32 devices in a mesh: dp: 4 (over y, x), ctx: 4 (over z), tp: 2 (over core).
Axes of the slice: x: 2, y: 2, z: 4, core: 2. Of those that a mesh axis runs over, the one named last changes fastest.
Arguments:
- tokens: bfloat16 [4, 2048, 1024], P('dp', 'ctx'), may hold values from -6 to 6
- query_weight: bfloat16 [1024, 1024], P('dp', 'tp'), may hold values from -0.1875 to 0.1875
- key_weight: bfloat16 [1024, 512], P('dp', 'tp'), may hold values from -0.1875 to 0.1875
- value_weight: bfloat16 [1024, 512], P('dp', 'tp'), may hold values from -0.1875 to 0.1875
- output_weight: bfloat16 [1024, 1024], P('tp', 'dp'), may hold values from -4 to 4
- gain_attn: bfloat16 [1024], P('dp'), may hold values from 0.5 to 1.5
- gain_moe: bfloat16 [1024], P('dp'), may hold values from 0.5 to 1.5
- expert_weights: bfloat16 [32, 3, 1024, 512], P('dp', None, None, 'tp'), may hold values from -0.375 to 0.375
- routes: int32 [4, 2048, 8], P('dp', 'ctx'), may hold values from 0 to 31, all different within a row
- gate_values: float32 [4, 2048, 8], P('dp', 'ctx'), may hold values from 0.05 to 0.2
- documents: int32 [4, 2048], P('dp', 'ctx'), may hold values from 0 to 2, never falling along the last dimension, each value on 1 to 1024 neighbouring positions
- pic_starts: int32 [4, 4], P('dp'), may hold values from 0 to 1792, as said below
- cotangent: bfloat16 [4, 2048, 1024], P('dp', 'ctx'), may hold values from -6 to 6
Outputs:
- layer_out: bfloat16 [4, 2048, 1024], P('dp', 'ctx')
- input_grad: bfloat16 [4, 2048, 1024], P('dp', 'ctx')
- query_w_grad: float32 [1024, 1024], P(('dp', 'ctx'), 'tp')
- key_w_grad: float32 [1024, 512], P(('dp', 'ctx'), 'tp')
- value_w_grad: float32 [1024, 512], P(('dp', 'ctx'), 'tp')
- output_w_grad: float32 [1024, 1024], P('tp', ('dp', 'ctx'))
- gain_attn_grad: float32 [1024], P(('dp', 'ctx'))
- gain_moe_grad: float32 [1024], P(('dp', 'ctx'))
- expert_grad: float32 [32, 3, 1024, 512], P('dp', None, 'ctx', 'tp')
The draws below stay inside these ranges and needn't reach their ends.
Inputs may be any that keep to these rules, and one draw needn't show every extreme that they name: `routes`: each token names 8 different experts. `documents`: document numbers never fall along a sequence; a document holds at most 1024 positions. `pic_starts`: span j of a sequence lies inside positions j * (512) to (j + 1) (512) - 1.
All inputs are finite; a program needn't handle non-finite values.
Results may differ from the reference program's by a relative error of at most 0.02.
Values may be sent and summed in bfloat16 or wider, within the bound.
A program may use at most 448 MiB of HBM per device.

```python
import math
import jax
import jax.numpy as jnp
import numpy as np
from jax import lax

MODEL_DIM = 1024
QUERY_HEADS = 16
KEY_VALUE_HEADS = 8
HEAD_DIM = 64
FF = 512
EXPERTS = 32
TOP = 8
SEQUENCES_LOCAL = 1
CONTEXT_LENGTH = 512
PIC = 256
NPIC = 4
DOCS = 3
SEQUENCE_LENGTH = 2048
SEQS = 4
CAP = 144
N_DP = 4
N_CTX = 4


def draw_pic_starts(key, part):
    width_slot = SEQUENCE_LENGTH // NPIC
    own_key = jax.random.fold_in(key, 7)
    offsets = jax.random.randint(own_key, (SEQS, NPIC), 0, width_slot - PIC + 1).astype(jnp.int32)
    offsets = offsets.at[0, 0].set(0)
    offsets = offsets.at[0, NPIC - 1].set(width_slot - PIC)
    return (jnp.arange(NPIC, dtype=jnp.int32)[None, :] * width_slot + offsets).astype(jnp.int32)


def shard_levels(rng, shape, cuts, low, high):
    def one(axis_at, shards_of):
        steps = jax.random.uniform(jax.random.fold_in(jax.random.fold_in(rng, 6), axis_at), (shards_of,), jnp.float32, low / len(cuts), high / len(cuts))
        return jnp.repeat(jnp.exp(steps), shape[axis_at] // shards_of).reshape((-1,) + (1,) * (len(shape) - axis_at - 1))

    gain = one(*cuts[0])
    for cut in cuts[1:]:
        gain = gain * one(*cut)
    return gain


def choose_distinct(key, rows, count, top, lift):
    order = jax.random.permutation(jax.random.fold_in(key, 1), count)
    favour = order
    for power in range(3):
        favour = favour * favour // count
    favour = favour * lift // count
    chance = jax.random.randint(jax.random.fold_in(key, 2), (rows, count), 0, 4096) + favour
    fixed_rows = jax.random.permutation(jax.random.fold_in(key, 3), rows)[jnp.arange(count) % rows]
    chance = jnp.where(jnp.arange(rows)[:, None] == fixed_rows[None, :], 1 << 14, chance)
    priority = chance * count + jnp.arange(count)
    return lax.top_k(priority.astype(jnp.int32), top)[1].astype(jnp.int32)


def profile(number_of, total, reach, skew):
    portions = [(1 << 20) // math.isqrt(standing ** skew) + 1 for standing in range(2, number_of + 1)]
    rest, given = total - reach - (number_of - 1), [1] * (number_of - 1)
    while rest > 0:
        candidates = [i for i in range(number_of - 1) if given[i] < reach]
        whole, left = sum([portions[i] for i in candidates]), rest
        for i in candidates:
            extra = min(reach - given[i], max(1, left * portions[i] // whole), rest)
            given[i] = given[i] + extra
            rest = rest - extra
    return np.array([reach] + given)


def ragged_sizes(key, amount, total, reach, slope):
    if amount == 2:
        one = jax.random.randint(key, (), max(1, total - reach), min(reach, total - 1) + 1)
        return jnp.stack([one, total - one])
    tallies = jnp.asarray(profile(amount, total, reach, slope), jnp.int32)
    twos = (amount - 1) // 2
    source_of, sink = tallies[1:1 + 2 * twos:2], tallies[2:2 + 2 * twos:2]
    margin = jnp.minimum(source_of - 1, reach - sink)
    passed = jax.random.randint(jax.random.fold_in(key, 1), (twos,), 0, 1 << 20) % (margin + 1)
    tallies = tallies.at[1:1 + 2 * twos:2].set(source_of - passed).at[2:2 + 2 * twos:2].set(sink + passed)
    return tallies[jax.random.permutation(jax.random.fold_in(key, 2), amount)]


def bell_draw(key, dims, width, most, split=(), kind=jnp.bfloat16):
    level = shard_levels(key, dims, split, -0.22, 0.18) if split else 1.0
    values = jax.random.normal(key, dims, jnp.float32) * width * level
    return jnp.minimum(jnp.maximum(values, -most), most).astype(kind)


def setup_inputs(seed: int = 0) -> dict:
    splits = jax.random.split(jax.random.key(seed), 14)
    tokens = bell_draw(splits[0], (SEQS, SEQUENCE_LENGTH, MODEL_DIM), 1.0, 6.0, ((0, 4), (1, 4)))
    query_weight = bell_draw(splits[1], (MODEL_DIM, QUERY_HEADS * HEAD_DIM), MODEL_DIM ** -0.5, 0.1875, ((0, 4), (1, 2)))
    key_weight = bell_draw(splits[2], (MODEL_DIM, KEY_VALUE_HEADS * HEAD_DIM), MODEL_DIM ** -0.5, 0.1875, ((0, 4), (1, 2)))
    value_weight = bell_draw(splits[3], (MODEL_DIM, KEY_VALUE_HEADS * HEAD_DIM), MODEL_DIM ** -0.5, 0.1875, ((0, 4), (1, 2)))
    output_weight = bell_draw(splits[4], (QUERY_HEADS * HEAD_DIM, MODEL_DIM), (max(HEAD_DIM // 32, 1)) ** -0.5, 4.0, ((0, 2), (1, 4)))
    gain_attn = jnp.clip(1.0 + 0.1 * jax.random.normal(splits[5], (MODEL_DIM,), jnp.float32), 0.5, 1.5).astype(jnp.bfloat16)
    gain_moe = jnp.clip(1.0 + 0.1 * jax.random.normal(splits[6], (MODEL_DIM,), jnp.float32), 0.5, 1.5).astype(jnp.bfloat16)
    expert_weights = bell_draw(splits[7], (EXPERTS, 3, MODEL_DIM, FF), (MODEL_DIM // 4) ** -0.5, 0.375, ((0, 4), (3, 2)))
    routes = choose_distinct(splits[8], SEQS * SEQUENCE_LENGTH, EXPERTS, TOP, 2048).reshape((SEQS, SEQUENCE_LENGTH, TOP))
    gate_values = jnp.clip(0.05 + 0.15 * jax.random.uniform(splits[9], (SEQS, SEQUENCE_LENGTH, TOP), jnp.float32) ** shard_levels(splits[9], (SEQS, SEQUENCE_LENGTH, TOP), ((0, 4), (1, 4)), -0.2, 0.2), 0.05, 0.2)
    documents = jax.vmap(lambda own: jnp.searchsorted(jnp.cumsum(ragged_sizes(own, DOCS, SEQUENCE_LENGTH, SEQUENCE_LENGTH // 2, 0)), jnp.arange(SEQUENCE_LENGTH), side="right"))(jax.random.split(splits[10], SEQS)).reshape((SEQS, SEQUENCE_LENGTH)).astype(jnp.int32)
    pic_starts = draw_pic_starts(jax.random.fold_in(splits[13], 71), 0)
    cotangent = bell_draw(splits[12], (SEQS, SEQUENCE_LENGTH, MODEL_DIM), 1.0, 6.0, ((0, 4), (1, 4)))
    return dict(tokens=tokens, query_weight=query_weight, key_weight=key_weight, value_weight=value_weight, output_weight=output_weight, gain_attn=gain_attn, gain_moe=gain_moe, expert_weights=expert_weights, routes=routes, gate_values=gate_values, documents=documents, pic_starts=pic_starts, cotangent=cotangent)


@jax.custom_vjp
def reduced_cast(v):
    return lax.optimization_barrier(v.astype(jnp.bfloat16)).astype(jnp.float32)

@jax.custom_vjp
def reduced_cast_gradient(v):
    return v

def low_keep(v):
    return (reduced_cast(v), None)

def low_pass(kept, grad):
    return (grad,)

def back_keep(v):
    return (v, None)

def back_low(kept, grad):
    return (reduced_cast(grad),)
reduced_cast.defvjp(low_keep, low_pass)
reduced_cast_gradient.defvjp(back_keep, back_low)
TOP_PRECISION = lax.Precision.HIGHEST
EPSILON = 1e-06
THETA = 10000.0

def rms_norm(tensor, gain_vec):
    return tensor * lax.rsqrt(lax.optimization_barrier(jnp.mean(tensor * tensor, axis=-1, keepdims=True)) + EPSILON) * gain_vec

def apply_rotary(tensor, token_positions):
    half_dim = tensor.shape[-1] // 2
    inverse = THETA ** (-(jnp.arange(half_dim, dtype=jnp.float32) * 2.0 / tensor.shape[-1]))
    angles = token_positions.astype(jnp.float32)[:, None] * inverse[None, :]
    cosine = jnp.cos(angles)[:, None, :]
    sine_of = jnp.sin(angles)[:, None, :]
    first_half = tensor[..., :half_dim]
    second_half = tensor[..., half_dim:]
    return jnp.concatenate([first_half * cosine - second_half * sine_of, second_half * cosine + first_half * sine_of], axis=-1)

def picture_of(starts, token_positions):
    inside = (token_positions[:, None] >= starts[None, :]) & (token_positions[:, None] < starts[None, :] + PIC)
    labels = jnp.arange(starts.shape[0], dtype=jnp.int32) + 1
    return (lax.optimization_barrier(jnp.sum(jnp.where(inside, labels[None, :], 0), axis=-1)) - 1).astype(jnp.int32)

def permitted(q_doc, q_pic, q_place, k_doc, k_pic, k_place):
    same_doc = q_doc[:, None] == k_doc[None, :]
    earlier = k_place[None, :] <= q_place[:, None]
    picture = (q_pic[:, None] >= 0) & (q_pic[:, None] == k_pic[None, :])
    return same_doc & (earlier | picture)

def dispatch(chosen):
    onehot = (chosen[:, None] == jnp.arange(EXPERTS, dtype=jnp.int32)[None, :]).astype(jnp.int32)
    before = (jnp.cumsum(onehot, axis=0) - onehot).astype(jnp.int32)
    position = lax.optimization_barrier(jnp.sum(before * onehot, axis=-1)).astype(jnp.int32)
    return jnp.where(position < CAP, chosen * CAP + position, EXPERTS * CAP).astype(jnp.int32)

def slot_table(slot_ids, tok_count):
    owners = (jnp.arange(slot_ids.shape[0], dtype=jnp.int32) // TOP).astype(jnp.int32)
    slot_owner = jnp.full((EXPERTS * CAP + 1,), tok_count, jnp.int32).at[slot_ids].set(owners)
    return slot_owner[:EXPERTS * CAP]

def attend_one_sequence(inputs):
    query_rotated, key_rotated, values, document_index, picture_index = inputs
    query_groups = QUERY_HEADS // KEY_VALUE_HEADS
    token_positions = jnp.arange(SEQUENCE_LENGTH, dtype=jnp.int32)
    query_rows_all = query_rotated.reshape(N_CTX, CONTEXT_LENGTH, KEY_VALUE_HEADS, query_groups, HEAD_DIM)
    blocks = (query_rows_all, document_index.reshape(N_CTX, CONTEXT_LENGTH), picture_index.reshape(N_CTX, CONTEXT_LENGTH), token_positions.reshape(N_CTX, CONTEXT_LENGTH))

    def one_block(block_in):
        q_block, q_doc, q_pic, q_place = block_in
        raw_scores = reduced_cast_gradient(jnp.einsum('qhgd,khd->hgqk', q_block, key_rotated, precision=TOP_PRECISION))
        allowed = permitted(q_doc, q_pic, q_place, document_index, picture_index, token_positions)
        scores = jnp.where(allowed[None, None], raw_scores * HEAD_DIM ** (-0.5), -jnp.inf)
        attn_probs = reduced_cast(jax.nn.softmax(scores, axis=-1))
        expert_mixture = jnp.einsum('hgqk,khd->qhgd', attn_probs, values, precision=TOP_PRECISION)
        return expert_mixture.reshape(CONTEXT_LENGTH, QUERY_HEADS * HEAD_DIM)
    return lax.map(jax.checkpoint(one_block), blocks).reshape(SEQUENCE_LENGTH, QUERY_HEADS * HEAD_DIM)

def expert_group(inputs, experts):
    normalized_input, chosen, gate_vals = inputs
    tok_count = normalized_input.shape[0]
    slot_ids = dispatch(chosen)
    slot_owner = slot_table(slot_ids, tok_count)
    padded = jnp.concatenate([normalized_input, jnp.zeros((1, MODEL_DIM), jnp.float32)], axis=0)
    slot_rows = padded[slot_owner].reshape(EXPERTS, CAP, MODEL_DIM)
    gate_pre = reduced_cast_gradient(jnp.einsum('ecd,edf->ecf', slot_rows, experts[:, 0], precision=TOP_PRECISION))
    up_pre = reduced_cast_gradient(jnp.einsum('ecd,edf->ecf', slot_rows, experts[:, 1], precision=TOP_PRECISION))
    activation = reduced_cast(jax.nn.silu(gate_pre) * up_pre)
    result = reduced_cast_gradient(jnp.einsum('ecf,edf->ecd', activation, experts[:, 2], precision=TOP_PRECISION))
    flat_out = jnp.concatenate([result.reshape(EXPERTS * CAP, MODEL_DIM), jnp.zeros((1, MODEL_DIM), jnp.float32)], axis=0)
    picked = flat_out[slot_ids].reshape(tok_count, TOP, MODEL_DIM)
    return lax.optimization_barrier(jnp.sum(picked * gate_vals.reshape(tok_count, TOP)[:, :, None], axis=1))

def layer(tokens, query_weight, key_weight, value_weight, output_weight, gain_attn, gain_moe, experts, chosen, gate_vals, document_index, picture_index):
    normalized_input = reduced_cast(rms_norm(tokens, gain_attn))
    query_projected = reduced_cast_gradient(jnp.einsum('unh,hg->ung', normalized_input, query_weight, precision=TOP_PRECISION))
    key_projected = reduced_cast_gradient(jnp.einsum('unh,hg->ung', normalized_input, key_weight, precision=TOP_PRECISION))
    value_projected = reduced_cast_gradient(reduced_cast(jnp.einsum('unh,hg->ung', normalized_input, value_weight, precision=TOP_PRECISION)))
    token_positions = jnp.arange(SEQUENCE_LENGTH, dtype=jnp.int32)
    query_rotated = reduced_cast(apply_rotary(query_projected.reshape(SEQUENCES_LOCAL, SEQUENCE_LENGTH, QUERY_HEADS, HEAD_DIM), token_positions))
    key_rotated = reduced_cast(apply_rotary(key_projected.reshape(SEQUENCES_LOCAL, SEQUENCE_LENGTH, KEY_VALUE_HEADS, HEAD_DIM), token_positions))
    expert_mixture = lax.map(attend_one_sequence, (query_rotated, key_rotated, value_projected.reshape(SEQUENCES_LOCAL, SEQUENCE_LENGTH, KEY_VALUE_HEADS, HEAD_DIM), document_index, picture_index))
    expert_mixture = reduced_cast_gradient(reduced_cast(expert_mixture))
    attention_output = reduced_cast_gradient(jnp.einsum('xik,kv->xiv', expert_mixture, output_weight, precision=TOP_PRECISION))
    hidden = tokens + attention_output
    normed_two = reduced_cast(rms_norm(hidden, gain_moe))
    grouped = normed_two.reshape(SEQUENCES_LOCAL, N_CTX, CONTEXT_LENGTH, MODEL_DIM).transpose(1, 0, 2, 3).reshape(N_CTX, SEQUENCES_LOCAL * CONTEXT_LENGTH, MODEL_DIM)
    group_routes = chosen.reshape(SEQUENCES_LOCAL, N_CTX, CONTEXT_LENGTH, TOP).transpose(1, 0, 2, 3).reshape(N_CTX, SEQUENCES_LOCAL * CONTEXT_LENGTH * TOP)
    group_gates = gate_vals.reshape(SEQUENCES_LOCAL, N_CTX, CONTEXT_LENGTH, TOP).transpose(1, 0, 2, 3).reshape(N_CTX, SEQUENCES_LOCAL * CONTEXT_LENGTH * TOP)

    def run_group(inputs):
        return expert_group(inputs, experts)
    moe_out = lax.map(jax.checkpoint(run_group), (grouped, group_routes, group_gates))
    moe_out = moe_out.reshape(N_CTX, SEQUENCES_LOCAL, CONTEXT_LENGTH, MODEL_DIM).transpose(1, 0, 2, 3).reshape(SEQUENCES_LOCAL, SEQUENCE_LENGTH, MODEL_DIM)
    return hidden + moe_out

def reference(tokens, query_weight, key_weight, value_weight, output_weight, gain_attn, gain_moe, expert_weights, routes, gate_values, documents, pic_starts, cotangent):
    weights = (query_weight.astype(jnp.float32), key_weight.astype(jnp.float32), value_weight.astype(jnp.float32), output_weight.astype(jnp.float32), gain_attn.astype(jnp.float32), gain_moe.astype(jnp.float32), expert_weights.astype(jnp.float32))
    token_positions = jnp.arange(SEQUENCE_LENGTH, dtype=jnp.int32)
    pictures = jax.vmap(picture_of, in_axes=(0, None))(pic_starts, token_positions)

    def slabs(source):
        return source.reshape((N_DP, SEQUENCES_LOCAL) + source.shape[1:])

    def step(totals, inputs):
        x_slab, grad_slab, route_slab, gate_slab, doc_slab, pic_slab = inputs

        def forward(x_in, query_w, key_w, value_w, output_w, attn_gain, moe_gain, expert_w):
            return layer(x_in, query_w, key_w, value_w, output_w, attn_gain, moe_gain, expert_w, route_slab, gate_slab, doc_slab, pic_slab)
        output, pullback = jax.vjp(forward, x_slab.astype(jnp.float32), *weights)
        grad_list = pullback(grad_slab.astype(jnp.float32))
        new_totals = tuple((total + grad for total, grad in zip(totals, grad_list[1:])))
        return (new_totals, (output.astype(jnp.bfloat16), grad_list[0].astype(jnp.bfloat16)))
    zero_totals = tuple((jnp.zeros(weight.shape, jnp.float32) for weight in weights))
    totals, (outputs, input_grads) = lax.scan(step, zero_totals, (slabs(tokens), slabs(cotangent), slabs(routes), slabs(gate_values.astype(jnp.float32)), slabs(documents), slabs(pictures)))
    return (outputs.reshape(SEQS, SEQUENCE_LENGTH, MODEL_DIM), input_grads.reshape(SEQS, SEQUENCE_LENGTH, MODEL_DIM), totals[0], totals[1], totals[2], totals[3], totals[4], totals[5], totals[6])
```

```python
import jax
import jax.numpy as jnp
from jax import lax
from jax.sharding import PartitionSpec as P

HEAD_DIM = 64
TOP = 8
PIC = 256
CAP = 144


EPSILON = 1e-06
THETA = 10000.0
NEG_FILL = -1e30


def rms_norm(tensor, gain_vec):
    return (
        tensor * lax.rsqrt(jnp.mean(tensor * tensor, axis=-1, keepdims=True) + EPSILON) * gain_vec
    )


def apply_rotary(tensor, token_positions):
    half_dim = tensor.shape[-1] // 2
    inverse = THETA ** (-(jnp.arange(half_dim, dtype=jnp.float32) * 2.0 / tensor.shape[-1]))
    angles = token_positions.astype(jnp.float32)[:, None] * inverse[None, :]
    cosine = jnp.cos(angles)[:, None, :]
    sine_of = jnp.sin(angles)[:, None, :]
    first_half = tensor[..., :half_dim]
    second_half = tensor[..., half_dim:]
    return jnp.concatenate(
        [first_half * cosine - second_half * sine_of, second_half * cosine + first_half * sine_of],
        axis=-1,
    )


def picture_of(starts, token_positions):
    inside = (token_positions[:, None] >= starts[None, :]) & (
        token_positions[:, None] < starts[None, :] + PIC
    )
    labels = jnp.arange(starts.shape[0], dtype=jnp.int32) + 1
    return jnp.sum(jnp.where(inside, labels[None, :], 0), axis=-1) - 1


def permitted(q_doc, q_pic, q_place, k_doc, k_pic, k_place):
    same_doc = q_doc[:, None] == k_doc[None, :]
    earlier = k_place[None, :] <= q_place[:, None]
    picture = (q_pic[:, None] >= 0) & (q_pic[:, None] == k_pic[None, :])
    return same_doc & (earlier | picture)


def gated_product(gate_pre, up_pre):
    return jax.nn.silu(gate_pre) * up_pre


def expert_backward(weight_rows, slot_rows, slot_grads):
    gate_pre = jnp.einsum(
        "ecd,edf->ecf", slot_rows, weight_rows[:, 0], preferred_element_type=jnp.float32
    )
    up_pre = jnp.einsum(
        "ecd,edf->ecf", slot_rows, weight_rows[:, 1], preferred_element_type=jnp.float32
    )
    activation, pullback = jax.vjp(gated_product, gate_pre, up_pre)
    act_grad = jnp.einsum(
        "ecd,edf->ecf", slot_grads, weight_rows[:, 2], preferred_element_type=jnp.float32
    )
    gate_grad, up_grad = pullback(act_grad)
    gate_low = gate_grad.astype(jnp.bfloat16)
    up_low = up_grad.astype(jnp.bfloat16)
    act_low = activation.astype(jnp.bfloat16)
    input_back = jnp.einsum(
        "ecf,edf->ecd", gate_low, weight_rows[:, 0], preferred_element_type=jnp.float32
    )
    input_back = input_back + jnp.einsum(
        "ecf,edf->ecd", up_low, weight_rows[:, 1], preferred_element_type=jnp.float32
    )
    return (input_back, gate_low, up_low, act_low)


def expert_weight_grads(slot_rows, slot_grads, gate_low, up_low, act_low):
    gate_part = jnp.einsum("ecd,ecf->edf", slot_rows, gate_low, preferred_element_type=jnp.float32)
    up_part = jnp.einsum("ecd,ecf->edf", slot_rows, up_low, preferred_element_type=jnp.float32)
    down_part = jnp.einsum("ecd,ecf->edf", slot_grads, act_low, preferred_element_type=jnp.float32)
    return jnp.stack([gate_part, up_part, down_part], axis=1)


def body(
    tokens,
    query_weight,
    key_weight,
    value_weight,
    output_weight,
    gain_attn,
    gain_moe,
    expert_weights,
    routes,
    gate_values,
    documents,
    pic_starts,
    cotangent,
):
    seq_dev, block_len, model_width = tokens.shape
    ctx_size = lax.axis_size("ctx")
    length = block_len * ctx_size
    tok_rows = seq_dev * block_len
    offset = lax.axis_index("ctx") * block_len
    query_full, key_full, value_full, output_full, gain_one, gain_two = (
        lax.all_gather(query_weight, "dp", axis=0, tiled=True),
        lax.all_gather(key_weight, "dp", axis=0, tiled=True),
        lax.all_gather(value_weight, "dp", axis=0, tiled=True),
        lax.all_gather(output_weight, "dp", axis=1, tiled=True),
        lax.all_gather(gain_attn, "dp", axis=0, tiled=True),
        lax.all_gather(gain_moe, "dp", axis=0, tiled=True),
    )
    q_heads = query_full.shape[1] // HEAD_DIM
    kv_heads = key_full.shape[1] // HEAD_DIM
    query_groups = q_heads // kv_heads
    kv_width = kv_heads * HEAD_DIM
    score_scale = HEAD_DIM ** (-0.5)
    local_places = offset + jnp.arange(block_len, dtype=jnp.int32)
    all_places = jnp.arange(length, dtype=jnp.int32)
    pictures = jax.vmap(picture_of, in_axes=(0, None))(pic_starts, all_places)
    local_pics = lax.dynamic_slice_in_dim(pictures, offset, block_len, 1)

    def sum_heads(partial_sum):
        return lax.psum(partial_sum, "tp")

    x_flat = tokens.reshape(tok_rows, model_width).astype(jnp.float32)
    gain_first = gain_one.astype(jnp.float32)
    gain_second = gain_two.astype(jnp.float32)
    normed_one = rms_norm(x_flat, gain_first).astype(jnp.bfloat16)
    query_projected = jnp.dot(normed_one, query_full, preferred_element_type=jnp.float32).reshape(
        seq_dev, block_len, q_heads, HEAD_DIM
    )
    key_projected = jnp.dot(normed_one, key_full, preferred_element_type=jnp.float32).reshape(
        seq_dev, block_len, kv_heads, HEAD_DIM
    )
    value_low = jnp.dot(normed_one, value_full, preferred_element_type=jnp.float32).astype(
        jnp.bfloat16
    )
    query_rotated = apply_rotary(query_projected, local_places).astype(jnp.bfloat16)
    key_rotated = apply_rotary(key_projected, local_places).astype(jnp.bfloat16)
    q_group = query_rotated.reshape(seq_dev, block_len, kv_heads, query_groups, HEAD_DIM)
    kv_local = jnp.concatenate(
        [
            key_rotated.reshape(seq_dev, block_len, kv_width),
            value_low.reshape(seq_dev, block_len, kv_width),
        ],
        axis=-1,
    )
    kv_all, doc_all = (
        lax.all_gather(kv_local, "ctx", axis=1, tiled=True),
        lax.all_gather(documents.astype(jnp.bfloat16), "ctx", axis=1, tiled=True),
    )
    doc_keys = doc_all.astype(jnp.int32)
    starts = jnp.arange(ctx_size, dtype=jnp.int32) * block_len
    stat_shape = (seq_dev, kv_heads, query_groups, block_len)
    acc_shape = (seq_dev, block_len, kv_heads, query_groups, HEAD_DIM)

    def key_block(first_row, row_count):
        kv_part = lax.dynamic_slice_in_dim(kv_all, first_row, row_count, 1)
        key_rows = kv_part[..., :kv_width].reshape(seq_dev, row_count, kv_heads, HEAD_DIM)
        val_rows = kv_part[..., kv_width:].reshape(seq_dev, row_count, kv_heads, HEAD_DIM)
        raw_scores = jnp.einsum(
            "sqhgd,skhd->shgqk", q_group, key_rows, preferred_element_type=jnp.float32
        )
        k_places = first_row + jnp.arange(row_count, dtype=jnp.int32)
        k_docs = lax.dynamic_slice_in_dim(doc_keys, first_row, row_count, 1)
        k_pics = lax.dynamic_slice_in_dim(pictures, first_row, row_count, 1)
        allowed = jax.vmap(permitted, in_axes=(0, 0, None, 0, 0, None))(
            documents, local_pics, local_places, k_docs, k_pics, k_places
        )
        scores = jnp.where(allowed[:, None, None], raw_scores * score_scale, -jnp.inf)
        return (scores, key_rows, val_rows)

    def stat_step(stat_carry, first_row):
        run_max, run_sum = stat_carry
        scores = key_block(first_row, block_len)[0]
        new_max = jnp.maximum(run_max, jnp.max(scores, axis=-1))
        run_sum = run_sum * jnp.exp(run_max - new_max) + jnp.sum(
            jnp.exp(scores - new_max[..., None]), axis=-1
        )
        return ((new_max, run_sum), None)

    stats = lax.scan(
        stat_step,
        (jnp.full(stat_shape, NEG_FILL, jnp.float32), jnp.zeros(stat_shape, jnp.float32)),
        starts,
    )[0]
    log_total = stats[0] + jnp.log(stats[1])

    def mix_step(running, first_row):
        scores, key_rows, val_rows = key_block(first_row, block_len)
        probs_low = jnp.exp(scores - log_total[..., None]).astype(jnp.bfloat16)
        return (
            running
            + jnp.einsum(
                "shgqk,skhd->sqhgd", probs_low, val_rows, preferred_element_type=jnp.float32
            ),
            None,
        )

    expert_mixture = lax.scan(mix_step, jnp.zeros(acc_shape, jnp.float32), starts)[0]
    mixture_low = expert_mixture.reshape(tok_rows, q_heads * HEAD_DIM).astype(jnp.bfloat16)
    attention_output = sum_heads(
        jnp.dot(mixture_low, output_full, preferred_element_type=jnp.float32)
    )
    hidden = x_flat + attention_output
    normed_two = rms_norm(hidden, gain_second).astype(jnp.bfloat16)
    own = expert_weights.shape[0]
    chosen_all = lax.all_gather(routes.reshape(tok_rows, TOP), "dp", axis=0)
    gates_all = lax.all_gather(gate_values.reshape(tok_rows, TOP), "dp", axis=0)
    grad_all = lax.all_gather(cotangent.reshape(tok_rows, model_width), "dp", axis=0)
    rows_all = lax.all_gather(normed_two, "dp", axis=0)
    groups = rows_all.shape[0]
    first_own = lax.axis_index("dp") * own
    named = chosen_all[..., None] == first_own + jnp.arange(own, dtype=jnp.int32)
    names = jnp.any(named, axis=2)
    gate_of = jnp.sum(jnp.where(named, gates_all[..., None], 0.0), axis=2)
    earlier = jnp.tril(jnp.ones((tok_rows, tok_rows), jnp.bfloat16), -1)
    place = jnp.einsum(
        "rq,gqe->gre", earlier, names.astype(jnp.bfloat16), preferred_element_type=jnp.float32
    ).astype(jnp.int32)
    place = jnp.where(names & (place < CAP), place, -1)
    picks = place.transpose(0, 2, 1)[:, :, None, :] == jnp.arange(CAP, dtype=jnp.int32)[:, None]
    slot_gate = jnp.sum(jnp.where(picks, gate_of.transpose(0, 2, 1)[:, :, None, :], 0.0), axis=-1)
    picks = picks.astype(jnp.bfloat16)
    slot_rows = (
        jnp.einsum("gesr,grd->egsd", picks, rows_all, preferred_element_type=jnp.float32)
        .astype(jnp.bfloat16)
        .reshape(own, groups * CAP, model_width)
    )
    gate_col = slot_gate.transpose(1, 0, 2).reshape(own, groups * CAP, 1)
    slot_grads = (
        jnp.einsum("gesr,grd->egsd", picks, grad_all, preferred_element_type=jnp.float32).reshape(
            own, groups * CAP, model_width
        )
        * gate_col
    ).astype(jnp.bfloat16)
    out_grad = cotangent.reshape(tok_rows, model_width).astype(jnp.float32)
    slot_back, gate_low, up_low, act_low = expert_backward(expert_weights, slot_rows, slot_grads)
    slot_out = jnp.einsum(
        "ecf,edf->ecd", act_low, expert_weights[:, 2], preferred_element_type=jnp.float32
    )

    def combine(slots):
        part = jnp.einsum(
            "gesr,egsd->grd",
            picks,
            slots.astype(jnp.bfloat16).reshape(own, groups, CAP, model_width),
            preferred_element_type=jnp.float32,
        )
        mine = lax.psum_scatter(
            part.astype(jnp.bfloat16).reshape(groups * tok_rows, model_width),
            "dp",
            scatter_dimension=0,
            tiled=True,
        )
        return sum_heads(mine.astype(jnp.float32))

    normed_two_grad = combine(slot_back)
    expert_part = expert_weight_grads(slot_rows, slot_grads, gate_low, up_low, act_low).astype(
        jnp.bfloat16
    )
    layer_out = hidden + combine(slot_out * gate_col)
    hidden_pull = jax.vjp(rms_norm, hidden, gain_second)[1]
    hidden_norm_grad, gain_second_grad = hidden_pull(normed_two_grad)
    hidden_grad = out_grad + hidden_norm_grad
    hidden_low = hidden_grad.astype(jnp.bfloat16)
    output_grad = jnp.einsum(
        "re,rd->ed", mixture_low, hidden_low, preferred_element_type=jnp.float32
    )
    mix_grad = (
        jnp.einsum("rd,ed->re", hidden_low, output_full, preferred_element_type=jnp.float32)
        .astype(jnp.bfloat16)
        .reshape(acc_shape)
    )

    def delta_step(running, first_row):
        scores, key_rows, val_rows = key_block(first_row, block_len)
        attn_probs = jnp.exp(scores - log_total[..., None])
        prob_grad = jnp.einsum(
            "sqhgd,skhd->shgqk", mix_grad, val_rows, preferred_element_type=jnp.float32
        )
        return (running + jnp.sum(attn_probs * prob_grad, axis=-1), None)

    row_delta = lax.scan(delta_step, jnp.zeros(stat_shape, jnp.float32), starts)[0]

    def score_grads(scores, val_rows):
        attn_probs = jnp.exp(scores - log_total[..., None])
        prob_grad = jnp.einsum(
            "sqhgd,skhd->shgqk", mix_grad, val_rows, preferred_element_type=jnp.float32
        )
        score_low = (attn_probs * (prob_grad - row_delta[..., None]) * score_scale).astype(
            jnp.bfloat16
        )
        return (attn_probs, score_low)

    def query_step(running, first_row):
        scores, key_rows, val_rows = key_block(first_row, block_len)
        score_low = score_grads(scores, val_rows)[1]
        return (
            running
            + jnp.einsum(
                "shgqk,skhd->sqhgd", score_low, key_rows, preferred_element_type=jnp.float32
            ),
            None,
        )

    q_rot_grad = lax.scan(query_step, jnp.zeros(acc_shape, jnp.float32), starts)[0]
    row_count = block_len * lax.axis_size("ctx")
    scores, key_rows, val_rows = key_block(jnp.int32(0), row_count)
    attn_probs, score_low = score_grads(scores, val_rows)
    val_grad = jnp.einsum(
        "shgqk,sqhgd->skhd",
        attn_probs.astype(jnp.bfloat16),
        mix_grad,
        preferred_element_type=jnp.float32,
    )
    key_grad = jnp.einsum(
        "shgqk,sqhgd->skhd", score_low, q_group, preferred_element_type=jnp.float32
    )
    joined_kv = jnp.concatenate(
        [
            key_grad.reshape(seq_dev, row_count, kv_width),
            val_grad.reshape(seq_dev, row_count, kv_width),
        ],
        axis=-1,
    )
    kv_term = lax.psum_scatter(
        jnp.transpose(joined_kv, (1, 0, 2)), "ctx", scatter_dimension=0, tiled=True
    )
    kv_back = jnp.transpose(kv_term, (1, 0, 2))
    k_rot_grad = kv_back[..., :kv_width].reshape(seq_dev, block_len, kv_heads, HEAD_DIM)
    value_grad_low = kv_back[..., kv_width:].reshape(tok_rows, kv_width).astype(jnp.bfloat16)

    def rotate_here(tensor):
        return apply_rotary(tensor, local_places)

    query_grad_low = (
        jax.vjp(rotate_here, query_projected)[1](
            q_rot_grad.reshape(seq_dev, block_len, q_heads, HEAD_DIM)
        )[0]
        .reshape(tok_rows, q_heads * HEAD_DIM)
        .astype(jnp.bfloat16)
    )
    key_grad_low = (
        jax.vjp(rotate_here, key_projected)[1](k_rot_grad)[0]
        .reshape(tok_rows, kv_width)
        .astype(jnp.bfloat16)
    )
    query_w_grad = jnp.einsum(
        "rd,re->de", normed_one, query_grad_low, preferred_element_type=jnp.float32
    )
    key_w_grad = jnp.einsum(
        "rd,re->de", normed_one, key_grad_low, preferred_element_type=jnp.float32
    )
    value_w_grad = jnp.einsum(
        "rd,re->de", normed_one, value_grad_low, preferred_element_type=jnp.float32
    )
    normed_one_part = jnp.einsum(
        "re,de->rd", query_grad_low, query_full, preferred_element_type=jnp.float32
    )
    normed_one_part = normed_one_part + jnp.einsum(
        "re,de->rd", key_grad_low, key_full, preferred_element_type=jnp.float32
    )
    normed_one_part = normed_one_part + jnp.einsum(
        "re,de->rd", value_grad_low, value_full, preferred_element_type=jnp.float32
    )
    normed_one_grad = sum_heads(normed_one_part)
    x_pull = jax.vjp(rms_norm, x_flat, gain_first)[1]
    x_norm_grad, gain_first_grad = x_pull(normed_one_grad)
    input_grad = (
        (hidden_grad + x_norm_grad).astype(jnp.bfloat16).reshape(seq_dev, block_len, model_width)
    )
    attn_sums = (
        lax.psum_scatter(
            query_w_grad.astype(jnp.bfloat16), "dp", scatter_dimension=0, tiled=True
        ).astype(jnp.float32),
        lax.psum_scatter(
            key_w_grad.astype(jnp.bfloat16), "dp", scatter_dimension=0, tiled=True
        ).astype(jnp.float32),
        lax.psum_scatter(
            value_w_grad.astype(jnp.bfloat16), "dp", scatter_dimension=0, tiled=True
        ).astype(jnp.float32),
        lax.psum_scatter(
            output_grad.astype(jnp.bfloat16), "dp", scatter_dimension=1, tiled=True
        ).astype(jnp.float32),
        lax.psum_scatter(
            gain_first_grad.astype(jnp.bfloat16), "dp", scatter_dimension=0, tiled=True
        ).astype(jnp.float32),
        lax.psum_scatter(
            gain_second_grad.astype(jnp.bfloat16), "dp", scatter_dimension=0, tiled=True
        ).astype(jnp.float32),
    )
    owned = (
        lax.psum_scatter(
            attn_sums[0].astype(jnp.bfloat16), "ctx", scatter_dimension=0, tiled=True
        ).astype(jnp.float32),
        lax.psum_scatter(
            attn_sums[1].astype(jnp.bfloat16), "ctx", scatter_dimension=0, tiled=True
        ).astype(jnp.float32),
        lax.psum_scatter(
            attn_sums[2].astype(jnp.bfloat16), "ctx", scatter_dimension=0, tiled=True
        ).astype(jnp.float32),
        lax.psum_scatter(
            attn_sums[3].astype(jnp.bfloat16), "ctx", scatter_dimension=1, tiled=True
        ).astype(jnp.float32),
        lax.psum_scatter(
            attn_sums[4].astype(jnp.bfloat16), "ctx", scatter_dimension=0, tiled=True
        ).astype(jnp.float32),
        lax.psum_scatter(
            attn_sums[5].astype(jnp.bfloat16), "ctx", scatter_dimension=0, tiled=True
        ).astype(jnp.float32),
        lax.psum_scatter(expert_part, "ctx", scatter_dimension=2, tiled=True).astype(jnp.float32),
    )
    return (
        layer_out.astype(jnp.bfloat16).reshape(seq_dev, block_len, model_width),
        input_grad,
        owned[0],
        owned[1],
        owned[2],
        owned[3],
        owned[4],
        owned[5],
        owned[6],
    )


def solution(mesh):
    return jax.shard_map(
        body,
        mesh=mesh,
        in_specs=(
            P("dp", "ctx", None),
            P("dp", "tp"),
            P("dp", "tp"),
            P("dp", "tp"),
            P("tp", "dp"),
            P("dp"),
            P("dp"),
            P("dp", None, None, "tp"),
            P("dp", "ctx", None),
            P("dp", "ctx", None),
            P("dp", "ctx"),
            P("dp", None),
            P("dp", "ctx", None),
        ),
        out_specs=(
            P("dp", "ctx", None),
            P("dp", "ctx", None),
            P(("dp", "ctx"), "tp"),
            P(("dp", "ctx"), "tp"),
            P(("dp", "ctx"), "tp"),
            P("tp", ("dp", "ctx")),
            P(("dp", "ctx")),
            P(("dp", "ctx")),
            P("dp", None, "ctx", "tp"),
        ),
        check_vma=False,
    )
```

```python
import functools

import jax
import jax.numpy as jnp
from jax import lax
from jax.experimental import pallas as pl
from jax.experimental.pallas import tpu as pltpu
from jax.sharding import PartitionSpec as P

HEAD_DIM = 64
TOP = 8
PIC = 256
CAP = 144

EPSILON = 1e-06
THETA = 10000.0
NEG_FILL = -1e30


KEY_ROWS = 256
NT = (((1,), (1,)), ((), ()))
LIMIT = 60 * 1024 * 1024


def seen_bias(flags, j, blocks, kinfo_ref, qinfo_ref):
    rows = pl.ds(pl.multiple_of(j * KEY_ROWS, KEY_ROWS), KEY_ROWS)
    q_doc, q_pic = qinfo_ref[0:1, :], qinfo_ref[1:2, :]
    k_doc, k_pic = kinfo_ref[rows, 0:1], kinfo_ref[rows, 1:2]
    q_place = flags[blocks] + lax.broadcasted_iota(jnp.int32, q_doc.shape, 1)
    k_place = j * KEY_ROWS + lax.broadcasted_iota(jnp.int32, k_doc.shape, 0)
    seen = (k_doc == q_doc) & ((k_place <= q_place) | ((k_pic == q_pic) & (q_pic >= 0)))
    return rows, jnp.where(seen, 0.0, NEG_FILL)


def attend_kernel(
    flags, q_ref, kv_ref, kinfo_ref, qinfo_ref, out_w_ref, mix_ref, full_ref, log_ref, part_ref,
    acc, top, total,
):
    blocks = kv_ref.shape[0] // KEY_ROWS
    kv_width = kv_ref.shape[1] // 2
    heads, kv_heads = q_ref.shape[1] // HEAD_DIM, kv_width // HEAD_DIM
    top[...] = jnp.full(top.shape, NEG_FILL, jnp.float32)
    total[...] = jnp.zeros(total.shape, jnp.float32)
    acc[...] = jnp.zeros(acc.shape, jnp.float32)

    def step(j, carry):
        @pl.when(flags[j] > 0)
        def _():
            rows, bias = seen_bias(flags, j, blocks, kinfo_ref, qinfo_ref)
            for g in range(kv_heads):
                key = kv_ref[rows, g * HEAD_DIM : (g + 1) * HEAD_DIM]
                val = kv_ref[rows, kv_width + g * HEAD_DIM : kv_width + (g + 1) * HEAD_DIM]
                val_t = jnp.transpose(val.astype(jnp.float32)).astype(jnp.bfloat16)
                for h in range(g * heads // kv_heads, (g + 1) * heads // kv_heads):
                    at = slice(h * HEAD_DIM, (h + 1) * HEAD_DIM)
                    scores = bias + lax.dot_general(
                        key, q_ref[:, at], NT, preferred_element_type=jnp.float32
                    )
                    old = top[h : h + 1, :]
                    new = jnp.maximum(old, jnp.max(scores, axis=0, keepdims=True))
                    probs = jnp.exp(scores - new)
                    fade = jnp.exp(old - new)
                    total[h : h + 1, :] = total[h : h + 1, :] * fade + jnp.sum(
                        probs, axis=0, keepdims=True
                    )
                    acc[at, :] = acc[at, :] * fade + jnp.dot(
                        val_t, probs.astype(jnp.bfloat16), preferred_element_type=jnp.float32
                    )
                    top[h : h + 1, :] = new

        return carry

    lax.fori_loop(0, blocks, step, 0)
    log_ref[...] = top[...] + jnp.log(total[...])
    for h in range(heads):
        at = slice(h * HEAD_DIM, (h + 1) * HEAD_DIM)
        acc[at, :] = acc[at, :] / total[h : h + 1, :]
    full = jnp.transpose(acc[...])
    full_ref[...] = full
    mix_ref[...] = full.astype(jnp.bfloat16)
    part_ref[...] = jnp.dot(
        mix_ref[...], out_w_ref[...], preferred_element_type=jnp.float32
    ).astype(jnp.bfloat16)


def attend_back_kernel(
    flags, q_ref, kv_ref, kinfo_ref, qinfo_ref, log_ref, full_ref, grad_ref, dq_ref, dkv_ref,
    acc, delta,
):
    blocks = kv_ref.shape[0] // KEY_ROWS
    kv_width = kv_ref.shape[1] // 2
    heads, kv_heads = q_ref.shape[1] // HEAD_DIM, kv_width // HEAD_DIM
    acc[...] = jnp.transpose(full_ref[...] * grad_ref[...].astype(jnp.float32))
    for h in range(heads):
        delta[h : h + 1, :] = jnp.sum(
            acc[h * HEAD_DIM : (h + 1) * HEAD_DIM, :], axis=0, keepdims=True
        )
    acc[...] = jnp.zeros(acc.shape, jnp.float32)

    def step(j, carry):
        @pl.when(flags[j] > 0)
        def _():
            rows, bias = seen_bias(flags, j, blocks, kinfo_ref, qinfo_ref)
            for g in range(kv_heads):
                k_at = slice(g * HEAD_DIM, (g + 1) * HEAD_DIM)
                v_at = slice(kv_width + g * HEAD_DIM, kv_width + (g + 1) * HEAD_DIM)
                key, val = kv_ref[rows, k_at], kv_ref[rows, v_at]
                key_t = jnp.transpose(key.astype(jnp.float32)).astype(jnp.bfloat16)
                dk = jnp.zeros((KEY_ROWS, HEAD_DIM), jnp.float32)
                dv = jnp.zeros((KEY_ROWS, HEAD_DIM), jnp.float32)
                for h in range(g * heads // kv_heads, (g + 1) * heads // kv_heads):
                    at = slice(h * HEAD_DIM, (h + 1) * HEAD_DIM)
                    q_rows, g_rows = q_ref[:, at], grad_ref[:, at]
                    scores = bias + lax.dot_general(
                        key, q_rows, NT, preferred_element_type=jnp.float32
                    )
                    probs = jnp.exp(scores - log_ref[h : h + 1, :])
                    prob_grad = lax.dot_general(
                        val, g_rows, NT, preferred_element_type=jnp.float32
                    )
                    slope = (probs * (prob_grad - delta[h : h + 1, :])).astype(jnp.bfloat16)
                    dv += jnp.dot(
                        probs.astype(jnp.bfloat16), g_rows, preferred_element_type=jnp.float32
                    )
                    dk += jnp.dot(slope, q_rows, preferred_element_type=jnp.float32)
                    acc[at, :] += jnp.dot(key_t, slope, preferred_element_type=jnp.float32)
                dkv_ref[rows, k_at] = dk.astype(dkv_ref.dtype)
                dkv_ref[rows, v_at] = dv.astype(dkv_ref.dtype)

        @pl.when(flags[j] == 0)
        def _():
            rows = pl.ds(pl.multiple_of(j * KEY_ROWS, KEY_ROWS), KEY_ROWS)
            dkv_ref[rows, :] = jnp.zeros((KEY_ROWS, dkv_ref.shape[1]), dkv_ref.dtype)

        return carry

    lax.fori_loop(0, blocks, step, 0)
    dq_ref[...] = jnp.transpose(acc[...]) * (HEAD_DIM**-0.5)


def whole_vmem(count):
    return [pl.BlockSpec(memory_space=pltpu.VMEM)] * count


def attend(flags, q, kv, kinfo, qinfo, out_w):
    rows, width = q.shape
    heads = width // HEAD_DIM
    return pl.pallas_call(
        attend_kernel,
        name="attend",
        in_specs=[pl.BlockSpec(memory_space=pltpu.SMEM)] + whole_vmem(5),
        out_specs=whole_vmem(4),
        out_shape=[
            jax.ShapeDtypeStruct((rows, width), jnp.bfloat16),
            jax.ShapeDtypeStruct((rows, width), jnp.float32),
            jax.ShapeDtypeStruct((heads, rows), jnp.float32),
            jax.ShapeDtypeStruct((rows, out_w.shape[1]), jnp.bfloat16),
        ],
        scratch_shapes=[
            pltpu.VMEM((width, rows), jnp.float32),
            pltpu.VMEM((heads, rows), jnp.float32),
            pltpu.VMEM((heads, rows), jnp.float32),
        ],
        compiler_params=pltpu.CompilerParams(vmem_limit_bytes=LIMIT),
    )(flags, q, kv, kinfo, qinfo, out_w)


def attend_back(flags, q, kv, kinfo, qinfo, log_total, full, grad):
    rows, width = q.shape
    return pl.pallas_call(
        attend_back_kernel,
        name="attend_back",
        in_specs=[pl.BlockSpec(memory_space=pltpu.SMEM)] + whole_vmem(7),
        out_specs=whole_vmem(2),
        out_shape=[
            jax.ShapeDtypeStruct((rows, width), jnp.float32),
            jax.ShapeDtypeStruct(kv.shape, jnp.bfloat16),
        ],
        scratch_shapes=[
            pltpu.VMEM((width, rows), jnp.float32),
            pltpu.VMEM((width // HEAD_DIM, rows), jnp.float32),
        ],
        compiler_params=pltpu.CompilerParams(vmem_limit_bytes=LIMIT),
    )(flags, q, kv, kinfo, qinfo, log_total, full, grad)


def block_flags(pic_starts, q_docs, k_docs, offset):
    block_len, length = q_docs.shape[0], k_docs.shape[0]
    docs = k_docs.reshape(length // KEY_ROWS, KEY_ROWS)
    first = jnp.arange(length // KEY_ROWS, dtype=jnp.int32) * KEY_ROWS
    same = (docs[:, 0] <= q_docs[-1]) & (docs[:, -1] >= q_docs[0])
    spans = (
        (pic_starts[None, :] < offset + block_len)
        & (pic_starts[None, :] + PIC > offset)
        & (pic_starts[None, :] < first[:, None] + KEY_ROWS)
        & (pic_starts[None, :] + PIC > first[:, None])
    )
    needed = same & ((first < offset + block_len) | jnp.any(spans, axis=1))
    return jnp.concatenate([needed.astype(jnp.int32), offset[None].astype(jnp.int32)])


MESH = pl.DeviceIdType.MESH


def place_on(axes):
    index, size = 0, 1
    for axis in axes:
        index = index * lax.axis_size(axis) + lax.axis_index(axis)
        size *= lax.axis_size(axis)
    return index, size


def peer_id(axes, index):
    ids = {}
    for axis in reversed(axes):
        count = lax.axis_size(axis)
        ids[axis] = lax.rem(index, count)
        index = lax.div(index, count)
    return ids


def greet(groups):
    barrier = pltpu.get_barrier_semaphore()
    count = 0
    for axes in groups:
        me, size = place_on(axes)

        def signal(k, carry, axes=axes, me=me, size=size):
            pl.semaphore_signal(
                barrier,
                inc=1,
                device_id=peer_id(axes, lax.rem(me + k, size)),
                device_id_type=MESH,
            )
            return carry

        lax.fori_loop(1, size, signal, 0)
        count += size - 1
    pl.semaphore_wait(barrier, count)


def spread_kernel(axes_of, *refs):
    count = len(axes_of)
    ins, outs, sems = refs[:count], refs[count : 2 * count], refs[2 * count :]
    groups = []
    for axes in axes_of:
        if axes not in groups:
            groups.append(axes)
    greet(groups)

    def copy(i, k):
        me, size = place_on(axes_of[i])
        return pltpu.make_async_remote_copy(
            src_ref=ins[i],
            dst_ref=outs[i].at[me],
            send_sem=sems[2 * i].at[k],
            recv_sem=sems[2 * i + 1].at[k],
            device_id=peer_id(axes_of[i], lax.rem(me + k, size)),
            device_id_type=MESH,
        )

    def start(i, k):
        copy(i, k).start()
        return 0

    def finish(i, k):
        copy(i, k).wait()
        return 0

    for i in range(count):
        lax.fori_loop(1, place_on(axes_of[i])[1], lambda k, c, i=i: start(i, k), 0)
    for i in range(count):
        outs[i][place_on(axes_of[i])[0]] = ins[i][...]
    for i in range(count):
        lax.fori_loop(1, place_on(axes_of[i])[1], lambda k, c, i=i: finish(i, k), 0)


def spread(arrays, axes_of, ident, name):
    sizes = [place_on(axes)[1] for axes in axes_of]
    scratch = []
    for size in sizes:
        scratch += [pltpu.SemaphoreType.DMA((size,)), pltpu.SemaphoreType.DMA((size,))]
    return pl.pallas_call(
        functools.partial(spread_kernel, tuple(axes_of)),
        name=name,
        in_specs=whole_vmem(len(arrays)),
        out_specs=whole_vmem(len(arrays)),
        out_shape=[
            jax.ShapeDtypeStruct((size,) + a.shape, a.dtype) for size, a in zip(sizes, arrays)
        ],
        scratch_shapes=scratch,
        compiler_params=pltpu.CompilerParams(
            collective_id=ident, has_side_effects=True, vmem_limit_bytes=LIMIT
        ),
    )(*arrays)


def swap_sum_kernel(axes, x_ref, out_ref, held, send, recv):
    me, size = place_on(axes)
    greet([axes])

    def copy(k):
        peer = lax.rem(me + k, size)
        return pltpu.make_async_remote_copy(
            src_ref=x_ref.at[peer],
            dst_ref=held.at[k],
            send_sem=send.at[k],
            recv_sem=recv.at[k],
            device_id=peer_id(axes, peer),
            device_id_type=MESH,
        )

    def start(k, carry):
        copy(k).start()
        return carry

    def finish(k, carry):
        copy(k).wait()
        out_ref[...] += held[k].astype(jnp.float32)
        return carry

    lax.fori_loop(1, size, start, 0)
    out_ref[...] = x_ref[me].astype(jnp.float32)
    lax.fori_loop(1, size, finish, 0)


def swap_sum(x, axes, ident, name):
    size = place_on(axes)[1]
    return pl.pallas_call(
        functools.partial(swap_sum_kernel, tuple(axes)),
        name=name,
        in_specs=whole_vmem(1),
        out_specs=pl.BlockSpec(memory_space=pltpu.VMEM),
        out_shape=jax.ShapeDtypeStruct(x.shape[1:], jnp.float32),
        scratch_shapes=[
            pltpu.VMEM(x.shape, x.dtype),
            pltpu.SemaphoreType.DMA((size,)),
            pltpu.SemaphoreType.DMA((size,)),
        ],
        compiler_params=pltpu.CompilerParams(
            collective_id=ident, has_side_effects=True, vmem_limit_bytes=LIMIT
        ),
    )(x)


def pair_copy(ref, dst, sems, k):
    return pltpu.make_async_remote_copy(
        src_ref=ref,
        dst_ref=dst,
        send_sem=sems[0].at[k],
        recv_sem=sems[1].at[k],
        device_id={"tp": 1 - lax.axis_index("tp")},
        device_id_type=MESH,
    )


def share_rows_kernel(
    part_ref, x_ref, gain_ref, hidden_ref, all_ref, held, normed, send, recv, up_send, up_recv
):
    me, size = place_on(("dp",))
    half = part_ref.shape[0] // 2
    core = lax.axis_index("tp")
    mine = pl.ds(pl.multiple_of(core * half, half), half)
    greet([("dp",), ("tp",)])
    swap = pair_copy(part_ref, held, (up_send, up_recv), 0)
    swap.start()
    swap.wait()

    def norm(rows):
        total = (
            x_ref[rows, :].astype(jnp.float32)
            + (part_ref[rows, :].astype(jnp.float32) + held[rows, :].astype(jnp.float32))
        )
        hidden_ref[rows, :] = total
        scale = lax.rsqrt(jnp.mean(total * total, axis=-1, keepdims=True) + EPSILON)
        normed[rows, :] = (total * scale * gain_ref[...]).astype(jnp.bfloat16)

    def copy(k):
        return pltpu.make_async_remote_copy(
            src_ref=normed.at[mine],
            dst_ref=all_ref.at[me, mine],
            send_sem=send.at[k],
            recv_sem=recv.at[k],
            device_id={"dp": lax.rem(me + k, size)},
            device_id_type=MESH,
        )

    def relay(k):
        source = lax.rem(me + size - k, size)
        return pair_copy(all_ref.at[source, mine], all_ref.at[source, mine], (up_send, up_recv), k)

    def start(k, carry):
        copy(k).start()
        return carry

    def forward(k, carry):
        copy(k).wait_recv()
        relay(k).start()
        return carry

    def finish(k, carry):
        copy(k).wait_send()
        relay(k).wait()
        return carry

    norm(mine)
    lax.fori_loop(1, size, start, 0)
    norm(pl.ds(pl.multiple_of((1 - core) * half, half), half))
    all_ref[me] = normed[...]
    lax.fori_loop(1, size, forward, 0)
    lax.fori_loop(1, size, finish, 0)


def share_rows(part, x, gain, ident):
    size = lax.axis_size("dp")
    rows, width = part.shape
    sems = pltpu.SemaphoreType.DMA((size,))
    return pl.pallas_call(
        share_rows_kernel,
        name="share_rows",
        in_specs=whole_vmem(3),
        out_specs=whole_vmem(2),
        out_shape=[
            jax.ShapeDtypeStruct((rows, width), jnp.float32),
            jax.ShapeDtypeStruct((size, rows, width), jnp.bfloat16),
        ],
        scratch_shapes=[
            pltpu.VMEM((rows, width), jnp.bfloat16),
            pltpu.VMEM((rows, width), jnp.bfloat16),
            sems,
            sems,
            sems,
            sems,
        ],
        compiler_params=pltpu.CompilerParams(
            collective_id=ident, has_side_effects=True, vmem_limit_bytes=LIMIT
        ),
    )(part, x, gain)


def return_rows_kernel(
    part_ref, out_ref, held, summed, landed, sent, send, recv, up_send, up_recv
):
    me, size = place_on(("dp",))
    half = part_ref.shape[1] // 2
    core = lax.axis_index("tp")
    mine = pl.ds(pl.multiple_of(core * half, half), half)
    theirs = pl.ds(pl.multiple_of((1 - core) * half, half), half)
    greet([("dp",), ("tp",)])

    def swap(k):
        group = lax.rem(me + k, size)
        return pair_copy(part_ref.at[group, theirs], held.at[k], (up_send, up_recv), k)

    def copy(k):
        return pltpu.make_async_remote_copy(
            src_ref=summed.at[k],
            dst_ref=landed.at[k],
            send_sem=send.at[k],
            recv_sem=recv.at[k],
            device_id={"dp": lax.rem(me + k, size)},
            device_id_type=MESH,
        )

    def total(k):
        group = lax.rem(me + k, size)
        return part_ref[group, mine].astype(jnp.float32) + held[k].astype(jnp.float32)

    def first(k, carry):
        swap(lax.rem(k, size)).start()
        return carry

    def second(k, carry):
        swap(k).wait_recv()
        summed[k] = total(k).astype(jnp.bfloat16)
        copy(k).start()
        return carry

    def third(k, carry):
        copy(k).wait_recv()
        out_ref[mine, :] += landed[k].astype(jnp.float32)
        return carry

    def finish(k, carry):
        swap(k).wait_send()
        copy(k).wait_send()
        return carry

    lax.fori_loop(1, size + 1, first, 0)
    lax.fori_loop(1, size, second, 0)
    swap(0).wait()
    out_ref[mine, :] = total(0)
    lax.fori_loop(1, size, third, 0)
    sent[...] = out_ref[mine, :].astype(jnp.bfloat16)
    out_ref[mine, :] = sent[...].astype(jnp.float32)
    last = pair_copy(sent, summed.at[0], (up_send, up_recv), size)
    last.start()
    lax.fori_loop(1, size, finish, 0)
    last.wait()
    out_ref[theirs, :] = summed[0].astype(jnp.float32)


def return_rows(part, ident, name):
    size, rows, width = part.shape
    blocks = pltpu.VMEM((size, rows // 2, width), jnp.bfloat16)
    sems, more = pltpu.SemaphoreType.DMA((size,)), pltpu.SemaphoreType.DMA((size + 1,))
    return pl.pallas_call(
        return_rows_kernel,
        name=name,
        in_specs=whole_vmem(1),
        out_specs=pl.BlockSpec(memory_space=pltpu.VMEM),
        out_shape=jax.ShapeDtypeStruct((rows, width), jnp.float32),
        scratch_shapes=[
            blocks,
            blocks,
            blocks,
            pltpu.VMEM((rows // 2, width), jnp.bfloat16),
            sems,
            sems,
            more,
            more,
        ],
        compiler_params=pltpu.CompilerParams(
            collective_id=ident, has_side_effects=True, vmem_limit_bytes=LIMIT
        ),
    )(part)


def back_blocks(ctx_size, block_len, length):
    return min(ctx_size - 1, -(-(length // 2 - 1) // block_len))


def ahead_blocks(block_len, length, spans):
    return 0 if block_len % (length // spans) == 0 else 1


def greet_line():
    me, size = lax.axis_index("ctx"), lax.axis_size("ctx")
    barrier = pltpu.get_barrier_semaphore()
    for step in (1, -1):
        other = me + step

        @pl.when((other >= 0) & (other < size))
        def _(other=other):
            pl.semaphore_signal(
                barrier, inc=1, device_id={"ctx": other}, device_id_type=MESH
            )

    inner = (me > 0) & (me < size - 1)

    @pl.when(inner)
    def _():
        pl.semaphore_wait(barrier, 2)

    @pl.when(jnp.logical_not(inner))
    def _():
        pl.semaphore_wait(barrier, 1)


def line_copy(src, dst, sems, k, other):
    return pltpu.make_async_remote_copy(
        src_ref=src,
        dst_ref=dst,
        send_sem=sems[0].at[k],
        recv_sem=sems[1].at[k],
        device_id={"ctx": other},
        device_id_type=MESH,
    )


def window_kernel(back, ahead, kv_ref, all_ref, send, recv):
    me, size = lax.axis_index("ctx"), lax.axis_size("ctx")
    greet_line()
    right, left = me + 1, me - 1
    if ahead:

        @pl.when(left >= 0)
        def _():
            line_copy(kv_ref, all_ref.at[me], (send, recv), back, left).start()

    for s in range(back):
        src = kv_ref if s == 0 else all_ref.at[lax.rem(me + size - s, size)]
        block = lax.rem(me + size - s, size)
        came = lax.rem(me + size - s - 1, size)

        @pl.when((right < size) & (me - s >= 0))
        def _(src=src, block=block, s=s):
            line_copy(src, all_ref.at[block], (send, recv), s, right).start()

        if s == 0:
            all_ref[me] = kv_ref[...]

        @pl.when(me - s - 1 >= 0)
        def _(came=came, s=s):
            line_copy(kv_ref, all_ref.at[came], (send, recv), s, right).wait_recv()

    for s in range(back):

        @pl.when((right < size) & (me - s >= 0))
        def _(s=s):
            line_copy(kv_ref, all_ref.at[me], (send, recv), s, right).wait_send()

    if ahead:

        @pl.when(left >= 0)
        def _():
            line_copy(kv_ref, all_ref.at[me], (send, recv), back, left).wait_send()

        @pl.when(right < size)
        def _():
            line_copy(kv_ref, all_ref.at[me], (send, recv), back, left).wait_recv()


def window(kv, back, ahead, ident):
    return pl.pallas_call(
        functools.partial(window_kernel, back, ahead),
        name="window",
        in_specs=whole_vmem(1),
        out_specs=pl.BlockSpec(memory_space=pltpu.VMEM),
        out_shape=jax.ShapeDtypeStruct((lax.axis_size("ctx"),) + kv.shape, kv.dtype),
        scratch_shapes=[
            pltpu.SemaphoreType.DMA((back + 1,)),
            pltpu.SemaphoreType.DMA((back + 1,)),
        ],
        compiler_params=pltpu.CompilerParams(
            collective_id=ident, has_side_effects=True, vmem_limit_bytes=LIMIT
        ),
    )(kv)


def window_sum_kernel(back, ahead, grad_ref, out_ref, going, came, send, recv):
    me, size = lax.axis_index("ctx"), lax.axis_size("ctx")
    greet_line()
    right, left = me + 1, me - 1
    if ahead:

        @pl.when(right < size)
        def _():
            line_copy(
                grad_ref.at[lax.rem(me + 1, size)], came.at[0], (send, recv), 0, right
            ).start()

    for s in range(back, 0, -1):
        piece = lax.rem(me + size - s, size)

        own = grad_ref.at[piece]
        if s == back:

            @pl.when(me - s >= 0)
            def _(own=own, s=s):
                line_copy(own, came.at[s], (send, recv), s, left).start()

        else:

            @pl.when((me - s >= 0) & (right < size))
            def _(piece=piece, s=s):
                line_copy(going.at[s], came.at[s + 1], (send, recv), s + 1, left).wait_recv()
                going[s] = (
                    grad_ref[piece].astype(jnp.float32) + came[s + 1].astype(jnp.float32)
                ).astype(going.dtype)
                line_copy(going.at[s], came.at[s], (send, recv), s, left).start()

            @pl.when((me - s >= 0) & (right >= size))
            def _(own=own, s=s):
                line_copy(own, came.at[s], (send, recv), s, left).start()

    out_ref[...] = grad_ref[me].astype(jnp.float32)

    @pl.when(right < size)
    def _():
        line_copy(going.at[1], came.at[1], (send, recv), 1, left).wait_recv()
        out_ref[...] += came[1].astype(jnp.float32)

    if ahead:

        @pl.when(left >= 0)
        def _():
            line_copy(going.at[1], came.at[0], (send, recv), 0, left).wait_recv()
            out_ref[...] += came[0].astype(jnp.float32)

        @pl.when(right < size)
        def _():
            line_copy(going.at[1], came.at[0], (send, recv), 0, right).wait_send()

    for s in range(back, 0, -1):

        @pl.when(me - s >= 0)
        def _(s=s):
            line_copy(going.at[s], came.at[s], (send, recv), s, left).wait_send()


def window_sum(grad, back, ahead, ident):
    held = pltpu.VMEM((back + 1,) + grad.shape[1:], grad.dtype)
    return pl.pallas_call(
        functools.partial(window_sum_kernel, back, ahead),
        name="window_sum",
        in_specs=whole_vmem(1),
        out_specs=pl.BlockSpec(memory_space=pltpu.VMEM),
        out_shape=jax.ShapeDtypeStruct(grad.shape[1:], jnp.float32),
        scratch_shapes=[
            held,
            held,
            pltpu.SemaphoreType.DMA((back + 1,)),
            pltpu.SemaphoreType.DMA((back + 1,)),
        ],
        compiler_params=pltpu.CompilerParams(
            collective_id=ident, has_side_effects=True, vmem_limit_bytes=LIMIT
        ),
    )(grad)


def rms_norm(tensor, gain_vec):
    return (
        tensor * lax.rsqrt(jnp.mean(tensor * tensor, axis=-1, keepdims=True) + EPSILON) * gain_vec
    )


def norm_back(x, gain, grad):
    scale = lax.rsqrt(jnp.mean(x * x, axis=-1, keepdims=True) + EPSILON)
    unit = x * scale
    pull = grad * gain
    return (
        scale * (pull - unit * jnp.mean(pull * unit, axis=-1, keepdims=True)),
        jnp.sum(grad * unit, axis=0),
    )


def rotary_tables(token_positions, heads):
    half_dim = HEAD_DIM // 2
    inverse = THETA ** (-(jnp.arange(half_dim, dtype=jnp.float32) * 2.0 / HEAD_DIM))
    angles = token_positions.astype(jnp.float32)[:, None] * inverse[None, :]
    return jnp.cos(angles)[:, None, :], jnp.sin(angles)[:, None, :]


def rotate(tensor, tables, sign):
    rows, width = tensor.shape
    parts = tensor.reshape(rows, width // HEAD_DIM, 2, HEAD_DIM // 2)
    cosine, sine = tables
    first, second = parts[:, :, 0], parts[:, :, 1]
    sine = sine * sign
    return jnp.stack([first * cosine - second * sine, second * cosine + first * sine], 2).reshape(
        rows, width
    )


def picture_of(starts, token_positions):
    inside = (token_positions[:, None] >= starts[None, :]) & (
        token_positions[:, None] < starts[None, :] + PIC
    )
    labels = jnp.arange(starts.shape[0], dtype=jnp.int32) + 1
    return jnp.sum(jnp.where(inside, labels[None, :], 0), axis=-1) - 1


def silu_parts(gate_pre):
    sig = jax.nn.sigmoid(gate_pre)
    return gate_pre * sig, sig * (1.0 + gate_pre * (1.0 - sig))


def experts(weights, chosen_all, gates_all, rows_all, grad_all):
    own, _, model_width, _ = weights.shape
    groups, tok_rows, _ = rows_all.shape
    first_own = lax.axis_index("dp") * own
    named = chosen_all[..., None] == first_own + jnp.arange(own, dtype=jnp.int32)
    names = jnp.any(named, axis=2)
    gate_of = jnp.sum(jnp.where(named, gates_all[..., None], 0.0), axis=2)
    earlier = jnp.tril(jnp.ones((tok_rows, tok_rows), jnp.bfloat16), -1)
    place = jnp.einsum(
        "rq,gqe->gre", earlier, names.astype(jnp.bfloat16), preferred_element_type=jnp.float32
    ).astype(jnp.int32)
    place = jnp.where(names & (place < CAP), place, -1)
    picks = place.transpose(0, 2, 1)[:, :, None, :] == jnp.arange(CAP, dtype=jnp.int32)[:, None]
    slot_gate = jnp.sum(jnp.where(picks, gate_of.transpose(0, 2, 1)[:, :, None, :], 0.0), axis=-1)
    picks = picks.astype(jnp.bfloat16)
    gate_col = slot_gate.transpose(1, 0, 2).reshape(own, groups * CAP, 1)

    def take(source):
        return jnp.einsum(
            "gesr,grd->egsd", picks, source, preferred_element_type=jnp.float32
        ).reshape(own, groups * CAP, model_width)

    def into(slots, matrix):
        return jnp.einsum("ecd,edf->ecf", slots, matrix, preferred_element_type=jnp.float32)

    def back(slots, matrix):
        return jnp.einsum("ecf,edf->ecd", slots, matrix, preferred_element_type=jnp.float32)

    def outer(left, right):
        return jnp.einsum("ecd,ecf->edf", left, right, preferred_element_type=jnp.float32)

    def combine(slots):
        return jnp.einsum(
            "gesr,egsd->grd",
            picks,
            slots.astype(jnp.bfloat16).reshape(own, groups, CAP, model_width),
            preferred_element_type=jnp.float32,
        ).astype(jnp.bfloat16)

    slot_rows = take(rows_all).astype(jnp.bfloat16)
    slot_grads = (take(grad_all) * gate_col).astype(jnp.bfloat16)
    gate_pre, up_pre = into(slot_rows, weights[:, 0]), into(slot_rows, weights[:, 1])
    silu, slope = silu_parts(gate_pre)
    act_grad = into(slot_grads, weights[:, 2])
    gate_low = (act_grad * up_pre * slope).astype(jnp.bfloat16)
    up_low = (act_grad * silu).astype(jnp.bfloat16)
    act_low = (silu * up_pre).astype(jnp.bfloat16)
    back_part = combine(back(gate_low, weights[:, 0]) + back(up_low, weights[:, 1]))
    out_part = combine(back(act_low, weights[:, 2]) * gate_col)
    weight_part = jnp.stack(
        [outer(slot_rows, gate_low), outer(slot_rows, up_low), outer(slot_grads, act_low)], axis=1
    ).astype(jnp.bfloat16)
    return out_part, back_part, weight_part


def body(
    tokens,
    query_weight,
    key_weight,
    value_weight,
    output_weight,
    gain_attn,
    gain_moe,
    expert_weights,
    routes,
    gate_values,
    documents,
    pic_starts,
    cotangent,
):
    _, block_len, model_width = tokens.shape
    dp_size, ctx_size = lax.axis_size("dp"), lax.axis_size("ctx")
    length = block_len * ctx_size
    offset = lax.axis_index("ctx") * block_len
    back = back_blocks(ctx_size, block_len, length)
    ahead = ahead_blocks(block_len, length, pic_starts.shape[1])
    q_width, kv_width = query_weight.shape[1], key_weight.shape[1]

    joined_w = jnp.concatenate([query_weight, key_weight, value_weight], axis=1)
    gains = jnp.stack([gain_attn, gain_moe]).astype(jnp.float32)
    joined_all, gains_all, docs_all, chosen_all, gates_all = spread(
        [
            joined_w,
            gains,
            documents,
            routes.reshape(block_len * TOP // 128, 128),
            gate_values.reshape(block_len * TOP // 128, 128),
        ],
        [("dp",), ("dp",), ("ctx",), ("dp",), ("dp",)],
        1,
        "spread_weights",
    )
    output_weight, cot, joined_all = lax.optimization_barrier(
        (output_weight, cotangent[0], joined_all)
    )
    output_full = lax.all_gather(output_weight, "dp", axis=1, tiled=True)
    grad_all = lax.all_gather(cot, "dp", axis=0)
    chosen_all = chosen_all.reshape(dp_size, block_len, TOP)
    gates_all = gates_all.reshape(dp_size, block_len, TOP)
    joined_full = joined_all.reshape(model_width, -1)
    gain_rows = gains_all.transpose(1, 0, 2).reshape(2, 1, model_width)
    docs_all = docs_all.reshape(length)

    pictures = picture_of(pic_starts[0], jnp.arange(length, dtype=jnp.int32))
    flags = block_flags(pic_starts[0], documents[0], docs_all, offset)
    kinfo = jnp.stack([docs_all, pictures], axis=1)
    qinfo = jnp.stack([documents[0], lax.dynamic_slice_in_dim(pictures, offset, block_len)])
    tables = rotary_tables(offset + jnp.arange(block_len, dtype=jnp.int32), 1)

    x = tokens[0].astype(jnp.float32)
    normed_one = rms_norm(x, gain_rows[0]).astype(jnp.bfloat16)
    projected = jnp.dot(normed_one, joined_full, preferred_element_type=jnp.float32)
    rotated = rotate(projected[:, : q_width + kv_width], tables, 1.0).astype(jnp.bfloat16)
    query = rotated[:, :q_width] * jnp.bfloat16(HEAD_DIM**-0.5)
    kv = jnp.concatenate(
        [rotated[:, q_width:], projected[:, q_width + kv_width :].astype(jnp.bfloat16)], axis=1
    )
    kv_all = window(kv, back, ahead, 2).reshape(length, 2 * kv_width)
    mixture, mix_full, log_total, attn_part = attend(
        flags, query, kv_all, kinfo, qinfo, output_full
    )
    hidden, rows_all = share_rows(attn_part, tokens[0], gain_rows[1], 3)
    out_part, back_part, weight_part = experts(
        expert_weights, chosen_all, gates_all, rows_all, grad_all
    )
    expert_grad = lax.psum_scatter(weight_part, "ctx", scatter_dimension=2, tiled=True)
    normed_two_grad = return_rows(back_part, 4, "return_grads")
    layer_out = hidden + return_rows(out_part, 5, "return_rows")

    norm_grad, gain_two_grad = norm_back(hidden, gain_rows[1], normed_two_grad)
    hidden_grad = cotangent[0].astype(jnp.float32) + norm_grad
    hidden_low = hidden_grad.astype(jnp.bfloat16)
    output_grad = lax.dot_general(
        hidden_low, mixture, (((0,), (0,)), ((), ())), preferred_element_type=jnp.float32
    )
    mix_grad = lax.dot_general(
        hidden_low, output_full, NT, preferred_element_type=jnp.float32
    ).astype(jnp.bfloat16)
    q_rot_grad, kv_part = attend_back(
        flags, query, kv_all, kinfo, qinfo, log_total, mix_full, mix_grad
    )
    kv_back = window_sum(kv_part.reshape(ctx_size, block_len, 2 * kv_width), back, ahead, 6)
    qk_grad = rotate(jnp.concatenate([q_rot_grad, kv_back[:, :kv_width]], axis=1), tables, -1.0)
    joined_grad = jnp.concatenate([qk_grad, kv_back[:, kv_width:]], axis=1).astype(jnp.bfloat16)
    joined_w_grad = lax.dot_general(
        normed_one, joined_grad, (((0,), (0,)), ((), ())), preferred_element_type=jnp.float32
    )
    normed_part = lax.dot_general(
        joined_grad, joined_full, NT, preferred_element_type=jnp.float32
    ).astype(jnp.bfloat16)
    (both,) = spread([normed_part], [("tp",)], 7, "spread_normed")
    normed_one_grad = both[0].astype(jnp.float32) + both[1].astype(jnp.float32)
    x_norm_grad, gain_one_grad = norm_back(x, gain_rows[0], normed_one_grad)
    input_grad = (hidden_grad + x_norm_grad).astype(jnp.bfloat16)

    sums = jnp.concatenate(
        [
            joined_w_grad,
            output_grad,
            gain_one_grad[:, None],
            gain_two_grad[:, None],
            jnp.zeros((model_width, 126), jnp.float32),
        ],
        axis=1,
    ).astype(jnp.bfloat16)
    width = sums.shape[1]
    part = swap_sum(sums.reshape(dp_size, -1, width), ("dp",), 8, "sum_dp").astype(jnp.bfloat16)
    owned = swap_sum(part.reshape(ctx_size, -1, width), ("ctx",), 9, "sum_ctx")
    v_end = q_width + 2 * kv_width
    return (
        layer_out.astype(jnp.bfloat16)[None],
        input_grad[None],
        owned[:, :q_width],
        owned[:, q_width : q_width + kv_width],
        owned[:, q_width + kv_width : v_end],
        owned[:, v_end : v_end + q_width].T,
        owned[:, v_end + q_width],
        owned[:, v_end + q_width + 1],
        expert_grad.astype(jnp.float32),
    )


def solution(mesh):
    return jax.shard_map(
        body,
        mesh=mesh,
        in_specs=(
            P("dp", "ctx", None),
            P("dp", "tp"),
            P("dp", "tp"),
            P("dp", "tp"),
            P("tp", "dp"),
            P("dp"),
            P("dp"),
            P("dp", None, None, "tp"),
            P("dp", "ctx", None),
            P("dp", "ctx", None),
            P("dp", "ctx"),
            P("dp", None),
            P("dp", "ctx", None),
        ),
        out_specs=(
            P("dp", "ctx", None),
            P("dp", "ctx", None),
            P(("dp", "ctx"), "tp"),
            P(("dp", "ctx"), "tp"),
            P(("dp", "ctx"), "tp"),
            P("tp", ("dp", "ctx")),
            P(("dp", "ctx")),
            P(("dp", "ctx")),
            P("dp", None, "ctx", "tp"),
        ),
        check_vma=False,
    )
```

```python
import functools

import jax
import jax.numpy as jnp
from jax import lax
from jax.experimental import pallas as pl
from jax.experimental.pallas import tpu as pltpu
from jax.sharding import PartitionSpec as P

HEAD_DIM = 64
TOP = 8
PIC = 256
CAP = 144

EPSILON = 1e-06
THETA = 10000.0
NEG_FILL = -1e30


KEY_ROWS = 256
NT = (((1,), (1,)), ((), ()))
LIMIT = 60 * 1024 * 1024


def seen_bias(flags, j, blocks, kinfo_ref, qinfo_ref):
    rows = pl.ds(pl.multiple_of(j * KEY_ROWS, KEY_ROWS), KEY_ROWS)
    q_doc, q_pic = qinfo_ref[0:1, :], qinfo_ref[1:2, :]
    k_doc, k_pic = kinfo_ref[rows, 0:1], kinfo_ref[rows, 1:2]
    q_place = flags[blocks] + lax.broadcasted_iota(jnp.int32, q_doc.shape, 1)
    k_place = j * KEY_ROWS + lax.broadcasted_iota(jnp.int32, k_doc.shape, 0)
    seen = (k_doc == q_doc) & ((k_place <= q_place) | ((k_pic == q_pic) & (q_pic >= 0)))
    return rows, jnp.where(seen, 0.0, NEG_FILL)


def attend_kernel(
    flags, q_ref, kv_ref, kinfo_ref, qinfo_ref, out_w_ref, mix_ref, full_ref, log_ref, part_ref,
    acc, top, total,
):
    blocks = kv_ref.shape[0] // KEY_ROWS
    kv_width = kv_ref.shape[1] // 2
    heads, kv_heads = q_ref.shape[1] // HEAD_DIM, kv_width // HEAD_DIM
    top[...] = jnp.full(top.shape, NEG_FILL, jnp.float32)
    total[...] = jnp.zeros(total.shape, jnp.float32)
    acc[...] = jnp.zeros(acc.shape, jnp.float32)

    def step(j, carry):
        @pl.when(flags[j] > 0)
        def _():
            rows, bias = seen_bias(flags, j, blocks, kinfo_ref, qinfo_ref)
            for g in range(kv_heads):
                key = kv_ref[rows, g * HEAD_DIM : (g + 1) * HEAD_DIM]
                val = kv_ref[rows, kv_width + g * HEAD_DIM : kv_width + (g + 1) * HEAD_DIM]
                val_t = jnp.transpose(val.astype(jnp.float32)).astype(jnp.bfloat16)
                for h in range(g * heads // kv_heads, (g + 1) * heads // kv_heads):
                    at = slice(h * HEAD_DIM, (h + 1) * HEAD_DIM)
                    scores = bias + lax.dot_general(
                        key, q_ref[:, at], NT, preferred_element_type=jnp.float32
                    )
                    old = top[h : h + 1, :]
                    new = jnp.maximum(old, jnp.max(scores, axis=0, keepdims=True))
                    probs = jnp.exp(scores - new)
                    fade = jnp.exp(old - new)
                    total[h : h + 1, :] = total[h : h + 1, :] * fade + jnp.sum(
                        probs, axis=0, keepdims=True
                    )
                    acc[at, :] = acc[at, :] * fade + jnp.dot(
                        val_t, probs.astype(jnp.bfloat16), preferred_element_type=jnp.float32
                    )
                    top[h : h + 1, :] = new

        return carry

    lax.fori_loop(0, blocks, step, 0)
    log_ref[...] = top[...] + jnp.log(total[...])
    for h in range(heads):
        at = slice(h * HEAD_DIM, (h + 1) * HEAD_DIM)
        acc[at, :] = acc[at, :] / total[h : h + 1, :]
    full = jnp.transpose(acc[...])
    full_ref[...] = full
    mix_ref[...] = full.astype(jnp.bfloat16)
    part_ref[...] = jnp.dot(
        mix_ref[...], out_w_ref[...], preferred_element_type=jnp.float32
    ).astype(jnp.bfloat16)


def attend_back_kernel(
    flags, q_ref, kv_ref, kinfo_ref, qinfo_ref, log_ref, full_ref, grad_ref, dq_ref, dkv_ref,
    acc, delta,
):
    blocks = kv_ref.shape[0] // KEY_ROWS
    kv_width = kv_ref.shape[1] // 2
    heads, kv_heads = q_ref.shape[1] // HEAD_DIM, kv_width // HEAD_DIM
    acc[...] = jnp.transpose(full_ref[...] * grad_ref[...].astype(jnp.float32))
    for h in range(heads):
        delta[h : h + 1, :] = jnp.sum(
            acc[h * HEAD_DIM : (h + 1) * HEAD_DIM, :], axis=0, keepdims=True
        )
    acc[...] = jnp.zeros(acc.shape, jnp.float32)

    def step(j, carry):
        @pl.when(flags[j] > 0)
        def _():
            rows, bias = seen_bias(flags, j, blocks, kinfo_ref, qinfo_ref)
            for g in range(kv_heads):
                k_at = slice(g * HEAD_DIM, (g + 1) * HEAD_DIM)
                v_at = slice(kv_width + g * HEAD_DIM, kv_width + (g + 1) * HEAD_DIM)
                key, val = kv_ref[rows, k_at], kv_ref[rows, v_at]
                key_t = jnp.transpose(key.astype(jnp.float32)).astype(jnp.bfloat16)
                dk = jnp.zeros((KEY_ROWS, HEAD_DIM), jnp.float32)
                dv = jnp.zeros((KEY_ROWS, HEAD_DIM), jnp.float32)
                for h in range(g * heads // kv_heads, (g + 1) * heads // kv_heads):
                    at = slice(h * HEAD_DIM, (h + 1) * HEAD_DIM)
                    q_rows, g_rows = q_ref[:, at], grad_ref[:, at]
                    scores = bias + lax.dot_general(
                        key, q_rows, NT, preferred_element_type=jnp.float32
                    )
                    probs = jnp.exp(scores - log_ref[h : h + 1, :])
                    prob_grad = lax.dot_general(
                        val, g_rows, NT, preferred_element_type=jnp.float32
                    )
                    slope = (probs * (prob_grad - delta[h : h + 1, :])).astype(jnp.bfloat16)
                    dv += jnp.dot(
                        probs.astype(jnp.bfloat16), g_rows, preferred_element_type=jnp.float32
                    )
                    dk += jnp.dot(slope, q_rows, preferred_element_type=jnp.float32)
                    acc[at, :] += jnp.dot(key_t, slope, preferred_element_type=jnp.float32)
                dkv_ref[rows, k_at] = dk.astype(dkv_ref.dtype)
                dkv_ref[rows, v_at] = dv.astype(dkv_ref.dtype)

        @pl.when(flags[j] == 0)
        def _():
            rows = pl.ds(pl.multiple_of(j * KEY_ROWS, KEY_ROWS), KEY_ROWS)
            dkv_ref[rows, :] = jnp.zeros((KEY_ROWS, dkv_ref.shape[1]), dkv_ref.dtype)

        return carry

    lax.fori_loop(0, blocks, step, 0)
    dq_ref[...] = jnp.transpose(acc[...]) * (HEAD_DIM**-0.5)


def whole_vmem(count):
    return [pl.BlockSpec(memory_space=pltpu.VMEM)] * count


def attend(flags, q, kv, kinfo, qinfo, out_w):
    rows, width = q.shape
    heads = width // HEAD_DIM
    return pl.pallas_call(
        attend_kernel,
        name="attend",
        in_specs=[pl.BlockSpec(memory_space=pltpu.SMEM)] + whole_vmem(5),
        out_specs=whole_vmem(4),
        out_shape=[
            jax.ShapeDtypeStruct((rows, width), jnp.bfloat16),
            jax.ShapeDtypeStruct((rows, width), jnp.float32),
            jax.ShapeDtypeStruct((heads, rows), jnp.float32),
            jax.ShapeDtypeStruct((rows, out_w.shape[1]), jnp.bfloat16),
        ],
        scratch_shapes=[
            pltpu.VMEM((width, rows), jnp.float32),
            pltpu.VMEM((heads, rows), jnp.float32),
            pltpu.VMEM((heads, rows), jnp.float32),
        ],
        compiler_params=pltpu.CompilerParams(vmem_limit_bytes=LIMIT),
    )(flags, q, kv, kinfo, qinfo, out_w)


def attend_back(flags, q, kv, kinfo, qinfo, log_total, full, grad):
    rows, width = q.shape
    return pl.pallas_call(
        attend_back_kernel,
        name="attend_back",
        in_specs=[pl.BlockSpec(memory_space=pltpu.SMEM)] + whole_vmem(7),
        out_specs=whole_vmem(2),
        out_shape=[
            jax.ShapeDtypeStruct((rows, width), jnp.float32),
            jax.ShapeDtypeStruct(kv.shape, jnp.bfloat16),
        ],
        scratch_shapes=[
            pltpu.VMEM((width, rows), jnp.float32),
            pltpu.VMEM((width // HEAD_DIM, rows), jnp.float32),
        ],
        compiler_params=pltpu.CompilerParams(vmem_limit_bytes=LIMIT),
    )(flags, q, kv, kinfo, qinfo, log_total, full, grad)


def block_flags(pic_starts, q_docs, k_docs, offset):
    block_len, length = q_docs.shape[0], k_docs.shape[0]
    docs = k_docs.reshape(length // KEY_ROWS, KEY_ROWS)
    first = jnp.arange(length // KEY_ROWS, dtype=jnp.int32) * KEY_ROWS
    same = (docs[:, 0] <= q_docs[-1]) & (docs[:, -1] >= q_docs[0])
    spans = (
        (pic_starts[None, :] < offset + block_len)
        & (pic_starts[None, :] + PIC > offset)
        & (pic_starts[None, :] < first[:, None] + KEY_ROWS)
        & (pic_starts[None, :] + PIC > first[:, None])
    )
    needed = same & ((first < offset + block_len) | jnp.any(spans, axis=1))
    return jnp.concatenate([needed.astype(jnp.int32), offset[None].astype(jnp.int32)])


MESH = pl.DeviceIdType.MESH


def place_on(axes):
    index, size = 0, 1
    for axis in axes:
        index = index * lax.axis_size(axis) + lax.axis_index(axis)
        size *= lax.axis_size(axis)
    return index, size


def peer_id(axes, index):
    ids = {}
    for axis in reversed(axes):
        count = lax.axis_size(axis)
        ids[axis] = lax.rem(index, count)
        index = lax.div(index, count)
    return ids


def greet(groups):
    barrier = pltpu.get_barrier_semaphore()
    count = 0
    for axes in groups:
        me, size = place_on(axes)

        def signal(k, carry, axes=axes, me=me, size=size):
            pl.semaphore_signal(
                barrier,
                inc=1,
                device_id=peer_id(axes, lax.rem(me + k, size)),
                device_id_type=MESH,
            )
            return carry

        lax.fori_loop(1, size, signal, 0)
        count += size - 1
    pl.semaphore_wait(barrier, count)


def spread_kernel(axes_of, *refs):
    count = len(axes_of)
    ins, outs, sems = refs[:count], refs[count : 2 * count], refs[2 * count :]
    groups = []
    for axes in axes_of:
        if axes not in groups:
            groups.append(axes)
    greet(groups)

    def copy(i, k):
        me, size = place_on(axes_of[i])
        return pltpu.make_async_remote_copy(
            src_ref=ins[i],
            dst_ref=outs[i].at[me],
            send_sem=sems[2 * i].at[k],
            recv_sem=sems[2 * i + 1].at[k],
            device_id=peer_id(axes_of[i], lax.rem(me + k, size)),
            device_id_type=MESH,
        )

    def start(i, k):
        copy(i, k).start()
        return 0

    def finish(i, k):
        copy(i, k).wait()
        return 0

    for i in range(count):
        lax.fori_loop(1, place_on(axes_of[i])[1], lambda k, c, i=i: start(i, k), 0)
    for i in range(count):
        outs[i][place_on(axes_of[i])[0]] = ins[i][...]
    for i in range(count):
        lax.fori_loop(1, place_on(axes_of[i])[1], lambda k, c, i=i: finish(i, k), 0)


def spread(arrays, axes_of, ident, name):
    sizes = [place_on(axes)[1] for axes in axes_of]
    scratch = []
    for size in sizes:
        scratch += [pltpu.SemaphoreType.DMA((size,)), pltpu.SemaphoreType.DMA((size,))]
    return pl.pallas_call(
        functools.partial(spread_kernel, tuple(axes_of)),
        name=name,
        in_specs=whole_vmem(len(arrays)),
        out_specs=whole_vmem(len(arrays)),
        out_shape=[
            jax.ShapeDtypeStruct((size,) + a.shape, a.dtype) for size, a in zip(sizes, arrays)
        ],
        scratch_shapes=scratch,
        compiler_params=pltpu.CompilerParams(
            collective_id=ident, has_side_effects=True, vmem_limit_bytes=LIMIT
        ),
    )(*arrays)


def swap_sum_kernel(axes, x_ref, out_ref, held, send, recv):
    me, size = place_on(axes)
    greet([axes])

    def copy(k):
        peer = lax.rem(me + k, size)
        return pltpu.make_async_remote_copy(
            src_ref=x_ref.at[peer],
            dst_ref=held.at[k],
            send_sem=send.at[k],
            recv_sem=recv.at[k],
            device_id=peer_id(axes, peer),
            device_id_type=MESH,
        )

    def start(k, carry):
        copy(k).start()
        return carry

    def finish(k, carry):
        copy(k).wait()
        out_ref[...] += held[k].astype(jnp.float32)
        return carry

    lax.fori_loop(1, size, start, 0)
    out_ref[...] = x_ref[me].astype(jnp.float32)
    lax.fori_loop(1, size, finish, 0)


def swap_sum(x, axes, ident, name):
    size = place_on(axes)[1]
    return pl.pallas_call(
        functools.partial(swap_sum_kernel, tuple(axes)),
        name=name,
        in_specs=whole_vmem(1),
        out_specs=pl.BlockSpec(memory_space=pltpu.VMEM),
        out_shape=jax.ShapeDtypeStruct(x.shape[1:], jnp.float32),
        scratch_shapes=[
            pltpu.VMEM(x.shape, x.dtype),
            pltpu.SemaphoreType.DMA((size,)),
            pltpu.SemaphoreType.DMA((size,)),
        ],
        compiler_params=pltpu.CompilerParams(
            collective_id=ident, has_side_effects=True, vmem_limit_bytes=LIMIT
        ),
    )(x)


def pair_copy(ref, dst, sems, k):
    return pltpu.make_async_remote_copy(
        src_ref=ref,
        dst_ref=dst,
        send_sem=sems[0].at[k],
        recv_sem=sems[1].at[k],
        device_id={"tp": 1 - lax.axis_index("tp")},
        device_id_type=MESH,
    )


def share_rows_kernel(
    part_ref, x_ref, gain_ref, hidden_ref, all_ref, held, normed, send, recv, up_send, up_recv
):
    me, size = place_on(("dp",))
    half = part_ref.shape[0] // 2
    core = lax.axis_index("tp")
    mine = pl.ds(pl.multiple_of(core * half, half), half)
    greet([("dp",), ("tp",)])
    swap = pair_copy(part_ref, held, (up_send, up_recv), 0)
    swap.start()
    swap.wait()

    def norm(rows):
        total = (
            x_ref[rows, :].astype(jnp.float32)
            + (part_ref[rows, :].astype(jnp.float32) + held[rows, :].astype(jnp.float32))
        )
        hidden_ref[rows, :] = total
        scale = lax.rsqrt(jnp.mean(total * total, axis=-1, keepdims=True) + EPSILON)
        normed[rows, :] = (total * scale * gain_ref[...]).astype(jnp.bfloat16)

    def copy(k):
        return pltpu.make_async_remote_copy(
            src_ref=normed.at[mine],
            dst_ref=all_ref.at[me, mine],
            send_sem=send.at[k],
            recv_sem=recv.at[k],
            device_id={"dp": lax.rem(me + k, size)},
            device_id_type=MESH,
        )

    def relay(k):
        source = lax.rem(me + size - k, size)
        return pair_copy(all_ref.at[source, mine], all_ref.at[source, mine], (up_send, up_recv), k)

    def start(k, carry):
        copy(k).start()
        return carry

    def forward(k, carry):
        copy(k).wait_recv()
        relay(k).start()
        return carry

    def finish(k, carry):
        copy(k).wait_send()
        relay(k).wait()
        return carry

    norm(mine)
    lax.fori_loop(1, size, start, 0)
    norm(pl.ds(pl.multiple_of((1 - core) * half, half), half))
    all_ref[me] = normed[...]
    lax.fori_loop(1, size, forward, 0)
    lax.fori_loop(1, size, finish, 0)


def share_rows(part, x, gain, ident):
    size = lax.axis_size("dp")
    rows, width = part.shape
    sems = pltpu.SemaphoreType.DMA((size,))
    return pl.pallas_call(
        share_rows_kernel,
        name="share_rows",
        in_specs=whole_vmem(3),
        out_specs=whole_vmem(2),
        out_shape=[
            jax.ShapeDtypeStruct((rows, width), jnp.float32),
            jax.ShapeDtypeStruct((size, rows, width), jnp.bfloat16),
        ],
        scratch_shapes=[
            pltpu.VMEM((rows, width), jnp.bfloat16),
            pltpu.VMEM((rows, width), jnp.bfloat16),
            sems,
            sems,
            sems,
            sems,
        ],
        compiler_params=pltpu.CompilerParams(
            collective_id=ident, has_side_effects=True, vmem_limit_bytes=LIMIT
        ),
    )(part, x, gain)


def return_rows_kernel(
    part_ref, out_ref, held, summed, landed, sent, send, recv, up_send, up_recv
):
    me, size = place_on(("dp",))
    half = part_ref.shape[1] // 2
    core = lax.axis_index("tp")
    mine = pl.ds(pl.multiple_of(core * half, half), half)
    theirs = pl.ds(pl.multiple_of((1 - core) * half, half), half)
    greet([("dp",), ("tp",)])

    def swap(k):
        group = lax.rem(me + k, size)
        return pair_copy(part_ref.at[group, theirs], held.at[k], (up_send, up_recv), k)

    def copy(k):
        return pltpu.make_async_remote_copy(
            src_ref=summed.at[k],
            dst_ref=landed.at[k],
            send_sem=send.at[k],
            recv_sem=recv.at[k],
            device_id={"dp": lax.rem(me + k, size)},
            device_id_type=MESH,
        )

    def total(k):
        group = lax.rem(me + k, size)
        return part_ref[group, mine].astype(jnp.float32) + held[k].astype(jnp.float32)

    def first(k, carry):
        swap(lax.rem(k, size)).start()
        return carry

    def second(k, carry):
        swap(k).wait_recv()
        summed[k] = total(k).astype(jnp.bfloat16)
        copy(k).start()
        return carry

    def third(k, carry):
        copy(k).wait_recv()
        out_ref[mine, :] += landed[k].astype(jnp.float32)
        return carry

    def finish(k, carry):
        swap(k).wait_send()
        copy(k).wait_send()
        return carry

    lax.fori_loop(1, size + 1, first, 0)
    lax.fori_loop(1, size, second, 0)
    swap(0).wait()
    out_ref[mine, :] = total(0)
    lax.fori_loop(1, size, third, 0)
    sent[...] = out_ref[mine, :].astype(jnp.bfloat16)
    out_ref[mine, :] = sent[...].astype(jnp.float32)
    last = pair_copy(sent, summed.at[0], (up_send, up_recv), size)
    last.start()
    lax.fori_loop(1, size, finish, 0)
    last.wait()
    out_ref[theirs, :] = summed[0].astype(jnp.float32)


def return_rows(part, ident, name):
    size, rows, width = part.shape
    blocks = pltpu.VMEM((size, rows // 2, width), jnp.bfloat16)
    sems, more = pltpu.SemaphoreType.DMA((size,)), pltpu.SemaphoreType.DMA((size + 1,))
    return pl.pallas_call(
        return_rows_kernel,
        name=name,
        in_specs=whole_vmem(1),
        out_specs=pl.BlockSpec(memory_space=pltpu.VMEM),
        out_shape=jax.ShapeDtypeStruct((rows, width), jnp.float32),
        scratch_shapes=[
            blocks,
            blocks,
            blocks,
            pltpu.VMEM((rows // 2, width), jnp.bfloat16),
            sems,
            sems,
            more,
            more,
        ],
        compiler_params=pltpu.CompilerParams(
            collective_id=ident, has_side_effects=True, vmem_limit_bytes=LIMIT
        ),
    )(part)


def back_blocks(ctx_size, block_len, length):
    return min(ctx_size - 1, -(-(length // 2 - 1) // block_len))


def ahead_blocks(block_len, length, spans):
    return 0 if block_len % (length // spans) == 0 else 1


def greet_line():
    me, size = lax.axis_index("ctx"), lax.axis_size("ctx")
    barrier = pltpu.get_barrier_semaphore()
    for step in (1, -1):
        other = me + step

        @pl.when((other >= 0) & (other < size))
        def _(other=other):
            pl.semaphore_signal(
                barrier, inc=1, device_id={"ctx": other}, device_id_type=MESH
            )

    inner = (me > 0) & (me < size - 1)

    @pl.when(inner)
    def _():
        pl.semaphore_wait(barrier, 2)

    @pl.when(jnp.logical_not(inner))
    def _():
        pl.semaphore_wait(barrier, 1)


def line_copy(src, dst, sems, k, other):
    return pltpu.make_async_remote_copy(
        src_ref=src,
        dst_ref=dst,
        send_sem=sems[0].at[k],
        recv_sem=sems[1].at[k],
        device_id={"ctx": other},
        device_id_type=MESH,
    )


def window_kernel(back, ahead, kv_ref, all_ref, send, recv):
    me, size = lax.axis_index("ctx"), lax.axis_size("ctx")
    greet_line()
    right, left = me + 1, me - 1
    if ahead:

        @pl.when(left >= 0)
        def _():
            line_copy(kv_ref, all_ref.at[me], (send, recv), back, left).start()

    for s in range(back):
        src = kv_ref if s == 0 else all_ref.at[lax.rem(me + size - s, size)]
        block = lax.rem(me + size - s, size)
        came = lax.rem(me + size - s - 1, size)

        @pl.when((right < size) & (me - s >= 0))
        def _(src=src, block=block, s=s):
            line_copy(src, all_ref.at[block], (send, recv), s, right).start()

        if s == 0:
            all_ref[me] = kv_ref[...]

        @pl.when(me - s - 1 >= 0)
        def _(came=came, s=s):
            line_copy(kv_ref, all_ref.at[came], (send, recv), s, right).wait_recv()

    for s in range(back):

        @pl.when((right < size) & (me - s >= 0))
        def _(s=s):
            line_copy(kv_ref, all_ref.at[me], (send, recv), s, right).wait_send()

    if ahead:

        @pl.when(left >= 0)
        def _():
            line_copy(kv_ref, all_ref.at[me], (send, recv), back, left).wait_send()

        @pl.when(right < size)
        def _():
            line_copy(kv_ref, all_ref.at[me], (send, recv), back, left).wait_recv()


def window(kv, back, ahead, ident):
    return pl.pallas_call(
        functools.partial(window_kernel, back, ahead),
        name="window",
        in_specs=whole_vmem(1),
        out_specs=pl.BlockSpec(memory_space=pltpu.VMEM),
        out_shape=jax.ShapeDtypeStruct((lax.axis_size("ctx"),) + kv.shape, kv.dtype),
        scratch_shapes=[
            pltpu.SemaphoreType.DMA((back + 1,)),
            pltpu.SemaphoreType.DMA((back + 1,)),
        ],
        compiler_params=pltpu.CompilerParams(
            collective_id=ident, has_side_effects=True, vmem_limit_bytes=LIMIT
        ),
    )(kv)


def window_sum_kernel(back, ahead, grad_ref, out_ref, going, came, send, recv):
    me, size = lax.axis_index("ctx"), lax.axis_size("ctx")
    greet_line()
    right, left = me + 1, me - 1
    if ahead:

        @pl.when(right < size)
        def _():
            line_copy(
                grad_ref.at[lax.rem(me + 1, size)], came.at[0], (send, recv), 0, right
            ).start()

    for s in range(back, 0, -1):
        piece = lax.rem(me + size - s, size)

        own = grad_ref.at[piece]
        if s == back:

            @pl.when(me - s >= 0)
            def _(own=own, s=s):
                line_copy(own, came.at[s], (send, recv), s, left).start()

        else:

            @pl.when((me - s >= 0) & (right < size))
            def _(piece=piece, s=s):
                line_copy(going.at[s], came.at[s + 1], (send, recv), s + 1, left).wait_recv()
                going[s] = (
                    grad_ref[piece].astype(jnp.float32) + came[s + 1].astype(jnp.float32)
                ).astype(going.dtype)
                line_copy(going.at[s], came.at[s], (send, recv), s, left).start()

            @pl.when((me - s >= 0) & (right >= size))
            def _(own=own, s=s):
                line_copy(own, came.at[s], (send, recv), s, left).start()

    out_ref[...] = grad_ref[me].astype(jnp.float32)

    @pl.when(right < size)
    def _():
        line_copy(going.at[1], came.at[1], (send, recv), 1, left).wait_recv()
        out_ref[...] += came[1].astype(jnp.float32)

    if ahead:

        @pl.when(left >= 0)
        def _():
            line_copy(going.at[1], came.at[0], (send, recv), 0, left).wait_recv()
            out_ref[...] += came[0].astype(jnp.float32)

        @pl.when(right < size)
        def _():
            line_copy(going.at[1], came.at[0], (send, recv), 0, right).wait_send()

    for s in range(back, 0, -1):

        @pl.when(me - s >= 0)
        def _(s=s):
            line_copy(going.at[s], came.at[s], (send, recv), s, left).wait_send()


def window_sum(grad, back, ahead, ident):
    held = pltpu.VMEM((back + 1,) + grad.shape[1:], grad.dtype)
    return pl.pallas_call(
        functools.partial(window_sum_kernel, back, ahead),
        name="window_sum",
        in_specs=whole_vmem(1),
        out_specs=pl.BlockSpec(memory_space=pltpu.VMEM),
        out_shape=jax.ShapeDtypeStruct(grad.shape[1:], jnp.float32),
        scratch_shapes=[
            held,
            held,
            pltpu.SemaphoreType.DMA((back + 1,)),
            pltpu.SemaphoreType.DMA((back + 1,)),
        ],
        compiler_params=pltpu.CompilerParams(
            collective_id=ident, has_side_effects=True, vmem_limit_bytes=LIMIT
        ),
    )(grad)


GROUPS_AT_ONCE = 4


def experts_kernel(
    rows_ref, grads_ref, weights_ref, place_ref, gate_ref, place_col_ref, out_ref, back_ref,
    weight_grad_ref, slots, slot_grads, outs, backs,
):
    e = pl.program_id(1)
    groups, tok_rows, model_width = rows_ref.shape
    owners, part = weight_grad_ref.shape[1], weight_grad_ref.shape[5]
    slot_index = lax.broadcasted_iota(jnp.int32, (CAP, tok_rows), 0)
    gates = []
    for g in range(groups):
        picks = slot_index == place_ref[g, 0]
        gates.append(jnp.sum(jnp.where(picks, gate_ref[g, 0], 0.0), axis=1, keepdims=True))
        picks = picks.astype(jnp.float32).astype(jnp.bfloat16)
        at = slice(g * CAP, (g + 1) * CAP)
        slots[at, :] = jnp.dot(
            picks, rows_ref[g], preferred_element_type=jnp.float32
        ).astype(jnp.bfloat16)
        slot_grads[at, :] = (
            jnp.dot(picks, grads_ref[g], preferred_element_type=jnp.float32) * gates[g]
        ).astype(jnp.bfloat16)
    gate_w, up_w, down_w = (weights_ref.at[0, i] for i in range(3))
    gate_pre = jnp.dot(slots[...], gate_w[...], preferred_element_type=jnp.float32)
    up_pre = jnp.dot(slots[...], up_w[...], preferred_element_type=jnp.float32)
    act_grad = jnp.dot(slot_grads[...], down_w[...], preferred_element_type=jnp.float32)
    sig = 1.0 / (1.0 + jnp.exp(-gate_pre))
    silu = gate_pre * sig
    act_low = (silu * up_pre).astype(jnp.bfloat16)
    up_low = (act_grad * silu).astype(jnp.bfloat16)
    gate_low = (act_grad * up_pre * (sig * (1.0 + gate_pre * (1.0 - sig)))).astype(jnp.bfloat16)

    back = lax.dot_general(
        gate_low, gate_w[...], NT, preferred_element_type=jnp.float32
    ) + lax.dot_general(up_low, up_w[...], NT, preferred_element_type=jnp.float32)
    out = lax.dot_general(act_low, down_w[...], NT, preferred_element_type=jnp.float32)
    for g in range(groups):
        at = slice(g * CAP, (g + 1) * CAP)
        to = pl.ds(pl.multiple_of(e * CAP, CAP), CAP)
        backs[g, to, :] = back[at].astype(jnp.bfloat16)
        outs[g, to, :] = (out[at] * gates[g]).astype(jnp.bfloat16)

    for i, (low, source) in enumerate(
        ((gate_low, slots), (up_low, slots), (act_low, slot_grads))
    ):
        turned = jnp.transpose(low.astype(jnp.float32)).astype(jnp.bfloat16)
        total = jnp.dot(turned, source[...], preferred_element_type=jnp.float32)
        for c in range(owners):
            weight_grad_ref[0, c, 0, i] = total[:, c * part : (c + 1) * part].astype(
                weight_grad_ref.dtype
            )

    @pl.when(e == pl.num_programs(1) - 1)
    def _():
        slot_count = outs.shape[1]
        for g in range(groups):
            tiles = []
            for first in range(0, slot_count, 128):
                wide = min(128, slot_count - first)
                lane = first + lax.broadcasted_iota(jnp.int32, (tok_rows, wide), 1)
                hit = None
                for n in range(first // CAP, (first + wide - 1) // CAP + 1):
                    one = place_col_ref[g, :, n : n + 1] == lane - n * CAP
                    hit = one if hit is None else hit | one
                tiles.append(hit.astype(jnp.float32).astype(jnp.bfloat16))
            spread_picks = jnp.concatenate(tiles, axis=1)
            back_ref[g] = jnp.dot(
                spread_picks, backs[g], preferred_element_type=jnp.float32
            ).astype(jnp.bfloat16)
            out_ref[g] = jnp.dot(
                spread_picks, outs[g], preferred_element_type=jnp.float32
            ).astype(jnp.bfloat16)


def experts(weights, chosen_all, gates_all, rows_all, grad_all):
    own, _, model_width, hidden = weights.shape
    groups, tok_rows, _ = rows_all.shape
    owners = lax.axis_size("ctx")
    named = chosen_all[..., None] == lax.axis_index("dp") * own + jnp.arange(own, dtype=jnp.int32)
    names = jnp.any(named, axis=2)
    gate_of = jnp.sum(jnp.where(named, gates_all[..., None], 0.0), axis=2)
    earlier = jnp.tril(jnp.ones((tok_rows, tok_rows), jnp.bfloat16), -1)
    place = jnp.einsum(
        "rq,gqe->gre", earlier, names.astype(jnp.bfloat16), preferred_element_type=jnp.float32
    ).astype(jnp.int32)
    place = jnp.where(names & (place < CAP), place, -CAP * own)
    at_once = min(GROUPS_AT_ONCE, groups)
    chunks = groups // at_once
    part = model_width // owners
    rows_spec = pl.BlockSpec(
        (at_once, tok_rows, model_width), lambda c, e: (c, 0, 0), pipeline_mode=pl.Buffered(1)
    )
    line_spec = pl.BlockSpec((at_once, 1, 1, tok_rows), lambda c, e: (c, e, 0, 0))
    out_shape = jax.ShapeDtypeStruct(rows_all.shape, jnp.bfloat16)
    flops = own * groups * CAP * model_width * 2 * (9 * hidden + 4 * tok_rows)
    out_part, back_part, weight_part = pl.pallas_call(
        experts_kernel,
        name="experts",
        grid=(chunks, own),
        in_specs=[
            rows_spec,
            rows_spec,
            pl.BlockSpec((1, 3, model_width, hidden), lambda c, e: (e, 0, 0, 0)),
            line_spec,
            line_spec,
            pl.BlockSpec((at_once, tok_rows, own), lambda c, e: (c, 0, 0)),
        ],
        out_specs=[
            rows_spec,
            rows_spec,
            pl.BlockSpec((1, owners, 1, 3, hidden, part), lambda c, e: (c, 0, e, 0, 0, 0)),
        ],
        out_shape=[
            out_shape,
            out_shape,
            jax.ShapeDtypeStruct((chunks, owners, own, 3, hidden, part), jnp.bfloat16),
        ],
        scratch_shapes=[
            pltpu.VMEM((at_once * CAP, model_width), jnp.bfloat16),
            pltpu.VMEM((at_once * CAP, model_width), jnp.bfloat16),
            pltpu.VMEM((at_once, own * CAP, model_width), jnp.bfloat16),
            pltpu.VMEM((at_once, own * CAP, model_width), jnp.bfloat16),
        ],
        compiler_params=pltpu.CompilerParams(vmem_limit_bytes=LIMIT),
        cost_estimate=pl.CostEstimate(
            flops=flops, bytes_accessed=4 * weights.size, transcendentals=0
        ),
    )(
        rows_all,
        grad_all,
        weights,
        place.transpose(0, 2, 1)[:, :, None],
        gate_of.transpose(0, 2, 1)[:, :, None],
        place,
    )
    if chunks == 1:
        return out_part, back_part, weight_part[0]
    return out_part, back_part, jnp.sum(weight_part.astype(jnp.float32), axis=0).astype(
        jnp.bfloat16
    )


def rms_norm(tensor, gain_vec):
    return (
        tensor * lax.rsqrt(jnp.mean(tensor * tensor, axis=-1, keepdims=True) + EPSILON) * gain_vec
    )


def norm_back(x, gain, grad):
    scale = lax.rsqrt(jnp.mean(x * x, axis=-1, keepdims=True) + EPSILON)
    unit = x * scale
    pull = grad * gain
    return (
        scale * (pull - unit * jnp.mean(pull * unit, axis=-1, keepdims=True)),
        jnp.sum(grad * unit, axis=0),
    )


def rotary_tables(token_positions, heads):
    half_dim = HEAD_DIM // 2
    inverse = THETA ** (-(jnp.arange(half_dim, dtype=jnp.float32) * 2.0 / HEAD_DIM))
    angles = token_positions.astype(jnp.float32)[:, None] * inverse[None, :]
    return jnp.cos(angles)[:, None, :], jnp.sin(angles)[:, None, :]


def rotate(tensor, tables, sign):
    rows, width = tensor.shape
    parts = tensor.reshape(rows, width // HEAD_DIM, 2, HEAD_DIM // 2)
    cosine, sine = tables
    first, second = parts[:, :, 0], parts[:, :, 1]
    sine = sine * sign
    return jnp.stack([first * cosine - second * sine, second * cosine + first * sine], 2).reshape(
        rows, width
    )


def picture_of(starts, token_positions):
    inside = (token_positions[:, None] >= starts[None, :]) & (
        token_positions[:, None] < starts[None, :] + PIC
    )
    labels = jnp.arange(starts.shape[0], dtype=jnp.int32) + 1
    return jnp.sum(jnp.where(inside, labels[None, :], 0), axis=-1) - 1


def body(
    tokens,
    query_weight,
    key_weight,
    value_weight,
    output_weight,
    gain_attn,
    gain_moe,
    expert_weights,
    routes,
    gate_values,
    documents,
    pic_starts,
    cotangent,
):
    _, block_len, model_width = tokens.shape
    dp_size, ctx_size = lax.axis_size("dp"), lax.axis_size("ctx")
    length = block_len * ctx_size
    offset = lax.axis_index("ctx") * block_len
    back = back_blocks(ctx_size, block_len, length)
    ahead = ahead_blocks(block_len, length, pic_starts.shape[1])
    q_width, kv_width = query_weight.shape[1], key_weight.shape[1]

    joined_w = jnp.concatenate([query_weight, key_weight, value_weight], axis=1)
    gains = jnp.stack([gain_attn, gain_moe]).astype(jnp.float32)
    joined_all, gains_all, docs_all, chosen_all, gates_all = spread(
        [
            joined_w,
            gains,
            documents,
            routes.reshape(block_len * TOP // 128, 128),
            gate_values.reshape(block_len * TOP // 128, 128),
        ],
        [("dp",), ("dp",), ("ctx",), ("dp",), ("dp",)],
        1,
        "spread_weights",
    )
    output_weight, cot, joined_all = lax.optimization_barrier(
        (output_weight, cotangent[0], joined_all)
    )
    output_full = lax.all_gather(output_weight, "dp", axis=1, tiled=True)
    grad_all = lax.all_gather(cot, "dp", axis=0)
    chosen_all = chosen_all.reshape(dp_size, block_len, TOP)
    gates_all = gates_all.reshape(dp_size, block_len, TOP)
    joined_full = joined_all.reshape(model_width, -1)
    gain_rows = gains_all.transpose(1, 0, 2).reshape(2, 1, model_width)
    docs_all = docs_all.reshape(length)

    pictures = picture_of(pic_starts[0], jnp.arange(length, dtype=jnp.int32))
    flags = block_flags(pic_starts[0], documents[0], docs_all, offset)
    kinfo = jnp.stack([docs_all, pictures], axis=1)
    qinfo = jnp.stack([documents[0], lax.dynamic_slice_in_dim(pictures, offset, block_len)])
    tables = rotary_tables(offset + jnp.arange(block_len, dtype=jnp.int32), 1)

    x = tokens[0].astype(jnp.float32)
    normed_one = rms_norm(x, gain_rows[0]).astype(jnp.bfloat16)
    projected = jnp.dot(normed_one, joined_full, preferred_element_type=jnp.float32)
    rotated = rotate(projected[:, : q_width + kv_width], tables, 1.0).astype(jnp.bfloat16)
    query = rotated[:, :q_width] * jnp.bfloat16(HEAD_DIM**-0.5)
    kv = jnp.concatenate(
        [rotated[:, q_width:], projected[:, q_width + kv_width :].astype(jnp.bfloat16)], axis=1
    )
    kv_all = window(kv, back, ahead, 2).reshape(length, 2 * kv_width)
    mixture, mix_full, log_total, attn_part = attend(
        flags, query, kv_all, kinfo, qinfo, output_full
    )
    hidden, rows_all = share_rows(attn_part, tokens[0], gain_rows[1], 3)
    out_part, back_part, weight_part = experts(
        expert_weights, chosen_all, gates_all, rows_all, grad_all
    )
    expert_grad = lax.psum_scatter(weight_part, "ctx", scatter_dimension=0)
    normed_two_grad = return_rows(back_part, 4, "return_grads")
    layer_out = hidden + return_rows(out_part, 5, "return_rows")

    norm_grad, gain_two_grad = norm_back(hidden, gain_rows[1], normed_two_grad)
    hidden_grad = cotangent[0].astype(jnp.float32) + norm_grad
    hidden_low = hidden_grad.astype(jnp.bfloat16)
    output_grad = lax.dot_general(
        hidden_low, mixture, (((0,), (0,)), ((), ())), preferred_element_type=jnp.float32
    )
    mix_grad = lax.dot_general(
        hidden_low, output_full, NT, preferred_element_type=jnp.float32
    ).astype(jnp.bfloat16)
    q_rot_grad, kv_part = attend_back(
        flags, query, kv_all, kinfo, qinfo, log_total, mix_full, mix_grad
    )
    kv_back = window_sum(kv_part.reshape(ctx_size, block_len, 2 * kv_width), back, ahead, 6)
    qk_grad = rotate(jnp.concatenate([q_rot_grad, kv_back[:, :kv_width]], axis=1), tables, -1.0)
    joined_grad = jnp.concatenate([qk_grad, kv_back[:, kv_width:]], axis=1).astype(jnp.bfloat16)
    joined_w_grad = lax.dot_general(
        normed_one, joined_grad, (((0,), (0,)), ((), ())), preferred_element_type=jnp.float32
    )
    normed_part = lax.dot_general(
        joined_grad, joined_full, NT, preferred_element_type=jnp.float32
    ).astype(jnp.bfloat16)
    (both,) = spread([normed_part], [("tp",)], 7, "spread_normed")
    normed_one_grad = both[0].astype(jnp.float32) + both[1].astype(jnp.float32)
    x_norm_grad, gain_one_grad = norm_back(x, gain_rows[0], normed_one_grad)
    input_grad = (hidden_grad + x_norm_grad).astype(jnp.bfloat16)

    sums = jnp.concatenate(
        [
            joined_w_grad,
            output_grad,
            gain_one_grad[:, None],
            gain_two_grad[:, None],
            jnp.zeros((model_width, 126), jnp.float32),
        ],
        axis=1,
    ).astype(jnp.bfloat16)
    width = sums.shape[1]
    part = swap_sum(sums.reshape(dp_size, -1, width), ("dp",), 8, "sum_dp").astype(jnp.bfloat16)
    owned = swap_sum(part.reshape(ctx_size, -1, width), ("ctx",), 9, "sum_ctx")
    v_end = q_width + 2 * kv_width
    return (
        layer_out.astype(jnp.bfloat16)[None],
        input_grad[None],
        owned[:, :q_width],
        owned[:, q_width : q_width + kv_width],
        owned[:, q_width + kv_width : v_end],
        owned[:, v_end : v_end + q_width].T,
        owned[:, v_end + q_width],
        owned[:, v_end + q_width + 1],
        expert_grad.astype(jnp.float32).transpose(0, 1, 3, 2),
    )


def solution(mesh):
    return jax.shard_map(
        body,
        mesh=mesh,
        in_specs=(
            P("dp", "ctx", None),
            P("dp", "tp"),
            P("dp", "tp"),
            P("dp", "tp"),
            P("tp", "dp"),
            P("dp"),
            P("dp"),
            P("dp", None, None, "tp"),
            P("dp", "ctx", None),
            P("dp", "ctx", None),
            P("dp", "ctx"),
            P("dp", None),
            P("dp", "ctx", None),
        ),
        out_specs=(
            P("dp", "ctx", None),
            P("dp", "ctx", None),
            P(("dp", "ctx"), "tp"),
            P(("dp", "ctx"), "tp"),
            P(("dp", "ctx"), "tp"),
            P("tp", ("dp", "ctx")),
            P(("dp", "ctx")),
            P(("dp", "ctx")),
            P("dp", None, "ctx", "tp"),
        ),
        check_vma=False,
    )
```

```python
import functools

import jax
import jax.numpy as jnp
from jax import lax
from jax.experimental import pallas as pl
from jax.experimental.pallas import tpu as pltpu
from jax.sharding import PartitionSpec as P

HEAD_DIM = 64
TOP = 8
PIC = 256
CAP = 144

EPSILON = 1e-06
THETA = 10000.0
NEG_FILL = -1e30


KEY_ROWS = 256
NT = (((1,), (1,)), ((), ()))
LIMIT = 60 * 1024 * 1024


def seen_bias(flags, j, blocks, kinfo_ref, qinfo_ref):
    rows = pl.ds(pl.multiple_of(j * KEY_ROWS, KEY_ROWS), KEY_ROWS)
    q_doc, q_pic = qinfo_ref[0:1, :], qinfo_ref[1:2, :]
    k_doc, k_pic = kinfo_ref[rows, 0:1], kinfo_ref[rows, 1:2]
    q_place = flags[blocks] + lax.broadcasted_iota(jnp.int32, q_doc.shape, 1)
    k_place = j * KEY_ROWS + lax.broadcasted_iota(jnp.int32, k_doc.shape, 0)
    seen = (k_doc == q_doc) & ((k_place <= q_place) | ((k_pic == q_pic) & (q_pic >= 0)))
    return rows, jnp.where(seen, 0.0, NEG_FILL)


def attend_kernel(
    flags, q_ref, kv_ref, kinfo_ref, qinfo_ref, out_w_ref, mix_ref, full_ref, log_ref, part_ref,
    acc, top, total,
):
    blocks = kv_ref.shape[0] // KEY_ROWS
    kv_width = kv_ref.shape[1] // 2
    heads, kv_heads = q_ref.shape[1] // HEAD_DIM, kv_width // HEAD_DIM
    top[...] = jnp.full(top.shape, NEG_FILL, jnp.float32)
    total[...] = jnp.zeros(total.shape, jnp.float32)
    acc[...] = jnp.zeros(acc.shape, jnp.float32)

    def step(j, carry):
        @pl.when(flags[j] > 0)
        def _():
            rows, bias = seen_bias(flags, j, blocks, kinfo_ref, qinfo_ref)
            for g in range(kv_heads):
                key = kv_ref[rows, g * HEAD_DIM : (g + 1) * HEAD_DIM]
                val = kv_ref[rows, kv_width + g * HEAD_DIM : kv_width + (g + 1) * HEAD_DIM]
                val_t = jnp.transpose(val.astype(jnp.float32)).astype(jnp.bfloat16)
                for h in range(g * heads // kv_heads, (g + 1) * heads // kv_heads):
                    at = slice(h * HEAD_DIM, (h + 1) * HEAD_DIM)
                    scores = bias + lax.dot_general(
                        key, q_ref[:, at], NT, preferred_element_type=jnp.float32
                    )
                    old = top[h : h + 1, :]
                    new = jnp.maximum(old, jnp.max(scores, axis=0, keepdims=True))
                    probs = jnp.exp(scores - new)
                    fade = jnp.exp(old - new)
                    total[h : h + 1, :] = total[h : h + 1, :] * fade + jnp.sum(
                        probs, axis=0, keepdims=True
                    )
                    acc[at, :] = acc[at, :] * fade + jnp.dot(
                        val_t, probs.astype(jnp.bfloat16), preferred_element_type=jnp.float32
                    )
                    top[h : h + 1, :] = new

        return carry

    lax.fori_loop(0, blocks, step, 0)
    log_ref[...] = top[...] + jnp.log(total[...])
    for h in range(heads):
        at = slice(h * HEAD_DIM, (h + 1) * HEAD_DIM)
        acc[at, :] = acc[at, :] / total[h : h + 1, :]
    full = jnp.transpose(acc[...])
    full_ref[...] = full
    mix_ref[...] = full.astype(jnp.bfloat16)
    part_ref[...] = jnp.dot(
        mix_ref[...], out_w_ref[...], preferred_element_type=jnp.float32
    ).astype(jnp.bfloat16)


def attend_back_kernel(
    flags, q_ref, kv_ref, kinfo_ref, qinfo_ref, log_ref, full_ref, grad_ref, dq_ref, dkv_ref,
    acc, delta,
):
    blocks = kv_ref.shape[0] // KEY_ROWS
    kv_width = kv_ref.shape[1] // 2
    heads, kv_heads = q_ref.shape[1] // HEAD_DIM, kv_width // HEAD_DIM
    acc[...] = jnp.transpose(full_ref[...] * grad_ref[...].astype(jnp.float32))
    for h in range(heads):
        delta[h : h + 1, :] = jnp.sum(
            acc[h * HEAD_DIM : (h + 1) * HEAD_DIM, :], axis=0, keepdims=True
        )
    acc[...] = jnp.zeros(acc.shape, jnp.float32)

    def step(j, carry):
        @pl.when(flags[j] > 0)
        def _():
            rows, bias = seen_bias(flags, j, blocks, kinfo_ref, qinfo_ref)
            for g in range(kv_heads):
                k_at = slice(g * HEAD_DIM, (g + 1) * HEAD_DIM)
                v_at = slice(kv_width + g * HEAD_DIM, kv_width + (g + 1) * HEAD_DIM)
                key, val = kv_ref[rows, k_at], kv_ref[rows, v_at]
                key_t = jnp.transpose(key.astype(jnp.float32)).astype(jnp.bfloat16)
                dk = jnp.zeros((KEY_ROWS, HEAD_DIM), jnp.float32)
                dv = jnp.zeros((KEY_ROWS, HEAD_DIM), jnp.float32)
                for h in range(g * heads // kv_heads, (g + 1) * heads // kv_heads):
                    at = slice(h * HEAD_DIM, (h + 1) * HEAD_DIM)
                    q_rows, g_rows = q_ref[:, at], grad_ref[:, at]
                    scores = bias + lax.dot_general(
                        key, q_rows, NT, preferred_element_type=jnp.float32
                    )
                    probs = jnp.exp(scores - log_ref[h : h + 1, :])
                    prob_grad = lax.dot_general(
                        val, g_rows, NT, preferred_element_type=jnp.float32
                    )
                    slope = (probs * (prob_grad - delta[h : h + 1, :])).astype(jnp.bfloat16)
                    dv += jnp.dot(
                        probs.astype(jnp.bfloat16), g_rows, preferred_element_type=jnp.float32
                    )
                    dk += jnp.dot(slope, q_rows, preferred_element_type=jnp.float32)
                    acc[at, :] += jnp.dot(key_t, slope, preferred_element_type=jnp.float32)
                dkv_ref[rows, k_at] = dk.astype(dkv_ref.dtype)
                dkv_ref[rows, v_at] = dv.astype(dkv_ref.dtype)

        @pl.when(flags[j] == 0)
        def _():
            rows = pl.ds(pl.multiple_of(j * KEY_ROWS, KEY_ROWS), KEY_ROWS)
            dkv_ref[rows, :] = jnp.zeros((KEY_ROWS, dkv_ref.shape[1]), dkv_ref.dtype)

        return carry

    lax.fori_loop(0, blocks, step, 0)
    dq_ref[...] = jnp.transpose(acc[...]) * (HEAD_DIM**-0.5)


def whole_vmem(count):
    return [pl.BlockSpec(memory_space=pltpu.VMEM)] * count


def attend(flags, q, kv, kinfo, qinfo, out_w):
    rows, width = q.shape
    heads = width // HEAD_DIM
    return pl.pallas_call(
        attend_kernel,
        name="attend",
        in_specs=[pl.BlockSpec(memory_space=pltpu.SMEM)] + whole_vmem(5),
        out_specs=whole_vmem(4),
        out_shape=[
            jax.ShapeDtypeStruct((rows, width), jnp.bfloat16),
            jax.ShapeDtypeStruct((rows, width), jnp.float32),
            jax.ShapeDtypeStruct((heads, rows), jnp.float32),
            jax.ShapeDtypeStruct((rows, out_w.shape[1]), jnp.bfloat16),
        ],
        scratch_shapes=[
            pltpu.VMEM((width, rows), jnp.float32),
            pltpu.VMEM((heads, rows), jnp.float32),
            pltpu.VMEM((heads, rows), jnp.float32),
        ],
        compiler_params=pltpu.CompilerParams(vmem_limit_bytes=LIMIT),
    )(flags, q, kv, kinfo, qinfo, out_w)


def attend_back(flags, q, kv, kinfo, qinfo, log_total, full, grad):
    rows, width = q.shape
    return pl.pallas_call(
        attend_back_kernel,
        name="attend_back",
        in_specs=[pl.BlockSpec(memory_space=pltpu.SMEM)] + whole_vmem(7),
        out_specs=whole_vmem(2),
        out_shape=[
            jax.ShapeDtypeStruct((rows, width), jnp.float32),
            jax.ShapeDtypeStruct(kv.shape, jnp.bfloat16),
        ],
        scratch_shapes=[
            pltpu.VMEM((width, rows), jnp.float32),
            pltpu.VMEM((width // HEAD_DIM, rows), jnp.float32),
        ],
        compiler_params=pltpu.CompilerParams(vmem_limit_bytes=LIMIT),
    )(flags, q, kv, kinfo, qinfo, log_total, full, grad)


def block_flags(pic_starts, q_docs, k_docs, offset):
    block_len, length = q_docs.shape[0], k_docs.shape[0]
    docs = k_docs.reshape(length // KEY_ROWS, KEY_ROWS)
    first = jnp.arange(length // KEY_ROWS, dtype=jnp.int32) * KEY_ROWS
    same = (docs[:, 0] <= q_docs[-1]) & (docs[:, -1] >= q_docs[0])
    spans = (
        (pic_starts[None, :] < offset + block_len)
        & (pic_starts[None, :] + PIC > offset)
        & (pic_starts[None, :] < first[:, None] + KEY_ROWS)
        & (pic_starts[None, :] + PIC > first[:, None])
    )
    needed = same & ((first < offset + block_len) | jnp.any(spans, axis=1))
    return jnp.concatenate([needed.astype(jnp.int32), offset[None].astype(jnp.int32)])


MESH = pl.DeviceIdType.MESH
TN = (((0,), (0,)), ((), ()))


def place_on(axes):
    index, size = 0, 1
    for axis in axes:
        index = index * lax.axis_size(axis) + lax.axis_index(axis)
        size *= lax.axis_size(axis)
    return index, size


def greet(axes_list, line=False):
    barrier = pltpu.get_barrier_semaphore()
    count = 0
    for axis in axes_list:
        me, size = lax.axis_index(axis), lax.axis_size(axis)

        def signal(k, carry, axis=axis, me=me, size=size):
            pl.semaphore_signal(
                barrier, inc=1, device_id={axis: lax.rem(me + k, size)}, device_id_type=MESH
            )
            return carry

        lax.fori_loop(1, size, signal, 0)
        count += size - 1
    if not line:
        pl.semaphore_wait(barrier, count)
        return
    me, size = lax.axis_index("ctx"), lax.axis_size("ctx")
    for step in (1, -1):
        other = me + step

        @pl.when((other >= 0) & (other < size))
        def _(other=other):
            pl.semaphore_signal(barrier, inc=1, device_id={"ctx": other}, device_id_type=MESH)

    inner = (me > 0) & (me < size - 1)

    @pl.when(inner)
    def _():
        pl.semaphore_wait(barrier, count + 2)

    @pl.when(jnp.logical_not(inner))
    def _():
        pl.semaphore_wait(barrier, count + 1)


def remote(src, dst, sems, k, device_id):
    return pltpu.make_async_remote_copy(
        src_ref=src,
        dst_ref=dst,
        send_sem=sems[0].at[k],
        recv_sem=sems[1].at[k],
        device_id=device_id,
        device_id_type=MESH,
    )


def other_core():
    return {"tp": 1 - lax.axis_index("tp")}


def ahead_on(axis, k):
    return lax.rem(lax.axis_index(axis) + k, lax.axis_size(axis))


def each(count, do, first=1):
    def step(k, carry):
        do(k)
        return carry

    lax.fori_loop(first, count, step, 0)


def sem_pair(count):
    return [pltpu.SemaphoreType.DMA((count,)), pltpu.SemaphoreType.DMA((count,))]


def remote_params(ident):
    return pltpu.CompilerParams(
        collective_id=ident, has_side_effects=True, vmem_limit_bytes=LIMIT
    )


def halves(rows):
    half = rows // 2
    core = lax.axis_index("tp")
    return (
        pl.ds(pl.multiple_of(core * half, half), half),
        pl.ds(pl.multiple_of((1 - core) * half, half), half),
    )


def spread_kernel(axes_of, *refs):
    count = len(axes_of)
    ins, outs, sems = refs[:count], refs[count : 2 * count], refs[2 * count :]
    greet(sorted(set(axes_of)))

    def copy(i, k):
        return remote(
            ins[i],
            outs[i].at[lax.axis_index(axes_of[i])],
            sems[2 * i : 2 * i + 2],
            k,
            {axes_of[i]: ahead_on(axes_of[i], k)},
        )

    for i in range(count):
        each(lax.axis_size(axes_of[i]), lambda k, i=i: copy(i, k).start())
    for i in range(count):
        outs[i][lax.axis_index(axes_of[i])] = ins[i][...]
    for i in range(count):
        each(lax.axis_size(axes_of[i]), lambda k, i=i: copy(i, k).wait())


def spread(arrays, axes_of, ident, name):
    sizes = [lax.axis_size(axis) for axis in axes_of]
    return pl.pallas_call(
        functools.partial(spread_kernel, tuple(axes_of)),
        name=name,
        in_specs=whole_vmem(len(arrays)),
        out_specs=whole_vmem(len(arrays)),
        out_shape=[
            jax.ShapeDtypeStruct((size,) + a.shape, a.dtype) for size, a in zip(sizes, arrays)
        ],
        scratch_shapes=sum([sem_pair(size) for size in sizes], []),
        compiler_params=remote_params(ident),
    )(*arrays)


def turn(tile, cosine, sine):
    lane = lax.broadcasted_iota(jnp.int32, tile.shape, 1)
    half = HEAD_DIM // 2
    swapped = jnp.where(
        lax.rem(lane, HEAD_DIM) < half,
        pltpu.roll(tile, 2 * HEAD_DIM - half, 1),
        pltpu.roll(tile, half, 1),
    )
    return tile * cosine + swapped * sine


def row_scale(x):
    return lax.rsqrt(jnp.mean(x * x, axis=-1, keepdims=True) + EPSILON)


def norm_back(x, gain, grad):
    scale = row_scale(x)
    unit = x * scale
    pull = grad * gain
    return (
        scale * (pull - unit * jnp.mean(pull * unit, axis=-1, keepdims=True)),
        jnp.sum(grad * unit, axis=0, keepdims=True),
    )


def back_blocks(ctx_size, block_len, length):
    return min(ctx_size - 1, -(-(length // 2 - 1) // block_len))


def ahead_blocks(block_len, length, spans):
    return 0 if block_len % (length // spans) == 0 else 1


class RowGather:
    def __init__(self, source, target, dp_sems, tp_sems, first):
        self.source, self.target = source, target
        self.dp_sems, self.tp_sems, self.first = dp_sems, tp_sems, first
        self.mine, _ = halves(source.shape[0])
        self.size = lax.axis_size("dp")

    def copy(self, k):
        at = self.target.at[lax.axis_index("dp"), self.mine]
        return remote(
            self.source.at[self.mine], at, self.dp_sems, k, {"dp": ahead_on("dp", k)}
        )

    def relay(self, k):
        at = self.target.at[ahead_on("dp", self.size - k), self.mine]
        return remote(at, at, self.tp_sems, self.first + k, other_core())

    def start(self):
        each(self.size, lambda k: self.copy(k).start())

    def forward(self):
        def one(k):
            self.copy(k).wait_recv()
            self.relay(k).start()

        each(self.size, one)

    def finish(self):
        def one(k):
            self.copy(k).wait_send()
            self.relay(k).wait()

        each(self.size, one)


def project_kernel(
    back, ahead, q_width, x_ref, w_ref, gain_ref, cos_ref, sin_ref, cot_ref, normed_ref, q_ref,
    all_ref, cot_all_ref, kv_ref, line_send, line_recv, dp_send, dp_recv, tp_send, tp_recv,
):
    me, size = lax.axis_index("ctx"), lax.axis_size("ctx")
    greet(["dp", "tp"], line=True)
    rows_of = RowGather(cot_ref, cot_all_ref, (dp_send, dp_recv), (tp_send, tp_recv), 0)
    rows_of.start()
    x = x_ref[...].astype(jnp.float32)
    normed_ref[...] = (x * row_scale(x) * gain_ref[...]).astype(jnp.bfloat16)
    kv_width = kv_ref.shape[1] // 2
    wide = 2 * HEAD_DIM
    for first in range(q_width, q_width + 2 * kv_width, wide):
        tile = jnp.dot(
            normed_ref[...], w_ref[:, first : first + wide], preferred_element_type=jnp.float32
        )
        if first < q_width + kv_width:
            tile = turn(tile, cos_ref[...], -sin_ref[...])
        kv_ref[:, first - q_width : first - q_width + wide] = tile.astype(jnp.bfloat16)

    sems = (line_send, line_recv)
    right, left = me + 1, me - 1

    def hop(s):
        block = lax.rem(me + size - s, size)
        return remote(
            kv_ref if s == 0 else all_ref.at[block], all_ref.at[block], sems, s, {"ctx": right}
        )

    def arrive(s):
        return remote(kv_ref, all_ref.at[me], sems, s, {"ctx": right})

    def back_hop():
        return remote(kv_ref, all_ref.at[me], sems, back, {"ctx": left})

    if ahead:

        @pl.when(left >= 0)
        def _():
            back_hop().start()

    for s in range(back):

        @pl.when((right < size) & (me - s >= 0))
        def _(s=s):
            hop(s).start()

        if s == 0:
            all_ref[me] = kv_ref[...]
            for first in range(0, q_width, wide):
                tile = jnp.dot(
                    normed_ref[...],
                    w_ref[:, first : first + wide],
                    preferred_element_type=jnp.float32,
                )
                tile = turn(tile, cos_ref[...], -sin_ref[...]).astype(jnp.bfloat16)
                q_ref[:, first : first + wide] = (
                    tile.astype(jnp.float32) * HEAD_DIM**-0.5
                ).astype(jnp.bfloat16)

        @pl.when(me - s - 1 >= 0)
        def _(s=s):
            arrive(s).wait_recv()

    rows_of.forward()
    for s in range(back):

        @pl.when((right < size) & (me - s >= 0))
        def _(s=s):
            hop(s).wait_send()

    if ahead:

        @pl.when(left >= 0)
        def _():
            back_hop().wait_send()

        @pl.when(right < size)
        def _():
            back_hop().wait_recv()

    cot_all_ref[lax.axis_index("dp")] = cot_ref[...]
    rows_of.finish()


def project(x, w, gain, cosine, sine, cot, q_width, back, ahead, ident):
    rows, width = x.shape
    kv_cols = w.shape[1] - q_width
    dp_size, ctx_size = lax.axis_size("dp"), lax.axis_size("ctx")
    low = jnp.bfloat16
    return pl.pallas_call(
        functools.partial(project_kernel, back, ahead, q_width),
        name="project",
        in_specs=whole_vmem(6),
        out_specs=whole_vmem(4),
        out_shape=[
            jax.ShapeDtypeStruct((rows, width), low),
            jax.ShapeDtypeStruct((rows, q_width), low),
            jax.ShapeDtypeStruct((ctx_size, rows, kv_cols), low),
            jax.ShapeDtypeStruct((dp_size, rows, width), low),
        ],
        scratch_shapes=[
            pltpu.VMEM((rows, kv_cols), low),
            *sem_pair(back + 1),
            *sem_pair(dp_size),
            *sem_pair(dp_size),
        ],
        compiler_params=remote_params(ident),
    )(x, w, gain, cosine, sine, cot)


def share_rows_kernel(
    part_ref, x_ref, gain_ref, hidden_ref, all_ref, held, normed, dp_send, dp_recv, tp_send,
    tp_recv,
):
    mine, theirs = halves(part_ref.shape[0])
    greet(["dp", "tp"])
    size = lax.axis_size("dp")
    rows_of = RowGather(normed, all_ref, (dp_send, dp_recv), (tp_send, tp_recv), 1)
    first = remote(part_ref.at[theirs], held.at[theirs], (tp_send, tp_recv), 0, other_core())
    second = remote(part_ref.at[mine], held.at[mine], (tp_send, tp_recv), 1, other_core())
    first.start()
    second.start()

    def norm(rows):
        total = x_ref[rows, :].astype(jnp.float32) + (
            part_ref[rows, :].astype(jnp.float32) + held[rows, :].astype(jnp.float32)
        )
        hidden_ref[rows, :] = total
        normed[rows, :] = (total * row_scale(total) * gain_ref[...]).astype(jnp.bfloat16)

    first.wait()
    norm(mine)
    rows_of.start()
    second.wait()
    norm(theirs)
    all_ref[lax.axis_index("dp")] = normed[...]
    rows_of.forward()
    rows_of.finish()


def share_rows(part, x, gain, ident):
    size = lax.axis_size("dp")
    rows, width = part.shape
    return pl.pallas_call(
        share_rows_kernel,
        name="share_rows",
        in_specs=whole_vmem(3),
        out_specs=whole_vmem(2),
        out_shape=[
            jax.ShapeDtypeStruct((rows, width), jnp.float32),
            jax.ShapeDtypeStruct((size, rows, width), jnp.bfloat16),
        ],
        scratch_shapes=[
            pltpu.VMEM((rows, width), jnp.bfloat16),
            pltpu.VMEM((rows, width), jnp.bfloat16),
            *sem_pair(size),
            *sem_pair(size + 1),
        ],
        compiler_params=remote_params(ident),
    )(part, x, gain)


class RowReturn:
    def __init__(self, part, held, landed, total, sent, came, dp_sems, tp_sems):
        self.part, self.held, self.landed, self.total = part, held, landed, total
        self.sent, self.came, self.dp_sems, self.tp_sems = sent, came, dp_sems, tp_sems
        self.size = lax.axis_size("dp")
        self.mine, self.theirs = halves(part.shape[1])

    def swap(self, k):
        group = ahead_on("dp", k)
        return remote(
            self.part.at[group, self.theirs], self.held.at[k], self.tp_sems, k, other_core()
        )

    def copy(self, k):
        return remote(
            self.held.at[k], self.landed.at[k], self.dp_sems, k, {"dp": ahead_on("dp", k)}
        )

    def last(self):
        return remote(self.sent, self.came, self.tp_sems, self.size, other_core())

    def both(self, k):
        group = ahead_on("dp", k)
        return self.part[group, self.mine].astype(jnp.float32) + self.held[k].astype(jnp.float32)

    def start(self):
        each(self.size + 1, lambda k: self.swap(lax.rem(k, self.size)).start())

    def forward(self):
        def one(k):
            self.swap(k).wait_recv()
            self.held[k] = self.both(k).astype(jnp.bfloat16)
            self.copy(k).start()

        each(self.size, one)
        self.swap(0).wait()
        self.total[...] = self.both(0)

    def gather(self):
        def one(k):
            self.copy(k).wait_recv()
            self.total[...] += self.landed[k].astype(jnp.float32)

        each(self.size, one)
        self.sent[...] = self.total[...].astype(jnp.bfloat16)
        self.last().start()

    def finish(self):
        def one(k):
            self.swap(k).wait_send()
            self.copy(k).wait_send()

        each(self.size, one)
        self.last().wait()


def return_scratch(size, rows, width):
    low = jnp.bfloat16
    return [
        pltpu.VMEM((size, rows // 2, width), low),
        pltpu.VMEM((size, rows // 2, width), low),
        pltpu.VMEM((rows // 2, width), jnp.float32),
        pltpu.VMEM((rows // 2, width), low),
        pltpu.VMEM((rows // 2, width), low),
        *sem_pair(size),
        *sem_pair(size + 1),
    ]


def return_grads_kernel(
    part_ref, hidden_ref, cot_ref, gain_ref, out_w_ref, grad_ref, low_ref, mix_ref, gain_grad_ref,
    held, landed, total, sent, came, dp_send, dp_recv, tp_send, tp_recv,
):
    greet(["dp", "tp"])
    rows = RowReturn(
        part_ref, held, landed, total, sent, came, (dp_send, dp_recv), (tp_send, tp_recv)
    )
    rows.start()
    rows.forward()
    rows.gather()

    def turn_back(at, grads):
        x_grad, gain_grad = norm_back(
            hidden_ref[at, :], gain_ref[...], grads.astype(jnp.float32)
        )
        hidden_grad = cot_ref[at, :].astype(jnp.float32) + x_grad
        grad_ref[at, :] = hidden_grad
        low_ref[at, :] = hidden_grad.astype(jnp.bfloat16)
        mix_ref[at, :] = lax.dot_general(
            low_ref[at, :], out_w_ref[...], NT, preferred_element_type=jnp.float32
        ).astype(jnp.bfloat16)
        return gain_grad

    gain_mine = turn_back(rows.mine, sent[...])
    rows.finish()
    gain_theirs = turn_back(rows.theirs, came[...])
    gain_grad_ref[...] = gain_mine + gain_theirs


def return_grads(part, hidden, cot, gain, out_w, ident):
    size, rows, width = part.shape
    return pl.pallas_call(
        return_grads_kernel,
        name="return_grads",
        in_specs=whole_vmem(5),
        out_specs=whole_vmem(4),
        out_shape=[
            jax.ShapeDtypeStruct((rows, width), jnp.float32),
            jax.ShapeDtypeStruct((rows, width), jnp.bfloat16),
            jax.ShapeDtypeStruct((rows, out_w.shape[0]), jnp.bfloat16),
            jax.ShapeDtypeStruct((1, width), jnp.float32),
        ],
        scratch_shapes=return_scratch(size, rows, width),
        compiler_params=remote_params(ident),
    )(part, hidden, cot, gain, out_w)


def trade_kernel(
    back, ahead, kv_grad_ref, part_ref, hidden_ref, low_ref, mix_ref, kv_ref, out_ref, out_w_ref,
    going, came_kv, line_send, line_recv, held, landed, total, sent, came, dp_send, dp_recv,
    tp_send, tp_recv,
):
    me, size = lax.axis_index("ctx"), lax.axis_size("ctx")
    greet(["dp", "tp"], line=True)
    right, left = me + 1, me - 1
    sems = (line_send, line_recv)

    def hop(s, src):
        return remote(src, came_kv.at[s], sems, s, {"ctx": left})

    def forth():
        return remote(
            kv_grad_ref.at[lax.rem(me + 1, size)], came_kv.at[0], sems, 0, {"ctx": right}
        )

    def own_piece(s):
        return kv_grad_ref.at[lax.rem(me + size - s, size)]

    if ahead:

        @pl.when(right < size)
        def _():
            forth().start()

    @pl.when(me - back >= 0)
    def _():
        hop(back, own_piece(back)).start()

    rows = RowReturn(
        part_ref, held, landed, total, sent, came, (dp_send, dp_recv), (tp_send, tp_recv)
    )
    rows.start()
    rows.forward()
    turned = jnp.transpose(low_ref[...].astype(jnp.float32)).astype(jnp.bfloat16)
    grad = jnp.dot(turned, mix_ref[...], preferred_element_type=jnp.float32)
    piece = out_w_ref.shape[1]
    for i in range(out_w_ref.shape[0]):
        out_w_ref[i] = grad[i * piece : (i + 1) * piece].astype(jnp.bfloat16)

    for s in range(back - 1, 0, -1):

        @pl.when((me - s >= 0) & (right < size))
        def _(s=s):
            hop(s + 1, going.at[s]).wait_recv()
            going[s] = (
                own_piece(s)[...].astype(jnp.float32) + came_kv[s + 1].astype(jnp.float32)
            ).astype(going.dtype)
            hop(s, going.at[s]).start()

        @pl.when((me - s >= 0) & (right >= size))
        def _(s=s):
            hop(s, own_piece(s)).start()

    rows.gather()
    kv_ref[...] = kv_grad_ref[me].astype(jnp.float32)

    @pl.when(right < size)
    def _():
        hop(1, going.at[0]).wait_recv()
        kv_ref[...] += came_kv[1].astype(jnp.float32)

    if ahead:

        @pl.when(left >= 0)
        def _():
            forth().wait_recv()
            kv_ref[...] += came_kv[0].astype(jnp.float32)

        @pl.when(right < size)
        def _():
            forth().wait_send()

    for s in range(back, 0, -1):

        @pl.when(me - s >= 0)
        def _(s=s):
            hop(s, going.at[0]).wait_send()

    rows.finish()
    mine, theirs = rows.mine, rows.theirs
    out_ref[mine, :] = (hidden_ref[mine, :] + sent[...].astype(jnp.float32)).astype(jnp.bfloat16)
    out_ref[theirs, :] = (hidden_ref[theirs, :] + came[...].astype(jnp.float32)).astype(
        jnp.bfloat16
    )


def trade(kv_grad, part, hidden, low, mix, back, ahead, ident):
    size, rows, width = part.shape
    kv_shape = kv_grad.shape[1:]
    held = pltpu.VMEM((back + 1,) + kv_shape, kv_grad.dtype)
    return pl.pallas_call(
        functools.partial(trade_kernel, back, ahead),
        name="trade",
        in_specs=whole_vmem(5),
        out_specs=whole_vmem(3),
        out_shape=[
            jax.ShapeDtypeStruct(kv_shape, jnp.float32),
            jax.ShapeDtypeStruct((rows, width), jnp.bfloat16),
            jax.ShapeDtypeStruct((size, width // size, mix.shape[1]), jnp.bfloat16),
        ],
        scratch_shapes=[
            held, held, *sem_pair(back + 1), *return_scratch(size, rows, width)
        ],
        compiler_params=remote_params(ident),
    )(kv_grad, part, hidden, low, mix)


class PieceSum:
    def __init__(self, axis, source, landed, sems):
        self.axis, self.source, self.landed, self.sems = axis, source, landed, sems
        self.size = lax.axis_size(axis)

    def copy(self, k):
        peer = ahead_on(self.axis, k)
        return remote(
            self.source.at[peer], self.landed.at[k], self.sems, k, {self.axis: peer}
        )

    def send(self, k):
        self.copy(k).start()

    def total(self):
        each(self.size, lambda k: self.copy(k).wait_recv())
        whole = self.source[lax.axis_index(self.axis)].astype(jnp.float32)
        for k in range(1, self.size):
            whole += self.landed[k].astype(jnp.float32)
        return whole

    def finish(self):
        each(self.size, lambda k: self.copy(k).wait_send())


class WholeSum:
    def __init__(self, axis, source, landed, sems):
        self.axis, self.source, self.landed, self.sems = axis, source, landed, sems
        self.size = lax.axis_size(axis)

    def copy(self, k):
        return remote(
            self.source, self.landed.at[k], self.sems, k, {self.axis: ahead_on(self.axis, k)}
        )

    def start(self):
        each(self.size, lambda k: self.copy(k).start())

    def total(self):
        each(self.size, lambda k: self.copy(k).wait())
        whole = self.source[...]
        for k in range(1, self.size):
            whole += self.landed[k]
        return whole


def finish_kernel(
    dq_ref, dkv_ref, cos_ref, sin_ref, normed_ref, w_ref, x_ref, gain_ref, hidden_ref, out_w_ref,
    gain_two_ref, in_ref, own_ref, gains_ref, joined, turned, part, held, pieces, landed,
    out_landed, low, low_landed, gain_rows, gain_landed, gain_more, gain_more_landed, *sems,
):
    greet(["dp", "ctx", "tp"])
    pairs = [sems[2 * i : 2 * i + 2] for i in range(len(sems) // 2)]
    out_sum = PieceSum("dp", out_w_ref, out_landed, pairs[0])
    each(out_sum.size, out_sum.send)
    wide = 2 * HEAD_DIM
    q_width, kv_width = dq_ref.shape[1], dkv_ref.shape[1] // 2
    for first in range(0, q_width, wide):
        joined[:, first : first + wide] = turn(
            dq_ref[:, first : first + wide], cos_ref[...], sin_ref[...]
        ).astype(jnp.bfloat16)
    for first in range(0, kv_width, wide):
        joined[:, q_width + first : q_width + first + wide] = turn(
            dkv_ref[:, first : first + wide], cos_ref[...], sin_ref[...]
        ).astype(jnp.bfloat16)
    joined[:, q_width + kv_width :] = dkv_ref[:, kv_width:].astype(jnp.bfloat16)

    turned[...] = jnp.transpose(normed_ref[...].astype(jnp.float32)).astype(jnp.bfloat16)
    w_sum = PieceSum("dp", pieces, landed, pairs[1])
    rows = pieces.shape[1]

    def piece(k):
        peer = ahead_on("dp", k)
        at = pl.ds(pl.multiple_of(peer * rows, rows), rows)
        pieces[peer] = jnp.dot(
            turned[at, :], joined[...], preferred_element_type=jnp.float32
        ).astype(jnp.bfloat16)
        w_sum.send(k)

    each(w_sum.size, piece)
    part[...] = lax.dot_general(
        joined[...], w_ref[...], NT, preferred_element_type=jnp.float32
    ).astype(jnp.bfloat16)
    swap = remote(part, held, pairs[2], 0, other_core())
    swap.start()
    me = lax.axis_index("dp")
    own = pl.ds(pl.multiple_of(me * rows, rows), rows)
    pieces[me] = jnp.dot(
        turned[own, :], joined[...], preferred_element_type=jnp.float32
    ).astype(jnp.bfloat16)
    swap.wait()
    x_grad, gain_grad = norm_back(
        x_ref[...].astype(jnp.float32),
        gain_ref[...],
        part[...].astype(jnp.float32) + held[...].astype(jnp.float32),
    )
    in_ref[...] = (hidden_ref[...] + x_grad).astype(jnp.bfloat16)
    gain_rows[...] = jnp.zeros(gain_rows.shape, jnp.float32)
    gain_rows[0:1, :] = gain_grad
    gain_rows[1:2, :] = gain_two_ref[...]
    gain_sum = WholeSum("dp", gain_rows, gain_landed, pairs[3])
    gain_sum.start()

    out_total = out_sum.total()
    w_total = w_sum.total()
    cols = w_total.shape[1]
    few = low.shape[1]
    for c in range(low.shape[0]):
        low[c, :, :cols] = w_total[c * few : (c + 1) * few].astype(jnp.bfloat16)
        low[c, :, cols:] = out_total[c * few : (c + 1) * few].astype(jnp.bfloat16)
    low_sum = PieceSum("ctx", low, low_landed, pairs[4])
    each(low_sum.size, low_sum.send)
    gain_more[...] = gain_sum.total()
    more_sum = WholeSum("ctx", gain_more, gain_more_landed, pairs[5])
    more_sum.start()
    out_sum.finish()
    w_sum.finish()
    own_ref[...] = low_sum.total()
    low_sum.finish()
    gains_ref[...] = more_sum.total()


def finish(dq, dkv, cosine, sine, normed, w, x, gain, hidden_grad, out_w, gain_two, ident):
    rows, width = x.shape
    dp_size, ctx_size = lax.axis_size("dp"), lax.axis_size("ctx")
    cols, out_cols = w.shape[1], out_w.shape[2]
    few = width // dp_size // ctx_size
    low, high = jnp.bfloat16, jnp.float32
    return pl.pallas_call(
        finish_kernel,
        name="finish",
        in_specs=whole_vmem(11),
        out_specs=whole_vmem(3),
        out_shape=[
            jax.ShapeDtypeStruct((rows, width), low),
            jax.ShapeDtypeStruct((few, cols + out_cols), high),
            jax.ShapeDtypeStruct((8, width), high),
        ],
        scratch_shapes=[
            pltpu.VMEM((rows, cols), low),
            pltpu.VMEM((width, rows), low),
            pltpu.VMEM((rows, width), low),
            pltpu.VMEM((rows, width), low),
            pltpu.VMEM((dp_size, width // dp_size, cols), low),
            pltpu.VMEM((dp_size, width // dp_size, cols), low),
            pltpu.VMEM(out_w.shape, low),
            pltpu.VMEM((ctx_size, few, cols + out_cols), low),
            pltpu.VMEM((ctx_size, few, cols + out_cols), low),
            pltpu.VMEM((8, width), high),
            pltpu.VMEM((dp_size, 8, width), high),
            pltpu.VMEM((8, width), high),
            pltpu.VMEM((ctx_size, 8, width), high),
            *sem_pair(dp_size),
            *sem_pair(dp_size),
            *sem_pair(1),
            *sem_pair(dp_size),
            *sem_pair(ctx_size),
            *sem_pair(ctx_size),
        ],
        compiler_params=remote_params(ident),
    )(dq, dkv, cosine, sine, normed, w, x, gain, hidden_grad, out_w, gain_two)


GROUPS_AT_ONCE = 4


def experts_kernel(
    more, rows_ref, grads_ref, weights_ref, place_ref, gate_ref, place_col_ref, *refs
):
    before, refs = (refs[:2], refs[2:]) if more else (None, refs)
    out_ref, back_ref, weight_grad_ref, slots, slot_grads, outs, backs = refs
    e = pl.program_id(1)
    groups, tok_rows, model_width = rows_ref.shape
    owners, part = weight_grad_ref.shape[1], weight_grad_ref.shape[5]
    slot_index = lax.broadcasted_iota(jnp.int32, (CAP, tok_rows), 0)
    gates = []
    for g in range(groups):
        picks = slot_index == place_ref[g, 0]
        gates.append(jnp.sum(jnp.where(picks, gate_ref[g, 0], 0.0), axis=1, keepdims=True))
        picks = picks.astype(jnp.float32).astype(jnp.bfloat16)
        at = slice(g * CAP, (g + 1) * CAP)
        slots[at, :] = jnp.dot(
            picks, rows_ref[g], preferred_element_type=jnp.float32
        ).astype(jnp.bfloat16)
        slot_grads[at, :] = (
            jnp.dot(picks, grads_ref[g], preferred_element_type=jnp.float32) * gates[g]
        ).astype(jnp.bfloat16)
    gate_w, up_w, down_w = (weights_ref.at[0, i] for i in range(3))
    gate_pre = jnp.dot(slots[...], gate_w[...], preferred_element_type=jnp.float32)
    up_pre = jnp.dot(slots[...], up_w[...], preferred_element_type=jnp.float32)
    act_grad = jnp.dot(slot_grads[...], down_w[...], preferred_element_type=jnp.float32)
    sig = 1.0 / (1.0 + jnp.exp(-gate_pre))
    silu = gate_pre * sig
    act_low = (silu * up_pre).astype(jnp.bfloat16)
    up_low = (act_grad * silu).astype(jnp.bfloat16)
    gate_low = (act_grad * up_pre * (sig * (1.0 + gate_pre * (1.0 - sig)))).astype(jnp.bfloat16)

    back = lax.dot_general(
        gate_low, gate_w[...], NT, preferred_element_type=jnp.float32
    ) + lax.dot_general(up_low, up_w[...], NT, preferred_element_type=jnp.float32)
    out = lax.dot_general(act_low, down_w[...], NT, preferred_element_type=jnp.float32)
    for g in range(groups):
        at = slice(g * CAP, (g + 1) * CAP)
        to = pl.ds(pl.multiple_of(e * CAP, CAP), CAP)
        backs[g, to, :] = back[at].astype(jnp.bfloat16)
        outs[g, to, :] = (out[at] * gates[g]).astype(jnp.bfloat16)

    for i, (low, source) in enumerate(
        ((gate_low, slots), (up_low, slots), (act_low, slot_grads))
    ):
        turned = jnp.transpose(low.astype(jnp.float32)).astype(jnp.bfloat16)
        total = jnp.dot(turned, source[...], preferred_element_type=jnp.float32)
        for c in range(owners):
            weight_grad_ref[0, c, 0, i] = total[:, c * part : (c + 1) * part].astype(
                weight_grad_ref.dtype
            )

    @pl.when(e == pl.num_programs(1) - 1)
    def _():
        slot_count = outs.shape[1]
        for g in range(groups):
            tiles = []
            for first in range(0, slot_count, 128):
                wide = min(128, slot_count - first)
                lane = first + lax.broadcasted_iota(jnp.int32, (tok_rows, wide), 1)
                hit = None
                for n in range(first // CAP, (first + wide - 1) // CAP + 1):
                    one = place_col_ref[g, :, n : n + 1] == lane - n * CAP
                    hit = one if hit is None else hit | one
                tiles.append(hit.astype(jnp.float32).astype(jnp.bfloat16))
            spread_picks = jnp.concatenate(tiles, axis=1)
            for i, (to_ref, source) in enumerate(((back_ref, backs), (out_ref, outs))):
                total = jnp.dot(spread_picks, source[g], preferred_element_type=jnp.float32)
                if more:
                    total += before[1 - i][g].astype(jnp.float32)
                to_ref[g] = total.astype(jnp.bfloat16)


def expert_places(chosen_all, gates_all, own):
    tok_rows = chosen_all.shape[1]
    named = chosen_all[..., None] == lax.axis_index("dp") * own + jnp.arange(own, dtype=jnp.int32)
    names = jnp.any(named, axis=2)
    gate_of = jnp.sum(jnp.where(named, gates_all[..., None], 0.0), axis=2)
    earlier = jnp.tril(jnp.ones((tok_rows, tok_rows), jnp.bfloat16), -1)
    place = jnp.einsum(
        "rq,gqe->gre", earlier, names.astype(jnp.bfloat16), preferred_element_type=jnp.float32
    ).astype(jnp.int32)
    place = jnp.where(names & (place < CAP), place, -CAP * own)
    return (
        place,
        place.transpose(0, 2, 1)[:, :, None],
        gate_of.transpose(0, 2, 1)[:, :, None],
    )


def experts(weights, places, rows_all, grad_all, first, count, before):
    _, _, model_width, hidden = weights.shape
    place_cols, place_rows, gate_rows = places
    groups, tok_rows, _ = rows_all.shape
    owners = lax.axis_size("ctx")
    at_once = min(GROUPS_AT_ONCE, groups)
    chunks = groups // at_once
    part = model_width // owners
    rows_spec = pl.BlockSpec(
        (at_once, tok_rows, model_width), lambda c, e: (c, 0, 0), pipeline_mode=pl.Buffered(1)
    )
    line_spec = pl.BlockSpec((at_once, 1, 1, tok_rows), lambda c, e: (c, e + first, 0, 0))
    out_shape = jax.ShapeDtypeStruct(rows_all.shape, jnp.bfloat16)
    flops = count * groups * CAP * model_width * 2 * (9 * hidden + 4 * tok_rows)
    more = before is not None
    out_part, back_part, weight_part = pl.pallas_call(
        functools.partial(experts_kernel, more),
        name="experts",
        grid=(chunks, count),
        in_specs=[
            rows_spec,
            rows_spec,
            pl.BlockSpec((1, 3, model_width, hidden), lambda c, e: (e + first, 0, 0, 0)),
            line_spec,
            line_spec,
            pl.BlockSpec((at_once, tok_rows, count), lambda c, e: (c, 0, 0)),
        ]
        + [rows_spec] * (2 * more),
        out_specs=[
            rows_spec,
            rows_spec,
            pl.BlockSpec((1, owners, 1, 3, hidden, part), lambda c, e: (c, 0, e, 0, 0, 0)),
        ],
        out_shape=[
            out_shape,
            out_shape,
            jax.ShapeDtypeStruct((chunks, owners, count, 3, hidden, part), jnp.bfloat16),
        ],
        scratch_shapes=[
            pltpu.VMEM((at_once * CAP, model_width), jnp.bfloat16),
            pltpu.VMEM((at_once * CAP, model_width), jnp.bfloat16),
            pltpu.VMEM((at_once, count * CAP, model_width), jnp.bfloat16),
            pltpu.VMEM((at_once, count * CAP, model_width), jnp.bfloat16),
        ],
        compiler_params=pltpu.CompilerParams(vmem_limit_bytes=LIMIT),
        cost_estimate=pl.CostEstimate(
            flops=flops, bytes_accessed=4 * weights.size, transcendentals=0
        ),
    )(
        rows_all,
        grad_all,
        weights,
        place_rows,
        gate_rows,
        place_cols[:, :, first : first + count],
        *(before if more else ()),
    )
    if chunks == 1:
        return (out_part, back_part), weight_part[0]
    return (out_part, back_part), jnp.sum(weight_part.astype(jnp.float32), axis=0).astype(
        jnp.bfloat16
    )


def picture_of(starts, token_positions):
    inside = (token_positions[:, None] >= starts[None, :]) & (
        token_positions[:, None] < starts[None, :] + PIC
    )
    labels = jnp.arange(starts.shape[0], dtype=jnp.int32) + 1
    return jnp.sum(jnp.where(inside, labels[None, :], 0), axis=-1) - 1


def rotary_tables(token_positions):
    half_dim = HEAD_DIM // 2
    inverse = THETA ** (-(jnp.arange(half_dim, dtype=jnp.float32) * 2.0 / HEAD_DIM))
    angles = token_positions.astype(jnp.float32)[:, None] * inverse[None, :]
    cosine, sine = jnp.cos(angles), jnp.sin(angles)
    return jnp.concatenate([cosine] * 4, axis=1), jnp.concatenate([sine, -sine] * 2, axis=1)


def body(
    tokens,
    query_weight,
    key_weight,
    value_weight,
    output_weight,
    gain_attn,
    gain_moe,
    expert_weights,
    routes,
    gate_values,
    documents,
    pic_starts,
    cotangent,
):
    _, block_len, model_width = tokens.shape
    dp_size, ctx_size = lax.axis_size("dp"), lax.axis_size("ctx")
    length = block_len * ctx_size
    offset = lax.axis_index("ctx") * block_len
    back = back_blocks(ctx_size, block_len, length)
    ahead = ahead_blocks(block_len, length, pic_starts.shape[1])
    q_width, kv_width = query_weight.shape[1], key_weight.shape[1]
    own = expert_weights.shape[0]
    x, cot = tokens[0], cotangent[0]

    joined_w = jnp.concatenate([query_weight, key_weight, value_weight], axis=1)
    gains = jnp.stack([gain_attn, gain_moe]).astype(jnp.float32)
    joined_all, gains_all, docs_all, chosen_all, gates_all = spread(
        [
            joined_w,
            gains,
            documents,
            routes.reshape(block_len * TOP // 128, 128),
            gate_values.reshape(block_len * TOP // 128, 128),
        ],
        ["dp", "dp", "ctx", "dp", "dp"],
        1,
        "spread_weights",
    )
    output_weight, joined_all = lax.optimization_barrier((output_weight, joined_all))
    output_full = lax.all_gather(output_weight, "dp", axis=1, tiled=True)
    joined_full = joined_all.reshape(model_width, -1)
    gain_rows = gains_all.transpose(1, 0, 2).reshape(2, 1, model_width)
    docs_all = docs_all.reshape(length)
    cosine, sine = rotary_tables(offset + jnp.arange(block_len, dtype=jnp.int32))
    normed_one, query, kv_all, grad_all = project(
        x, joined_full, gain_rows[0], cosine, sine, cot, q_width, back, ahead, 2
    )
    kv_all = kv_all.reshape(length, 2 * kv_width)

    pictures = picture_of(pic_starts[0], jnp.arange(length, dtype=jnp.int32))
    flags = block_flags(pic_starts[0], documents[0], docs_all, offset)
    kinfo = jnp.stack([docs_all, pictures], axis=1)
    qinfo = jnp.stack([documents[0], lax.dynamic_slice_in_dim(pictures, offset, block_len)])
    places = expert_places(
        chosen_all.reshape(dp_size, block_len, TOP), gates_all.reshape(dp_size, block_len, TOP), own
    )
    mixture, mix_full, log_total, attn_part = attend(
        flags, query, kv_all, kinfo, qinfo, output_full
    )
    hidden, rows_all = share_rows(attn_part, x, gain_rows[1], 3)
    half = own // 2
    parts, grads_one = experts(expert_weights, places, rows_all, grad_all, 0, half, None)
    expert_one = lax.psum_scatter(grads_one, "ctx", scatter_dimension=0)
    (out_part, back_part), grads_two = experts(
        expert_weights, places, rows_all, grad_all, half, own - half, parts
    )
    hidden_grad, hidden_low, mix_grad, gain_two_grad = return_grads(
        back_part, hidden, cot, gain_rows[1], output_full, 4
    )
    q_rot_grad, kv_part = attend_back(
        flags, query, kv_all, kinfo, qinfo, log_total, mix_full, mix_grad
    )
    kv_back, layer_out, output_grad = trade(
        kv_part.reshape(ctx_size, block_len, 2 * kv_width),
        out_part,
        hidden,
        hidden_low,
        mixture,
        back,
        ahead,
        5,
    )
    grads_two, kv_back = lax.optimization_barrier((grads_two, kv_back))
    expert_two = lax.psum_scatter(grads_two, "ctx", scatter_dimension=0)
    input_grad, owned, gain_sums = finish(
        q_rot_grad,
        kv_back,
        cosine,
        sine,
        normed_one,
        joined_full,
        x,
        gain_rows[0],
        hidden_grad,
        output_grad,
        gain_two_grad,
        6,
    )
    few = owned.shape[0]
    here = (lax.axis_index("dp") * ctx_size + lax.axis_index("ctx")) * few
    gain_sums = lax.dynamic_slice_in_dim(gain_sums, here, few, 1)
    expert_grad = jnp.concatenate([expert_one, expert_two], axis=0)
    v_end = q_width + 2 * kv_width
    return (
        layer_out[None],
        input_grad[None],
        owned[:, :q_width],
        owned[:, q_width : q_width + kv_width],
        owned[:, q_width + kv_width : v_end],
        owned[:, v_end:].T,
        gain_sums[0],
        gain_sums[1],
        expert_grad.astype(jnp.float32).transpose(0, 1, 3, 2),
    )


def solution(mesh):
    return jax.shard_map(
        body,
        mesh=mesh,
        in_specs=(
            P("dp", "ctx", None),
            P("dp", "tp"),
            P("dp", "tp"),
            P("dp", "tp"),
            P("tp", "dp"),
            P("dp"),
            P("dp"),
            P("dp", None, None, "tp"),
            P("dp", "ctx", None),
            P("dp", "ctx", None),
            P("dp", "ctx"),
            P("dp", None),
            P("dp", "ctx", None),
        ),
        out_specs=(
            P("dp", "ctx", None),
            P("dp", "ctx", None),
            P(("dp", "ctx"), "tp"),
            P(("dp", "ctx"), "tp"),
            P(("dp", "ctx"), "tp"),
            P("tp", ("dp", "ctx")),
            P(("dp", "ctx")),
            P(("dp", "ctx")),
            P("dp", None, "ctx", "tp"),
        ),
        check_vma=False,
    )
```

```python
import functools

import jax
import jax.numpy as jnp
from jax import lax
from jax.experimental import pallas as pl
from jax.experimental.pallas import tpu as pltpu
from jax.sharding import PartitionSpec as P

HEAD_DIM = 64
TOP = 8
PIC = 256
CAP = 144

EPSILON = 1e-06
THETA = 10000.0
NEG_FILL = -1e30


KEY_ROWS = 256
NT = (((1,), (1,)), ((), ()))
LIMIT = 60 * 1024 * 1024


def seen_bias(flags, j, blocks, kinfo_ref, qinfo_ref):
    rows = pl.ds(pl.multiple_of(j * KEY_ROWS, KEY_ROWS), KEY_ROWS)
    q_doc, q_pic = qinfo_ref[0:1, :], qinfo_ref[1:2, :]
    k_doc, k_pic = kinfo_ref[rows, 0:1], kinfo_ref[rows, 1:2]
    q_place = flags[blocks] + lax.broadcasted_iota(jnp.int32, q_doc.shape, 1)
    k_place = j * KEY_ROWS + lax.broadcasted_iota(jnp.int32, k_doc.shape, 0)
    seen = (k_doc == q_doc) & ((k_place <= q_place) | ((k_pic == q_pic) & (q_pic >= 0)))
    return rows, jnp.where(seen, 0.0, NEG_FILL)


def attend_kernel(
    flags, q_ref, kv_ref, kinfo_ref, qinfo_ref, out_w_ref, mix_ref, full_ref, log_ref, part_ref,
    acc, top, total,
):
    blocks = kv_ref.shape[0] // KEY_ROWS
    kv_width = kv_ref.shape[1] // 2
    heads, kv_heads = q_ref.shape[1] // HEAD_DIM, kv_width // HEAD_DIM
    top[...] = jnp.full(top.shape, NEG_FILL, jnp.float32)
    total[...] = jnp.zeros(total.shape, jnp.float32)
    acc[...] = jnp.zeros(acc.shape, jnp.float32)

    def step(j, carry):
        @pl.when(flags[j] > 0)
        def _():
            rows, bias = seen_bias(flags, j, blocks, kinfo_ref, qinfo_ref)
            for g in range(kv_heads):
                key = kv_ref[rows, g * HEAD_DIM : (g + 1) * HEAD_DIM]
                val = kv_ref[rows, kv_width + g * HEAD_DIM : kv_width + (g + 1) * HEAD_DIM]
                val_t = jnp.transpose(val.astype(jnp.float32)).astype(jnp.bfloat16)
                for h in range(g * heads // kv_heads, (g + 1) * heads // kv_heads):
                    at = slice(h * HEAD_DIM, (h + 1) * HEAD_DIM)
                    scores = bias + lax.dot_general(
                        key, q_ref[:, at], NT, preferred_element_type=jnp.float32
                    )
                    old = top[h : h + 1, :]
                    new = jnp.maximum(old, jnp.max(scores, axis=0, keepdims=True))
                    probs = jnp.exp(scores - new)
                    fade = jnp.exp(old - new)
                    total[h : h + 1, :] = total[h : h + 1, :] * fade + jnp.sum(
                        probs, axis=0, keepdims=True
                    )
                    acc[at, :] = acc[at, :] * fade + jnp.dot(
                        val_t, probs.astype(jnp.bfloat16), preferred_element_type=jnp.float32
                    )
                    top[h : h + 1, :] = new

        return carry

    lax.fori_loop(0, blocks, step, 0)
    log_ref[...] = top[...] + jnp.log(total[...])
    for h in range(heads):
        at = slice(h * HEAD_DIM, (h + 1) * HEAD_DIM)
        acc[at, :] = acc[at, :] / total[h : h + 1, :]
    full = jnp.transpose(acc[...])
    full_ref[...] = full
    mix_ref[...] = full.astype(jnp.bfloat16)
    part_ref[...] = jnp.dot(
        mix_ref[...], out_w_ref[...], preferred_element_type=jnp.float32
    ).astype(jnp.bfloat16)


def attend_back_kernel(
    flags, q_ref, kv_ref, kinfo_ref, qinfo_ref, log_ref, full_ref, grad_ref, dq_ref, dkv_ref,
    acc, delta,
):
    blocks = kv_ref.shape[0] // KEY_ROWS
    kv_width = kv_ref.shape[1] // 2
    heads, kv_heads = q_ref.shape[1] // HEAD_DIM, kv_width // HEAD_DIM
    acc[...] = jnp.transpose(full_ref[...] * grad_ref[...].astype(jnp.float32))
    for h in range(heads):
        delta[h : h + 1, :] = jnp.sum(
            acc[h * HEAD_DIM : (h + 1) * HEAD_DIM, :], axis=0, keepdims=True
        )
    acc[...] = jnp.zeros(acc.shape, jnp.float32)

    def step(j, carry):
        @pl.when(flags[j] > 0)
        def _():
            rows, bias = seen_bias(flags, j, blocks, kinfo_ref, qinfo_ref)
            for g in range(kv_heads):
                k_at = slice(g * HEAD_DIM, (g + 1) * HEAD_DIM)
                v_at = slice(kv_width + g * HEAD_DIM, kv_width + (g + 1) * HEAD_DIM)
                key, val = kv_ref[rows, k_at], kv_ref[rows, v_at]
                key_t = jnp.transpose(key.astype(jnp.float32)).astype(jnp.bfloat16)
                dk = jnp.zeros((KEY_ROWS, HEAD_DIM), jnp.float32)
                dv = jnp.zeros((KEY_ROWS, HEAD_DIM), jnp.float32)
                for h in range(g * heads // kv_heads, (g + 1) * heads // kv_heads):
                    at = slice(h * HEAD_DIM, (h + 1) * HEAD_DIM)
                    q_rows, g_rows = q_ref[:, at], grad_ref[:, at]
                    scores = bias + lax.dot_general(
                        key, q_rows, NT, preferred_element_type=jnp.float32
                    )
                    probs = jnp.exp(scores - log_ref[h : h + 1, :])
                    prob_grad = lax.dot_general(
                        val, g_rows, NT, preferred_element_type=jnp.float32
                    )
                    slope = (probs * (prob_grad - delta[h : h + 1, :])).astype(jnp.bfloat16)
                    dv += jnp.dot(
                        probs.astype(jnp.bfloat16), g_rows, preferred_element_type=jnp.float32
                    )
                    dk += jnp.dot(slope, q_rows, preferred_element_type=jnp.float32)
                    acc[at, :] += jnp.dot(key_t, slope, preferred_element_type=jnp.float32)
                dkv_ref[rows, k_at] = dk.astype(dkv_ref.dtype)
                dkv_ref[rows, v_at] = dv.astype(dkv_ref.dtype)

        @pl.when(flags[j] == 0)
        def _():
            rows = pl.ds(pl.multiple_of(j * KEY_ROWS, KEY_ROWS), KEY_ROWS)
            dkv_ref[rows, :] = jnp.zeros((KEY_ROWS, dkv_ref.shape[1]), dkv_ref.dtype)

        return carry

    lax.fori_loop(0, blocks, step, 0)
    dq_ref[...] = jnp.transpose(acc[...]) * (HEAD_DIM**-0.5)


def whole_vmem(count):
    return [pl.BlockSpec(memory_space=pltpu.VMEM)] * count


def attend(flags, q, kv, kinfo, qinfo, out_w):
    rows, width = q.shape
    heads = width // HEAD_DIM
    return pl.pallas_call(
        attend_kernel,
        name="attend",
        in_specs=[pl.BlockSpec(memory_space=pltpu.SMEM)] + whole_vmem(5),
        out_specs=whole_vmem(4),
        out_shape=[
            jax.ShapeDtypeStruct((rows, width), jnp.bfloat16),
            jax.ShapeDtypeStruct((rows, width), jnp.float32),
            jax.ShapeDtypeStruct((heads, rows), jnp.float32),
            jax.ShapeDtypeStruct((rows, out_w.shape[1]), jnp.bfloat16),
        ],
        scratch_shapes=[
            pltpu.VMEM((width, rows), jnp.float32),
            pltpu.VMEM((heads, rows), jnp.float32),
            pltpu.VMEM((heads, rows), jnp.float32),
        ],
        compiler_params=pltpu.CompilerParams(vmem_limit_bytes=LIMIT),
    )(flags, q, kv, kinfo, qinfo, out_w)


def attend_back(flags, q, kv, kinfo, qinfo, log_total, full, grad):
    rows, width = q.shape
    return pl.pallas_call(
        attend_back_kernel,
        name="attend_back",
        in_specs=[pl.BlockSpec(memory_space=pltpu.SMEM)] + whole_vmem(7),
        out_specs=whole_vmem(2),
        out_shape=[
            jax.ShapeDtypeStruct((rows, width), jnp.float32),
            jax.ShapeDtypeStruct(kv.shape, jnp.bfloat16),
        ],
        scratch_shapes=[
            pltpu.VMEM((width, rows), jnp.float32),
            pltpu.VMEM((width // HEAD_DIM, rows), jnp.float32),
        ],
        compiler_params=pltpu.CompilerParams(vmem_limit_bytes=LIMIT),
    )(flags, q, kv, kinfo, qinfo, log_total, full, grad)


def block_flags(pic_starts, q_docs, k_docs, offset):
    block_len, length = q_docs.shape[0], k_docs.shape[0]
    docs = k_docs.reshape(length // KEY_ROWS, KEY_ROWS)
    first = jnp.arange(length // KEY_ROWS, dtype=jnp.int32) * KEY_ROWS
    same = (docs[:, 0] <= q_docs[-1]) & (docs[:, -1] >= q_docs[0])
    spans = (
        (pic_starts[None, :] < offset + block_len)
        & (pic_starts[None, :] + PIC > offset)
        & (pic_starts[None, :] < first[:, None] + KEY_ROWS)
        & (pic_starts[None, :] + PIC > first[:, None])
    )
    needed = same & ((first < offset + block_len) | jnp.any(spans, axis=1))
    return jnp.concatenate([needed.astype(jnp.int32), offset[None].astype(jnp.int32)])


MESH = pl.DeviceIdType.MESH


def greet(axes_list, line=False):
    barrier = pltpu.get_barrier_semaphore()
    count = 0
    for axis in axes_list:
        me, size = lax.axis_index(axis), lax.axis_size(axis)

        def signal(k, carry, axis=axis, me=me, size=size):
            pl.semaphore_signal(
                barrier, inc=1, device_id={axis: lax.rem(me + k, size)}, device_id_type=MESH
            )
            return carry

        lax.fori_loop(1, size, signal, 0)
        count += size - 1
    if not line:
        pl.semaphore_wait(barrier, count)
        return
    me, size = lax.axis_index("ctx"), lax.axis_size("ctx")
    for step in (1, -1):
        other = me + step

        @pl.when((other >= 0) & (other < size))
        def _(other=other):
            pl.semaphore_signal(barrier, inc=1, device_id={"ctx": other}, device_id_type=MESH)

    inner = (me > 0) & (me < size - 1)

    @pl.when(inner)
    def _():
        pl.semaphore_wait(barrier, count + 2)

    @pl.when(jnp.logical_not(inner))
    def _():
        pl.semaphore_wait(barrier, count + 1)


def remote(src, dst, sems, k, device_id):
    return pltpu.make_async_remote_copy(
        src_ref=src,
        dst_ref=dst,
        send_sem=sems[0].at[k],
        recv_sem=sems[1].at[k],
        device_id=device_id,
        device_id_type=MESH,
    )


def other_core():
    return {"tp": 1 - lax.axis_index("tp")}


def ahead_on(axis, k):
    return lax.rem(lax.axis_index(axis) + k, lax.axis_size(axis))


def each(count, do, first=1):
    def step(k, carry):
        do(k)
        return carry

    lax.fori_loop(first, count, step, 0)


def sem_pair(count):
    return [pltpu.SemaphoreType.DMA((count,)), pltpu.SemaphoreType.DMA((count,))]


def remote_params(ident):
    return pltpu.CompilerParams(
        collective_id=ident, has_side_effects=True, vmem_limit_bytes=LIMIT
    )


def halves(rows):
    half = rows // 2
    core = lax.axis_index("tp")
    return (
        pl.ds(pl.multiple_of(core * half, half), half),
        pl.ds(pl.multiple_of((1 - core) * half, half), half),
    )


def spread_kernel(axes_of, *refs):
    count = len(axes_of)
    ins, outs, sems = refs[:count], refs[count : 2 * count], refs[2 * count :]
    greet(sorted(set(axes_of)))

    def copy(i, k):
        return remote(
            ins[i],
            outs[i].at[lax.axis_index(axes_of[i])],
            sems[2 * i : 2 * i + 2],
            k,
            {axes_of[i]: ahead_on(axes_of[i], k)},
        )

    for i in range(count):
        each(lax.axis_size(axes_of[i]), lambda k, i=i: copy(i, k).start())
    for i in range(count):
        outs[i][lax.axis_index(axes_of[i])] = ins[i][...]
    for i in range(count):
        each(lax.axis_size(axes_of[i]), lambda k, i=i: copy(i, k).wait())


def spread(arrays, axes_of, ident):
    sizes = [lax.axis_size(axis) for axis in axes_of]
    return pl.pallas_call(
        functools.partial(spread_kernel, tuple(axes_of)),
        in_specs=whole_vmem(len(arrays)),
        out_specs=whole_vmem(len(arrays)),
        out_shape=[
            jax.ShapeDtypeStruct((size,) + a.shape, a.dtype) for size, a in zip(sizes, arrays)
        ],
        scratch_shapes=sum([sem_pair(size) for size in sizes], []),
        compiler_params=remote_params(ident),
    )(*arrays)


def turn(tile, cosine, sine):
    lane = lax.broadcasted_iota(jnp.int32, tile.shape, 1)
    half = HEAD_DIM // 2
    swapped = jnp.where(
        lax.rem(lane, HEAD_DIM) < half,
        pltpu.roll(tile, 2 * HEAD_DIM - half, 1),
        pltpu.roll(tile, half, 1),
    )
    return tile * cosine + swapped * sine


def row_scale(x):
    return lax.rsqrt(jnp.mean(x * x, axis=-1, keepdims=True) + EPSILON)


def norm_back(x, gain, grad):
    scale = row_scale(x)
    unit = x * scale
    pull = grad * gain
    return (
        scale * (pull - unit * jnp.mean(pull * unit, axis=-1, keepdims=True)),
        jnp.sum(grad * unit, axis=0, keepdims=True),
    )


def back_blocks(ctx_size, block_len, length):
    return min(ctx_size - 1, -(-(length // 2 - 1) // block_len))


def ahead_blocks(block_len, length, spans):
    return 0 if block_len % (length // spans) == 0 else 1


class RowGather:
    def __init__(self, source, target, dp_sems, tp_sems, first):
        self.source, self.target = source, target
        self.dp_sems, self.tp_sems, self.first = dp_sems, tp_sems, first
        self.mine, _ = halves(source.shape[0])
        self.size = lax.axis_size("dp")

    def copy(self, k):
        at = self.target.at[lax.axis_index("dp"), self.mine]
        return remote(
            self.source.at[self.mine], at, self.dp_sems, k, {"dp": ahead_on("dp", k)}
        )

    def relay(self, k):
        at = self.target.at[ahead_on("dp", self.size - k), self.mine]
        return remote(at, at, self.tp_sems, self.first + k, other_core())

    def start(self):
        each(self.size, lambda k: self.copy(k).start())

    def forward(self):
        def one(k):
            self.copy(k).wait_recv()
            self.relay(k).start()

        each(self.size, one)

    def finish(self):
        def one(k):
            self.copy(k).wait_send()
            self.relay(k).wait()

        each(self.size, one)


def project_kernel(
    back, ahead, q_width, x_ref, w_ref, gain_ref, cos_ref, sin_ref, cot_ref, normed_ref, q_ref,
    all_ref, cot_all_ref, kv_ref, line_send, line_recv, dp_send, dp_recv, tp_send, tp_recv,
):
    me, size = lax.axis_index("ctx"), lax.axis_size("ctx")
    greet(["dp", "tp"], line=True)
    rows_of = RowGather(cot_ref, cot_all_ref, (dp_send, dp_recv), (tp_send, tp_recv), 0)
    rows_of.start()
    x = x_ref[...].astype(jnp.float32)
    normed_ref[...] = (x * row_scale(x) * gain_ref[...]).astype(jnp.bfloat16)
    kv_width = kv_ref.shape[1] // 2
    wide = 2 * HEAD_DIM
    for first in range(q_width, q_width + 2 * kv_width, wide):
        tile = jnp.dot(
            normed_ref[...], w_ref[:, first : first + wide], preferred_element_type=jnp.float32
        )
        if first < q_width + kv_width:
            tile = turn(tile, cos_ref[...], -sin_ref[...])
        kv_ref[:, first - q_width : first - q_width + wide] = tile.astype(jnp.bfloat16)

    sems = (line_send, line_recv)
    right, left = me + 1, me - 1

    def hop(s):
        block = lax.rem(me + size - s, size)
        return remote(
            kv_ref if s == 0 else all_ref.at[block], all_ref.at[block], sems, s, {"ctx": right}
        )

    def arrive(s):
        return remote(kv_ref, all_ref.at[me], sems, s, {"ctx": right})

    def back_hop():
        return remote(kv_ref, all_ref.at[me], sems, back, {"ctx": left})

    if ahead:

        @pl.when(left >= 0)
        def _():
            back_hop().start()

    for s in range(back):

        @pl.when((right < size) & (me - s >= 0))
        def _(s=s):
            hop(s).start()

        if s == 0:
            all_ref[me] = kv_ref[...]
            for first in range(0, q_width, wide):
                tile = jnp.dot(
                    normed_ref[...],
                    w_ref[:, first : first + wide],
                    preferred_element_type=jnp.float32,
                )
                tile = turn(tile, cos_ref[...], -sin_ref[...]).astype(jnp.bfloat16)
                q_ref[:, first : first + wide] = (
                    tile.astype(jnp.float32) * HEAD_DIM**-0.5
                ).astype(jnp.bfloat16)

        @pl.when(me - s - 1 >= 0)
        def _(s=s):
            arrive(s).wait_recv()

    rows_of.forward()
    for s in range(back):

        @pl.when((right < size) & (me - s >= 0))
        def _(s=s):
            hop(s).wait_send()

    if ahead:

        @pl.when(left >= 0)
        def _():
            back_hop().wait_send()

        @pl.when(right < size)
        def _():
            back_hop().wait_recv()

    cot_all_ref[lax.axis_index("dp")] = cot_ref[...]
    rows_of.finish()


def project(x, w, gain, cosine, sine, cot, q_width, back, ahead, ident):
    rows, width = x.shape
    kv_cols = w.shape[1] - q_width
    dp_size, ctx_size = lax.axis_size("dp"), lax.axis_size("ctx")
    low = jnp.bfloat16
    return pl.pallas_call(
        functools.partial(project_kernel, back, ahead, q_width),
        name="project",
        in_specs=whole_vmem(6),
        out_specs=whole_vmem(4),
        out_shape=[
            jax.ShapeDtypeStruct((rows, width), low),
            jax.ShapeDtypeStruct((rows, q_width), low),
            jax.ShapeDtypeStruct((ctx_size, rows, kv_cols), low),
            jax.ShapeDtypeStruct((dp_size, rows, width), low),
        ],
        scratch_shapes=[
            pltpu.VMEM((rows, kv_cols), low),
            *sem_pair(back + 1),
            *sem_pair(dp_size),
            *sem_pair(dp_size),
        ],
        compiler_params=remote_params(ident),
    )(x, w, gain, cosine, sine, cot)


def share_rows_kernel(
    part_ref, x_ref, gain_ref, hidden_ref, all_ref, held, normed, dp_send, dp_recv, tp_send,
    tp_recv,
):
    mine, theirs = halves(part_ref.shape[0])
    greet(["dp", "tp"])
    rows_of = RowGather(normed, all_ref, (dp_send, dp_recv), (tp_send, tp_recv), 1)
    first = remote(part_ref.at[theirs], held.at[theirs], (tp_send, tp_recv), 0, other_core())
    second = remote(part_ref.at[mine], held.at[mine], (tp_send, tp_recv), 1, other_core())
    first.start()
    second.start()

    def norm(rows):
        total = x_ref[rows, :].astype(jnp.float32) + (
            part_ref[rows, :].astype(jnp.float32) + held[rows, :].astype(jnp.float32)
        )
        hidden_ref[rows, :] = total
        normed[rows, :] = (total * row_scale(total) * gain_ref[...]).astype(jnp.bfloat16)

    first.wait()
    norm(mine)
    rows_of.start()
    second.wait()
    norm(theirs)
    all_ref[lax.axis_index("dp")] = normed[...]
    rows_of.forward()
    rows_of.finish()


def share_rows(part, x, gain, ident):
    size = lax.axis_size("dp")
    rows, width = part.shape
    return pl.pallas_call(
        share_rows_kernel,
        name="share_rows",
        in_specs=whole_vmem(3),
        out_specs=whole_vmem(2),
        out_shape=[
            jax.ShapeDtypeStruct((rows, width), jnp.float32),
            jax.ShapeDtypeStruct((size, rows, width), jnp.bfloat16),
        ],
        scratch_shapes=[
            pltpu.VMEM((rows, width), jnp.bfloat16),
            pltpu.VMEM((rows, width), jnp.bfloat16),
            *sem_pair(size),
            *sem_pair(size + 1),
        ],
        compiler_params=remote_params(ident),
    )(part, x, gain)


class RowReturn:
    def __init__(self, part, held, landed, total, sent, came, dp_sems, tp_sems):
        self.part, self.held, self.landed, self.total = part, held, landed, total
        self.sent, self.came, self.dp_sems, self.tp_sems = sent, came, dp_sems, tp_sems
        self.size = lax.axis_size("dp")
        self.mine, self.theirs = halves(part.shape[1])

    def swap(self, k):
        group = ahead_on("dp", k)
        return remote(
            self.part.at[group, self.theirs], self.held.at[k], self.tp_sems, k, other_core()
        )

    def copy(self, k):
        return remote(
            self.held.at[k], self.landed.at[k], self.dp_sems, k, {"dp": ahead_on("dp", k)}
        )

    def last(self):
        return remote(self.sent, self.came, self.tp_sems, self.size, other_core())

    def both(self, k):
        group = ahead_on("dp", k)
        return self.part[group, self.mine].astype(jnp.float32) + self.held[k].astype(jnp.float32)

    def start(self):
        each(self.size + 1, lambda k: self.swap(lax.rem(k, self.size)).start())

    def forward(self):
        def one(k):
            self.swap(k).wait_recv()
            self.held[k] = self.both(k).astype(jnp.bfloat16)
            self.copy(k).start()

        each(self.size, one)
        self.swap(0).wait()
        self.total[...] = self.both(0)

    def gather(self):
        def one(k):
            self.copy(k).wait_recv()
            self.total[...] += self.landed[k].astype(jnp.float32)

        each(self.size, one)
        self.sent[...] = self.total[...].astype(jnp.bfloat16)
        self.last().start()

    def finish(self):
        def one(k):
            self.swap(k).wait_send()
            self.copy(k).wait_send()

        each(self.size, one)
        self.last().wait()


def return_scratch(size, rows, width):
    low = jnp.bfloat16
    return [
        pltpu.VMEM((size, rows // 2, width), low),
        pltpu.VMEM((size, rows // 2, width), low),
        pltpu.VMEM((rows // 2, width), jnp.float32),
        pltpu.VMEM((rows // 2, width), low),
        pltpu.VMEM((rows // 2, width), low),
        *sem_pair(size),
        *sem_pair(size + 1),
    ]


def return_grads_kernel(
    part_ref, hidden_ref, cot_ref, gain_ref, out_w_ref, grad_ref, low_ref, mix_ref, gain_grad_ref,
    held, landed, total, sent, came, dp_send, dp_recv, tp_send, tp_recv,
):
    greet(["dp", "tp"])
    rows = RowReturn(
        part_ref, held, landed, total, sent, came, (dp_send, dp_recv), (tp_send, tp_recv)
    )
    rows.start()
    rows.forward()
    rows.gather()

    def turn_back(at, grads):
        x_grad, gain_grad = norm_back(
            hidden_ref[at, :], gain_ref[...], grads.astype(jnp.float32)
        )
        hidden_grad = cot_ref[at, :].astype(jnp.float32) + x_grad
        grad_ref[at, :] = hidden_grad
        low_ref[at, :] = hidden_grad.astype(jnp.bfloat16)
        mix_ref[at, :] = lax.dot_general(
            low_ref[at, :], out_w_ref[...], NT, preferred_element_type=jnp.float32
        ).astype(jnp.bfloat16)
        return gain_grad

    gain_mine = turn_back(rows.mine, sent[...])
    rows.finish()
    gain_theirs = turn_back(rows.theirs, came[...])
    gain_grad_ref[...] = gain_mine + gain_theirs


def return_grads(part, hidden, cot, gain, out_w, ident):
    size, rows, width = part.shape
    return pl.pallas_call(
        return_grads_kernel,
        name="return_grads",
        in_specs=whole_vmem(5),
        out_specs=whole_vmem(4),
        out_shape=[
            jax.ShapeDtypeStruct((rows, width), jnp.float32),
            jax.ShapeDtypeStruct((rows, width), jnp.bfloat16),
            jax.ShapeDtypeStruct((rows, out_w.shape[0]), jnp.bfloat16),
            jax.ShapeDtypeStruct((1, width), jnp.float32),
        ],
        scratch_shapes=return_scratch(size, rows, width),
        compiler_params=remote_params(ident),
    )(part, hidden, cot, gain, out_w)


def trade_kernel(
    back, ahead, kv_grad_ref, part_ref, hidden_ref, low_ref, mix_ref, kv_ref, out_ref, out_w_ref,
    going, came_kv, line_send, line_recv, held, landed, total, sent, came, dp_send, dp_recv,
    tp_send, tp_recv,
):
    me, size = lax.axis_index("ctx"), lax.axis_size("ctx")
    greet(["dp", "tp"], line=True)
    right, left = me + 1, me - 1
    sems = (line_send, line_recv)

    def hop(s, src):
        return remote(src, came_kv.at[s], sems, s, {"ctx": left})

    def forth():
        return remote(
            kv_grad_ref.at[lax.rem(me + 1, size)], came_kv.at[0], sems, 0, {"ctx": right}
        )

    def own_piece(s):
        return kv_grad_ref.at[lax.rem(me + size - s, size)]

    if ahead:

        @pl.when(right < size)
        def _():
            forth().start()

    @pl.when(me - back >= 0)
    def _():
        hop(back, own_piece(back)).start()

    rows = RowReturn(
        part_ref, held, landed, total, sent, came, (dp_send, dp_recv), (tp_send, tp_recv)
    )
    rows.start()
    rows.forward()
    turned = jnp.transpose(low_ref[...].astype(jnp.float32)).astype(jnp.bfloat16)
    grad = jnp.dot(turned, mix_ref[...], preferred_element_type=jnp.float32)
    piece = out_w_ref.shape[1]
    for i in range(out_w_ref.shape[0]):
        out_w_ref[i] = grad[i * piece : (i + 1) * piece].astype(jnp.bfloat16)

    for s in range(back - 1, 0, -1):

        @pl.when((me - s >= 0) & (right < size))
        def _(s=s):
            hop(s + 1, going.at[s]).wait_recv()
            going[s] = (
                own_piece(s)[...].astype(jnp.float32) + came_kv[s + 1].astype(jnp.float32)
            ).astype(going.dtype)
            hop(s, going.at[s]).start()

        @pl.when((me - s >= 0) & (right >= size))
        def _(s=s):
            hop(s, own_piece(s)).start()

    rows.gather()
    kv_ref[...] = kv_grad_ref[me].astype(jnp.float32)

    @pl.when(right < size)
    def _():
        hop(1, going.at[0]).wait_recv()
        kv_ref[...] += came_kv[1].astype(jnp.float32)

    if ahead:

        @pl.when(left >= 0)
        def _():
            forth().wait_recv()
            kv_ref[...] += came_kv[0].astype(jnp.float32)

        @pl.when(right < size)
        def _():
            forth().wait_send()

    for s in range(back, 0, -1):

        @pl.when(me - s >= 0)
        def _(s=s):
            hop(s, going.at[0]).wait_send()

    rows.finish()
    mine, theirs = rows.mine, rows.theirs
    out_ref[mine, :] = (hidden_ref[mine, :] + sent[...].astype(jnp.float32)).astype(jnp.bfloat16)
    out_ref[theirs, :] = (hidden_ref[theirs, :] + came[...].astype(jnp.float32)).astype(
        jnp.bfloat16
    )


def trade(kv_grad, part, hidden, low, mix, back, ahead, ident):
    size, rows, width = part.shape
    kv_shape = kv_grad.shape[1:]
    held = pltpu.VMEM((back + 1,) + kv_shape, kv_grad.dtype)
    return pl.pallas_call(
        functools.partial(trade_kernel, back, ahead),
        name="trade",
        in_specs=whole_vmem(5),
        out_specs=whole_vmem(3),
        out_shape=[
            jax.ShapeDtypeStruct(kv_shape, jnp.float32),
            jax.ShapeDtypeStruct((rows, width), jnp.bfloat16),
            jax.ShapeDtypeStruct((size, width // size, mix.shape[1]), jnp.bfloat16),
        ],
        scratch_shapes=[
            held, held, *sem_pair(back + 1), *return_scratch(size, rows, width)
        ],
        compiler_params=remote_params(ident),
    )(kv_grad, part, hidden, low, mix)


class PieceSum:
    def __init__(self, axis, source, landed, sems):
        self.axis, self.source, self.landed, self.sems = axis, source, landed, sems
        self.size = lax.axis_size(axis)

    def copy(self, k):
        peer = ahead_on(self.axis, k)
        return remote(
            self.source.at[peer], self.landed.at[k], self.sems, k, {self.axis: peer}
        )

    def send(self, k):
        self.copy(k).start()

    def total(self):
        each(self.size, lambda k: self.copy(k).wait_recv())
        whole = self.source[lax.axis_index(self.axis)].astype(jnp.float32)
        for k in range(1, self.size):
            whole += self.landed[k].astype(jnp.float32)
        return whole

    def finish(self):
        each(self.size, lambda k: self.copy(k).wait_send())


class WholeSum:
    def __init__(self, axis, source, landed, sems):
        self.axis, self.source, self.landed, self.sems = axis, source, landed, sems
        self.size = lax.axis_size(axis)

    def copy(self, k):
        return remote(
            self.source, self.landed.at[k], self.sems, k, {self.axis: ahead_on(self.axis, k)}
        )

    def start(self):
        each(self.size, lambda k: self.copy(k).start())

    def total(self):
        each(self.size, lambda k: self.copy(k).wait())
        whole = self.source[...]
        for k in range(1, self.size):
            whole += self.landed[k]
        return whole


def finish_kernel(
    dq_ref, dkv_ref, cos_ref, sin_ref, normed_ref, w_ref, x_ref, gain_ref, hidden_ref, out_w_ref,
    gain_two_ref, in_ref, own_ref, gains_ref, joined, turned, part, held, pieces, landed,
    out_landed, low, low_landed, gain_rows, gain_landed, gain_more, gain_more_landed, *sems,
):
    greet(["dp", "ctx", "tp"])
    pairs = [sems[2 * i : 2 * i + 2] for i in range(len(sems) // 2)]
    out_sum = PieceSum("dp", out_w_ref, out_landed, pairs[0])
    each(out_sum.size, out_sum.send)
    wide = 2 * HEAD_DIM
    q_width, kv_width = dq_ref.shape[1], dkv_ref.shape[1] // 2
    for first in range(0, q_width, wide):
        joined[:, first : first + wide] = turn(
            dq_ref[:, first : first + wide], cos_ref[...], sin_ref[...]
        ).astype(jnp.bfloat16)
    for first in range(0, kv_width, wide):
        joined[:, q_width + first : q_width + first + wide] = turn(
            dkv_ref[:, first : first + wide], cos_ref[...], sin_ref[...]
        ).astype(jnp.bfloat16)
    joined[:, q_width + kv_width :] = dkv_ref[:, kv_width:].astype(jnp.bfloat16)

    turned[...] = jnp.transpose(normed_ref[...].astype(jnp.float32)).astype(jnp.bfloat16)
    w_sum = PieceSum("dp", pieces, landed, pairs[1])
    rows = pieces.shape[1]

    def piece(k):
        peer = ahead_on("dp", k)
        at = pl.ds(pl.multiple_of(peer * rows, rows), rows)
        pieces[peer] = jnp.dot(
            turned[at, :], joined[...], preferred_element_type=jnp.float32
        ).astype(jnp.bfloat16)
        w_sum.send(k)

    each(w_sum.size, piece)
    part[...] = lax.dot_general(
        joined[...], w_ref[...], NT, preferred_element_type=jnp.float32
    ).astype(jnp.bfloat16)
    swap = remote(part, held, pairs[2], 0, other_core())
    swap.start()
    me = lax.axis_index("dp")
    own = pl.ds(pl.multiple_of(me * rows, rows), rows)
    pieces[me] = jnp.dot(
        turned[own, :], joined[...], preferred_element_type=jnp.float32
    ).astype(jnp.bfloat16)
    swap.wait()
    x_grad, gain_grad = norm_back(
        x_ref[...].astype(jnp.float32),
        gain_ref[...],
        part[...].astype(jnp.float32) + held[...].astype(jnp.float32),
    )
    in_ref[...] = (hidden_ref[...] + x_grad).astype(jnp.bfloat16)
    gain_rows[...] = jnp.zeros(gain_rows.shape, jnp.float32)
    gain_rows[0:1, :] = gain_grad
    gain_rows[1:2, :] = gain_two_ref[...]
    gain_sum = WholeSum("dp", gain_rows, gain_landed, pairs[3])
    gain_sum.start()

    out_total = out_sum.total()
    w_total = w_sum.total()
    cols = w_total.shape[1]
    few = low.shape[1]
    for c in range(low.shape[0]):
        low[c, :, :cols] = w_total[c * few : (c + 1) * few].astype(jnp.bfloat16)
        low[c, :, cols:] = out_total[c * few : (c + 1) * few].astype(jnp.bfloat16)
    low_sum = PieceSum("ctx", low, low_landed, pairs[4])
    each(low_sum.size, low_sum.send)
    gain_more[...] = gain_sum.total()
    more_sum = WholeSum("ctx", gain_more, gain_more_landed, pairs[5])
    more_sum.start()
    out_sum.finish()
    w_sum.finish()
    own_ref[...] = low_sum.total()
    low_sum.finish()
    gains_ref[...] = more_sum.total()


def finish(dq, dkv, cosine, sine, normed, w, x, gain, hidden_grad, out_w, gain_two, ident):
    rows, width = x.shape
    dp_size, ctx_size = lax.axis_size("dp"), lax.axis_size("ctx")
    cols, out_cols = w.shape[1], out_w.shape[2]
    few = width // dp_size // ctx_size
    low, high = jnp.bfloat16, jnp.float32
    return pl.pallas_call(
        finish_kernel,
        name="finish",
        in_specs=whole_vmem(11),
        out_specs=whole_vmem(3),
        out_shape=[
            jax.ShapeDtypeStruct((rows, width), low),
            jax.ShapeDtypeStruct((few, cols + out_cols), high),
            jax.ShapeDtypeStruct((8, width), high),
        ],
        scratch_shapes=[
            pltpu.VMEM((rows, cols), low),
            pltpu.VMEM((width, rows), low),
            pltpu.VMEM((rows, width), low),
            pltpu.VMEM((rows, width), low),
            pltpu.VMEM((dp_size, width // dp_size, cols), low),
            pltpu.VMEM((dp_size, width // dp_size, cols), low),
            pltpu.VMEM(out_w.shape, low),
            pltpu.VMEM((ctx_size, few, cols + out_cols), low),
            pltpu.VMEM((ctx_size, few, cols + out_cols), low),
            pltpu.VMEM((8, width), high),
            pltpu.VMEM((dp_size, 8, width), high),
            pltpu.VMEM((8, width), high),
            pltpu.VMEM((ctx_size, 8, width), high),
            *sem_pair(dp_size),
            *sem_pair(dp_size),
            *sem_pair(1),
            *sem_pair(dp_size),
            *sem_pair(ctx_size),
            *sem_pair(ctx_size),
        ],
        compiler_params=remote_params(ident),
    )(dq, dkv, cosine, sine, normed, w, x, gain, hidden_grad, out_w, gain_two)


GROUPS_AT_ONCE = 4


def experts_kernel(
    more, rows_ref, grads_ref, weights_ref, place_ref, gate_ref, place_col_ref, *refs
):
    before, refs = (refs[:2], refs[2:]) if more else (None, refs)
    out_ref, back_ref, weight_grad_ref, slots, slot_grads, outs, backs = refs
    e = pl.program_id(1)
    groups, tok_rows, _ = rows_ref.shape
    owners, part = weight_grad_ref.shape[1], weight_grad_ref.shape[5]
    slot_index = lax.broadcasted_iota(jnp.int32, (CAP, tok_rows), 0)
    gates = []
    for g in range(groups):
        picks = slot_index == place_ref[g, 0]
        gates.append(jnp.sum(jnp.where(picks, gate_ref[g, 0], 0.0), axis=1, keepdims=True))
        picks = picks.astype(jnp.float32).astype(jnp.bfloat16)
        at = slice(g * CAP, (g + 1) * CAP)
        slots[at, :] = jnp.dot(
            picks, rows_ref[g], preferred_element_type=jnp.float32
        ).astype(jnp.bfloat16)
        slot_grads[at, :] = (
            jnp.dot(picks, grads_ref[g], preferred_element_type=jnp.float32) * gates[g]
        ).astype(jnp.bfloat16)
    gate_w, up_w, down_w = (weights_ref.at[0, i] for i in range(3))
    gate_pre = jnp.dot(slots[...], gate_w[...], preferred_element_type=jnp.float32)
    up_pre = jnp.dot(slots[...], up_w[...], preferred_element_type=jnp.float32)
    act_grad = jnp.dot(slot_grads[...], down_w[...], preferred_element_type=jnp.float32)
    sig = 1.0 / (1.0 + jnp.exp(-gate_pre))
    silu = gate_pre * sig
    act_low = (silu * up_pre).astype(jnp.bfloat16)
    up_low = (act_grad * silu).astype(jnp.bfloat16)
    gate_low = (act_grad * up_pre * (sig * (1.0 + gate_pre * (1.0 - sig)))).astype(jnp.bfloat16)

    back = lax.dot_general(
        gate_low, gate_w[...], NT, preferred_element_type=jnp.float32
    ) + lax.dot_general(up_low, up_w[...], NT, preferred_element_type=jnp.float32)
    out = lax.dot_general(act_low, down_w[...], NT, preferred_element_type=jnp.float32)
    for g in range(groups):
        at = slice(g * CAP, (g + 1) * CAP)
        to = pl.ds(pl.multiple_of(e * CAP, CAP), CAP)
        backs[g, to, :] = back[at].astype(jnp.bfloat16)
        outs[g, to, :] = (out[at] * gates[g]).astype(jnp.bfloat16)

    for i, (low, source) in enumerate(
        ((gate_low, slots), (up_low, slots), (act_low, slot_grads))
    ):
        turned = jnp.transpose(low.astype(jnp.float32)).astype(jnp.bfloat16)
        total = jnp.dot(turned, source[...], preferred_element_type=jnp.float32)
        for c in range(owners):
            weight_grad_ref[0, c, 0, i] = total[:, c * part : (c + 1) * part].astype(
                weight_grad_ref.dtype
            )

    @pl.when(e == pl.num_programs(1) - 1)
    def _():
        slot_count = outs.shape[1]
        for g in range(groups):
            tiles = []
            for first in range(0, slot_count, 128):
                wide = min(128, slot_count - first)
                lane = first + lax.broadcasted_iota(jnp.int32, (tok_rows, wide), 1)
                hit = None
                for n in range(first // CAP, (first + wide - 1) // CAP + 1):
                    one = place_col_ref[g, :, n : n + 1] == lane - n * CAP
                    hit = one if hit is None else hit | one
                tiles.append(hit.astype(jnp.float32).astype(jnp.bfloat16))
            spread_picks = jnp.concatenate(tiles, axis=1)
            for i, (to_ref, source) in enumerate(((back_ref, backs), (out_ref, outs))):
                total = jnp.dot(spread_picks, source[g], preferred_element_type=jnp.float32)
                if more:
                    total += before[1 - i][g].astype(jnp.float32)
                to_ref[g] = total.astype(jnp.bfloat16)


def expert_places(chosen_all, gates_all, own):
    tok_rows = chosen_all.shape[1]
    named = chosen_all[..., None] == lax.axis_index("dp") * own + jnp.arange(own, dtype=jnp.int32)
    names = jnp.any(named, axis=2)
    gate_of = jnp.sum(jnp.where(named, gates_all[..., None], 0.0), axis=2)
    earlier = jnp.tril(jnp.ones((tok_rows, tok_rows), jnp.bfloat16), -1)
    place = jnp.einsum(
        "rq,gqe->gre", earlier, names.astype(jnp.bfloat16), preferred_element_type=jnp.float32
    ).astype(jnp.int32)
    place = jnp.where(names & (place < CAP), place, -CAP * own)
    return (
        place,
        place.transpose(0, 2, 1)[:, :, None],
        gate_of.transpose(0, 2, 1)[:, :, None],
    )


def experts(weights, places, rows_all, grad_all, first, count, before):
    _, _, model_width, hidden = weights.shape
    place_cols, place_rows, gate_rows = places
    groups, tok_rows, _ = rows_all.shape
    owners = lax.axis_size("ctx")
    at_once = min(GROUPS_AT_ONCE, groups)
    chunks = groups // at_once
    part = model_width // owners
    rows_spec = pl.BlockSpec(
        (at_once, tok_rows, model_width), lambda c, e: (c, 0, 0), pipeline_mode=pl.Buffered(1)
    )
    line_spec = pl.BlockSpec((at_once, 1, 1, tok_rows), lambda c, e: (c, e + first, 0, 0))
    out_shape = jax.ShapeDtypeStruct(rows_all.shape, jnp.bfloat16)
    flops = count * groups * CAP * model_width * 2 * (9 * hidden + 4 * tok_rows)
    more = before is not None
    out_part, back_part, weight_part = pl.pallas_call(
        functools.partial(experts_kernel, more),
        name="experts",
        grid=(chunks, count),
        in_specs=[
            rows_spec,
            rows_spec,
            pl.BlockSpec((1, 3, model_width, hidden), lambda c, e: (e + first, 0, 0, 0)),
            line_spec,
            line_spec,
            pl.BlockSpec((at_once, tok_rows, count), lambda c, e: (c, 0, 0)),
        ]
        + [rows_spec] * (2 * more),
        out_specs=[
            rows_spec,
            rows_spec,
            pl.BlockSpec((1, owners, 1, 3, hidden, part), lambda c, e: (c, 0, e, 0, 0, 0)),
        ],
        out_shape=[
            out_shape,
            out_shape,
            jax.ShapeDtypeStruct((chunks, owners, count, 3, hidden, part), jnp.bfloat16),
        ],
        scratch_shapes=[
            pltpu.VMEM((at_once * CAP, model_width), jnp.bfloat16),
            pltpu.VMEM((at_once * CAP, model_width), jnp.bfloat16),
            pltpu.VMEM((at_once, count * CAP, model_width), jnp.bfloat16),
            pltpu.VMEM((at_once, count * CAP, model_width), jnp.bfloat16),
        ],
        compiler_params=pltpu.CompilerParams(vmem_limit_bytes=LIMIT),
        cost_estimate=pl.CostEstimate(
            flops=flops, bytes_accessed=4 * weights.size, transcendentals=0
        ),
    )(
        rows_all,
        grad_all,
        weights,
        place_rows,
        gate_rows,
        place_cols[:, :, first : first + count],
        *(before if more else ()),
    )
    if chunks == 1:
        return (out_part, back_part), weight_part[0]
    return (out_part, back_part), jnp.sum(weight_part.astype(jnp.float32), axis=0).astype(
        jnp.bfloat16
    )


def picture_of(starts, token_positions):
    inside = (token_positions[:, None] >= starts[None, :]) & (
        token_positions[:, None] < starts[None, :] + PIC
    )
    labels = jnp.arange(starts.shape[0], dtype=jnp.int32) + 1
    return jnp.sum(jnp.where(inside, labels[None, :], 0), axis=-1) - 1


def rotary_tables(token_positions):
    half_dim = HEAD_DIM // 2
    inverse = THETA ** (-(jnp.arange(half_dim, dtype=jnp.float32) * 2.0 / HEAD_DIM))
    angles = token_positions.astype(jnp.float32)[:, None] * inverse[None, :]
    cosine, sine = jnp.cos(angles), jnp.sin(angles)
    return jnp.concatenate([cosine] * 4, axis=1), jnp.concatenate([sine, -sine] * 2, axis=1)


def body(
    tokens,
    query_weight,
    key_weight,
    value_weight,
    output_weight,
    gain_attn,
    gain_moe,
    expert_weights,
    routes,
    gate_values,
    documents,
    pic_starts,
    cotangent,
):
    _, block_len, model_width = tokens.shape
    dp_size, ctx_size = lax.axis_size("dp"), lax.axis_size("ctx")
    length = block_len * ctx_size
    offset = lax.axis_index("ctx") * block_len
    back = back_blocks(ctx_size, block_len, length)
    ahead = ahead_blocks(block_len, length, pic_starts.shape[1])
    q_width, kv_width = query_weight.shape[1], key_weight.shape[1]
    own = expert_weights.shape[0]
    x, cot = tokens[0], cotangent[0]

    joined_w = jnp.concatenate([query_weight, key_weight, value_weight], axis=1)
    gains = jnp.stack([gain_attn, gain_moe]).astype(jnp.float32)
    joined_all, gains_all, docs_all, chosen_all, gates_all = spread(
        [
            joined_w,
            gains,
            documents,
            routes.reshape(block_len * TOP // 128, 128),
            gate_values.reshape(block_len * TOP // 128, 128),
        ],
        ["dp", "dp", "ctx", "dp", "dp"],
        1,
    )
    output_weight, joined_all = lax.optimization_barrier((output_weight, joined_all))
    output_full = lax.all_gather(output_weight, "dp", axis=1, tiled=True)
    joined_full = joined_all.reshape(model_width, -1)
    gain_rows = gains_all.transpose(1, 0, 2).reshape(2, 1, model_width)
    docs_all = docs_all.reshape(length)
    cosine, sine = rotary_tables(offset + jnp.arange(block_len, dtype=jnp.int32))
    normed_one, query, kv_all, grad_all = project(
        x, joined_full, gain_rows[0], cosine, sine, cot, q_width, back, ahead, 2
    )
    kv_all = kv_all.reshape(length, 2 * kv_width)

    pictures = picture_of(pic_starts[0], jnp.arange(length, dtype=jnp.int32))
    flags = block_flags(pic_starts[0], documents[0], docs_all, offset)
    kinfo = jnp.stack([docs_all, pictures], axis=1)
    qinfo = jnp.stack([documents[0], lax.dynamic_slice_in_dim(pictures, offset, block_len)])
    places = expert_places(
        chosen_all.reshape(dp_size, block_len, TOP), gates_all.reshape(dp_size, block_len, TOP), own
    )
    mixture, mix_full, log_total, attn_part = attend(
        flags, query, kv_all, kinfo, qinfo, output_full
    )
    hidden, rows_all = share_rows(attn_part, x, gain_rows[1], 3)
    half = own // 2
    parts, grads_one = experts(expert_weights, places, rows_all, grad_all, 0, half, None)
    expert_one = lax.psum_scatter(grads_one, "ctx", scatter_dimension=0)
    (out_part, back_part), grads_two = experts(
        expert_weights, places, rows_all, grad_all, half, own - half, parts
    )
    hidden_grad, hidden_low, mix_grad, gain_two_grad = return_grads(
        back_part, hidden, cot, gain_rows[1], output_full, 4
    )
    q_rot_grad, kv_part = attend_back(
        flags, query, kv_all, kinfo, qinfo, log_total, mix_full, mix_grad
    )
    kv_back, layer_out, output_grad = trade(
        kv_part.reshape(ctx_size, block_len, 2 * kv_width),
        out_part,
        hidden,
        hidden_low,
        mixture,
        back,
        ahead,
        5,
    )
    grads_two, kv_back = lax.optimization_barrier((grads_two, kv_back))
    expert_two = lax.psum_scatter(grads_two, "ctx", scatter_dimension=0)
    input_grad, owned, gain_sums = finish(
        q_rot_grad,
        kv_back,
        cosine,
        sine,
        normed_one,
        joined_full,
        x,
        gain_rows[0],
        hidden_grad,
        output_grad,
        gain_two_grad,
        6,
    )
    few = owned.shape[0]
    here = (lax.axis_index("dp") * ctx_size + lax.axis_index("ctx")) * few
    gain_sums = lax.dynamic_slice_in_dim(gain_sums, here, few, 1)
    expert_grad = jnp.concatenate([expert_one, expert_two], axis=0)
    v_end = q_width + 2 * kv_width
    return (
        layer_out[None],
        input_grad[None],
        owned[:, :q_width],
        owned[:, q_width : q_width + kv_width],
        owned[:, q_width + kv_width : v_end],
        owned[:, v_end:].T,
        gain_sums[0],
        gain_sums[1],
        expert_grad.astype(jnp.float32).transpose(0, 1, 3, 2),
    )


def solution(mesh):
    return jax.shard_map(
        body,
        mesh=mesh,
        in_specs=(
            P("dp", "ctx", None),
            P("dp", "tp"),
            P("dp", "tp"),
            P("dp", "tp"),
            P("tp", "dp"),
            P("dp"),
            P("dp"),
            P("dp", None, None, "tp"),
            P("dp", "ctx", None),
            P("dp", "ctx", None),
            P("dp", "ctx"),
            P("dp", None),
            P("dp", "ctx", None),
        ),
        out_specs=(
            P("dp", "ctx", None),
            P("dp", "ctx", None),
            P(("dp", "ctx"), "tp"),
            P(("dp", "ctx"), "tp"),
            P(("dp", "ctx"), "tp"),
            P("tp", ("dp", "ctx")),
            P(("dp", "ctx")),
            P(("dp", "ctx")),
            P("dp", None, "ctx", "tp"),
        ),
        check_vma=False,
    )
```

```python
import functools

import jax
import jax.numpy as jnp
from jax import lax
from jax.experimental import pallas as pl
from jax.experimental.pallas import tpu as pltpu
from jax.sharding import PartitionSpec as P

HEAD_DIM = 64
PIC = 256
CAP = 144

EPSILON = 1e-06
THETA = 10000.0
NEG_FILL = -1e30


KEY_ROWS = 256
NT = (((1,), (1,)), ((), ()))
LIMIT = 63 * 1024 * 1024


def whole_vmem(count):
    return [pl.BlockSpec(memory_space=pltpu.VMEM)] * count


def picture_ids(starts_ref, places):
    ids = jnp.full(places.shape, -1, jnp.int32)
    for j in range(starts_ref.shape[1]):
        start = starts_ref[0, j]
        ids += jnp.where((places >= start) & (places < start + PIC), j + 1, 0)
    return ids


def as_column(row):
    tall = jnp.broadcast_to(row.astype(jnp.float32), (8, row.shape[1]))
    return jnp.transpose(tall)[:, 0:1].astype(jnp.int32)


class Masks:
    def __init__(self, docs_ref, starts_ref, column):
        self.docs_ref, self.starts_ref, self.column = docs_ref, starts_ref, column
        self.rows = docs_ref.shape[2]
        me = lax.axis_index("ctx")
        self.q_doc = docs_ref[me]
        self.q_place = me * self.rows + lax.broadcasted_iota(jnp.int32, (1, self.rows), 1)
        self.q_pic = picture_ids(starts_ref, self.q_place)

    def open(self, block):
        self.column[...] = jnp.broadcast_to(
            as_column(self.docs_ref[block]), self.column.shape
        )

    def bias(self, block, rows, first):
        k_doc = self.column[rows, 0:1]
        k_place = block * self.rows + first + lax.broadcasted_iota(jnp.int32, k_doc.shape, 0)
        k_pic = picture_ids(self.starts_ref, k_place)
        seen = (k_doc == self.q_doc) & (
            (k_place <= self.q_place) | ((k_pic == self.q_pic) & (self.q_pic >= 0))
        )
        return jnp.where(seen, 0.0, NEG_FILL)


def attend_block(masks, block, q_ref, kv_ref, acc, top, total):
    kv_width = kv_ref.shape[1] // 2
    heads, kv_heads = q_ref.shape[1] // HEAD_DIM, kv_width // HEAD_DIM
    masks.open(block)

    def step(j, carry):
        first = pl.multiple_of(j * KEY_ROWS, KEY_ROWS)
        rows = pl.ds(first, KEY_ROWS)
        bias = masks.bias(block, rows, first)
        for g in range(kv_heads):
            key = kv_ref[rows, g * HEAD_DIM : (g + 1) * HEAD_DIM]
            val = kv_ref[rows, kv_width + g * HEAD_DIM : kv_width + (g + 1) * HEAD_DIM]
            val_t = jnp.transpose(val.astype(jnp.float32)).astype(jnp.bfloat16)
            for h in range(g * heads // kv_heads, (g + 1) * heads // kv_heads):
                at = slice(h * HEAD_DIM, (h + 1) * HEAD_DIM)
                scores = bias + lax.dot_general(
                    key, q_ref[:, at], NT, preferred_element_type=jnp.float32
                )
                old = top[h : h + 1, :]
                new = jnp.maximum(old, jnp.max(scores, axis=0, keepdims=True))
                probs = jnp.exp(scores - new)
                fade = jnp.exp(old - new)
                total[h : h + 1, :] = total[h : h + 1, :] * fade + jnp.sum(
                    probs, axis=0, keepdims=True
                )
                acc[at, :] = acc[at, :] * fade + jnp.dot(
                    val_t, probs.astype(jnp.bfloat16), preferred_element_type=jnp.float32
                )
                top[h : h + 1, :] = new
        return carry

    lax.fori_loop(0, kv_ref.shape[0] // KEY_ROWS, step, 0)


def attend_back_block(masks, block, q_ref, kv_ref, log_ref, delta, grad_ref, acc, dkv_ref):
    kv_width = kv_ref.shape[1] // 2
    heads, kv_heads = q_ref.shape[1] // HEAD_DIM, kv_width // HEAD_DIM
    masks.open(block)

    def step(j, carry):
        first = pl.multiple_of(j * KEY_ROWS, KEY_ROWS)
        rows = pl.ds(first, KEY_ROWS)
        bias = masks.bias(block, rows, first)
        for g in range(kv_heads):
            k_at = slice(g * HEAD_DIM, (g + 1) * HEAD_DIM)
            v_at = slice(kv_width + g * HEAD_DIM, kv_width + (g + 1) * HEAD_DIM)
            key, val = kv_ref[rows, k_at], kv_ref[rows, v_at]
            key_t = jnp.transpose(key.astype(jnp.float32)).astype(jnp.bfloat16)
            dk = jnp.zeros((KEY_ROWS, HEAD_DIM), jnp.float32)
            dv = jnp.zeros((KEY_ROWS, HEAD_DIM), jnp.float32)
            for h in range(g * heads // kv_heads, (g + 1) * heads // kv_heads):
                at = slice(h * HEAD_DIM, (h + 1) * HEAD_DIM)
                q_rows, g_rows = q_ref[:, at], grad_ref[:, at]
                scores = bias + lax.dot_general(
                    key, q_rows, NT, preferred_element_type=jnp.float32
                )
                probs = jnp.exp(scores - log_ref[h : h + 1, :])
                prob_grad = lax.dot_general(val, g_rows, NT, preferred_element_type=jnp.float32)
                slope = (probs * (prob_grad - delta[h : h + 1, :])).astype(jnp.bfloat16)
                dv += jnp.dot(
                    probs.astype(jnp.bfloat16), g_rows, preferred_element_type=jnp.float32
                )
                dk += jnp.dot(slope, q_rows, preferred_element_type=jnp.float32)
                acc[at, :] += jnp.dot(key_t, slope, preferred_element_type=jnp.float32)
            dkv_ref[rows, k_at] = dk.astype(dkv_ref.dtype)
            dkv_ref[rows, v_at] = dv.astype(dkv_ref.dtype)
        return carry

    lax.fori_loop(0, kv_ref.shape[0] // KEY_ROWS, step, 0)


def attend_back_kernel(
    back, ahead, starts_ref, q_ref, kv_ref, docs_ref, log_ref, full_ref, grad_ref, dq_ref,
    dkv_ref, acc, delta, column,
):
    me, size = lax.axis_index("ctx"), lax.axis_size("ctx")
    acc[...] = jnp.transpose(full_ref[...] * grad_ref[...].astype(jnp.float32))
    for h in range(delta.shape[0]):
        delta[h : h + 1, :] = jnp.sum(
            acc[h * HEAD_DIM : (h + 1) * HEAD_DIM, :], axis=0, keepdims=True
        )
    acc[...] = jnp.zeros(acc.shape, jnp.float32)
    masks = Masks(docs_ref, starts_ref, column)

    def step(s, carry):
        block = me + ahead - s

        @pl.when((block >= 0) & (block < size))
        def _():
            attend_back_block(
                masks, block, q_ref, kv_ref.at[block], log_ref, delta, grad_ref, acc,
                dkv_ref.at[block],
            )

        return carry

    lax.fori_loop(0, back + ahead + 1, step, 0)
    dq_ref[...] = jnp.transpose(acc[...]) * (HEAD_DIM**-0.5)


def attend_back(starts, q, kv, docs, log_total, full, grad, back, ahead):
    rows, width = q.shape
    return pl.pallas_call(
        functools.partial(attend_back_kernel, back, ahead),
        name="attend_back",
        in_specs=[pl.BlockSpec(memory_space=pltpu.SMEM)] + whole_vmem(6),
        out_specs=whole_vmem(2),
        out_shape=[
            jax.ShapeDtypeStruct((rows, width), jnp.float32),
            jax.ShapeDtypeStruct(kv.shape, jnp.bfloat16),
        ],
        scratch_shapes=[
            pltpu.VMEM((width, rows), jnp.float32),
            pltpu.VMEM((width // HEAD_DIM, rows), jnp.float32),
            pltpu.VMEM((rows, 8), jnp.int32),
        ],
        compiler_params=pltpu.CompilerParams(vmem_limit_bytes=LIMIT),
    )(starts, q, kv, docs, log_total, full, grad)


MESH = pl.DeviceIdType.MESH


def greet(axes_list, line=False):
    barrier = pltpu.get_barrier_semaphore()
    count = 0
    for axis in axes_list:
        me, size = lax.axis_index(axis), lax.axis_size(axis)

        def signal(k, carry, axis=axis, me=me, size=size):
            pl.semaphore_signal(
                barrier, inc=1, device_id={axis: lax.rem(me + k, size)}, device_id_type=MESH
            )
            return carry

        lax.fori_loop(1, size, signal, 0)
        count += size - 1
    if not line:
        pl.semaphore_wait(barrier, count)
        return
    me, size = lax.axis_index("ctx"), lax.axis_size("ctx")
    for step in (1, -1):
        other = me + step

        @pl.when((other >= 0) & (other < size))
        def _(other=other):
            pl.semaphore_signal(barrier, inc=1, device_id={"ctx": other}, device_id_type=MESH)

    inner = (me > 0) & (me < size - 1)

    @pl.when(inner)
    def _():
        pl.semaphore_wait(barrier, count + 2)

    @pl.when(jnp.logical_not(inner))
    def _():
        pl.semaphore_wait(barrier, count + 1)


def remote(src, dst, sems, k, device_id):
    return pltpu.make_async_remote_copy(
        src_ref=src,
        dst_ref=dst,
        send_sem=sems[0].at[k],
        recv_sem=sems[1].at[k],
        device_id=device_id,
        device_id_type=MESH,
    )


def other_core():
    return {"tp": 1 - lax.axis_index("tp")}


def ahead_on(axis, k):
    return lax.rem(lax.axis_index(axis) + k, lax.axis_size(axis))


def each(count, do, first=1):
    def step(k, carry):
        do(k)
        return carry

    lax.fori_loop(first, count, step, 0)


def sem_pair(count):
    return [pltpu.SemaphoreType.DMA((count,)), pltpu.SemaphoreType.DMA((count,))]


def remote_params(ident):
    return pltpu.CompilerParams(
        collective_id=ident, has_side_effects=True, vmem_limit_bytes=LIMIT
    )


def halves(rows):
    half = rows // 2
    core = lax.axis_index("tp")
    return (
        pl.ds(pl.multiple_of(core * half, half), half),
        pl.ds(pl.multiple_of((1 - core) * half, half), half),
    )


def turn(tile, cosine, sine):
    lane = lax.broadcasted_iota(jnp.int32, tile.shape, 1)
    half = HEAD_DIM // 2
    swapped = jnp.where(
        lax.rem(lane, HEAD_DIM) < half,
        pltpu.roll(tile, 2 * HEAD_DIM - half, 1),
        pltpu.roll(tile, half, 1),
    )
    return tile * cosine + swapped * sine


def row_scale(x):
    return lax.rsqrt(jnp.mean(x * x, axis=-1, keepdims=True) + EPSILON)


def norm_back(x, gain, grad):
    scale = row_scale(x)
    unit = x * scale
    pull = grad * gain
    return (
        scale * (pull - unit * jnp.mean(pull * unit, axis=-1, keepdims=True)),
        jnp.sum(grad * unit, axis=0, keepdims=True),
    )


def back_blocks(ctx_size, block_len, length):
    return min(ctx_size - 1, -(-(length // 2 - 1) // block_len))


def ahead_blocks(block_len, length, spans):
    return 0 if block_len % (length // spans) == 0 else 1


class RowGather:
    def __init__(self, source, target, dp_sems, tp_sems, first):
        self.source, self.target = source, target
        self.dp_sems, self.tp_sems, self.first = dp_sems, tp_sems, first
        self.mine, _ = halves(source.shape[0])
        self.size = lax.axis_size("dp")

    def copy(self, k):
        at = self.target.at[lax.axis_index("dp"), self.mine]
        return remote(
            self.source.at[self.mine], at, self.dp_sems, k, {"dp": ahead_on("dp", k)}
        )

    def relay(self, k):
        at = self.target.at[ahead_on("dp", self.size - k), self.mine]
        return remote(at, at, self.tp_sems, self.first + k, other_core())

    def start(self):
        each(self.size, lambda k: self.copy(k).start())

    def forward(self):
        def one(k):
            self.copy(k).wait_recv()
            self.relay(k).start()

        each(self.size, one)

    def finish(self):
        def one(k):
            self.copy(k).wait_send()
            self.relay(k).wait()

        each(self.size, one)


class RowReturn:
    def __init__(self, part, held, landed, total, sent, came, dp_sems, tp_sems):
        self.part, self.held, self.landed, self.total = part, held, landed, total
        self.sent, self.came, self.dp_sems, self.tp_sems = sent, came, dp_sems, tp_sems
        self.size = lax.axis_size("dp")
        self.mine, self.theirs = halves(part.shape[1])

    def swap(self, k):
        group = ahead_on("dp", k)
        return remote(
            self.part.at[group, self.theirs], self.held.at[k], self.tp_sems, k, other_core()
        )

    def copy(self, k):
        return remote(
            self.held.at[k], self.landed.at[k], self.dp_sems, k, {"dp": ahead_on("dp", k)}
        )

    def last(self):
        return remote(self.sent, self.came, self.tp_sems, self.size, other_core())

    def both(self, k):
        group = ahead_on("dp", k)
        return self.part[group, self.mine].astype(jnp.float32) + self.held[k].astype(jnp.float32)

    def start(self):
        each(self.size + 1, lambda k: self.swap(lax.rem(k, self.size)).start())

    def forward(self):
        def one(k):
            self.swap(k).wait_recv()
            self.held[k] = self.both(k).astype(jnp.bfloat16)
            self.copy(k).start()

        each(self.size, one)
        self.swap(0).wait()
        self.total[...] = self.both(0)

    def gather(self):
        def one(k):
            self.copy(k).wait_recv()
            self.total[...] += self.landed[k].astype(jnp.float32)

        each(self.size, one)
        self.sent[...] = self.total[...].astype(jnp.bfloat16)
        self.last().start()

    def finish(self):
        def one(k):
            self.swap(k).wait_send()
            self.copy(k).wait_send()

        each(self.size, one)
        self.last().wait()


def return_scratch(size, rows, width):
    low = jnp.bfloat16
    return [
        pltpu.VMEM((size, rows // 2, width), low),
        pltpu.VMEM((size, rows // 2, width), low),
        pltpu.VMEM((rows // 2, width), jnp.float32),
        pltpu.VMEM((rows // 2, width), low),
        pltpu.VMEM((rows // 2, width), low),
        *sem_pair(size),
        *sem_pair(size + 1),
    ]


def return_grads_kernel(
    part_ref, hidden_ref, cot_ref, gain_ref, out_w_ref, grad_ref, low_ref, mix_ref, gain_grad_ref,
    held, landed, total, sent, came, dp_send, dp_recv, tp_send, tp_recv,
):
    greet(["dp", "tp"])
    rows = RowReturn(
        part_ref, held, landed, total, sent, came, (dp_send, dp_recv), (tp_send, tp_recv)
    )
    rows.start()
    rows.forward()
    rows.gather()

    def turn_back(at, grads):
        x_grad, gain_grad = norm_back(
            hidden_ref[at, :], gain_ref[1:2, :], grads.astype(jnp.float32)
        )
        hidden_grad = cot_ref[at, :].astype(jnp.float32) + x_grad
        grad_ref[at, :] = hidden_grad
        low_ref[at, :] = hidden_grad.astype(jnp.bfloat16)
        piece = out_w_ref.shape[2]
        mix = None
        for i in range(out_w_ref.shape[0]):
            one = lax.dot_general(
                low_ref[at, i * piece : (i + 1) * piece],
                out_w_ref[i],
                NT,
                preferred_element_type=jnp.float32,
            )
            mix = one if mix is None else mix + one
        mix_ref[at, :] = mix.astype(jnp.bfloat16)
        return gain_grad

    gain_mine = turn_back(rows.mine, sent[...])
    rows.finish()
    gain_theirs = turn_back(rows.theirs, came[...])
    gain_grad_ref[...] = gain_mine + gain_theirs


def return_grads(part, hidden, cot, gain, out_w, ident):
    size, rows, width = part.shape
    return pl.pallas_call(
        return_grads_kernel,
        name="return_grads",
        in_specs=whole_vmem(5),
        out_specs=whole_vmem(4),
        out_shape=[
            jax.ShapeDtypeStruct((rows, width), jnp.float32),
            jax.ShapeDtypeStruct((rows, width), jnp.bfloat16),
            jax.ShapeDtypeStruct((rows, out_w.shape[1]), jnp.bfloat16),
            jax.ShapeDtypeStruct((1, width), jnp.float32),
        ],
        scratch_shapes=return_scratch(size, rows, width),
        compiler_params=remote_params(ident),
    )(part, hidden, cot, gain, out_w)


def trade_kernel(
    back, ahead, kv_grad_ref, part_ref, hidden_ref, low_ref, mix_ref, kv_ref, out_ref, out_w_ref,
    going, came_kv, line_send, line_recv, held, landed, total, sent, came, dp_send, dp_recv,
    tp_send, tp_recv,
):
    me, size = lax.axis_index("ctx"), lax.axis_size("ctx")
    greet(["dp", "tp"], line=True)
    right, left = me + 1, me - 1
    sems = (line_send, line_recv)

    def hop(s, src):
        return remote(src, came_kv.at[s], sems, s, {"ctx": left})

    def forth():
        return remote(
            kv_grad_ref.at[lax.rem(me + 1, size)], came_kv.at[0], sems, 0, {"ctx": right}
        )

    def own_piece(s):
        return kv_grad_ref.at[lax.rem(me + size - s, size)]

    if ahead:

        @pl.when(right < size)
        def _():
            forth().start()

    @pl.when(me - back >= 0)
    def _():
        hop(back, own_piece(back)).start()

    rows = RowReturn(
        part_ref, held, landed, total, sent, came, (dp_send, dp_recv), (tp_send, tp_recv)
    )
    rows.start()
    rows.forward()
    turned = jnp.transpose(low_ref[...].astype(jnp.float32)).astype(jnp.bfloat16)
    grad = jnp.dot(turned, mix_ref[...], preferred_element_type=jnp.float32)
    piece = out_w_ref.shape[1]
    for i in range(out_w_ref.shape[0]):
        out_w_ref[i] = grad[i * piece : (i + 1) * piece].astype(jnp.bfloat16)

    for s in range(back - 1, 0, -1):

        @pl.when((me - s >= 0) & (right < size))
        def _(s=s):
            hop(s + 1, going.at[s]).wait_recv()
            going[s] = (
                own_piece(s)[...].astype(jnp.float32) + came_kv[s + 1].astype(jnp.float32)
            ).astype(going.dtype)
            hop(s, going.at[s]).start()

        @pl.when((me - s >= 0) & (right >= size))
        def _(s=s):
            hop(s, own_piece(s)).start()

    rows.gather()
    kv_ref[...] = kv_grad_ref[me].astype(jnp.float32)

    @pl.when(right < size)
    def _():
        hop(1, going.at[0]).wait_recv()
        kv_ref[...] += came_kv[1].astype(jnp.float32)

    if ahead:

        @pl.when(left >= 0)
        def _():
            forth().wait_recv()
            kv_ref[...] += came_kv[0].astype(jnp.float32)

        @pl.when(right < size)
        def _():
            forth().wait_send()

    for s in range(back, 0, -1):

        @pl.when(me - s >= 0)
        def _(s=s):
            hop(s, going.at[0]).wait_send()

    rows.finish()
    mine, theirs = rows.mine, rows.theirs
    out_ref[mine, :] = (hidden_ref[mine, :] + sent[...].astype(jnp.float32)).astype(jnp.bfloat16)
    out_ref[theirs, :] = (hidden_ref[theirs, :] + came[...].astype(jnp.float32)).astype(
        jnp.bfloat16
    )


def trade(kv_grad, part, hidden, low, mix, back, ahead, ident):
    size, rows, width = part.shape
    kv_shape = kv_grad.shape[1:]
    held = pltpu.VMEM((back + 1,) + kv_shape, kv_grad.dtype)
    return pl.pallas_call(
        functools.partial(trade_kernel, back, ahead),
        name="trade",
        in_specs=whole_vmem(5),
        out_specs=whole_vmem(3),
        out_shape=[
            jax.ShapeDtypeStruct(kv_shape, jnp.float32),
            jax.ShapeDtypeStruct((rows, width), jnp.bfloat16),
            jax.ShapeDtypeStruct((size, width // size, mix.shape[1]), jnp.bfloat16),
        ],
        scratch_shapes=[
            held, held, *sem_pair(back + 1), *return_scratch(size, rows, width)
        ],
        compiler_params=remote_params(ident),
    )(kv_grad, part, hidden, low, mix)


class PieceSum:
    def __init__(self, axis, source, landed, sems):
        self.axis, self.source, self.landed, self.sems = axis, source, landed, sems
        self.size = lax.axis_size(axis)

    def copy(self, k):
        peer = ahead_on(self.axis, k)
        return remote(
            self.source.at[peer], self.landed.at[k], self.sems, k, {self.axis: peer}
        )

    def send(self, k):
        self.copy(k).start()

    def total(self):
        each(self.size, lambda k: self.copy(k).wait_recv())
        whole = self.source[lax.axis_index(self.axis)].astype(jnp.float32)
        for k in range(1, self.size):
            whole += self.landed[k].astype(jnp.float32)
        return whole

    def finish(self):
        each(self.size, lambda k: self.copy(k).wait_send())


class WholeSum:
    def __init__(self, axis, source, landed, sems):
        self.axis, self.source, self.landed, self.sems = axis, source, landed, sems
        self.size = lax.axis_size(axis)

    def copy(self, k):
        return remote(
            self.source, self.landed.at[k], self.sems, k, {self.axis: ahead_on(self.axis, k)}
        )

    def start(self):
        each(self.size, lambda k: self.copy(k).start())

    def total(self):
        each(self.size, lambda k: self.copy(k).wait())
        whole = self.source[...]
        for k in range(1, self.size):
            whole += self.landed[k]
        return whole


def finish_kernel(
    dq_ref, dkv_ref, cos_ref, sin_ref, normed_ref, w_ref, x_ref, gain_ref, hidden_ref, out_w_ref,
    gain_two_ref, in_ref, own_ref, gains_ref, joined, turned, part, held, pieces, landed,
    out_landed, low, low_landed, gain_rows, gain_landed, gain_more, gain_more_landed, *sems,
):
    greet(["dp", "ctx", "tp"])
    pairs = [sems[2 * i : 2 * i + 2] for i in range(len(sems) // 2)]
    out_sum = PieceSum("dp", out_w_ref, out_landed, pairs[0])
    each(out_sum.size, out_sum.send)
    wide = 2 * HEAD_DIM
    q_width, kv_width = dq_ref.shape[1], dkv_ref.shape[1] // 2
    for first in range(0, q_width, wide):
        joined[:, first : first + wide] = turn(
            dq_ref[:, first : first + wide], cos_ref[...], sin_ref[...]
        ).astype(jnp.bfloat16)
    for first in range(0, kv_width, wide):
        joined[:, q_width + first : q_width + first + wide] = turn(
            dkv_ref[:, first : first + wide], cos_ref[...], sin_ref[...]
        ).astype(jnp.bfloat16)
    joined[:, q_width + kv_width :] = dkv_ref[:, kv_width:].astype(jnp.bfloat16)

    turned[...] = jnp.transpose(normed_ref[...].astype(jnp.float32)).astype(jnp.bfloat16)
    w_sum = PieceSum("dp", pieces, landed, pairs[1])
    rows = pieces.shape[1]

    def piece(k):
        peer = ahead_on("dp", k)
        at = pl.ds(pl.multiple_of(peer * rows, rows), rows)
        pieces[peer] = jnp.dot(
            turned[at, :], joined[...], preferred_element_type=jnp.float32
        ).astype(jnp.bfloat16)
        w_sum.send(k)

    each(w_sum.size, piece)
    for i in range(w_ref.shape[0]):
        part[:, i * rows : (i + 1) * rows] = lax.dot_general(
            joined[...], w_ref[i], NT, preferred_element_type=jnp.float32
        ).astype(jnp.bfloat16)
    swap = remote(part, held, pairs[2], 0, other_core())
    swap.start()
    me = lax.axis_index("dp")
    own = pl.ds(pl.multiple_of(me * rows, rows), rows)
    pieces[me] = jnp.dot(
        turned[own, :], joined[...], preferred_element_type=jnp.float32
    ).astype(jnp.bfloat16)
    swap.wait()
    x_grad, gain_grad = norm_back(
        x_ref[...].astype(jnp.float32),
        gain_ref[0:1, :],
        part[...].astype(jnp.float32) + held[...].astype(jnp.float32),
    )
    in_ref[...] = (hidden_ref[...] + x_grad).astype(jnp.bfloat16)
    gain_rows[...] = jnp.zeros(gain_rows.shape, jnp.float32)
    gain_rows[0:1, :] = gain_grad
    gain_rows[1:2, :] = gain_two_ref[...]
    gain_sum = WholeSum("dp", gain_rows, gain_landed, pairs[3])
    gain_sum.start()

    out_total = out_sum.total()
    w_total = w_sum.total()
    cols = w_total.shape[1]
    few = low.shape[1]
    for c in range(low.shape[0]):
        low[c, :, :cols] = w_total[c * few : (c + 1) * few].astype(jnp.bfloat16)
        low[c, :, cols:] = out_total[c * few : (c + 1) * few].astype(jnp.bfloat16)
    low_sum = PieceSum("ctx", low, low_landed, pairs[4])
    each(low_sum.size, low_sum.send)
    gain_more[...] = gain_sum.total()
    more_sum = WholeSum("ctx", gain_more, gain_more_landed, pairs[5])
    more_sum.start()
    out_sum.finish()
    w_sum.finish()
    own_ref[...] = low_sum.total()
    low_sum.finish()
    gains_ref[...] = more_sum.total()


def finish(dq, dkv, cosine, sine, normed, w, x, gain, hidden_grad, out_w, gain_two, ident):
    rows, width = x.shape
    dp_size, ctx_size = lax.axis_size("dp"), lax.axis_size("ctx")
    cols, out_cols = w.shape[2], out_w.shape[2]
    few = width // dp_size // ctx_size
    low, high = jnp.bfloat16, jnp.float32
    return pl.pallas_call(
        finish_kernel,
        name="finish",
        in_specs=whole_vmem(11),
        out_specs=whole_vmem(3),
        out_shape=[
            jax.ShapeDtypeStruct((rows, width), low),
            jax.ShapeDtypeStruct((few, cols + out_cols), high),
            jax.ShapeDtypeStruct((8, width), high),
        ],
        scratch_shapes=[
            pltpu.VMEM((rows, cols), low),
            pltpu.VMEM((width, rows), low),
            pltpu.VMEM((rows, width), low),
            pltpu.VMEM((rows, width), low),
            pltpu.VMEM((dp_size, width // dp_size, cols), low),
            pltpu.VMEM((dp_size, width // dp_size, cols), low),
            pltpu.VMEM(out_w.shape, low),
            pltpu.VMEM((ctx_size, few, cols + out_cols), low),
            pltpu.VMEM((ctx_size, few, cols + out_cols), low),
            pltpu.VMEM((8, width), high),
            pltpu.VMEM((dp_size, 8, width), high),
            pltpu.VMEM((8, width), high),
            pltpu.VMEM((ctx_size, 8, width), high),
            *sem_pair(dp_size),
            *sem_pair(dp_size),
            *sem_pair(1),
            *sem_pair(dp_size),
            *sem_pair(ctx_size),
            *sem_pair(ctx_size),
        ],
        compiler_params=remote_params(ident),
    )(dq, dkv, cosine, sine, normed, w, x, gain, hidden_grad, out_w, gain_two)


class Everyone:
    def __init__(self, axis, target, sems):
        self.axis, self.target, self.sems = axis, target, sems
        self.size = lax.axis_size(axis)

    def copy(self, k):
        at = self.target.at[lax.axis_index(self.axis)]
        return remote(at, at, self.sems, k, {self.axis: ahead_on(self.axis, k)})

    def start(self):
        each(self.size, lambda k: self.copy(k).start())

    def arrive(self):
        each(self.size, lambda k: self.copy(k).wait_recv())

    def finish(self):
        each(self.size, lambda k: self.copy(k).wait_send())


def find_places(first, own, routes_ref, gates_ref, earlier, place_ref, gate_ref, column_ref):
    _, tokens = routes_ref.shape[1:]

    def group(g, carry):
        routes, gates = routes_ref[g], gates_ref[g]
        names, values = [], []
        for e in range(own):
            named = routes == first + e
            names.append(jnp.max(named.astype(jnp.float32), axis=0, keepdims=True))
            values.append(jnp.sum(jnp.where(named, gates, 0.0), axis=0, keepdims=True))
        spare = jnp.zeros((8 - own % 8 if own % 8 else 0, tokens), jnp.float32)
        names = jnp.concatenate(names + ([spare] if spare.shape[0] else []), axis=0)
        place = jnp.dot(
            names.astype(jnp.bfloat16), earlier[...], preferred_element_type=jnp.float32
        )
        place = jnp.where((names > 0.0) & (place < CAP), place, -float(CAP * own))
        for e in range(own):
            place_ref[g, e] = place[e : e + 1].astype(jnp.int32)
            gate_ref[g, e] = values[e]
        column_ref[g] = jnp.transpose(place)[:, :own].astype(jnp.int32)
        return carry

    lax.fori_loop(0, routes_ref.shape[0], group, 0)


def front_kernel(
    back, ahead, own, starts_ref, x_ref, cot_ref, q_w_ref, k_w_ref, v_w_ref, out_w_ref, gains_ref,
    docs_ref, routes_ref, gates_ref, cos_ref, sin_ref, w_all, out_w_all, gain_rows, docs_all,
    normed_ref, q_ref, kv_all, mix_ref, full_ref, log_ref, hidden_ref, rows_all, cot_all,
    place_ref, gate_ref, column_ref, gains_all, routes_all, gates_all, acc, top, total, column,
    part, held, normed_two, earlier, *sems,
):
    me, size = lax.axis_index("ctx"), lax.axis_size("ctx")
    dp = lax.axis_index("dp")
    pairs = [sems[2 * i : 2 * i + 2] for i in range(len(sems) // 2)]
    q_width, kv_width = q_w_ref.shape[1], k_w_ref.shape[1]
    dp_size, piece = w_all.shape[:2]
    w_all[dp, :, :q_width] = q_w_ref[...]
    w_all[dp, :, q_width : q_width + kv_width] = k_w_ref[...]
    w_all[dp, :, q_width + kv_width :] = v_w_ref[...]
    gains_all[dp] = gains_ref[...]
    docs_all[me] = docs_ref[...]
    routes_all[dp] = routes_ref[...]
    gates_all[dp] = gates_ref[...]
    out_w_all[dp] = out_w_ref[...]
    greet(["dp", "ctx", "tp"])
    gains = Everyone("dp", gains_all, pairs[0])
    weights = Everyone("dp", w_all, pairs[1])
    docs = Everyone("ctx", docs_all, pairs[2])
    routes = Everyone("dp", routes_all, pairs[3])
    gates = Everyone("dp", gates_all, pairs[4])
    out_w = Everyone("dp", out_w_all, pairs[5])
    for one in (gains, weights, docs, routes, gates):
        one.start()

    token = lax.broadcasted_iota(jnp.int32, earlier.shape, 0)
    later = lax.broadcasted_iota(jnp.int32, earlier.shape, 1)
    earlier[...] = (token < later).astype(jnp.float32).astype(jnp.bfloat16)
    top[...] = jnp.full(top.shape, NEG_FILL, jnp.float32)
    total[...] = jnp.zeros(total.shape, jnp.float32)
    acc[...] = jnp.zeros(acc.shape, jnp.float32)
    gains.arrive()
    for i in range(dp_size):
        gain_rows[:, i * piece : (i + 1) * piece] = gains_all[i]
    x = x_ref[...].astype(jnp.float32)
    normed_ref[...] = (x * row_scale(x) * gain_rows[0:1, :]).astype(jnp.bfloat16)
    routes.arrive()
    gates.arrive()
    docs.arrive()
    find_places(dp * own, own, routes_all, gates_all, earlier, place_ref, gate_ref, column_ref)
    weights.arrive()
    out_w.start()
    cot_rows = RowGather(cot_ref, cot_all, pairs[6], pairs[7], 0)
    cot_rows.start()

    wide, tile = 4 * HEAD_DIM, 2 * HEAD_DIM

    def project(first):
        whole = jnp.dot(
            normed_ref[:, :piece], w_all[0, :, first : first + wide],
            preferred_element_type=jnp.float32,
        )
        for i in range(1, dp_size):
            whole += jnp.dot(
                normed_ref[:, i * piece : (i + 1) * piece], w_all[i, :, first : first + wide],
                preferred_element_type=jnp.float32,
            )
        return [whole[:, :tile], whole[:, tile:]]

    for first in range(q_width, q_width + 2 * kv_width, wide):
        for i, part_of in enumerate(project(first)):
            if first < q_width + kv_width:
                part_of = turn(part_of, cos_ref[...], -sin_ref[...])
            at = first - q_width + i * tile
            kv_all[me, :, at : at + tile] = part_of.astype(jnp.bfloat16)

    right, left = me + 1, me - 1
    line = pairs[8]

    def hop(s):
        at = kv_all.at[lax.rem(me + size - s, size)]
        return remote(at, at, line, s, {"ctx": right})

    def back_hop():
        return remote(kv_all.at[me], kv_all.at[me], line, back, {"ctx": left})

    if back:

        @pl.when(right < size)
        def _():
            hop(0).start()

    if ahead:

        @pl.when(left >= 0)
        def _():
            back_hop().start()

    for first in range(0, q_width, wide):
        for i, part_of in enumerate(project(first)):
            turned = turn(part_of, cos_ref[...], -sin_ref[...]).astype(jnp.bfloat16)
            at = first + i * tile
            q_ref[:, at : at + tile] = (turned.astype(jnp.float32) * HEAD_DIM**-0.5).astype(
                jnp.bfloat16
            )
    masks = Masks(docs_all, starts_ref, column)

    def visit(s):
        @pl.when(me - s >= 0)
        def _():
            block = lax.rem(me + size - s, size)

            @pl.when(s > 0)
            def _():
                hop(s - 1).wait_recv()

            @pl.when((s > 0) & (s < back) & (right < size))
            def _():
                hop(s).start()

            attend_block(masks, block, q_ref, kv_all.at[block], acc, top, total)

    each(back + 1, visit, 0)
    if ahead:

        @pl.when(right < size)
        def _():
            block = lax.rem(me + 1, size)
            back_hop().wait_recv()
            attend_block(masks, block, q_ref, kv_all.at[block], acc, top, total)

    log_ref[...] = top[...] + jnp.log(total[...])
    for h in range(total.shape[0]):
        at = slice(h * HEAD_DIM, (h + 1) * HEAD_DIM)
        acc[at, :] = acc[at, :] / total[h : h + 1, :]
    full_ref[...] = jnp.transpose(acc[...])
    mix_ref[...] = full_ref[...].astype(jnp.bfloat16)
    out_w.arrive()
    for i in range(dp_size):
        part[:, i * piece : (i + 1) * piece] = jnp.dot(
            mix_ref[...], out_w_all[i], preferred_element_type=jnp.float32
        ).astype(jnp.bfloat16)

    mine, theirs = halves(part.shape[0])
    rows = RowGather(normed_two, rows_all, pairs[9], pairs[10], 1)
    first = remote(part.at[theirs], held.at[theirs], pairs[10], 0, other_core())
    second = remote(part.at[mine], held.at[mine], pairs[10], 1, other_core())
    first.start()
    second.start()

    def norm(at):
        whole = x_ref[at, :].astype(jnp.float32) + (
            part[at, :].astype(jnp.float32) + held[at, :].astype(jnp.float32)
        )
        hidden_ref[at, :] = whole
        normed_two[at, :] = (whole * row_scale(whole) * gain_rows[1:2, :]).astype(jnp.bfloat16)

    first.wait()
    norm(mine)
    rows.start()
    second.wait()
    norm(theirs)
    rows_all[dp] = normed_two[...]
    cot_all[dp] = cot_ref[...]
    cot_rows.forward()
    rows.forward()
    for one in (gains, weights, docs, routes, gates, out_w):
        one.finish()

    def sent(s):
        @pl.when((right < size) & (me - s >= 0))
        def _():
            hop(s).wait_send()

    each(back, sent, 0)
    if ahead:

        @pl.when(left >= 0)
        def _():
            back_hop().wait_send()

    cot_rows.finish()
    rows.finish()


def front(
    starts, x, cot, q_w, k_w, v_w, out_w, gains, docs, routes, gates, cosine, sine, own, back,
    ahead, ident,
):
    rows, width = x.shape
    dp_size, ctx_size = lax.axis_size("dp"), lax.axis_size("ctx")
    q_width, kv_cols = q_w.shape[1], 2 * k_w.shape[1]
    piece, heads = q_w.shape[0], q_width // HEAD_DIM
    low, high, whole = jnp.bfloat16, jnp.float32, jnp.int32
    shapes = [
        ((dp_size, piece, q_width + kv_cols), low),
        ((dp_size,) + out_w.shape, low),
        ((2, width), high),
        ((ctx_size, 1, rows), whole),
        ((rows, width), low),
        ((rows, q_width), low),
        ((ctx_size, rows, kv_cols), low),
        ((rows, q_width), low),
        ((rows, q_width), high),
        ((heads, rows), high),
        ((rows, width), high),
        ((dp_size, rows, width), low),
        ((dp_size, rows, width), low),
        ((dp_size, own, 1, rows), whole),
        ((dp_size, own, 1, rows), high),
        ((dp_size, rows, own), whole),
    ]
    return pl.pallas_call(
        functools.partial(front_kernel, back, ahead, own),
        name="front",
        in_specs=[pl.BlockSpec(memory_space=pltpu.SMEM)] + whole_vmem(12),
        out_specs=whole_vmem(len(shapes)),
        out_shape=[jax.ShapeDtypeStruct(*shape) for shape in shapes],
        scratch_shapes=[
            pltpu.VMEM((dp_size,) + gains.shape, high),
            pltpu.VMEM((dp_size,) + routes.shape, whole),
            pltpu.VMEM((dp_size,) + gates.shape, high),
            pltpu.VMEM((q_width, rows), high),
            pltpu.VMEM((heads, rows), high),
            pltpu.VMEM((heads, rows), high),
            pltpu.VMEM((rows, 8), whole),
            pltpu.VMEM((rows, width), low),
            pltpu.VMEM((rows, width), low),
            pltpu.VMEM((rows, width), low),
            pltpu.VMEM((rows, rows), low),
            *sem_pair(dp_size),
            *sem_pair(dp_size),
            *sem_pair(ctx_size),
            *sem_pair(dp_size),
            *sem_pair(dp_size),
            *sem_pair(dp_size),
            *sem_pair(dp_size),
            *sem_pair(dp_size),
            *sem_pair(back + 1),
            *sem_pair(dp_size),
            *sem_pair(dp_size + 1),
        ],
        compiler_params=remote_params(ident),
    )(starts, x, cot, q_w, k_w, v_w, out_w, gains, docs, routes, gates, cosine, sine)


GROUPS_AT_ONCE = 4


def experts_kernel(
    more, rows_ref, grads_ref, weights_ref, place_ref, gate_ref, place_col_ref, *refs
):
    before, refs = (refs[:2], refs[2:]) if more else (None, refs)
    out_ref, back_ref, weight_grad_ref, slots, slot_grads, outs, backs = refs
    e = pl.program_id(1)
    groups, tok_rows, _ = rows_ref.shape
    owners, part = weight_grad_ref.shape[1], weight_grad_ref.shape[5]
    slot_index = lax.broadcasted_iota(jnp.int32, (CAP, tok_rows), 0)
    gates = []
    for g in range(groups):
        picks = slot_index == place_ref[g, 0]
        gates.append(jnp.sum(jnp.where(picks, gate_ref[g, 0], 0.0), axis=1, keepdims=True))
        picks = picks.astype(jnp.float32).astype(jnp.bfloat16)
        at = slice(g * CAP, (g + 1) * CAP)
        slots[at, :] = jnp.dot(
            picks, rows_ref[g], preferred_element_type=jnp.float32
        ).astype(jnp.bfloat16)
        slot_grads[at, :] = (
            jnp.dot(picks, grads_ref[g], preferred_element_type=jnp.float32) * gates[g]
        ).astype(jnp.bfloat16)
    gate_w, up_w, down_w = (weights_ref.at[0, i] for i in range(3))
    gate_pre = jnp.dot(slots[...], gate_w[...], preferred_element_type=jnp.float32)
    up_pre = jnp.dot(slots[...], up_w[...], preferred_element_type=jnp.float32)
    act_grad = jnp.dot(slot_grads[...], down_w[...], preferred_element_type=jnp.float32)
    sig = 1.0 / (1.0 + jnp.exp(-gate_pre))
    silu = gate_pre * sig
    act_low = (silu * up_pre).astype(jnp.bfloat16)
    up_low = (act_grad * silu).astype(jnp.bfloat16)
    gate_low = (act_grad * up_pre * (sig * (1.0 + gate_pre * (1.0 - sig)))).astype(jnp.bfloat16)

    back = lax.dot_general(
        gate_low, gate_w[...], NT, preferred_element_type=jnp.float32
    ) + lax.dot_general(up_low, up_w[...], NT, preferred_element_type=jnp.float32)
    out = lax.dot_general(act_low, down_w[...], NT, preferred_element_type=jnp.float32)
    for g in range(groups):
        at = slice(g * CAP, (g + 1) * CAP)
        to = pl.ds(pl.multiple_of(e * CAP, CAP), CAP)
        backs[g, to, :] = back[at].astype(jnp.bfloat16)
        outs[g, to, :] = (out[at] * gates[g]).astype(jnp.bfloat16)

    for i, (low, source) in enumerate(
        ((gate_low, slots), (up_low, slots), (act_low, slot_grads))
    ):
        turned = jnp.transpose(low.astype(jnp.float32)).astype(jnp.bfloat16)
        total = jnp.dot(turned, source[...], preferred_element_type=jnp.float32)
        for c in range(owners):
            weight_grad_ref[0, c, 0, i] = total[:, c * part : (c + 1) * part].astype(
                weight_grad_ref.dtype
            )

    @pl.when(e == pl.num_programs(1) - 1)
    def _():
        slot_count = outs.shape[1]
        for g in range(groups):
            tiles = []
            for first in range(0, slot_count, 128):
                wide = min(128, slot_count - first)
                lane = first + lax.broadcasted_iota(jnp.int32, (tok_rows, wide), 1)
                hit = None
                for n in range(first // CAP, (first + wide - 1) // CAP + 1):
                    one = place_col_ref[g, :, n : n + 1] == lane - n * CAP
                    hit = one if hit is None else hit | one
                tiles.append(hit.astype(jnp.float32).astype(jnp.bfloat16))
            spread_picks = jnp.concatenate(tiles, axis=1)
            for i, (to_ref, source) in enumerate(((back_ref, backs), (out_ref, outs))):
                total = jnp.dot(spread_picks, source[g], preferred_element_type=jnp.float32)
                if more:
                    total += before[1 - i][g].astype(jnp.float32)
                to_ref[g] = total.astype(jnp.bfloat16)


def experts(weights, places, rows_all, grad_all, first, count, before):
    _, _, model_width, hidden = weights.shape
    place_rows, gate_rows, place_cols = places
    groups, tok_rows, _ = rows_all.shape
    owners = lax.axis_size("ctx")
    at_once = min(GROUPS_AT_ONCE, groups)
    chunks = groups // at_once
    part = model_width // owners
    rows_spec = pl.BlockSpec(
        (at_once, tok_rows, model_width), lambda c, e: (c, 0, 0), pipeline_mode=pl.Buffered(1)
    )
    line_spec = pl.BlockSpec((at_once, 1, 1, tok_rows), lambda c, e: (c, e + first, 0, 0))
    out_shape = jax.ShapeDtypeStruct(rows_all.shape, jnp.bfloat16)
    flops = count * groups * CAP * model_width * 2 * (9 * hidden + 4 * tok_rows)
    more = before is not None
    out_part, back_part, weight_part = pl.pallas_call(
        functools.partial(experts_kernel, more),
        name="experts",
        grid=(chunks, count),
        in_specs=[
            rows_spec,
            rows_spec,
            pl.BlockSpec((1, 3, model_width, hidden), lambda c, e: (e + first, 0, 0, 0)),
            line_spec,
            line_spec,
            pl.BlockSpec((at_once, tok_rows, count), lambda c, e: (c, 0, 0)),
        ]
        + [rows_spec] * (2 * more),
        out_specs=[
            rows_spec,
            rows_spec,
            pl.BlockSpec((1, owners, 1, 3, hidden, part), lambda c, e: (c, 0, e, 0, 0, 0)),
        ],
        out_shape=[
            out_shape,
            out_shape,
            jax.ShapeDtypeStruct((chunks, owners, count, 3, hidden, part), jnp.bfloat16),
        ],
        scratch_shapes=[
            pltpu.VMEM((at_once * CAP, model_width), jnp.bfloat16),
            pltpu.VMEM((at_once * CAP, model_width), jnp.bfloat16),
            pltpu.VMEM((at_once, count * CAP, model_width), jnp.bfloat16),
            pltpu.VMEM((at_once, count * CAP, model_width), jnp.bfloat16),
        ],
        compiler_params=pltpu.CompilerParams(vmem_limit_bytes=LIMIT),
        cost_estimate=pl.CostEstimate(
            flops=flops, bytes_accessed=4 * weights.size, transcendentals=0
        ),
    )(
        rows_all,
        grad_all,
        weights,
        place_rows,
        gate_rows,
        place_cols[:, :, first : first + count],
        *(before if more else ()),
    )
    if chunks == 1:
        return (out_part, back_part), weight_part[0]
    return (out_part, back_part), jnp.sum(weight_part.astype(jnp.float32), axis=0).astype(
        jnp.bfloat16
    )


def rotary_tables(token_positions):
    half_dim = HEAD_DIM // 2
    inverse = THETA ** (-(jnp.arange(half_dim, dtype=jnp.float32) * 2.0 / HEAD_DIM))
    angles = token_positions.astype(jnp.float32)[:, None] * inverse[None, :]
    cosine, sine = jnp.cos(angles), jnp.sin(angles)
    return jnp.concatenate([cosine] * 4, axis=1), jnp.concatenate([sine, -sine] * 2, axis=1)


def body(
    tokens,
    query_weight,
    key_weight,
    value_weight,
    output_weight,
    gain_attn,
    gain_moe,
    expert_weights,
    routes,
    gate_values,
    documents,
    pic_starts,
    cotangent,
):
    block_len = tokens.shape[1]
    ctx_size = lax.axis_size("ctx")
    length = block_len * ctx_size
    offset = lax.axis_index("ctx") * block_len
    back = back_blocks(ctx_size, block_len, length)
    ahead = ahead_blocks(block_len, length, pic_starts.shape[1])
    q_width, kv_width = query_weight.shape[1], key_weight.shape[1]
    own = expert_weights.shape[0]
    x, cot = tokens[0], cotangent[0]

    cosine, sine = rotary_tables(offset + jnp.arange(block_len, dtype=jnp.int32))
    (
        w_all,
        out_w_all,
        gain_rows,
        docs_all,
        normed_one,
        query,
        kv_all,
        mixture,
        mix_full,
        log_total,
        hidden,
        rows_all,
        grad_all,
        *places,
    ) = front(
        pic_starts,
        x,
        cot,
        query_weight,
        key_weight,
        value_weight,
        output_weight,
        jnp.stack([gain_attn, gain_moe]).astype(jnp.float32),
        documents,
        routes[0].T,
        gate_values[0].T,
        cosine,
        sine,
        own,
        back,
        ahead,
        1,
    )
    half = own // 2
    parts, grads_one = experts(expert_weights, places, rows_all, grad_all, 0, half, None)
    expert_one = lax.psum_scatter(grads_one, "ctx", scatter_dimension=0)
    (out_part, back_part), grads_two = experts(
        expert_weights, places, rows_all, grad_all, half, own - half, parts
    )
    hidden_grad, hidden_low, mix_grad, gain_two_grad = return_grads(
        back_part, hidden, cot, gain_rows, out_w_all, 2
    )
    q_rot_grad, kv_part = attend_back(
        pic_starts, query, kv_all, docs_all, log_total, mix_full, mix_grad, back, ahead
    )
    kv_back, layer_out, output_grad = trade(
        kv_part,
        out_part,
        hidden,
        hidden_low,
        mixture,
        back,
        ahead,
        3,
    )
    grads_two, kv_back = lax.optimization_barrier((grads_two, kv_back))
    expert_two = lax.psum_scatter(grads_two, "ctx", scatter_dimension=0)
    input_grad, owned, gain_sums = finish(
        q_rot_grad,
        kv_back,
        cosine,
        sine,
        normed_one,
        w_all,
        x,
        gain_rows,
        hidden_grad,
        output_grad,
        gain_two_grad,
        4,
    )
    few = owned.shape[0]
    here = (lax.axis_index("dp") * ctx_size + lax.axis_index("ctx")) * few
    gain_sums = lax.dynamic_slice_in_dim(gain_sums, here, few, 1)
    expert_grad = jnp.concatenate([expert_one, expert_two], axis=0)
    v_end = q_width + 2 * kv_width
    return (
        layer_out[None],
        input_grad[None],
        owned[:, :q_width],
        owned[:, q_width : q_width + kv_width],
        owned[:, q_width + kv_width : v_end],
        owned[:, v_end:].T,
        gain_sums[0],
        gain_sums[1],
        expert_grad.astype(jnp.float32).transpose(0, 1, 3, 2),
    )


def solution(mesh):
    return jax.shard_map(
        body,
        mesh=mesh,
        in_specs=(
            P("dp", "ctx", None),
            P("dp", "tp"),
            P("dp", "tp"),
            P("dp", "tp"),
            P("tp", "dp"),
            P("dp"),
            P("dp"),
            P("dp", None, None, "tp"),
            P("dp", "ctx", None),
            P("dp", "ctx", None),
            P("dp", "ctx"),
            P("dp", None),
            P("dp", "ctx", None),
        ),
        out_specs=(
            P("dp", "ctx", None),
            P("dp", "ctx", None),
            P(("dp", "ctx"), "tp"),
            P(("dp", "ctx"), "tp"),
            P(("dp", "ctx"), "tp"),
            P("tp", ("dp", "ctx")),
            P(("dp", "ctx")),
            P(("dp", "ctx")),
            P("dp", None, "ctx", "tp"),
        ),
        check_vma=False,
    )
```

```python
import functools

import jax
import jax.numpy as jnp
from jax import lax
from jax.experimental import pallas as pl
from jax.experimental.pallas import tpu as pltpu
from jax.sharding import PartitionSpec as P

HEAD_DIM = 64
PIC = 256
CAP = 144

EPSILON = 1e-06
THETA = 10000.0
NEG_FILL = -1e30


KEY_ROWS = 256
NT = (((1,), (1,)), ((), ()))
LIMIT = 67043328


def whole_vmem(count):
    return [pl.BlockSpec(memory_space=pltpu.VMEM)] * count


def picture_ids(starts_ref, places):
    ids = jnp.full(places.shape, -1, jnp.int32)
    for j in range(starts_ref.shape[1]):
        start = starts_ref[0, j]
        ids += jnp.where((places >= start) & (places < start + PIC), j + 1, 0)
    return ids


def as_column(row):
    tall = jnp.broadcast_to(row.astype(jnp.float32), (8, row.shape[1]))
    return jnp.transpose(tall)[:, 0:1].astype(jnp.int32)


class Masks:
    def __init__(self, docs_ref, starts_ref, column):
        self.docs_ref, self.starts_ref, self.column = docs_ref, starts_ref, column
        self.rows = docs_ref.shape[2]
        me = lax.axis_index("ctx")
        self.q_doc = docs_ref[me]
        self.q_place = me * self.rows + lax.broadcasted_iota(jnp.int32, (1, self.rows), 1)
        self.q_pic = picture_ids(starts_ref, self.q_place)

    def open(self, block):
        self.column[...] = jnp.broadcast_to(
            as_column(self.docs_ref[block]), self.column.shape
        )

    def bias(self, block, rows, first):
        k_doc = self.column[rows, 0:1]
        k_place = block * self.rows + first + lax.broadcasted_iota(jnp.int32, k_doc.shape, 0)
        k_pic = picture_ids(self.starts_ref, k_place)
        seen = (k_doc == self.q_doc) & (
            (k_place <= self.q_place) | ((k_pic == self.q_pic) & (self.q_pic >= 0))
        )
        return jnp.where(seen, 0.0, NEG_FILL)


def attend_block(masks, block, q_ref, kv_ref, acc, top, total):
    kv_width = kv_ref.shape[1] // 2
    heads, kv_heads = q_ref.shape[1] // HEAD_DIM, kv_width // HEAD_DIM
    masks.open(block)

    def step(j, carry):
        first = pl.multiple_of(j * KEY_ROWS, KEY_ROWS)
        rows = pl.ds(first, KEY_ROWS)
        bias = masks.bias(block, rows, first)
        for g in range(kv_heads):
            key = kv_ref[rows, g * HEAD_DIM : (g + 1) * HEAD_DIM]
            val = kv_ref[rows, kv_width + g * HEAD_DIM : kv_width + (g + 1) * HEAD_DIM]
            val_t = jnp.transpose(val.astype(jnp.float32)).astype(jnp.bfloat16)
            for h in range(g * heads // kv_heads, (g + 1) * heads // kv_heads):
                at = slice(h * HEAD_DIM, (h + 1) * HEAD_DIM)
                scores = bias + lax.dot_general(
                    key, q_ref[:, at], NT, preferred_element_type=jnp.float32
                )
                old = top[h : h + 1, :]
                new = jnp.maximum(old, jnp.max(scores, axis=0, keepdims=True))
                probs = jnp.exp(scores - new)
                fade = jnp.exp(old - new)
                total[h : h + 1, :] = total[h : h + 1, :] * fade + jnp.sum(
                    probs, axis=0, keepdims=True
                )
                acc[at, :] = acc[at, :] * fade + jnp.dot(
                    val_t, probs.astype(jnp.bfloat16), preferred_element_type=jnp.float32
                )
                top[h : h + 1, :] = new
        return carry

    lax.fori_loop(0, kv_ref.shape[0] // KEY_ROWS, step, 0)


def attend_back_block(
    masks, edges, block, q_ref, kv_ref, log_ref, delta, grad_ref, acc, dkv_ref
):
    kv_width = kv_ref.shape[1] // 2
    heads, kv_heads = q_ref.shape[1] // HEAD_DIM, kv_width // HEAD_DIM
    masks.open(block)
    count = kv_ref.shape[0] // KEY_ROWS
    me = lax.axis_index("ctx")
    q_first, q_last = edges[me * count, 0], edges[me * count + count - 1, 1]

    def step(j, carry):
        at = block * count + j
        same = (edges[at, 0] <= q_last) & (edges[at, 1] >= q_first)

        @pl.when(same)
        def _():
            inside(j)

        @pl.when(jnp.logical_not(same))
        def _():
            rows = pl.ds(pl.multiple_of(j * KEY_ROWS, KEY_ROWS), KEY_ROWS)
            dkv_ref[rows, :] = jnp.zeros((KEY_ROWS, dkv_ref.shape[1]), dkv_ref.dtype)

        return carry

    def inside(j):
        first = pl.multiple_of(j * KEY_ROWS, KEY_ROWS)
        rows = pl.ds(first, KEY_ROWS)
        bias = masks.bias(block, rows, first)
        for g in range(kv_heads):
            k_at = slice(g * HEAD_DIM, (g + 1) * HEAD_DIM)
            v_at = slice(kv_width + g * HEAD_DIM, kv_width + (g + 1) * HEAD_DIM)
            key, val = kv_ref[rows, k_at], kv_ref[rows, v_at]
            key_t = jnp.transpose(key.astype(jnp.float32)).astype(jnp.bfloat16)
            dk = jnp.zeros((KEY_ROWS, HEAD_DIM), jnp.float32)
            dv = jnp.zeros((KEY_ROWS, HEAD_DIM), jnp.float32)
            for h in range(g * heads // kv_heads, (g + 1) * heads // kv_heads):
                at = slice(h * HEAD_DIM, (h + 1) * HEAD_DIM)
                q_rows, g_rows = q_ref[:, at], grad_ref[:, at]
                scores = bias + lax.dot_general(
                    key, q_rows, NT, preferred_element_type=jnp.float32
                )
                probs = jnp.exp(scores - log_ref[h : h + 1, :])
                prob_grad = lax.dot_general(val, g_rows, NT, preferred_element_type=jnp.float32)
                slope = (probs * (prob_grad - delta[h : h + 1, :])).astype(jnp.bfloat16)
                dv += jnp.dot(
                    probs.astype(jnp.bfloat16), g_rows, preferred_element_type=jnp.float32
                )
                dk += jnp.dot(slope, q_rows, preferred_element_type=jnp.float32)
                acc[at, :] += jnp.dot(key_t, slope, preferred_element_type=jnp.float32)
            dkv_ref[rows, k_at] = dk.astype(dkv_ref.dtype)
            dkv_ref[rows, v_at] = dv.astype(dkv_ref.dtype)

    lax.fori_loop(0, count, step, 0)


def attend_back_kernel(
    back, ahead, starts_ref, edges, q_ref, kv_ref, docs_ref, log_ref, full_ref, grad_ref, dq_ref,
    dkv_ref, acc, delta, column,
):
    me, size = lax.axis_index("ctx"), lax.axis_size("ctx")
    acc[...] = jnp.transpose(full_ref[...] * grad_ref[...].astype(jnp.float32))
    for h in range(delta.shape[0]):
        delta[h : h + 1, :] = jnp.sum(
            acc[h * HEAD_DIM : (h + 1) * HEAD_DIM, :], axis=0, keepdims=True
        )
    acc[...] = jnp.zeros(acc.shape, jnp.float32)
    masks = Masks(docs_ref, starts_ref, column)

    def step(s, carry):
        block = me + ahead - s

        @pl.when((block >= 0) & (block < size))
        def _():
            attend_back_block(
                masks, edges, block, q_ref, kv_ref.at[block], log_ref, delta, grad_ref, acc,
                dkv_ref.at[block],
            )

        return carry

    lax.fori_loop(0, back + ahead + 1, step, 0)
    dq_ref[...] = jnp.transpose(acc[...]) * (HEAD_DIM**-0.5)


def attend_back(starts, q, kv, docs, log_total, full, grad, back, ahead):
    rows, width = q.shape
    by_block = docs.reshape(-1, KEY_ROWS)
    edges = jnp.concatenate([by_block[:, :1], by_block[:, -1:]], axis=1)
    return pl.pallas_call(
        functools.partial(attend_back_kernel, back, ahead),
        name="attend_back",
        in_specs=[pl.BlockSpec(memory_space=pltpu.SMEM)] * 2 + whole_vmem(6),
        out_specs=whole_vmem(2),
        out_shape=[
            jax.ShapeDtypeStruct((rows, width), jnp.float32),
            jax.ShapeDtypeStruct(kv.shape, jnp.bfloat16),
        ],
        scratch_shapes=[
            pltpu.VMEM((width, rows), jnp.float32),
            pltpu.VMEM((width // HEAD_DIM, rows), jnp.float32),
            pltpu.VMEM((rows, 8), jnp.int32),
        ],
        compiler_params=pltpu.CompilerParams(vmem_limit_bytes=LIMIT),
    )(starts, edges, q, kv, docs, log_total, full, grad)


MESH = pl.DeviceIdType.MESH


def greet(axes_list, line=False):
    barrier = pltpu.get_barrier_semaphore()
    count = 0
    for axis in axes_list:
        me, size = lax.axis_index(axis), lax.axis_size(axis)

        def signal(k, carry, axis=axis, me=me, size=size):
            pl.semaphore_signal(
                barrier, inc=1, device_id={axis: lax.rem(me + k, size)}, device_id_type=MESH
            )
            return carry

        lax.fori_loop(1, size, signal, 0)
        count += size - 1
    if not line:
        pl.semaphore_wait(barrier, count)
        return
    me, size = lax.axis_index("ctx"), lax.axis_size("ctx")
    for step in (1, -1):
        other = me + step

        @pl.when((other >= 0) & (other < size))
        def _(other=other):
            pl.semaphore_signal(barrier, inc=1, device_id={"ctx": other}, device_id_type=MESH)

    inner = (me > 0) & (me < size - 1)

    @pl.when(inner)
    def _():
        pl.semaphore_wait(barrier, count + 2)

    @pl.when(jnp.logical_not(inner))
    def _():
        pl.semaphore_wait(barrier, count + 1)


def remote(src, dst, sems, k, device_id):
    return pltpu.make_async_remote_copy(
        src_ref=src,
        dst_ref=dst,
        send_sem=sems[0].at[k],
        recv_sem=sems[1].at[k],
        device_id=device_id,
        device_id_type=MESH,
    )


def other_core():
    return {"tp": 1 - lax.axis_index("tp")}


def ahead_on(axis, k):
    return lax.rem(lax.axis_index(axis) + k, lax.axis_size(axis))


def each(count, do, first=1):
    def step(k, carry):
        do(k)
        return carry

    lax.fori_loop(first, count, step, 0)


def sem_pair(count):
    return [pltpu.SemaphoreType.DMA((count,)), pltpu.SemaphoreType.DMA((count,))]


def remote_params(ident):
    return pltpu.CompilerParams(
        collective_id=ident, has_side_effects=True, vmem_limit_bytes=LIMIT
    )


def halves(rows):
    half = rows // 2
    core = lax.axis_index("tp")
    return (
        pl.ds(pl.multiple_of(core * half, half), half),
        pl.ds(pl.multiple_of((1 - core) * half, half), half),
    )


def turn(tile, cosine, sine):
    lane = lax.broadcasted_iota(jnp.int32, tile.shape, 1)
    half = HEAD_DIM // 2
    swapped = jnp.where(
        lax.rem(lane, HEAD_DIM) < half,
        pltpu.roll(tile, 2 * HEAD_DIM - half, 1),
        pltpu.roll(tile, half, 1),
    )
    return tile * cosine + swapped * sine


def row_scale(x):
    return lax.rsqrt(jnp.mean(x * x, axis=-1, keepdims=True) + EPSILON)


def norm_back(x, gain, grad):
    scale = row_scale(x)
    unit = x * scale
    pull = grad * gain
    return (
        scale * (pull - unit * jnp.mean(pull * unit, axis=-1, keepdims=True)),
        jnp.sum(grad * unit, axis=0, keepdims=True),
    )


def back_blocks(ctx_size, block_len, length):
    return min(ctx_size - 1, -(-(length // 2 - 1) // block_len))


def ahead_blocks(block_len, length, spans):
    return 0 if block_len % (length // spans) == 0 else 1


class RowGather:
    def __init__(self, source, target, dp_sems, tp_sems, first):
        self.source, self.target = source, target
        self.dp_sems, self.tp_sems, self.first = dp_sems, tp_sems, first
        self.mine, _ = halves(source.shape[0])
        self.size = lax.axis_size("dp")

    def copy(self, k):
        at = self.target.at[lax.axis_index("dp"), self.mine]
        return remote(
            self.source.at[self.mine], at, self.dp_sems, k, {"dp": ahead_on("dp", k)}
        )

    def relay(self, k):
        at = self.target.at[ahead_on("dp", self.size - k), self.mine]
        return remote(at, at, self.tp_sems, self.first + k, other_core())

    def start(self):
        each(self.size, lambda k: self.copy(k).start())

    def forward(self):
        def one(k):
            self.copy(k).wait_recv()
            self.relay(k).start()

        each(self.size, one)

    def finish(self):
        def one(k):
            self.copy(k).wait_send()
            self.relay(k).wait()

        each(self.size, one)


def collect(places_ref, slots_ref, group):
    tok_rows, slot_count = places_ref.shape[1], slots_ref.shape[1]
    tiles = []
    for first in range(0, slot_count, 128):
        wide = min(128, slot_count - first)
        lane = first + lax.broadcasted_iota(jnp.int32, (tok_rows, wide), 1)
        hit = None
        for n in range(first // CAP, (first + wide - 1) // CAP + 1):
            one = places_ref[group, :, n : n + 1] == lane - n * CAP
            hit = one if hit is None else hit | one
        tiles.append(hit.astype(jnp.float32).astype(jnp.bfloat16))
    return jnp.dot(
        jnp.concatenate(tiles, axis=1), slots_ref[group], preferred_element_type=jnp.float32
    )


class RowReturn:
    def __init__(self, part, held, landed, total, sent, came, dp_sems, tp_sems):
        self.part, self.held, self.landed, self.total = part, held, landed, total
        self.sent, self.came, self.dp_sems, self.tp_sems = sent, came, dp_sems, tp_sems
        self.size = lax.axis_size("dp")
        self.mine, self.theirs = halves(part.shape[1])

    def swap(self, k):
        group = ahead_on("dp", k)
        return remote(
            self.part.at[group, self.theirs], self.held.at[k], self.tp_sems, k, other_core()
        )

    def copy(self, k):
        return remote(
            self.held.at[k], self.landed.at[k - 1], self.dp_sems, k, {"dp": ahead_on("dp", k)}
        )

    def last(self):
        return remote(self.sent, self.came, self.tp_sems, self.size, other_core())

    def both(self, k):
        group = ahead_on("dp", k)
        return self.part[group, self.mine].astype(jnp.float32) + self.held[k].astype(jnp.float32)

    def start(self, places_ref, slots_ref):
        def one(k):
            group = ahead_on("dp", k)
            self.part[group] = collect(places_ref, slots_ref, group).astype(jnp.bfloat16)
            self.swap(lax.rem(k, self.size)).start()

        each(self.size + 1, one)

    def forward(self):
        def one(k):
            self.swap(k).wait_recv()
            self.held[k] = self.both(k).astype(jnp.bfloat16)
            self.copy(k).start()

        each(self.size, one)
        self.swap(0).wait()
        self.total[...] = self.both(0)

    def gather(self):
        def one(k):
            self.copy(k).wait_recv()
            self.total[...] += self.landed[k - 1].astype(jnp.float32)

        each(self.size, one)
        self.sent[...] = self.total[...].astype(jnp.bfloat16)
        self.last().start()

    def finish(self):
        def one(k):
            self.swap(k).wait_send()
            self.copy(k).wait_send()

        each(self.size, one)
        self.last().wait()


def return_scratch(size, rows, width):
    low = jnp.bfloat16
    return [
        pltpu.VMEM((size, rows, width), low),
        pltpu.VMEM((size, rows // 2, width), low),
        pltpu.VMEM((size - 1, rows // 2, width), low),
        pltpu.VMEM((rows // 2, width), jnp.float32),
        pltpu.VMEM((rows // 2, width), low),
        pltpu.VMEM((rows // 2, width), low),
        *sem_pair(size),
        *sem_pair(size + 1),
    ]


def return_grads_kernel(
    slots_ref, places_ref, hidden_ref, cot_ref, gain_ref, out_w_ref, grad_ref, low_ref, mix_ref,
    gain_grad_ref, part, held, landed, total, sent, came, dp_send, dp_recv, tp_send, tp_recv,
):
    greet(["dp", "tp"])
    rows = RowReturn(
        part, held, landed, total, sent, came, (dp_send, dp_recv), (tp_send, tp_recv)
    )
    rows.start(places_ref, slots_ref)
    rows.forward()
    rows.gather()

    def turn_back(at, grads):
        x_grad, gain_grad = norm_back(
            hidden_ref[at, :], gain_ref[1:2, :], grads.astype(jnp.float32)
        )
        hidden_grad = cot_ref[at, :].astype(jnp.float32) + x_grad
        grad_ref[at, :] = hidden_grad
        low_ref[at, :] = hidden_grad.astype(jnp.bfloat16)
        piece = out_w_ref.shape[2]
        mix = None
        for i in range(out_w_ref.shape[0]):
            one = lax.dot_general(
                low_ref[at, i * piece : (i + 1) * piece],
                out_w_ref[i],
                NT,
                preferred_element_type=jnp.float32,
            )
            mix = one if mix is None else mix + one
        mix_ref[at, :] = mix.astype(jnp.bfloat16)
        return gain_grad

    gain_mine = turn_back(rows.mine, sent[...])
    rows.finish()
    gain_theirs = turn_back(rows.theirs, came[...])
    gain_grad_ref[...] = gain_mine + gain_theirs


def return_grads(slots, places, hidden, cot, gain, out_w, ident):
    size, (rows, width) = slots.shape[0], hidden.shape
    return pl.pallas_call(
        return_grads_kernel,
        name="return_grads",
        in_specs=whole_vmem(6),
        out_specs=whole_vmem(4),
        out_shape=[
            jax.ShapeDtypeStruct((rows, width), jnp.float32),
            jax.ShapeDtypeStruct((rows, width), jnp.bfloat16),
            jax.ShapeDtypeStruct((rows, out_w.shape[1]), jnp.bfloat16),
            jax.ShapeDtypeStruct((1, width), jnp.float32),
        ],
        scratch_shapes=return_scratch(size, rows, width),
        compiler_params=remote_params(ident),
    )(slots, places, hidden, cot, gain, out_w)


def trade_kernel(
    back, ahead, kv_grad_ref, slots_ref, places_ref, hidden_ref, low_ref, mix_ref, kv_ref, out_ref,
    out_w_ref, going, came_kv, line_send, line_recv, part, held, landed, total, sent, came, dp_send, dp_recv,
    tp_send, tp_recv,
):
    me, size = lax.axis_index("ctx"), lax.axis_size("ctx")
    greet(["dp", "tp"], line=True)
    right, left = me + 1, me - 1
    sems = (line_send, line_recv)

    def hop(s, src):
        return remote(src, came_kv.at[s], sems, s, {"ctx": left})

    def forth():
        return remote(
            kv_grad_ref.at[lax.rem(me + 1, size)], came_kv.at[0], sems, 0, {"ctx": right}
        )

    def own_piece(s):
        return kv_grad_ref.at[lax.rem(me + size - s, size)]

    if ahead:

        @pl.when(right < size)
        def _():
            forth().start()

    @pl.when(me - back >= 0)
    def _():
        hop(back, own_piece(back)).start()

    rows = RowReturn(
        part, held, landed, total, sent, came, (dp_send, dp_recv), (tp_send, tp_recv)
    )
    rows.start(places_ref, slots_ref)
    rows.forward()
    turned = jnp.transpose(low_ref[...].astype(jnp.float32)).astype(jnp.bfloat16)
    grad = jnp.dot(turned, mix_ref[...], preferred_element_type=jnp.float32)
    piece = out_w_ref.shape[1]
    for i in range(out_w_ref.shape[0]):
        out_w_ref[i] = grad[i * piece : (i + 1) * piece].astype(jnp.bfloat16)

    for s in range(back - 1, 0, -1):

        @pl.when((me - s >= 0) & (right < size))
        def _(s=s):
            hop(s + 1, going.at[s]).wait_recv()
            going[s] = (
                own_piece(s)[...].astype(jnp.float32) + came_kv[s + 1].astype(jnp.float32)
            ).astype(going.dtype)
            hop(s, going.at[s]).start()

        @pl.when((me - s >= 0) & (right >= size))
        def _(s=s):
            hop(s, own_piece(s)).start()

    rows.gather()
    kv_ref[...] = kv_grad_ref[me].astype(jnp.float32)

    @pl.when(right < size)
    def _():
        hop(1, going.at[0]).wait_recv()
        kv_ref[...] += came_kv[1].astype(jnp.float32)

    if ahead:

        @pl.when(left >= 0)
        def _():
            forth().wait_recv()
            kv_ref[...] += came_kv[0].astype(jnp.float32)

        @pl.when(right < size)
        def _():
            forth().wait_send()

    for s in range(back, 0, -1):

        @pl.when(me - s >= 0)
        def _(s=s):
            hop(s, going.at[0]).wait_send()

    rows.finish()
    mine, theirs = rows.mine, rows.theirs
    out_ref[mine, :] = (hidden_ref[mine, :] + sent[...].astype(jnp.float32)).astype(jnp.bfloat16)
    out_ref[theirs, :] = (hidden_ref[theirs, :] + came[...].astype(jnp.float32)).astype(
        jnp.bfloat16
    )


def trade(kv_grad, slots, places, hidden, low, mix, back, ahead, ident):
    size, (rows, width) = slots.shape[0], hidden.shape
    kv_shape = kv_grad.shape[1:]
    going = pltpu.VMEM((max(back, 1),) + kv_shape, kv_grad.dtype)
    came = pltpu.VMEM((back + 1,) + kv_shape, kv_grad.dtype)
    return pl.pallas_call(
        functools.partial(trade_kernel, back, ahead),
        name="trade",
        in_specs=whole_vmem(6),
        out_specs=whole_vmem(3),
        out_shape=[
            jax.ShapeDtypeStruct(kv_shape, jnp.float32),
            jax.ShapeDtypeStruct((rows, width), jnp.bfloat16),
            jax.ShapeDtypeStruct((size, width // size, mix.shape[1]), jnp.bfloat16),
        ],
        scratch_shapes=[
            going, came, *sem_pair(back + 1), *return_scratch(size, rows, width)
        ],
        compiler_params=remote_params(ident),
    )(kv_grad, slots, places, hidden, low, mix)


class PieceSum:
    def __init__(self, axis, source, landed, sems):
        self.axis, self.source, self.landed, self.sems = axis, source, landed, sems
        self.size = lax.axis_size(axis)

    def copy(self, k):
        peer = ahead_on(self.axis, k)
        return remote(
            self.source.at[peer], self.landed.at[k], self.sems, k, {self.axis: peer}
        )

    def send(self, k):
        self.copy(k).start()

    def total(self):
        each(self.size, lambda k: self.copy(k).wait_recv())
        whole = self.source[lax.axis_index(self.axis)].astype(jnp.float32)
        for k in range(1, self.size):
            whole += self.landed[k].astype(jnp.float32)
        return whole

    def finish(self):
        each(self.size, lambda k: self.copy(k).wait_send())


class WholeSum:
    def __init__(self, axis, source, landed, sems):
        self.axis, self.source, self.landed, self.sems = axis, source, landed, sems
        self.size = lax.axis_size(axis)

    def copy(self, k):
        return remote(
            self.source, self.landed.at[k], self.sems, k, {self.axis: ahead_on(self.axis, k)}
        )

    def start(self):
        each(self.size, lambda k: self.copy(k).start())

    def total(self):
        each(self.size, lambda k: self.copy(k).wait())
        whole = self.source[...]
        for k in range(1, self.size):
            whole += self.landed[k]
        return whole


def finish_kernel(
    dq_ref, dkv_ref, cos_ref, sin_ref, normed_ref, w_ref, x_ref, gain_ref, hidden_ref, out_w_ref,
    gain_two_ref, in_ref, own_ref, gains_ref, joined, turned, part, held, pieces, landed,
    out_landed, low, low_landed, gain_rows, gain_landed, gain_more, gain_more_landed, *sems,
):
    greet(["dp", "ctx", "tp"])
    pairs = [sems[2 * i : 2 * i + 2] for i in range(len(sems) // 2)]
    out_sum = PieceSum("dp", out_w_ref, out_landed, pairs[0])
    each(out_sum.size, out_sum.send)
    wide = 2 * HEAD_DIM
    q_width, kv_width = dq_ref.shape[1], dkv_ref.shape[1] // 2
    for first in range(0, q_width, wide):
        joined[:, first : first + wide] = turn(
            dq_ref[:, first : first + wide], cos_ref[...], sin_ref[...]
        ).astype(jnp.bfloat16)
    for first in range(0, kv_width, wide):
        joined[:, q_width + first : q_width + first + wide] = turn(
            dkv_ref[:, first : first + wide], cos_ref[...], sin_ref[...]
        ).astype(jnp.bfloat16)
    joined[:, q_width + kv_width :] = dkv_ref[:, kv_width:].astype(jnp.bfloat16)

    turned[...] = jnp.transpose(normed_ref[...].astype(jnp.float32)).astype(jnp.bfloat16)
    w_sum = PieceSum("dp", pieces, landed, pairs[1])
    rows = pieces.shape[1]

    def piece(k):
        peer = ahead_on("dp", k)
        at = pl.ds(pl.multiple_of(peer * rows, rows), rows)
        pieces[peer] = jnp.dot(
            turned[at, :], joined[...], preferred_element_type=jnp.float32
        ).astype(jnp.bfloat16)
        w_sum.send(k)

    each(w_sum.size, piece)
    for i in range(w_ref.shape[0]):
        part[:, i * rows : (i + 1) * rows] = lax.dot_general(
            joined[...], w_ref[i], NT, preferred_element_type=jnp.float32
        ).astype(jnp.bfloat16)
    swap = remote(part, held, pairs[2], 0, other_core())
    swap.start()
    me = lax.axis_index("dp")
    own = pl.ds(pl.multiple_of(me * rows, rows), rows)
    pieces[me] = jnp.dot(
        turned[own, :], joined[...], preferred_element_type=jnp.float32
    ).astype(jnp.bfloat16)
    swap.wait()
    x_grad, gain_grad = norm_back(
        x_ref[...].astype(jnp.float32),
        gain_ref[0:1, :],
        part[...].astype(jnp.float32) + held[...].astype(jnp.float32),
    )
    in_ref[...] = (hidden_ref[...] + x_grad).astype(jnp.bfloat16)
    gain_rows[...] = jnp.zeros(gain_rows.shape, jnp.float32)
    gain_rows[0:1, :] = gain_grad
    gain_rows[1:2, :] = gain_two_ref[...]
    gain_sum = WholeSum("dp", gain_rows, gain_landed, pairs[3])
    gain_sum.start()

    out_total = out_sum.total()
    w_total = w_sum.total()
    cols = w_total.shape[1]
    few = low.shape[1]
    for c in range(low.shape[0]):
        low[c, :, :cols] = w_total[c * few : (c + 1) * few].astype(jnp.bfloat16)
        low[c, :, cols:] = out_total[c * few : (c + 1) * few].astype(jnp.bfloat16)
    low_sum = PieceSum("ctx", low, low_landed, pairs[4])
    each(low_sum.size, low_sum.send)
    gain_more[...] = gain_sum.total()
    more_sum = WholeSum("ctx", gain_more, gain_more_landed, pairs[5])
    more_sum.start()
    out_sum.finish()
    w_sum.finish()
    own_ref[...] = low_sum.total()
    low_sum.finish()
    gains_ref[...] = more_sum.total()


def finish(dq, dkv, cosine, sine, normed, w, x, gain, hidden_grad, out_w, gain_two, ident):
    rows, width = x.shape
    dp_size, ctx_size = lax.axis_size("dp"), lax.axis_size("ctx")
    cols, out_cols = w.shape[2], out_w.shape[2]
    few = width // dp_size // ctx_size
    low, high = jnp.bfloat16, jnp.float32
    return pl.pallas_call(
        finish_kernel,
        name="finish",
        in_specs=whole_vmem(11),
        out_specs=whole_vmem(3),
        out_shape=[
            jax.ShapeDtypeStruct((rows, width), low),
            jax.ShapeDtypeStruct((few, cols + out_cols), high),
            jax.ShapeDtypeStruct((8, width), high),
        ],
        scratch_shapes=[
            pltpu.VMEM((rows, cols), low),
            pltpu.VMEM((width, rows), low),
            pltpu.VMEM((rows, width), low),
            pltpu.VMEM((rows, width), low),
            pltpu.VMEM((dp_size, width // dp_size, cols), low),
            pltpu.VMEM((dp_size, width // dp_size, cols), low),
            pltpu.VMEM(out_w.shape, low),
            pltpu.VMEM((ctx_size, few, cols + out_cols), low),
            pltpu.VMEM((ctx_size, few, cols + out_cols), low),
            pltpu.VMEM((8, width), high),
            pltpu.VMEM((dp_size, 8, width), high),
            pltpu.VMEM((8, width), high),
            pltpu.VMEM((ctx_size, 8, width), high),
            *sem_pair(dp_size),
            *sem_pair(dp_size),
            *sem_pair(1),
            *sem_pair(dp_size),
            *sem_pair(ctx_size),
            *sem_pair(ctx_size),
        ],
        compiler_params=remote_params(ident),
    )(dq, dkv, cosine, sine, normed, w, x, gain, hidden_grad, out_w, gain_two)


class Everyone:
    def __init__(self, axis, target, sems):
        self.axis, self.target, self.sems = axis, target, sems
        self.size = lax.axis_size(axis)

    def copy(self, k):
        at = self.target.at[lax.axis_index(self.axis)]
        return remote(at, at, self.sems, k, {self.axis: ahead_on(self.axis, k)})

    def start(self):
        each(self.size, lambda k: self.copy(k).start())

    def arrive(self):
        each(self.size, lambda k: self.copy(k).wait_recv())

    def finish(self):
        each(self.size, lambda k: self.copy(k).wait_send())


def find_places(first, own, routes_ref, gates_ref, earlier, place_ref, gate_ref, column_ref):
    _, tokens = routes_ref.shape[1:]

    def group(g, carry):
        routes, gates = routes_ref[g], gates_ref[g]
        names, values = [], []
        for e in range(own):
            named = routes == first + e
            names.append(jnp.max(named.astype(jnp.float32), axis=0, keepdims=True))
            values.append(jnp.sum(jnp.where(named, gates, 0.0), axis=0, keepdims=True))
        spare = jnp.zeros((8 - own % 8 if own % 8 else 0, tokens), jnp.float32)
        names = jnp.concatenate(names + ([spare] if spare.shape[0] else []), axis=0)
        place = jnp.dot(
            names.astype(jnp.bfloat16), earlier[...], preferred_element_type=jnp.float32
        )
        place = jnp.where((names > 0.0) & (place < CAP), place, -float(CAP * own))
        for e in range(own):
            place_ref[g, e] = place[e : e + 1].astype(jnp.int32)
            gate_ref[g, e] = values[e]
        column_ref[g] = jnp.transpose(place)[:, :own].astype(jnp.int32)
        return carry

    lax.fori_loop(0, routes_ref.shape[0], group, 0)


def front_kernel(
    back, ahead, own, starts_ref, x_ref, cot_ref, q_w_ref, k_w_ref, v_w_ref, out_w_ref, gains_ref,
    docs_ref, routes_ref, gates_ref, cos_ref, sin_ref, w_all, out_w_all, gain_rows, docs_all,
    normed_ref, q_ref, kv_all, mix_ref, full_ref, log_ref, hidden_ref, rows_all, cot_all,
    place_ref, gate_ref, column_ref, gains_all, routes_all, gates_all, acc, top, total, column,
    part, held, normed_two, earlier, *sems,
):
    me, size = lax.axis_index("ctx"), lax.axis_size("ctx")
    dp = lax.axis_index("dp")
    pairs = [sems[2 * i : 2 * i + 2] for i in range(len(sems) // 2)]
    q_width, kv_width = q_w_ref.shape[1], k_w_ref.shape[1]
    dp_size, piece = w_all.shape[:2]
    w_all[dp, :, :q_width] = q_w_ref[...]
    w_all[dp, :, q_width : q_width + kv_width] = k_w_ref[...]
    w_all[dp, :, q_width + kv_width :] = v_w_ref[...]
    gains_all[dp] = gains_ref[...]
    docs_all[me] = docs_ref[...]
    routes_all[dp] = routes_ref[...]
    gates_all[dp] = gates_ref[...]
    out_w_all[dp] = out_w_ref[...]
    greet(["dp", "ctx", "tp"])
    gains = Everyone("dp", gains_all, pairs[0])
    weights = Everyone("dp", w_all, pairs[1])
    docs = Everyone("ctx", docs_all, pairs[2])
    routes = Everyone("dp", routes_all, pairs[3])
    gates = Everyone("dp", gates_all, pairs[4])
    out_w = Everyone("dp", out_w_all, pairs[5])
    for one in (gains, weights, docs, routes, gates):
        one.start()

    token = lax.broadcasted_iota(jnp.int32, earlier.shape, 0)
    later = lax.broadcasted_iota(jnp.int32, earlier.shape, 1)
    earlier[...] = (token < later).astype(jnp.float32).astype(jnp.bfloat16)
    top[...] = jnp.full(top.shape, NEG_FILL, jnp.float32)
    total[...] = jnp.zeros(total.shape, jnp.float32)
    acc[...] = jnp.zeros(acc.shape, jnp.float32)
    gains.arrive()
    for i in range(dp_size):
        gain_rows[:, i * piece : (i + 1) * piece] = gains_all[i]
    x = x_ref[...].astype(jnp.float32)
    normed_ref[...] = (x * row_scale(x) * gain_rows[0:1, :]).astype(jnp.bfloat16)
    routes.arrive()
    gates.arrive()
    docs.arrive()
    find_places(dp * own, own, routes_all, gates_all, earlier, place_ref, gate_ref, column_ref)
    weights.arrive()
    out_w.start()
    cot_rows = RowGather(cot_ref, cot_all, pairs[6], pairs[7], 0)
    cot_rows.start()

    wide, tile = 4 * HEAD_DIM, 2 * HEAD_DIM

    def project(first):
        whole = jnp.dot(
            normed_ref[:, :piece], w_all[0, :, first : first + wide],
            preferred_element_type=jnp.float32,
        )
        for i in range(1, dp_size):
            whole += jnp.dot(
                normed_ref[:, i * piece : (i + 1) * piece], w_all[i, :, first : first + wide],
                preferred_element_type=jnp.float32,
            )
        return [whole[:, :tile], whole[:, tile:]]

    for first in range(q_width, q_width + 2 * kv_width, wide):
        for i, part_of in enumerate(project(first)):
            if first < q_width + kv_width:
                part_of = turn(part_of, cos_ref[...], -sin_ref[...])
            at = first - q_width + i * tile
            kv_all[me, :, at : at + tile] = part_of.astype(jnp.bfloat16)

    right, left = me + 1, me - 1
    line = pairs[8]

    def hop(s):
        at = kv_all.at[lax.rem(me + size - s, size)]
        return remote(at, at, line, s, {"ctx": right})

    def back_hop():
        return remote(kv_all.at[me], kv_all.at[me], line, back, {"ctx": left})

    if back:

        @pl.when(right < size)
        def _():
            hop(0).start()

    if ahead:

        @pl.when(left >= 0)
        def _():
            back_hop().start()

    for first in range(0, q_width, wide):
        for i, part_of in enumerate(project(first)):
            turned = turn(part_of, cos_ref[...], -sin_ref[...]).astype(jnp.bfloat16)
            at = first + i * tile
            q_ref[:, at : at + tile] = (turned.astype(jnp.float32) * HEAD_DIM**-0.5).astype(
                jnp.bfloat16
            )
    masks = Masks(docs_all, starts_ref, column)

    def visit(s):
        @pl.when(me - s >= 0)
        def _():
            block = lax.rem(me + size - s, size)

            @pl.when(s > 0)
            def _():
                hop(s - 1).wait_recv()

            @pl.when((s > 0) & (s < back) & (right < size))
            def _():
                hop(s).start()

            attend_block(masks, block, q_ref, kv_all.at[block], acc, top, total)

    each(back + 1, visit, 0)
    if ahead:

        @pl.when(right < size)
        def _():
            block = lax.rem(me + 1, size)
            back_hop().wait_recv()
            attend_block(masks, block, q_ref, kv_all.at[block], acc, top, total)

    log_ref[...] = top[...] + jnp.log(total[...])
    for h in range(total.shape[0]):
        at = slice(h * HEAD_DIM, (h + 1) * HEAD_DIM)
        acc[at, :] = acc[at, :] / total[h : h + 1, :]
    full_ref[...] = jnp.transpose(acc[...])
    mix_ref[...] = full_ref[...].astype(jnp.bfloat16)
    out_w.arrive()
    for i in range(dp_size):
        part[:, i * piece : (i + 1) * piece] = jnp.dot(
            mix_ref[...], out_w_all[i], preferred_element_type=jnp.float32
        ).astype(jnp.bfloat16)

    mine, theirs = halves(part.shape[0])
    rows = RowGather(normed_two, rows_all, pairs[9], pairs[10], 1)
    first = remote(part.at[theirs], held.at[theirs], pairs[10], 0, other_core())
    second = remote(part.at[mine], held.at[mine], pairs[10], 1, other_core())
    first.start()
    second.start()

    def norm(at):
        whole = x_ref[at, :].astype(jnp.float32) + (
            part[at, :].astype(jnp.float32) + held[at, :].astype(jnp.float32)
        )
        hidden_ref[at, :] = whole
        normed_two[at, :] = (whole * row_scale(whole) * gain_rows[1:2, :]).astype(jnp.bfloat16)

    first.wait()
    norm(mine)
    rows.start()
    second.wait()
    norm(theirs)
    rows_all[dp] = normed_two[...]
    cot_all[dp] = cot_ref[...]
    cot_rows.forward()
    rows.forward()
    for one in (gains, weights, docs, routes, gates, out_w):
        one.finish()

    def sent(s):
        @pl.when((right < size) & (me - s >= 0))
        def _():
            hop(s).wait_send()

    each(back, sent, 0)
    if ahead:

        @pl.when(left >= 0)
        def _():
            back_hop().wait_send()

    cot_rows.finish()
    rows.finish()


def front(
    starts, x, cot, q_w, k_w, v_w, out_w, gains, docs, routes, gates, cosine, sine, own, back,
    ahead, ident,
):
    rows, width = x.shape
    dp_size, ctx_size = lax.axis_size("dp"), lax.axis_size("ctx")
    q_width, kv_cols = q_w.shape[1], 2 * k_w.shape[1]
    piece, heads = q_w.shape[0], q_width // HEAD_DIM
    low, high, whole = jnp.bfloat16, jnp.float32, jnp.int32
    shapes = [
        ((dp_size, piece, q_width + kv_cols), low),
        ((dp_size,) + out_w.shape, low),
        ((2, width), high),
        ((ctx_size, 1, rows), whole),
        ((rows, width), low),
        ((rows, q_width), low),
        ((ctx_size, rows, kv_cols), low),
        ((rows, q_width), low),
        ((rows, q_width), high),
        ((heads, rows), high),
        ((rows, width), high),
        ((dp_size, rows, width), low),
        ((dp_size, rows, width), low),
        ((dp_size, own, 1, rows), whole),
        ((dp_size, own, 1, rows), high),
        ((dp_size, rows, own), whole),
    ]
    return pl.pallas_call(
        functools.partial(front_kernel, back, ahead, own),
        name="front",
        in_specs=[pl.BlockSpec(memory_space=pltpu.SMEM)] + whole_vmem(12),
        out_specs=whole_vmem(len(shapes)),
        out_shape=[jax.ShapeDtypeStruct(*shape) for shape in shapes],
        scratch_shapes=[
            pltpu.VMEM((dp_size,) + gains.shape, high),
            pltpu.VMEM((dp_size,) + routes.shape, whole),
            pltpu.VMEM((dp_size,) + gates.shape, high),
            pltpu.VMEM((q_width, rows), high),
            pltpu.VMEM((heads, rows), high),
            pltpu.VMEM((heads, rows), high),
            pltpu.VMEM((rows, 8), whole),
            pltpu.VMEM((rows, width), low),
            pltpu.VMEM((rows, width), low),
            pltpu.VMEM((rows, width), low),
            pltpu.VMEM((rows, rows), low),
            *sem_pair(dp_size),
            *sem_pair(dp_size),
            *sem_pair(ctx_size),
            *sem_pair(dp_size),
            *sem_pair(dp_size),
            *sem_pair(dp_size),
            *sem_pair(dp_size),
            *sem_pair(dp_size),
            *sem_pair(back + 1),
            *sem_pair(dp_size),
            *sem_pair(dp_size + 1),
        ],
        compiler_params=remote_params(ident),
    )(starts, x, cot, q_w, k_w, v_w, out_w, gains, docs, routes, gates, cosine, sine)


GROUPS_AT_ONCE = 4


def experts_kernel(more, rows_ref, grads_ref, weights_ref, place_ref, gate_ref, *refs):
    outs_ref, backs_ref, weight_grad_ref, slots, slot_grads = refs[2 * more :]
    groups, tok_rows, _ = rows_ref.shape
    owners, part = weight_grad_ref.shape[1], weight_grad_ref.shape[5]
    slot_index = lax.broadcasted_iota(jnp.int32, (CAP, tok_rows), 0)
    gates = []
    for g in range(groups):
        picks = slot_index == place_ref[g, 0]
        gates.append(jnp.sum(jnp.where(picks, gate_ref[g, 0], 0.0), axis=1, keepdims=True))
        picks = picks.astype(jnp.float32).astype(jnp.bfloat16)
        at = slice(g * CAP, (g + 1) * CAP)
        slots[at, :] = jnp.dot(
            picks, rows_ref[g], preferred_element_type=jnp.float32
        ).astype(jnp.bfloat16)
        slot_grads[at, :] = (
            jnp.dot(picks, grads_ref[g], preferred_element_type=jnp.float32) * gates[g]
        ).astype(jnp.bfloat16)
    gate_w, up_w, down_w = (weights_ref.at[0, i] for i in range(3))
    gate_pre = jnp.dot(slots[...], gate_w[...], preferred_element_type=jnp.float32)
    up_pre = jnp.dot(slots[...], up_w[...], preferred_element_type=jnp.float32)
    act_grad = jnp.dot(slot_grads[...], down_w[...], preferred_element_type=jnp.float32)
    sig = 1.0 / (1.0 + jnp.exp(-gate_pre))
    silu = gate_pre * sig
    act_low = (silu * up_pre).astype(jnp.bfloat16)
    up_low = (act_grad * silu).astype(jnp.bfloat16)
    gate_low = (act_grad * up_pre * (sig * (1.0 + gate_pre * (1.0 - sig)))).astype(jnp.bfloat16)

    back = lax.dot_general(
        gate_low, gate_w[...], NT, preferred_element_type=jnp.float32
    ) + lax.dot_general(up_low, up_w[...], NT, preferred_element_type=jnp.float32)
    out = lax.dot_general(act_low, down_w[...], NT, preferred_element_type=jnp.float32)
    for g in range(groups):
        at = slice(g * CAP, (g + 1) * CAP)
        backs_ref[g] = back[at].astype(jnp.bfloat16)
        outs_ref[g] = (out[at] * gates[g]).astype(jnp.bfloat16)

    for i, (low, source) in enumerate(
        ((gate_low, slots), (up_low, slots), (act_low, slot_grads))
    ):
        turned = jnp.transpose(low.astype(jnp.float32)).astype(jnp.bfloat16)
        total = jnp.dot(turned, source[...], preferred_element_type=jnp.float32)
        for c in range(owners):
            weight_grad_ref[0, c, 0, i] = total[:, c * part : (c + 1) * part].astype(
                weight_grad_ref.dtype
            )


def experts(weights, place_rows, gate_rows, rows_all, grad_all, first, count, before):
    own, _, model_width, hidden = weights.shape
    groups, tok_rows, _ = rows_all.shape
    owners = lax.axis_size("ctx")
    at_once = min(GROUPS_AT_ONCE, groups)
    chunks = groups // at_once
    part = model_width // owners
    rows_spec = pl.BlockSpec(
        (at_once, tok_rows, model_width), lambda c, e: (c, 0, 0), pipeline_mode=pl.Buffered(1)
    )
    line_spec = pl.BlockSpec((at_once, 1, 1, tok_rows), lambda c, e: (c, e + first, 0, 0))
    slots_spec = pl.BlockSpec((at_once, CAP, model_width), lambda c, e: (c, e + first, 0))
    slots_shape = jax.ShapeDtypeStruct((groups, own * CAP, model_width), jnp.bfloat16)
    flops = count * groups * CAP * model_width * 2 * (9 * hidden + 2 * tok_rows)
    more = before is not None
    outs, backs, weight_part = pl.pallas_call(
        functools.partial(experts_kernel, more),
        name="experts",
        grid=(chunks, count),
        in_specs=[
            rows_spec,
            rows_spec,
            pl.BlockSpec((1, 3, model_width, hidden), lambda c, e: (e + first, 0, 0, 0)),
            line_spec,
            line_spec,
        ]
        + [pl.BlockSpec(memory_space=pl.ANY)] * (2 * more),
        out_specs=[
            slots_spec,
            slots_spec,
            pl.BlockSpec((1, owners, 1, 3, hidden, part), lambda c, e: (c, 0, e, 0, 0, 0)),
        ],
        out_shape=[
            slots_shape,
            slots_shape,
            jax.ShapeDtypeStruct((chunks, owners, count, 3, hidden, part), jnp.bfloat16),
        ],
        scratch_shapes=[
            pltpu.VMEM((at_once * CAP, model_width), jnp.bfloat16),
            pltpu.VMEM((at_once * CAP, model_width), jnp.bfloat16),
        ],
        input_output_aliases={5: 0, 6: 1} if more else {},
        compiler_params=pltpu.CompilerParams(vmem_limit_bytes=LIMIT),
        cost_estimate=pl.CostEstimate(
            flops=flops, bytes_accessed=4 * weights.size, transcendentals=0
        ),
    )(rows_all, grad_all, weights, place_rows, gate_rows, *(before if more else ()))
    if chunks == 1:
        return (outs, backs), weight_part[0]
    return (outs, backs), jnp.sum(weight_part.astype(jnp.float32), axis=0).astype(jnp.bfloat16)


def unfold_kernel(more, sums_ref, *refs):
    out_ref = refs[more]
    for i in range(sums_ref.shape[1]):
        out_ref[0, i] = jnp.transpose(sums_ref[0, i].astype(jnp.float32))


def unfold(sums, own, first, before):
    count, three, hidden, part = sums.shape
    more = before is not None
    return pl.pallas_call(
        functools.partial(unfold_kernel, more),
        name="unfold",
        grid=(count,),
        in_specs=[pl.BlockSpec((1, three, hidden, part), lambda e: (e, 0, 0, 0))]
        + [pl.BlockSpec(memory_space=pl.ANY)] * more,
        out_specs=pl.BlockSpec((1, three, part, hidden), lambda e: (e + first, 0, 0, 0)),
        out_shape=jax.ShapeDtypeStruct((own, three, part, hidden), jnp.float32),
        input_output_aliases={1: 0} if more else {},
        compiler_params=pltpu.CompilerParams(vmem_limit_bytes=LIMIT),
    )(sums, *([before] if more else []))


def rotary_tables(token_positions):
    half_dim = HEAD_DIM // 2
    inverse = THETA ** (-(jnp.arange(half_dim, dtype=jnp.float32) * 2.0 / HEAD_DIM))
    angles = token_positions.astype(jnp.float32)[:, None] * inverse[None, :]
    cosine, sine = jnp.cos(angles), jnp.sin(angles)
    return jnp.concatenate([cosine] * 4, axis=1), jnp.concatenate([sine, -sine] * 2, axis=1)


def expert_counts(own):
    return (1, 2, 3, 2) if own == 8 else (own - own // 2, own // 2)


def scatter(grads):
    return lax.psum_scatter(grads, "ctx", scatter_dimension=0)


def body(
    tokens,
    query_weight,
    key_weight,
    value_weight,
    output_weight,
    gain_attn,
    gain_moe,
    expert_weights,
    routes,
    gate_values,
    documents,
    pic_starts,
    cotangent,
):
    block_len = tokens.shape[1]
    ctx_size = lax.axis_size("ctx")
    length = block_len * ctx_size
    offset = lax.axis_index("ctx") * block_len
    back = back_blocks(ctx_size, block_len, length)
    ahead = ahead_blocks(block_len, length, pic_starts.shape[1])
    q_width, kv_width = query_weight.shape[1], key_weight.shape[1]
    own = expert_weights.shape[0]
    x, cot = tokens[0], cotangent[0]

    cosine, sine = rotary_tables(offset + jnp.arange(block_len, dtype=jnp.int32))
    (
        w_all,
        out_w_all,
        gain_rows,
        docs_all,
        normed_one,
        query,
        kv_all,
        mixture,
        mix_full,
        log_total,
        hidden,
        rows_all,
        grad_all,
        *places,
    ) = front(
        pic_starts,
        x,
        cot,
        query_weight,
        key_weight,
        value_weight,
        output_weight,
        jnp.stack([gain_attn, gain_moe]).astype(jnp.float32),
        documents,
        routes[0].T,
        gate_values[0].T,
        cosine,
        sine,
        own,
        back,
        ahead,
        1,
    )
    place_rows, gate_rows, places = places
    counts = expert_counts(own)
    slots, sums = None, []
    first = 0
    for n, count in enumerate(counts):
        slots, grads = experts(
            expert_weights, place_rows, gate_rows, rows_all, grad_all, first, count, slots
        )
        if n < len(counts) - 1:
            sums.append((scatter(grads), first))
        first += count
    outs, backs = slots
    hidden_grad, hidden_low, mix_grad, gain_two_grad = return_grads(
        backs, places, hidden, cot, gain_rows, out_w_all, 2
    )
    q_rot_grad, kv_part = attend_back(
        pic_starts, query, kv_all, docs_all, log_total, mix_full, mix_grad, back, ahead
    )
    kv_back, layer_out, output_grad = trade(
        kv_part,
        outs,
        places,
        hidden,
        hidden_low,
        mixture,
        back,
        ahead,
        3,
    )
    grads, kv_back = lax.optimization_barrier((grads, kv_back))
    sums.append((scatter(grads), own - counts[-1]))
    input_grad, owned, gain_sums = finish(
        q_rot_grad,
        kv_back,
        cosine,
        sine,
        normed_one,
        w_all,
        x,
        gain_rows,
        hidden_grad,
        output_grad,
        gain_two_grad,
        4,
    )
    few = owned.shape[0]
    here = (lax.axis_index("dp") * ctx_size + lax.axis_index("ctx")) * few
    gain_sums = lax.dynamic_slice_in_dim(gain_sums, here, few, 1)
    expert_grad = None
    for part, first in sums:
        expert_grad = unfold(part, own, first, expert_grad)
    v_end = q_width + 2 * kv_width
    return (
        layer_out[None],
        input_grad[None],
        owned[:, :q_width],
        owned[:, q_width : q_width + kv_width],
        owned[:, q_width + kv_width : v_end],
        owned[:, v_end:].T,
        gain_sums[0],
        gain_sums[1],
        expert_grad,
    )


def solution(mesh):
    return jax.shard_map(
        body,
        mesh=mesh,
        in_specs=(
            P("dp", "ctx", None),
            P("dp", "tp"),
            P("dp", "tp"),
            P("dp", "tp"),
            P("tp", "dp"),
            P("dp"),
            P("dp"),
            P("dp", None, None, "tp"),
            P("dp", "ctx", None),
            P("dp", "ctx", None),
            P("dp", "ctx"),
            P("dp", None),
            P("dp", "ctx", None),
        ),
        out_specs=(
            P("dp", "ctx", None),
            P("dp", "ctx", None),
            P(("dp", "ctx"), "tp"),
            P(("dp", "ctx"), "tp"),
            P(("dp", "ctx"), "tp"),
            P("tp", ("dp", "ctx")),
            P(("dp", "ctx")),
            P(("dp", "ctx")),
            P("dp", None, "ctx", "tp"),
        ),
        check_vma=False,
    )
```

```python
import functools

import jax
import jax.numpy as jnp
from jax import lax
from jax.experimental import pallas as pl
from jax.experimental.pallas import tpu as pltpu
from jax.sharding import PartitionSpec as P

HEAD_DIM = 64
PIC = 256
CAP = 144

EPSILON = 1e-06
THETA = 10000.0
NEG_FILL = -1e30


KEY_ROWS = 256
NT = (((1,), (1,)), ((), ()))
LIMIT = 67043328


def whole_vmem(count):
    return [pl.BlockSpec(memory_space=pltpu.VMEM)] * count


def picture_ids(starts_ref, places):
    ids = jnp.full(places.shape, -1, jnp.int32)
    for j in range(starts_ref.shape[1]):
        start = starts_ref[0, j]
        ids += jnp.where((places >= start) & (places < start + PIC), j + 1, 0)
    return ids


def as_column(row):
    tall = jnp.broadcast_to(row.astype(jnp.float32), (8, row.shape[1]))
    return jnp.transpose(tall)[:, 0:1].astype(jnp.int32)


class Masks:
    def __init__(self, docs_ref, starts_ref, column):
        self.docs_ref, self.starts_ref, self.column = docs_ref, starts_ref, column
        self.rows = docs_ref.shape[2]
        me = lax.axis_index("ctx")
        self.q_doc = docs_ref[me]
        self.q_place = me * self.rows + lax.broadcasted_iota(jnp.int32, (1, self.rows), 1)
        self.q_pic = picture_ids(starts_ref, self.q_place)

    def open(self, block):
        self.column[...] = jnp.broadcast_to(
            as_column(self.docs_ref[block]), self.column.shape
        )

    def bias(self, block, rows, first):
        k_doc = self.column[rows, 0:1]
        k_place = block * self.rows + first + lax.broadcasted_iota(jnp.int32, k_doc.shape, 0)
        k_pic = picture_ids(self.starts_ref, k_place)
        seen = (k_doc == self.q_doc) & (
            (k_place <= self.q_place) | ((k_pic == self.q_pic) & (self.q_pic >= 0))
        )
        return jnp.where(seen, 0.0, NEG_FILL)


def attend_block(masks, block, q_ref, kv_ref, acc, top, total):
    kv_width = kv_ref.shape[1] // 2
    heads, kv_heads = q_ref.shape[1] // HEAD_DIM, kv_width // HEAD_DIM
    masks.open(block)

    def step(j, carry):
        first = pl.multiple_of(j * KEY_ROWS, KEY_ROWS)
        rows = pl.ds(first, KEY_ROWS)
        bias = masks.bias(block, rows, first)
        for g in range(kv_heads):
            key = kv_ref[rows, g * HEAD_DIM : (g + 1) * HEAD_DIM]
            val = kv_ref[rows, kv_width + g * HEAD_DIM : kv_width + (g + 1) * HEAD_DIM]
            val_t = jnp.transpose(val.astype(jnp.float32)).astype(jnp.bfloat16)
            for h in range(g * heads // kv_heads, (g + 1) * heads // kv_heads):
                at = slice(h * HEAD_DIM, (h + 1) * HEAD_DIM)
                scores = bias + lax.dot_general(
                    key, q_ref[:, at], NT, preferred_element_type=jnp.float32
                )
                old = top[h : h + 1, :]
                new = jnp.maximum(old, jnp.max(scores, axis=0, keepdims=True))
                probs = jnp.exp(scores - new)
                fade = jnp.exp(old - new)
                total[h : h + 1, :] = total[h : h + 1, :] * fade + jnp.sum(
                    probs, axis=0, keepdims=True
                )
                acc[at, :] = acc[at, :] * fade + jnp.dot(
                    val_t, probs.astype(jnp.bfloat16), preferred_element_type=jnp.float32
                )
                top[h : h + 1, :] = new
        return carry

    lax.fori_loop(0, kv_ref.shape[0] // KEY_ROWS, step, 0)


def attend_back_block(
    masks, edges, block, q_ref, kv_ref, log_ref, delta, grad_ref, acc, dkv_ref
):
    kv_width = kv_ref.shape[1] // 2
    heads, kv_heads = q_ref.shape[1] // HEAD_DIM, kv_width // HEAD_DIM
    masks.open(block)
    count = kv_ref.shape[0] // KEY_ROWS
    me = lax.axis_index("ctx")
    q_first, q_last = edges[me * count, 0], edges[me * count + count - 1, 1]

    def step(j, carry):
        at = block * count + j
        same = (edges[at, 0] <= q_last) & (edges[at, 1] >= q_first)

        @pl.when(same)
        def _():
            inside(j)

        @pl.when(jnp.logical_not(same))
        def _():
            rows = pl.ds(pl.multiple_of(j * KEY_ROWS, KEY_ROWS), KEY_ROWS)
            dkv_ref[rows, :] = jnp.zeros((KEY_ROWS, dkv_ref.shape[1]), dkv_ref.dtype)

        return carry

    def inside(j):
        first = pl.multiple_of(j * KEY_ROWS, KEY_ROWS)
        rows = pl.ds(first, KEY_ROWS)
        bias = masks.bias(block, rows, first)
        for g in range(kv_heads):
            k_at = slice(g * HEAD_DIM, (g + 1) * HEAD_DIM)
            v_at = slice(kv_width + g * HEAD_DIM, kv_width + (g + 1) * HEAD_DIM)
            key, val = kv_ref[rows, k_at], kv_ref[rows, v_at]
            key_t = jnp.transpose(key.astype(jnp.float32)).astype(jnp.bfloat16)
            dk = jnp.zeros((KEY_ROWS, HEAD_DIM), jnp.float32)
            dv = jnp.zeros((KEY_ROWS, HEAD_DIM), jnp.float32)
            for h in range(g * heads // kv_heads, (g + 1) * heads // kv_heads):
                at = slice(h * HEAD_DIM, (h + 1) * HEAD_DIM)
                q_rows, g_rows = q_ref[:, at], grad_ref[:, at]
                scores = bias + lax.dot_general(
                    key, q_rows, NT, preferred_element_type=jnp.float32
                )
                probs = jnp.exp(scores - log_ref[h : h + 1, :])
                prob_grad = lax.dot_general(val, g_rows, NT, preferred_element_type=jnp.float32)
                slope = (probs * (prob_grad - delta[h : h + 1, :])).astype(jnp.bfloat16)
                dv += jnp.dot(
                    probs.astype(jnp.bfloat16), g_rows, preferred_element_type=jnp.float32
                )
                dk += jnp.dot(slope, q_rows, preferred_element_type=jnp.float32)
                acc[at, :] += jnp.dot(key_t, slope, preferred_element_type=jnp.float32)
            dkv_ref[rows, k_at] = dk.astype(dkv_ref.dtype)
            dkv_ref[rows, v_at] = dv.astype(dkv_ref.dtype)

    lax.fori_loop(0, count, step, 0)


def attend_back_kernel(
    back, ahead, starts_ref, edges, q_ref, kv_ref, docs_ref, log_ref, full_ref, grad_ref, dq_ref,
    dkv_ref, acc, delta, column,
):
    me, size = lax.axis_index("ctx"), lax.axis_size("ctx")
    acc[...] = jnp.transpose(full_ref[...] * grad_ref[...].astype(jnp.float32))
    for h in range(delta.shape[0]):
        delta[h : h + 1, :] = jnp.sum(
            acc[h * HEAD_DIM : (h + 1) * HEAD_DIM, :], axis=0, keepdims=True
        )
    acc[...] = jnp.zeros(acc.shape, jnp.float32)
    masks = Masks(docs_ref, starts_ref, column)

    def step(s, carry):
        block = me + ahead - s

        @pl.when((block >= 0) & (block < size))
        def _():
            attend_back_block(
                masks, edges, block, q_ref, kv_ref.at[block], log_ref, delta, grad_ref, acc,
                dkv_ref.at[block],
            )

        return carry

    lax.fori_loop(0, back + ahead + 1, step, 0)
    dq_ref[...] = jnp.transpose(acc[...]) * (HEAD_DIM**-0.5)


def attend_back(starts, q, kv, docs, log_total, full, grad, back, ahead):
    rows, width = q.shape
    by_block = docs.reshape(-1, KEY_ROWS)
    edges = jnp.concatenate([by_block[:, :1], by_block[:, -1:]], axis=1)
    return pl.pallas_call(
        functools.partial(attend_back_kernel, back, ahead),
        name="attend_back",
        in_specs=[pl.BlockSpec(memory_space=pltpu.SMEM)] * 2 + whole_vmem(6),
        out_specs=whole_vmem(2),
        out_shape=[
            jax.ShapeDtypeStruct((rows, width), jnp.float32),
            jax.ShapeDtypeStruct(kv.shape, jnp.bfloat16),
        ],
        scratch_shapes=[
            pltpu.VMEM((width, rows), jnp.float32),
            pltpu.VMEM((width // HEAD_DIM, rows), jnp.float32),
            pltpu.VMEM((rows, 8), jnp.int32),
        ],
        compiler_params=pltpu.CompilerParams(vmem_limit_bytes=LIMIT),
    )(starts, edges, q, kv, docs, log_total, full, grad)


MESH = pl.DeviceIdType.MESH


def greet(axes_list, line=False):
    barrier = pltpu.get_barrier_semaphore()
    count = 0
    for axis in axes_list:
        me, size = lax.axis_index(axis), lax.axis_size(axis)

        def signal(k, carry, axis=axis, me=me, size=size):
            pl.semaphore_signal(
                barrier, inc=1, device_id={axis: lax.rem(me + k, size)}, device_id_type=MESH
            )
            return carry

        lax.fori_loop(1, size, signal, 0)
        count += size - 1
    if not line:
        pl.semaphore_wait(barrier, count)
        return
    me, size = lax.axis_index("ctx"), lax.axis_size("ctx")
    for step in (1, -1):
        other = me + step

        @pl.when((other >= 0) & (other < size))
        def _(other=other):
            pl.semaphore_signal(barrier, inc=1, device_id={"ctx": other}, device_id_type=MESH)

    inner = (me > 0) & (me < size - 1)

    @pl.when(inner)
    def _():
        pl.semaphore_wait(barrier, count + 2)

    @pl.when(jnp.logical_not(inner))
    def _():
        pl.semaphore_wait(barrier, count + 1)


def remote(src, dst, sems, k, device_id):
    return pltpu.make_async_remote_copy(
        src_ref=src,
        dst_ref=dst,
        send_sem=sems[0].at[k],
        recv_sem=sems[1].at[k],
        device_id=device_id,
        device_id_type=MESH,
    )


def other_core():
    return {"tp": 1 - lax.axis_index("tp")}


def ahead_on(axis, k):
    return lax.rem(lax.axis_index(axis) + k, lax.axis_size(axis))


def each(count, do, first=1):
    def step(k, carry):
        do(k)
        return carry

    lax.fori_loop(first, count, step, 0)


def sem_pair(count):
    return [pltpu.SemaphoreType.DMA((count,)), pltpu.SemaphoreType.DMA((count,))]


def remote_params(ident):
    return pltpu.CompilerParams(
        collective_id=ident, has_side_effects=True, vmem_limit_bytes=LIMIT
    )


def halves(rows):
    half = rows // 2
    core = lax.axis_index("tp")
    return (
        pl.ds(pl.multiple_of(core * half, half), half),
        pl.ds(pl.multiple_of((1 - core) * half, half), half),
    )


def turn(tile, cosine, sine):
    lane = lax.broadcasted_iota(jnp.int32, tile.shape, 1)
    half = HEAD_DIM // 2
    swapped = jnp.where(
        lax.rem(lane, HEAD_DIM) < half,
        pltpu.roll(tile, 2 * HEAD_DIM - half, 1),
        pltpu.roll(tile, half, 1),
    )
    return tile * cosine + swapped * sine


def row_scale(x):
    return lax.rsqrt(jnp.mean(x * x, axis=-1, keepdims=True) + EPSILON)


def norm_back(x, gain, grad):
    scale = row_scale(x)
    unit = x * scale
    pull = grad * gain
    return (
        scale * (pull - unit * jnp.mean(pull * unit, axis=-1, keepdims=True)),
        jnp.sum(grad * unit, axis=0, keepdims=True),
    )


def back_blocks(ctx_size, block_len, length):
    return min(ctx_size - 1, -(-(length // 2 - 1) // block_len))


def ahead_blocks(block_len, length, spans):
    return 0 if block_len % (length // spans) == 0 else 1


def grid_peers():
    me = lax.axis_index("dp")
    x, y = lax.rem(me, 2), lax.div(me, 2)
    return y * 2 + 1 - x, (1 - y) * 2 + x, 3 - me


class Gather:
    def __init__(self, target, sems, rows=None, source=None):
        self.target, self.sems, self.rows, self.source = target, sems, rows, source
        self.size = lax.axis_size("dp")
        self.grid = self.size == 4

    def at(self, place):
        return self.target.at[place] if self.rows is None else self.target.at[place, self.rows]

    def half(self, place, n):
        if self.rows is None:
            count = self.target.shape[1] // 2
            return self.target.at[place, pl.ds(n * count, count)]
        count = self.rows.size // 2
        first = pl.multiple_of(self.rows.start + n * count, count)
        return self.target.at[place, pl.ds(first, count)]

    def first(self, k, peer):
        place = self.at(lax.axis_index("dp"))
        source = place if self.source is None else self.source.at[self.rows]
        return remote(source, place, self.sems, k, {"dp": peer})

    def passed(self, k, place, n, peer):
        at = self.half(place, n)
        return remote(at, at, self.sems, k, {"dp": peer})

    def direct(self, k):
        return self.first(k, ahead_on("dp", k))

    def start(self):
        if not self.grid:
            each(self.size, lambda k: self.direct(k).start())
            return
        x, y, _ = grid_peers()
        self.first(0, x).start()
        self.first(1, y).start()

    def forward(self, came=None):
        if not self.grid:
            return
        x, y, _ = grid_peers()
        self.first(0, x).wait_recv()
        self.passed(2, x, 0, y).start()
        if came:
            came(0, self.at(x))
        self.first(1, y).wait_recv()
        self.passed(3, y, 1, x).start()
        if came:
            came(1, self.at(y))

    def arrive(self, came=None):
        if not self.grid:

            def one(k):
                self.direct(k).wait_recv()
                if came:
                    came(k, self.at(ahead_on("dp", self.size - k)))

            each(self.size, one)
            return
        x, _, diagonal = grid_peers()
        for n in range(2):
            self.passed(2 + n, diagonal, n, x).wait_recv()
            if came:
                came(2 + n, self.half(diagonal, n))

    def finish(self):
        if not self.grid:
            each(self.size, lambda k: self.direct(k).wait_send())
            return
        x, y, _ = grid_peers()
        self.first(0, x).wait_send()
        self.first(1, y).wait_send()
        self.passed(2, x, 0, y).wait_send()
        self.passed(3, y, 1, x).wait_send()


class RowGather:
    def __init__(self, source, target, dp_sems, tp_sems, first):
        mine, _ = halves(source.shape[0])
        self.gather = Gather(target, dp_sems, mine, source)
        self.tp_sems, self.after = tp_sems, first

    def relay(self, k, at):
        return remote(at, at, self.tp_sems, self.after + k, other_core())

    def came(self, k, at):
        self.relay(k, at).start()

    def start(self):
        self.gather.start()

    def forward(self):
        self.gather.forward(self.came)

    def arrive(self):
        self.gather.arrive(self.came)

    def finish(self):
        self.gather.finish()
        gather = self.gather
        if not gather.grid:
            each(
                gather.size,
                lambda k: self.relay(k, gather.at(ahead_on("dp", gather.size - k))).wait(),
            )
            return
        x, y, diagonal = grid_peers()
        self.relay(0, gather.at(x)).wait()
        self.relay(1, gather.at(y)).wait()
        self.relay(2, gather.half(diagonal, 0)).wait()
        self.relay(3, gather.half(diagonal, 1)).wait()


def collect(places_ref, slots_ref, group):
    tok_rows, slot_count = places_ref.shape[1], slots_ref.shape[1]
    tiles = []
    for first in range(0, slot_count, 128):
        wide = min(128, slot_count - first)
        lane = first + lax.broadcasted_iota(jnp.int32, (tok_rows, wide), 1)
        hit = None
        for n in range(first // CAP, (first + wide - 1) // CAP + 1):
            one = places_ref[group, :, n : n + 1] == lane - n * CAP
            hit = one if hit is None else hit | one
        tiles.append(hit.astype(jnp.float32).astype(jnp.bfloat16))
    return jnp.dot(
        jnp.concatenate(tiles, axis=1), slots_ref[group], preferred_element_type=jnp.float32
    )


class RowReturn:
    def __init__(self, part, held, landed, total, sent, came, dp_sems, tp_sems):
        self.part, self.held, self.landed, self.total = part, held, landed, total
        self.sent, self.came, self.dp_sems, self.tp_sems = sent, came, dp_sems, tp_sems
        self.size = lax.axis_size("dp")
        self.mine, self.theirs = halves(part.shape[1])

    def swap(self, k):
        group = ahead_on("dp", k)
        return remote(
            self.part.at[group, self.theirs], self.held.at[k], self.tp_sems, k, other_core()
        )

    def copy(self, k):
        return remote(
            self.held.at[k], self.landed.at[k - 1], self.dp_sems, k, {"dp": ahead_on("dp", k)}
        )

    def last(self):
        return remote(self.sent, self.came, self.tp_sems, self.size, other_core())

    def both(self, k):
        group = ahead_on("dp", k)
        return self.part[group, self.mine].astype(jnp.float32) + self.held[k].astype(jnp.float32)

    def start(self, places_ref, slots_ref):
        def one(k):
            group = ahead_on("dp", k)
            self.part[group] = collect(places_ref, slots_ref, group).astype(jnp.bfloat16)
            self.swap(lax.rem(k, self.size)).start()

        each(self.size + 1, one)

    def forward(self):
        def one(k):
            self.swap(k).wait_recv()
            self.held[k] = self.both(k).astype(jnp.bfloat16)
            self.copy(k).start()

        each(self.size, one)
        self.swap(0).wait()
        self.total[...] = self.both(0)

    def gather(self):
        def one(k):
            self.copy(k).wait_recv()
            self.total[...] += self.landed[k - 1].astype(jnp.float32)

        each(self.size, one)
        self.sent[...] = self.total[...].astype(jnp.bfloat16)
        self.last().start()

    def finish(self):
        def one(k):
            self.swap(k).wait_send()
            self.copy(k).wait_send()

        each(self.size, one)
        self.last().wait()


def return_scratch(size, rows, width):
    low = jnp.bfloat16
    return [
        pltpu.VMEM((size, rows, width), low),
        pltpu.VMEM((size, rows // 2, width), low),
        pltpu.VMEM((size - 1, rows // 2, width), low),
        pltpu.VMEM((rows // 2, width), jnp.float32),
        pltpu.VMEM((rows // 2, width), low),
        pltpu.VMEM((rows // 2, width), low),
        *sem_pair(size),
        *sem_pair(size + 1),
    ]


def return_grads_kernel(
    slots_ref, places_ref, hidden_ref, cot_ref, gain_ref, out_w_ref, grad_ref, low_ref, mix_ref,
    gain_grad_ref, part, held, landed, total, sent, came, dp_send, dp_recv, tp_send, tp_recv,
):
    greet(["dp", "tp"])
    rows = RowReturn(
        part, held, landed, total, sent, came, (dp_send, dp_recv), (tp_send, tp_recv)
    )
    rows.start(places_ref, slots_ref)
    rows.forward()
    rows.gather()

    def turn_back(at, grads):
        x_grad, gain_grad = norm_back(
            hidden_ref[at, :], gain_ref[1:2, :], grads.astype(jnp.float32)
        )
        hidden_grad = cot_ref[at, :].astype(jnp.float32) + x_grad
        grad_ref[at, :] = hidden_grad
        low_ref[at, :] = hidden_grad.astype(jnp.bfloat16)
        piece = out_w_ref.shape[2]
        mix = None
        for i in range(out_w_ref.shape[0]):
            one = lax.dot_general(
                low_ref[at, i * piece : (i + 1) * piece],
                out_w_ref[i],
                NT,
                preferred_element_type=jnp.float32,
            )
            mix = one if mix is None else mix + one
        mix_ref[at, :] = mix.astype(jnp.bfloat16)
        return gain_grad

    gain_mine = turn_back(rows.mine, sent[...])
    rows.finish()
    gain_theirs = turn_back(rows.theirs, came[...])
    gain_grad_ref[...] = gain_mine + gain_theirs


def return_grads(slots, places, hidden, cot, gain, out_w, ident):
    size, (rows, width) = slots.shape[0], hidden.shape
    return pl.pallas_call(
        return_grads_kernel,
        name="return_grads",
        in_specs=whole_vmem(6),
        out_specs=whole_vmem(4),
        out_shape=[
            jax.ShapeDtypeStruct((rows, width), jnp.float32),
            jax.ShapeDtypeStruct((rows, width), jnp.bfloat16),
            jax.ShapeDtypeStruct((rows, out_w.shape[1]), jnp.bfloat16),
            jax.ShapeDtypeStruct((1, width), jnp.float32),
        ],
        scratch_shapes=return_scratch(size, rows, width),
        compiler_params=remote_params(ident),
    )(slots, places, hidden, cot, gain, out_w)


def trade_kernel(
    back, ahead, kv_grad_ref, slots_ref, places_ref, low_ref, mix_ref, kv_ref, out_ref, out_w_ref,
    going, came_kv, line_send, line_recv, part, held, landed, total, sent, came, dp_send, dp_recv,
    tp_send, tp_recv,
):
    me, size = lax.axis_index("ctx"), lax.axis_size("ctx")
    greet(["dp", "tp"], line=True)
    right, left = me + 1, me - 1
    sems = (line_send, line_recv)

    def hop(s, src):
        return remote(src, came_kv.at[s], sems, s, {"ctx": left})

    def forth():
        return remote(
            kv_grad_ref.at[lax.rem(me + 1, size)], came_kv.at[0], sems, 0, {"ctx": right}
        )

    def own_piece(s):
        return kv_grad_ref.at[lax.rem(me + size - s, size)]

    if ahead:

        @pl.when(right < size)
        def _():
            forth().start()

    @pl.when(me - back >= 0)
    def _():
        hop(back, own_piece(back)).start()

    rows = RowReturn(
        part, held, landed, total, sent, came, (dp_send, dp_recv), (tp_send, tp_recv)
    )
    rows.start(places_ref, slots_ref)
    rows.forward()
    turned = jnp.transpose(low_ref[...].astype(jnp.float32)).astype(jnp.bfloat16)
    grad = jnp.dot(turned, mix_ref[...], preferred_element_type=jnp.float32)
    piece = out_w_ref.shape[1]
    for i in range(out_w_ref.shape[0]):
        out_w_ref[i] = grad[i * piece : (i + 1) * piece].astype(jnp.bfloat16)

    for s in range(back - 1, 0, -1):

        @pl.when((me - s >= 0) & (right < size))
        def _(s=s):
            hop(s + 1, going.at[s]).wait_recv()
            going[s] = (
                own_piece(s)[...].astype(jnp.float32) + came_kv[s + 1].astype(jnp.float32)
            ).astype(going.dtype)
            hop(s, going.at[s]).start()

        @pl.when((me - s >= 0) & (right >= size))
        def _(s=s):
            hop(s, own_piece(s)).start()

    rows.gather()
    kv_ref[...] = kv_grad_ref[me].astype(jnp.float32)

    @pl.when(right < size)
    def _():
        hop(1, going.at[0]).wait_recv()
        kv_ref[...] += came_kv[1].astype(jnp.float32)

    if ahead:

        @pl.when(left >= 0)
        def _():
            forth().wait_recv()
            kv_ref[...] += came_kv[0].astype(jnp.float32)

        @pl.when(right < size)
        def _():
            forth().wait_send()

    for s in range(back, 0, -1):

        @pl.when(me - s >= 0)
        def _(s=s):
            hop(s, going.at[0]).wait_send()

    rows.finish()
    out_ref[rows.mine, :] = sent[...]
    out_ref[rows.theirs, :] = came[...]


def trade(kv_grad, slots, places, low, mix, back, ahead, ident):
    size, (rows, width) = slots.shape[0], low.shape
    kv_shape = kv_grad.shape[1:]
    going = pltpu.VMEM((max(back, 1),) + kv_shape, kv_grad.dtype)
    came = pltpu.VMEM((back + 1,) + kv_shape, kv_grad.dtype)
    return pl.pallas_call(
        functools.partial(trade_kernel, back, ahead),
        name="trade",
        in_specs=whole_vmem(5),
        out_specs=whole_vmem(3),
        out_shape=[
            jax.ShapeDtypeStruct(kv_shape, jnp.float32),
            jax.ShapeDtypeStruct((rows, width), jnp.bfloat16),
            jax.ShapeDtypeStruct((size, width // size, mix.shape[1]), jnp.bfloat16),
        ],
        scratch_shapes=[
            going, came, *sem_pair(back + 1), *return_scratch(size, rows, width)
        ],
        compiler_params=remote_params(ident),
    )(kv_grad, slots, places, low, mix)


class PieceSum:
    def __init__(self, axis, source, landed, sems):
        self.axis, self.source, self.landed, self.sems = axis, source, landed, sems
        self.size = lax.axis_size(axis)

    def copy(self, k):
        peer = ahead_on(self.axis, k)
        return remote(
            self.source.at[peer], self.landed.at[k], self.sems, k, {self.axis: peer}
        )

    def send(self, k):
        self.copy(k).start()

    def total(self):
        each(self.size, lambda k: self.copy(k).wait_recv())
        whole = self.source[lax.axis_index(self.axis)].astype(jnp.float32)
        for k in range(1, self.size):
            whole += self.landed[k].astype(jnp.float32)
        return whole

    def finish(self):
        each(self.size, lambda k: self.copy(k).wait_send())


class WholeSum:
    def __init__(self, axis, source, landed, sems):
        self.axis, self.source, self.landed, self.sems = axis, source, landed, sems
        self.size = lax.axis_size(axis)

    def copy(self, k):
        return remote(
            self.source, self.landed.at[k], self.sems, k, {self.axis: ahead_on(self.axis, k)}
        )

    def start(self):
        each(self.size, lambda k: self.copy(k).start())

    def total(self):
        each(self.size, lambda k: self.copy(k).wait())
        whole = self.source[...]
        for k in range(1, self.size):
            whole += self.landed[k]
        return whole


def finish_kernel(
    dq_ref, dkv_ref, cos_ref, sin_ref, normed_ref, w_ref, x_ref, gain_ref, out_w_ref, gain_two_ref,
    in_ref, own_ref, gains_ref, joined, turned, part, held, pieces, landed,
    out_landed, low, low_landed, gain_rows, gain_landed, gain_more, gain_more_landed, *sems,
):
    greet(["dp", "ctx", "tp"])
    pairs = [sems[2 * i : 2 * i + 2] for i in range(len(sems) // 2)]
    out_sum = PieceSum("dp", out_w_ref, out_landed, pairs[0])
    each(out_sum.size, out_sum.send)
    wide = 2 * HEAD_DIM
    q_width, kv_width = dq_ref.shape[1], dkv_ref.shape[1] // 2
    tokens = dq_ref.shape[0]
    here = pl.ds(pl.multiple_of(lax.axis_index("ctx") * tokens, tokens), tokens)
    for first in range(0, q_width, wide):
        joined[:, first : first + wide] = turn(
            dq_ref[:, first : first + wide], cos_ref[here, :], sin_ref[here, :]
        ).astype(jnp.bfloat16)
    for first in range(0, kv_width, wide):
        joined[:, q_width + first : q_width + first + wide] = turn(
            dkv_ref[:, first : first + wide], cos_ref[here, :], sin_ref[here, :]
        ).astype(jnp.bfloat16)
    joined[:, q_width + kv_width :] = dkv_ref[:, kv_width:].astype(jnp.bfloat16)

    turned[...] = jnp.transpose(normed_ref[...].astype(jnp.float32)).astype(jnp.bfloat16)
    w_sum = PieceSum("dp", pieces, landed, pairs[1])
    rows = pieces.shape[1]

    def piece(k):
        peer = ahead_on("dp", k)
        at = pl.ds(pl.multiple_of(peer * rows, rows), rows)
        pieces[peer] = jnp.dot(
            turned[at, :], joined[...], preferred_element_type=jnp.float32
        ).astype(jnp.bfloat16)
        w_sum.send(k)

    each(w_sum.size, piece)
    for i in range(w_ref.shape[0]):
        part[:, i * rows : (i + 1) * rows] = lax.dot_general(
            joined[...], w_ref[i], NT, preferred_element_type=jnp.float32
        ).astype(jnp.bfloat16)
    swap = remote(part, held, pairs[2], 0, other_core())
    swap.start()
    me = lax.axis_index("dp")
    own = pl.ds(pl.multiple_of(me * rows, rows), rows)
    pieces[me] = jnp.dot(
        turned[own, :], joined[...], preferred_element_type=jnp.float32
    ).astype(jnp.bfloat16)
    swap.wait()
    x_grad, gain_grad = norm_back(
        x_ref[...].astype(jnp.float32),
        gain_ref[0:1, :],
        part[...].astype(jnp.float32) + held[...].astype(jnp.float32),
    )
    in_ref[...] = x_grad
    gain_rows[...] = jnp.zeros(gain_rows.shape, jnp.float32)
    gain_rows[0:1, :] = gain_grad
    gain_rows[1:2, :] = gain_two_ref[...]
    gain_sum = WholeSum("dp", gain_rows, gain_landed, pairs[3])
    gain_sum.start()

    out_total = out_sum.total()
    w_total = w_sum.total()
    cols = w_total.shape[1]
    few = low.shape[1]
    for c in range(low.shape[0]):
        low[c, :, :cols] = w_total[c * few : (c + 1) * few].astype(jnp.bfloat16)
        low[c, :, cols:] = out_total[c * few : (c + 1) * few].astype(jnp.bfloat16)
    low_sum = PieceSum("ctx", low, low_landed, pairs[4])
    each(low_sum.size, low_sum.send)
    gain_more[...] = gain_sum.total()
    more_sum = WholeSum("ctx", gain_more, gain_more_landed, pairs[5])
    more_sum.start()
    out_sum.finish()
    w_sum.finish()
    own_ref[...] = low_sum.total()
    low_sum.finish()
    gains_ref[...] = more_sum.total()


def finish(dq, dkv, cosine, sine, normed, w, x, gain, out_w, gain_two, ident):
    rows, width = x.shape
    dp_size, ctx_size = lax.axis_size("dp"), lax.axis_size("ctx")
    cols, out_cols = w.shape[2], out_w.shape[2]
    few = width // dp_size // ctx_size
    low, high = jnp.bfloat16, jnp.float32
    return pl.pallas_call(
        finish_kernel,
        name="finish",
        in_specs=whole_vmem(10),
        out_specs=whole_vmem(3),
        out_shape=[
            jax.ShapeDtypeStruct((rows, width), high),
            jax.ShapeDtypeStruct((few, cols + out_cols), high),
            jax.ShapeDtypeStruct((8, width), high),
        ],
        scratch_shapes=[
            pltpu.VMEM((rows, cols), low),
            pltpu.VMEM((width, rows), low),
            pltpu.VMEM((rows, width), low),
            pltpu.VMEM((rows, width), low),
            pltpu.VMEM((dp_size, width // dp_size, cols), low),
            pltpu.VMEM((dp_size, width // dp_size, cols), low),
            pltpu.VMEM(out_w.shape, low),
            pltpu.VMEM((ctx_size, few, cols + out_cols), low),
            pltpu.VMEM((ctx_size, few, cols + out_cols), low),
            pltpu.VMEM((8, width), high),
            pltpu.VMEM((dp_size, 8, width), high),
            pltpu.VMEM((8, width), high),
            pltpu.VMEM((ctx_size, 8, width), high),
            *sem_pair(dp_size),
            *sem_pair(dp_size),
            *sem_pair(1),
            *sem_pair(dp_size),
            *sem_pair(ctx_size),
            *sem_pair(ctx_size),
        ],
        compiler_params=remote_params(ident),
    )(dq, dkv, cosine, sine, normed, w, x, gain, out_w, gain_two)


class Everyone:
    def __init__(self, axis, target, sems):
        self.axis, self.target, self.sems = axis, target, sems
        self.size = lax.axis_size(axis)

    def copy(self, k):
        at = self.target.at[lax.axis_index(self.axis)]
        return remote(at, at, self.sems, k, {self.axis: ahead_on(self.axis, k)})

    def start(self):
        each(self.size, lambda k: self.copy(k).start())

    def arrive(self):
        each(self.size, lambda k: self.copy(k).wait_recv())

    def finish(self):
        each(self.size, lambda k: self.copy(k).wait_send())


def find_places(first, own, routes_ref, gates_ref, earlier, place_ref, gate_ref, column_ref):
    _, tokens = routes_ref.shape[1:]

    def group(g, carry):
        routes, gates = routes_ref[g], gates_ref[g]
        names, values = [], []
        for e in range(own):
            named = routes == first + e
            names.append(jnp.max(named.astype(jnp.float32), axis=0, keepdims=True))
            values.append(jnp.sum(jnp.where(named, gates, 0.0), axis=0, keepdims=True))
        spare = jnp.zeros((8 - own % 8 if own % 8 else 0, tokens), jnp.float32)
        names = jnp.concatenate(names + ([spare] if spare.shape[0] else []), axis=0)
        place = jnp.dot(
            names.astype(jnp.bfloat16), earlier[...], preferred_element_type=jnp.float32
        )
        place = jnp.where((names > 0.0) & (place < CAP), place, -float(CAP * own))
        for e in range(own):
            place_ref[g, e] = place[e : e + 1].astype(jnp.int32)
            gate_ref[g, e] = values[e]
        column_ref[g] = jnp.transpose(place)[:, :own].astype(jnp.int32)
        return carry

    lax.fori_loop(0, routes_ref.shape[0], group, 0)


class LineRows:
    def __init__(self, x_ref, x_all, back, ahead, line_sems, tp_sems):
        self.x_ref, self.x_all, self.back, self.ahead = x_ref, x_all, back, ahead
        self.line_sems, self.tp_sems = line_sems, tp_sems
        self.me, self.size = lax.axis_index("ctx"), lax.axis_size("ctx")
        self.mine, _ = halves(x_ref.shape[0])

    def block(self, s):
        return lax.rem(self.me + self.size - s, self.size)

    def sends(self, s):
        return (self.me + 1 < self.size) & (self.me - s >= 0)

    def hop(self, s):
        at = self.x_all.at[self.block(s), self.mine]
        source = self.x_ref.at[self.mine] if isinstance(s, int) and s == 0 else at
        return remote(source, at, self.line_sems, s, {"ctx": self.me + 1})

    def back_hop(self):
        at = self.x_all.at[self.me, self.mine]
        return remote(
            self.x_ref.at[self.mine], at, self.line_sems, self.back, {"ctx": self.me - 1}
        )

    def relay(self, k, block):
        at = self.x_all.at[block, self.mine]
        return remote(at, at, self.tp_sems, k, other_core())

    def start(self):
        if self.back:
            pl.when(self.sends(0))(lambda: self.hop(0).start())
        if self.ahead:
            pl.when(self.me >= 1)(lambda: self.back_hop().start())

    def step(self, s):
        @pl.when(self.me - s - 1 >= 0)
        def _():
            self.hop(s).wait_recv()
            self.relay(s, self.block(s + 1)).start()

        if s + 1 < self.back:
            pl.when(self.sends(s + 1))(lambda: self.hop(s + 1).start())

    def step_back(self):
        if self.ahead:

            @pl.when(self.me + 1 < self.size)
            def _():
                self.back_hop().wait_recv()
                self.relay(self.back, self.block(self.size - 1)).start()

    def finish(self):
        for s in range(self.back):
            pl.when(self.sends(s))(lambda s=s: self.hop(s).wait_send())
        if self.ahead:
            pl.when(self.me >= 1)(lambda: self.back_hop().wait_send())


def front_kernel(
    back, ahead, own, starts_ref, x_ref, cot_ref, q_w_ref, k_w_ref, v_w_ref, out_w_ref, gains_ref,
    docs_ref, routes_ref, gates_ref, cos_ref, sin_ref, w_out, out_w_out, gain_rows, docs_all,
    normed_out, q_ref, kv_out, mix_ref, full_out, log_ref, hidden_out, rows_out, cot_out,
    place_ref, gate_ref, column_ref, w_all, out_w_all, normed, kv_all, full, hidden, x_all,
    gains_all, routes_all, gates_all, acc, top, total, column, part, held,
    normed_two, *sems,
):
    me, size = lax.axis_index("ctx"), lax.axis_size("ctx")
    dp = lax.axis_index("dp")
    local = sems[-1]
    pairs = [sems[2 * i : 2 * i + 2] for i in range(len(sems) // 2)]
    q_width, kv_width = q_w_ref.shape[1], k_w_ref.shape[1]
    dp_size, piece = w_all.shape[:2]
    block_rows = x_ref.shape[0]

    def flush(i, source, target):
        return pltpu.make_async_copy(source, target, local.at[i])

    w_all[dp, :, :q_width] = q_w_ref[...]
    w_all[dp, :, q_width : q_width + kv_width] = k_w_ref[...]
    w_all[dp, :, q_width + kv_width :] = v_w_ref[...]
    gains_all[dp] = gains_ref[...]
    docs_all[me] = docs_ref[...]
    routes_all[dp] = routes_ref[...]
    gates_all[dp] = gates_ref[...]
    greet(["dp", "ctx", "tp"])
    weights = Gather(w_all, pairs[1])
    gains = Everyone("dp", gains_all, pairs[0])
    docs = Everyone("ctx", docs_all, pairs[2])
    routes = Everyone("dp", routes_all, pairs[3])
    gates = Everyone("dp", gates_all, pairs[4])
    out_w = Gather(out_w_all, pairs[5])
    line = LineRows(x_ref, x_all, back, ahead, pairs[8], pairs[11])
    for one in (gains, weights, line, docs, routes, gates):
        one.start()

    out_w_all[dp] = out_w_ref[...]
    x_all[me] = x_ref[...]
    token = lax.broadcasted_iota(jnp.int32, (block_rows, block_rows), 0)
    later = lax.broadcasted_iota(jnp.int32, (block_rows, block_rows), 1)
    normed_two[:, :block_rows] = (token < later).astype(jnp.float32).astype(jnp.bfloat16)
    top[...] = jnp.full(top.shape, NEG_FILL, jnp.float32)
    total[...] = jnp.zeros(total.shape, jnp.float32)
    acc[...] = jnp.zeros(acc.shape, jnp.float32)
    gains.arrive()
    for i in range(dp_size):
        gain_rows[:, i * piece : (i + 1) * piece] = gains_all[i]

    def norm_rows(source):
        x = source.astype(jnp.float32)
        return (x * row_scale(x) * gain_rows[0:1, :]).astype(jnp.bfloat16)

    normed[...] = norm_rows(x_ref[...])
    flush(0, normed, normed_out).start()
    routes.arrive()
    gates.arrive()
    docs.arrive()
    if back:
        line.step(0)
    weights.forward()
    find_places(
        dp * own, own, routes_all, gates_all, normed_two.at[:, :block_rows], place_ref, gate_ref,
        column_ref,
    )
    weights.arrive()
    flush(1, w_all, w_out).start()
    out_w.start()
    cot_rows = RowGather(cot_ref, cot_out, pairs[6], pairs[7], 0)
    cot_rows.start()
    last = 2 + back + 1 + ahead
    flush(last + 3, cot_ref, cot_out.at[dp]).start()

    wide, tile = 4 * HEAD_DIM, 2 * HEAD_DIM

    def project(source, first):
        whole = jnp.dot(
            source[:, :piece], w_all[0, :, first : first + wide],
            preferred_element_type=jnp.float32,
        )
        for i in range(1, dp_size):
            whole += jnp.dot(
                source[:, i * piece : (i + 1) * piece], w_all[i, :, first : first + wide],
                preferred_element_type=jnp.float32,
            )
        return [whole[:, :tile], whole[:, tile:]]

    def tables(block):
        at = pl.ds(pl.multiple_of(block * block_rows, block_rows), block_rows)
        return cos_ref[at, :], -sin_ref[at, :]

    for first in range(0, q_width, wide):
        for i, part_of in enumerate(project(normed, first)):
            turned = turn(part_of, *tables(me)).astype(jnp.bfloat16)
            at = first + i * tile
            q_ref[:, at : at + tile] = (turned.astype(jnp.float32) * HEAD_DIM**-0.5).astype(
                jnp.bfloat16
            )
    for s in range(1, back):
        line.step(s)
    line.step_back()
    masks = Masks(docs_all, starts_ref, column)

    def visit(s, block):
        @pl.when(s > 0)
        def _():
            line.relay(s - 1, block).wait()

        part[...] = norm_rows(x_all[block])
        for first in range(q_width, q_width + 2 * kv_width, wide):
            for i, part_of in enumerate(project(part, first)):
                if first < q_width + kv_width:
                    part_of = turn(part_of, *tables(block))
                at = first - q_width + i * tile
                kv_all[block, :, at : at + tile] = part_of.astype(jnp.bfloat16)
        flush(2 + s, kv_all.at[block], kv_out.at[block]).start()
        attend_block(masks, block, q_ref, kv_all.at[block], acc, top, total)

    def step(s):
        pl.when(me - s >= 0)(lambda: visit(s, lax.rem(me + size - s, size)))

        @pl.when(s == min(1, back))
        def _():
            out_w.forward()
            cot_rows.forward()

    each(back + 1, step, 0)
    if ahead:

        @pl.when(me + 1 < size)
        def _():
            visit(back + 1, lax.rem(me + 1, size))

    log_ref[...] = top[...] + jnp.log(total[...])
    for h in range(total.shape[0]):
        at = slice(h * HEAD_DIM, (h + 1) * HEAD_DIM)
        acc[at, :] = acc[at, :] / total[h : h + 1, :]
    full[...] = jnp.transpose(acc[...])
    mix_ref[...] = full[...].astype(jnp.bfloat16)
    out_w.arrive()
    cot_rows.arrive()
    for i in range(dp_size):
        part[:, i * piece : (i + 1) * piece] = jnp.dot(
            mix_ref[...], out_w_all[i], preferred_element_type=jnp.float32
        ).astype(jnp.bfloat16)

    mine, theirs = halves(block_rows)
    rows = RowGather(normed_two, rows_out, pairs[9], pairs[10], 2)
    first = remote(part.at[theirs], held.at[theirs], pairs[10], 0, other_core())
    second = remote(part.at[mine], held.at[mine], pairs[10], 1, other_core())
    first.start()
    second.start()
    flush(last, full, full_out).start()
    flush(last + 1, out_w_all, out_w_out).start()

    def norm(at):
        whole = x_ref[at, :].astype(jnp.float32) + (
            part[at, :].astype(jnp.float32) + held[at, :].astype(jnp.float32)
        )
        hidden[at, :] = whole
        normed_two[at, :] = (whole * row_scale(whole) * gain_rows[1:2, :]).astype(jnp.bfloat16)

    first.wait()
    norm(mine)
    rows.start()
    second.wait()
    norm(theirs)
    flush(last + 2, hidden, hidden_out).start()
    flush(last + 4, normed_two, rows_out.at[dp]).start()
    cot_rows.finish()
    for one in (gains, weights, docs, routes, gates, out_w, line):
        one.finish()
    rows.forward()
    rows.arrive()
    rows.finish()
    flush(0, normed, normed_out).wait()
    flush(1, w_all, w_out).wait()

    def kept(s):
        @pl.when(me - s >= 0)
        def _():
            flush(2 + s, kv_all.at[me], kv_out.at[me]).wait()

    each(back + 1, kept, 0)
    if ahead:
        pl.when(me + 1 < size)(lambda: flush(3 + back, kv_all.at[me], kv_out.at[me]).wait())
    flush(last, full, full_out).wait()
    flush(last + 1, out_w_all, out_w_out).wait()
    flush(last + 2, hidden, hidden_out).wait()
    flush(last + 3, cot_ref, cot_out.at[dp]).wait()
    flush(last + 4, normed_two, rows_out.at[dp]).wait()


def front(
    starts, x, cot, q_w, k_w, v_w, out_w, gains, docs, routes, gates, cosine, sine, own, back,
    ahead, ident,
):
    rows, width = x.shape
    dp_size, ctx_size = lax.axis_size("dp"), lax.axis_size("ctx")
    q_width, kv_cols = q_w.shape[1], 2 * k_w.shape[1]
    piece, heads = q_w.shape[0], q_width // HEAD_DIM
    low, high, whole = jnp.bfloat16, jnp.float32, jnp.int32
    far = [
        ((dp_size, piece, q_width + kv_cols), low),
        ((dp_size,) + out_w.shape, low),
        ((rows, width), low),
        ((ctx_size, rows, kv_cols), low),
        ((rows, q_width), high),
        ((rows, width), high),
        ((dp_size, rows, width), low),
        ((dp_size, rows, width), low),
    ]
    shapes = [
        far[0],
        far[1],
        ((2, width), high),
        ((ctx_size, 1, rows), whole),
        far[2],
        ((rows, q_width), low),
        far[3],
        ((rows, q_width), low),
        far[4],
        ((heads, rows), high),
        far[5],
        far[6],
        far[7],
        ((dp_size, own, 1, rows), whole),
        ((dp_size, own, 1, rows), high),
        ((dp_size, rows, own), whole),
    ]
    return pl.pallas_call(
        functools.partial(front_kernel, back, ahead, own),
        name="front",
        in_specs=[pl.BlockSpec(memory_space=pltpu.SMEM)] + whole_vmem(12),
        out_specs=[
            pl.BlockSpec(memory_space=pl.ANY if shape in far else pltpu.VMEM) for shape in shapes
        ],
        out_shape=[jax.ShapeDtypeStruct(*shape) for shape in shapes],
        scratch_shapes=[
            *[pltpu.VMEM(*shape) for shape in far[:6]],
            pltpu.VMEM((ctx_size, rows, width), low),
            pltpu.VMEM((dp_size,) + gains.shape, high),
            pltpu.VMEM((dp_size,) + routes.shape, whole),
            pltpu.VMEM((dp_size,) + gates.shape, high),
            pltpu.VMEM((q_width, rows), high),
            pltpu.VMEM((heads, rows), high),
            pltpu.VMEM((heads, rows), high),
            pltpu.VMEM((rows, 8), whole),
            pltpu.VMEM((rows, width), low),
            pltpu.VMEM((rows, width), low),
            pltpu.VMEM((rows, width), low),
            *sem_pair(dp_size),
            *sem_pair(dp_size),
            *sem_pair(ctx_size),
            *sem_pair(dp_size),
            *sem_pair(dp_size),
            *sem_pair(dp_size),
            *sem_pair(dp_size),
            *sem_pair(dp_size),
            *sem_pair(back + 1),
            *sem_pair(dp_size),
            *sem_pair(dp_size + 2),
            *sem_pair(back + 1),
            pltpu.SemaphoreType.DMA((8 + back + ahead,)),
        ],
        compiler_params=remote_params(ident),
    )(starts, x, cot, q_w, k_w, v_w, out_w, gains, docs, routes, gates, cosine, sine)


GROUPS_AT_ONCE = 4


def experts_kernel(more, rows_ref, grads_ref, weights_ref, place_ref, gate_ref, *refs):
    outs_ref, backs_ref, weight_grad_ref, slots, slot_grads = refs[2 * more :]
    groups, tok_rows, _ = rows_ref.shape
    owners, part = weight_grad_ref.shape[1], weight_grad_ref.shape[5]
    slot_index = lax.broadcasted_iota(jnp.int32, (CAP, tok_rows), 0)
    gates = []
    for g in range(groups):
        picks = slot_index == place_ref[g, 0]
        gates.append(jnp.sum(jnp.where(picks, gate_ref[g, 0], 0.0), axis=1, keepdims=True))
        picks = picks.astype(jnp.float32).astype(jnp.bfloat16)
        at = slice(g * CAP, (g + 1) * CAP)
        slots[at, :] = jnp.dot(
            picks, rows_ref[g], preferred_element_type=jnp.float32
        ).astype(jnp.bfloat16)
        slot_grads[at, :] = (
            jnp.dot(picks, grads_ref[g], preferred_element_type=jnp.float32) * gates[g]
        ).astype(jnp.bfloat16)
    gate_w, up_w, down_w = (weights_ref.at[0, i] for i in range(3))
    gate_pre = jnp.dot(slots[...], gate_w[...], preferred_element_type=jnp.float32)
    up_pre = jnp.dot(slots[...], up_w[...], preferred_element_type=jnp.float32)
    act_grad = jnp.dot(slot_grads[...], down_w[...], preferred_element_type=jnp.float32)
    sig = 1.0 / (1.0 + jnp.exp(-gate_pre))
    silu = gate_pre * sig
    act_low = (silu * up_pre).astype(jnp.bfloat16)
    up_low = (act_grad * silu).astype(jnp.bfloat16)
    gate_low = (act_grad * up_pre * (sig * (1.0 + gate_pre * (1.0 - sig)))).astype(jnp.bfloat16)

    back = lax.dot_general(
        gate_low, gate_w[...], NT, preferred_element_type=jnp.float32
    ) + lax.dot_general(up_low, up_w[...], NT, preferred_element_type=jnp.float32)
    out = lax.dot_general(act_low, down_w[...], NT, preferred_element_type=jnp.float32)
    for g in range(groups):
        at = slice(g * CAP, (g + 1) * CAP)
        backs_ref[g] = back[at].astype(jnp.bfloat16)
        outs_ref[g] = (out[at] * gates[g]).astype(jnp.bfloat16)

    for i, (low, source) in enumerate(
        ((gate_low, slots), (up_low, slots), (act_low, slot_grads))
    ):
        turned = jnp.transpose(low.astype(jnp.float32)).astype(jnp.bfloat16)
        total = jnp.dot(turned, source[...], preferred_element_type=jnp.float32)
        for c in range(owners):
            weight_grad_ref[0, c, 0, i] = total[:, c * part : (c + 1) * part].astype(
                weight_grad_ref.dtype
            )


def experts(weights, place_rows, gate_rows, rows_all, grad_all, first, count, before):
    own, _, model_width, hidden = weights.shape
    groups, tok_rows, _ = rows_all.shape
    owners = lax.axis_size("ctx")
    at_once = min(GROUPS_AT_ONCE, groups)
    chunks = groups // at_once
    part = model_width // owners
    rows_spec = pl.BlockSpec(
        (at_once, tok_rows, model_width), lambda c, e: (c, 0, 0), pipeline_mode=pl.Buffered(1)
    )
    line_spec = pl.BlockSpec((at_once, 1, 1, tok_rows), lambda c, e: (c, e + first, 0, 0))
    slots_spec = pl.BlockSpec((at_once, CAP, model_width), lambda c, e: (c, e + first, 0))
    slots_shape = jax.ShapeDtypeStruct((groups, own * CAP, model_width), jnp.bfloat16)
    flops = count * groups * CAP * model_width * 2 * (9 * hidden + 2 * tok_rows)
    more = before is not None
    outs, backs, weight_part = pl.pallas_call(
        functools.partial(experts_kernel, more),
        name="experts",
        grid=(chunks, count),
        in_specs=[
            rows_spec,
            rows_spec,
            pl.BlockSpec((1, 3, model_width, hidden), lambda c, e: (e + first, 0, 0, 0)),
            line_spec,
            line_spec,
        ]
        + [pl.BlockSpec(memory_space=pl.ANY)] * (2 * more),
        out_specs=[
            slots_spec,
            slots_spec,
            pl.BlockSpec((1, owners, 1, 3, hidden, part), lambda c, e: (c, 0, e, 0, 0, 0)),
        ],
        out_shape=[
            slots_shape,
            slots_shape,
            jax.ShapeDtypeStruct((chunks, owners, count, 3, hidden, part), jnp.bfloat16),
        ],
        scratch_shapes=[
            pltpu.VMEM((at_once * CAP, model_width), jnp.bfloat16),
            pltpu.VMEM((at_once * CAP, model_width), jnp.bfloat16),
        ],
        input_output_aliases={5: 0, 6: 1} if more else {},
        compiler_params=pltpu.CompilerParams(vmem_limit_bytes=LIMIT),
        cost_estimate=pl.CostEstimate(
            flops=flops, bytes_accessed=4 * weights.size, transcendentals=0
        ),
    )(rows_all, grad_all, weights, place_rows, gate_rows, *(before if more else ()))
    if chunks == 1:
        return (outs, backs), weight_part[0]
    return (outs, backs), jnp.sum(weight_part.astype(jnp.float32), axis=0).astype(jnp.bfloat16)


def unfold_kernel(more, sums_ref, *refs):
    out_ref = refs[more]
    for i in range(sums_ref.shape[1]):
        out_ref[0, i] = jnp.transpose(sums_ref[0, i].astype(jnp.float32))


def unfold(sums, own, first, before):
    count, three, hidden, part = sums.shape
    more = before is not None
    return pl.pallas_call(
        functools.partial(unfold_kernel, more),
        name="unfold",
        grid=(count,),
        in_specs=[pl.BlockSpec((1, three, hidden, part), lambda e: (e, 0, 0, 0))]
        + [pl.BlockSpec(memory_space=pl.ANY)] * more,
        out_specs=pl.BlockSpec((1, three, part, hidden), lambda e: (e + first, 0, 0, 0)),
        out_shape=jax.ShapeDtypeStruct((own, three, part, hidden), jnp.float32),
        input_output_aliases={1: 0} if more else {},
        compiler_params=pltpu.CompilerParams(vmem_limit_bytes=LIMIT),
    )(sums, *([before] if more else []))


def rotary_tables(token_positions):
    half_dim = HEAD_DIM // 2
    inverse = THETA ** (-(jnp.arange(half_dim, dtype=jnp.float32) * 2.0 / HEAD_DIM))
    angles = token_positions.astype(jnp.float32)[:, None] * inverse[None, :]
    cosine, sine = jnp.cos(angles), jnp.sin(angles)
    return jnp.concatenate([cosine] * 4, axis=1), jnp.concatenate([sine, -sine] * 2, axis=1)


def expert_counts(own):
    return (1, 2, 3, 2) if own == 8 else (own - own // 2, own // 2)


def scatter(grads):
    return lax.psum_scatter(grads, "ctx", scatter_dimension=0)


def body(
    tokens,
    query_weight,
    key_weight,
    value_weight,
    output_weight,
    gain_attn,
    gain_moe,
    expert_weights,
    routes,
    gate_values,
    documents,
    pic_starts,
    cotangent,
):
    block_len = tokens.shape[1]
    ctx_size = lax.axis_size("ctx")
    length = block_len * ctx_size
    back = back_blocks(ctx_size, block_len, length)
    ahead = ahead_blocks(block_len, length, pic_starts.shape[1])
    q_width, kv_width = query_weight.shape[1], key_weight.shape[1]
    own = expert_weights.shape[0]
    x, cot = tokens[0], cotangent[0]

    cosine, sine = rotary_tables(jnp.arange(length, dtype=jnp.int32))
    (
        w_all,
        out_w_all,
        gain_rows,
        docs_all,
        normed_one,
        query,
        kv_all,
        mixture,
        mix_full,
        log_total,
        hidden,
        rows_all,
        grad_all,
        *places,
    ) = front(
        pic_starts,
        x,
        cot,
        query_weight,
        key_weight,
        value_weight,
        output_weight,
        jnp.stack([gain_attn, gain_moe]).astype(jnp.float32),
        documents,
        routes[0].T,
        gate_values[0].T,
        cosine,
        sine,
        own,
        back,
        ahead,
        1,
    )
    place_rows, gate_rows, places = places
    counts = expert_counts(own)
    slots, sums = None, []
    first = 0
    for n, count in enumerate(counts):
        slots, grads = experts(
            expert_weights, place_rows, gate_rows, rows_all, grad_all, first, count, slots
        )
        if n < len(counts) - 1:
            sums.append((scatter(grads), first))
        first += count
    outs, backs = slots
    hidden_grad, hidden_low, mix_grad, gain_two_grad = return_grads(
        backs, places, hidden, cot, gain_rows, out_w_all, 2
    )
    q_rot_grad, kv_part = attend_back(
        pic_starts, query, kv_all, docs_all, log_total, mix_full, mix_grad, back, ahead
    )
    kv_back, expert_sum, output_grad = trade(
        kv_part,
        outs,
        places,
        hidden_low,
        mixture,
        back,
        ahead,
        3,
    )
    grads, kv_back = lax.optimization_barrier((grads, kv_back))
    sums.append((scatter(grads), own - counts[-1]))
    x_grad, owned, gain_sums = finish(
        q_rot_grad,
        kv_back,
        cosine,
        sine,
        normed_one,
        w_all,
        x,
        gain_rows,
        output_grad,
        gain_two_grad,
        4,
    )
    few = owned.shape[0]
    here = (lax.axis_index("dp") * ctx_size + lax.axis_index("ctx")) * few
    gain_sums = lax.dynamic_slice_in_dim(gain_sums, here, few, 1)
    expert_grad = None
    for part, first in sums:
        expert_grad = unfold(part, own, first, expert_grad)
    v_end = q_width + 2 * kv_width
    return (
        (hidden + expert_sum.astype(jnp.float32)).astype(jnp.bfloat16)[None],
        (hidden_grad + x_grad).astype(jnp.bfloat16)[None],
        owned[:, :q_width],
        owned[:, q_width : q_width + kv_width],
        owned[:, q_width + kv_width : v_end],
        owned[:, v_end:].T,
        gain_sums[0],
        gain_sums[1],
        expert_grad,
    )


def solution(mesh):
    return jax.shard_map(
        body,
        mesh=mesh,
        in_specs=(
            P("dp", "ctx", None),
            P("dp", "tp"),
            P("dp", "tp"),
            P("dp", "tp"),
            P("tp", "dp"),
            P("dp"),
            P("dp"),
            P("dp", None, None, "tp"),
            P("dp", "ctx", None),
            P("dp", "ctx", None),
            P("dp", "ctx"),
            P("dp", None),
            P("dp", "ctx", None),
        ),
        out_specs=(
            P("dp", "ctx", None),
            P("dp", "ctx", None),
            P(("dp", "ctx"), "tp"),
            P(("dp", "ctx"), "tp"),
            P(("dp", "ctx"), "tp"),
            P("tp", ("dp", "ctx")),
            P(("dp", "ctx")),
            P(("dp", "ctx")),
            P("dp", None, "ctx", "tp"),
        ),
        check_vma=False,
    )
```

```python
import functools

import jax
import jax.numpy as jnp
from jax import lax
from jax.experimental import pallas as pl
from jax.experimental.pallas import tpu as pltpu
from jax.sharding import PartitionSpec as P

HEAD_DIM = 64
PIC = 256
CAP = 144

EPSILON = 1e-06
THETA = 10000.0
NEG_FILL = -1e30


KEY_ROWS = 256
NT = (((1,), (1,)), ((), ()))
LIMIT = 67043328


def whole_vmem(count):
    return [pl.BlockSpec(memory_space=pltpu.VMEM)] * count


def picture_ids(starts_ref, places):
    ids = jnp.full(places.shape, -1, jnp.int32)
    for j in range(starts_ref.shape[1]):
        start = starts_ref[0, j]
        ids += jnp.where((places >= start) & (places < start + PIC), j + 1, 0)
    return ids


def as_column(row):
    tall = jnp.broadcast_to(row.astype(jnp.float32), (8, row.shape[1]))
    return jnp.transpose(tall)[:, 0:1].astype(jnp.int32)


class Masks:
    def __init__(self, docs_ref, starts_ref, column):
        self.docs_ref, self.starts_ref, self.column = docs_ref, starts_ref, column
        self.rows = docs_ref.shape[2]
        me = lax.axis_index("ctx")
        self.q_doc = docs_ref[me]
        self.q_place = me * self.rows + lax.broadcasted_iota(jnp.int32, (1, self.rows), 1)
        self.q_pic = picture_ids(starts_ref, self.q_place)

    def open(self, block):
        self.column[...] = jnp.broadcast_to(
            as_column(self.docs_ref[block]), self.column.shape
        )

    def bias(self, block, rows, first):
        k_doc = self.column[rows, 0:1]
        k_place = block * self.rows + first + lax.broadcasted_iota(jnp.int32, k_doc.shape, 0)
        k_pic = picture_ids(self.starts_ref, k_place)
        seen = (k_doc == self.q_doc) & (
            (k_place <= self.q_place) | ((k_pic == self.q_pic) & (self.q_pic >= 0))
        )
        return jnp.where(seen, 0.0, NEG_FILL)


def attend_block(masks, block, q_ref, kv_ref, acc, top, total):
    kv_width = kv_ref.shape[1] // 2
    heads, kv_heads = q_ref.shape[1] // HEAD_DIM, kv_width // HEAD_DIM
    masks.open(block)

    def step(j, carry):
        first = pl.multiple_of(j * KEY_ROWS, KEY_ROWS)
        rows = pl.ds(first, KEY_ROWS)
        bias = masks.bias(block, rows, first)
        for g in range(kv_heads):
            key = kv_ref[rows, g * HEAD_DIM : (g + 1) * HEAD_DIM]
            val = kv_ref[rows, kv_width + g * HEAD_DIM : kv_width + (g + 1) * HEAD_DIM]
            val_t = jnp.transpose(val.astype(jnp.float32)).astype(jnp.bfloat16)
            for h in range(g * heads // kv_heads, (g + 1) * heads // kv_heads):
                at = slice(h * HEAD_DIM, (h + 1) * HEAD_DIM)
                scores = bias + lax.dot_general(
                    key, q_ref[:, at], NT, preferred_element_type=jnp.float32
                )
                old = top[h : h + 1, :]
                new = jnp.maximum(old, jnp.max(scores, axis=0, keepdims=True))
                probs = jnp.exp(scores - new)
                fade = jnp.exp(old - new)
                total[h : h + 1, :] = total[h : h + 1, :] * fade + jnp.sum(
                    probs, axis=0, keepdims=True
                )
                acc[at, :] = acc[at, :] * fade + jnp.dot(
                    val_t, probs.astype(jnp.bfloat16), preferred_element_type=jnp.float32
                )
                top[h : h + 1, :] = new
        return carry

    lax.fori_loop(0, kv_ref.shape[0] // KEY_ROWS, step, 0)


def attend_back_block(
    masks, edges, block, q_ref, kv_ref, log_ref, delta, grad_ref, acc, dkv_ref
):
    kv_width = kv_ref.shape[1] // 2
    heads, kv_heads = q_ref.shape[1] // HEAD_DIM, kv_width // HEAD_DIM
    masks.open(block)
    count = kv_ref.shape[0] // KEY_ROWS
    me = lax.axis_index("ctx")
    q_first, q_last = edges[me * count, 0], edges[me * count + count - 1, 1]

    def step(j, carry):
        at = block * count + j
        same = (edges[at, 0] <= q_last) & (edges[at, 1] >= q_first)

        @pl.when(same)
        def _():
            inside(j)

        @pl.when(jnp.logical_not(same))
        def _():
            rows = pl.ds(pl.multiple_of(j * KEY_ROWS, KEY_ROWS), KEY_ROWS)
            dkv_ref[rows, :] = jnp.zeros((KEY_ROWS, dkv_ref.shape[1]), dkv_ref.dtype)

        return carry

    def inside(j):
        first = pl.multiple_of(j * KEY_ROWS, KEY_ROWS)
        rows = pl.ds(first, KEY_ROWS)
        bias = masks.bias(block, rows, first)
        for g in range(kv_heads):
            k_at = slice(g * HEAD_DIM, (g + 1) * HEAD_DIM)
            v_at = slice(kv_width + g * HEAD_DIM, kv_width + (g + 1) * HEAD_DIM)
            key, val = kv_ref[rows, k_at], kv_ref[rows, v_at]
            key_t = jnp.transpose(key.astype(jnp.float32)).astype(jnp.bfloat16)
            dk = jnp.zeros((KEY_ROWS, HEAD_DIM), jnp.float32)
            dv = jnp.zeros((KEY_ROWS, HEAD_DIM), jnp.float32)
            for h in range(g * heads // kv_heads, (g + 1) * heads // kv_heads):
                at = slice(h * HEAD_DIM, (h + 1) * HEAD_DIM)
                q_rows, g_rows = q_ref[:, at], grad_ref[:, at]
                scores = bias + lax.dot_general(
                    key, q_rows, NT, preferred_element_type=jnp.float32
                )
                probs = jnp.exp(scores - log_ref[h : h + 1, :])
                prob_grad = lax.dot_general(val, g_rows, NT, preferred_element_type=jnp.float32)
                slope = (probs * (prob_grad - delta[h : h + 1, :])).astype(jnp.bfloat16)
                dv += jnp.dot(
                    probs.astype(jnp.bfloat16), g_rows, preferred_element_type=jnp.float32
                )
                dk += jnp.dot(slope, q_rows, preferred_element_type=jnp.float32)
                acc[at, :] += jnp.dot(key_t, slope, preferred_element_type=jnp.float32)
            dkv_ref[rows, k_at] = dk.astype(dkv_ref.dtype)
            dkv_ref[rows, v_at] = dv.astype(dkv_ref.dtype)

    lax.fori_loop(0, count, step, 0)


def attend_back_kernel(
    back, ahead, starts_ref, edges, q_ref, kv_ref, docs_ref, log_ref, full_ref, grad_ref, dq_ref,
    dkv_ref, acc, delta, column,
):
    me, size = lax.axis_index("ctx"), lax.axis_size("ctx")
    acc[...] = jnp.transpose(full_ref[...] * grad_ref[...].astype(jnp.float32))
    for h in range(delta.shape[0]):
        delta[h : h + 1, :] = jnp.sum(
            acc[h * HEAD_DIM : (h + 1) * HEAD_DIM, :], axis=0, keepdims=True
        )
    acc[...] = jnp.zeros(acc.shape, jnp.float32)
    masks = Masks(docs_ref, starts_ref, column)

    def step(s, carry):
        block = me + ahead - s

        @pl.when((block >= 0) & (block < size))
        def _():
            attend_back_block(
                masks, edges, block, q_ref, kv_ref.at[block], log_ref, delta, grad_ref, acc,
                dkv_ref.at[block],
            )

        return carry

    lax.fori_loop(0, back + ahead + 1, step, 0)
    dq_ref[...] = jnp.transpose(acc[...]) * (HEAD_DIM**-0.5)


def attend_back(starts, q, kv, docs, log_total, full, grad, back, ahead):
    rows, width = q.shape
    by_block = docs.reshape(-1, KEY_ROWS)
    edges = jnp.concatenate([by_block[:, :1], by_block[:, -1:]], axis=1)
    return pl.pallas_call(
        functools.partial(attend_back_kernel, back, ahead),
        name="attend_back",
        in_specs=[pl.BlockSpec(memory_space=pltpu.SMEM)] * 2 + whole_vmem(6),
        out_specs=whole_vmem(2),
        out_shape=[
            jax.ShapeDtypeStruct((rows, width), jnp.float32),
            jax.ShapeDtypeStruct(kv.shape, jnp.bfloat16),
        ],
        scratch_shapes=[
            pltpu.VMEM((width, rows), jnp.float32),
            pltpu.VMEM((width // HEAD_DIM, rows), jnp.float32),
            pltpu.VMEM((rows, 8), jnp.int32),
        ],
        compiler_params=pltpu.CompilerParams(vmem_limit_bytes=LIMIT),
    )(starts, edges, q, kv, docs, log_total, full, grad)


MESH = pl.DeviceIdType.MESH


def greet(axes_list, line=False):
    barrier = pltpu.get_barrier_semaphore()
    count = 0
    for axis in axes_list:
        me, size = lax.axis_index(axis), lax.axis_size(axis)

        def signal(k, carry, axis=axis, me=me, size=size):
            pl.semaphore_signal(
                barrier, inc=1, device_id={axis: lax.rem(me + k, size)}, device_id_type=MESH
            )
            return carry

        lax.fori_loop(1, size, signal, 0)
        count += size - 1
    if not line:
        pl.semaphore_wait(barrier, count)
        return
    me, size = lax.axis_index("ctx"), lax.axis_size("ctx")
    for step in (1, -1):
        other = me + step

        @pl.when((other >= 0) & (other < size))
        def _(other=other):
            pl.semaphore_signal(barrier, inc=1, device_id={"ctx": other}, device_id_type=MESH)

    inner = (me > 0) & (me < size - 1)

    @pl.when(inner)
    def _():
        pl.semaphore_wait(barrier, count + 2)

    @pl.when(jnp.logical_not(inner))
    def _():
        pl.semaphore_wait(barrier, count + 1)


def remote(src, dst, sems, k, device_id):
    return pltpu.make_async_remote_copy(
        src_ref=src,
        dst_ref=dst,
        send_sem=sems[0].at[k],
        recv_sem=sems[1].at[k],
        device_id=device_id,
        device_id_type=MESH,
    )


def other_core():
    return {"tp": 1 - lax.axis_index("tp")}


def ahead_on(axis, k):
    return lax.rem(lax.axis_index(axis) + k, lax.axis_size(axis))


def each(count, do, first=1):
    def step(k, carry):
        do(k)
        return carry

    lax.fori_loop(first, count, step, 0)


def sem_pair(count):
    return [pltpu.SemaphoreType.DMA((count,)), pltpu.SemaphoreType.DMA((count,))]


def remote_params(ident):
    return pltpu.CompilerParams(
        collective_id=ident, has_side_effects=True, vmem_limit_bytes=LIMIT
    )


def halves(rows):
    half = rows // 2
    core = lax.axis_index("tp")
    return (
        pl.ds(pl.multiple_of(core * half, half), half),
        pl.ds(pl.multiple_of((1 - core) * half, half), half),
    )


def turn(tile, cosine, sine):
    lane = lax.broadcasted_iota(jnp.int32, tile.shape, 1)
    half = HEAD_DIM // 2
    swapped = jnp.where(
        lax.rem(lane, HEAD_DIM) < half,
        pltpu.roll(tile, 2 * HEAD_DIM - half, 1),
        pltpu.roll(tile, half, 1),
    )
    return tile * cosine + swapped * sine


def block_tables(cos_ref, sin_ref, rows, block):
    start = pl.ds(rows + block, 1)
    in_cos, in_sin = cos_ref[:rows, :], sin_ref[:rows, :]
    at_cos, at_sin = cos_ref[start, :], sin_ref[start, :]
    return in_cos * at_cos - in_sin * at_sin, in_sin * at_cos + in_cos * at_sin


def row_scale(x):
    return lax.rsqrt(jnp.mean(x * x, axis=-1, keepdims=True) + EPSILON)


def norm_back(x, gain, grad):
    scale = row_scale(x)
    unit = x * scale
    pull = grad * gain
    return (
        scale * (pull - unit * jnp.mean(pull * unit, axis=-1, keepdims=True)),
        jnp.sum(grad * unit, axis=0, keepdims=True),
    )


def back_blocks(ctx_size, block_len, length):
    return min(ctx_size - 1, -(-(length // 2 - 1) // block_len))


def ahead_blocks(block_len, length, spans):
    return 0 if block_len % (length // spans) == 0 else 1


def grid_peers():
    me = lax.axis_index("dp")
    x, y = lax.rem(me, 2), lax.div(me, 2)
    return y * 2 + 1 - x, (1 - y) * 2 + x, 3 - me


class Gather:
    def __init__(self, target, sems, rows=None, source=None):
        self.target, self.sems, self.rows, self.source = target, sems, rows, source
        self.size = lax.axis_size("dp")
        self.grid = self.size == 4

    def at(self, place):
        return self.target.at[place] if self.rows is None else self.target.at[place, self.rows]

    def half(self, place, n):
        if self.rows is None:
            count = self.target.shape[1] // 2
            return self.target.at[place, pl.ds(n * count, count)]
        count = self.rows.size // 2
        first = pl.multiple_of(self.rows.start + n * count, count)
        return self.target.at[place, pl.ds(first, count)]

    def first(self, k, peer):
        place = self.at(lax.axis_index("dp"))
        source = place if self.source is None else self.source.at[self.rows]
        return remote(source, place, self.sems, k, {"dp": peer})

    def passed(self, k, place, n, peer):
        at = self.half(place, n)
        return remote(at, at, self.sems, k, {"dp": peer})

    def direct(self, k):
        return self.first(k, ahead_on("dp", k))

    def start(self):
        if not self.grid:
            each(self.size, lambda k: self.direct(k).start())
            return
        x, y, _ = grid_peers()
        self.first(0, x).start()
        self.first(1, y).start()

    def forward(self, came=None):
        if not self.grid:
            return
        x, y, _ = grid_peers()
        self.first(0, x).wait_recv()
        self.passed(2, x, 0, y).start()
        if came:
            came(0, self.at(x))
        self.first(1, y).wait_recv()
        self.passed(3, y, 1, x).start()
        if came:
            came(1, self.at(y))

    def arrive(self, came=None):
        if not self.grid:

            def one(k):
                self.direct(k).wait_recv()
                if came:
                    came(k, self.at(ahead_on("dp", self.size - k)))

            each(self.size, one)
            return
        x, _, diagonal = grid_peers()
        for n in range(2):
            self.passed(2 + n, diagonal, n, x).wait_recv()
            if came:
                came(2 + n, self.half(diagonal, n))

    def finish(self):
        if not self.grid:
            each(self.size, lambda k: self.direct(k).wait_send())
            return
        x, y, _ = grid_peers()
        self.first(0, x).wait_send()
        self.first(1, y).wait_send()
        self.passed(2, x, 0, y).wait_send()
        self.passed(3, y, 1, x).wait_send()


class RowGather:
    def __init__(self, source, target, dp_sems, tp_sems, first):
        mine, _ = halves(source.shape[0])
        self.gather = Gather(target, dp_sems, mine, source)
        self.tp_sems, self.after = tp_sems, first

    def relay(self, k, at):
        return remote(at, at, self.tp_sems, self.after + k, other_core())

    def came(self, k, at):
        self.relay(k, at).start()

    def start(self):
        self.gather.start()

    def forward(self):
        self.gather.forward(self.came)

    def arrive(self):
        self.gather.arrive(self.came)

    def finish(self):
        self.gather.finish()
        gather = self.gather
        if not gather.grid:
            each(
                gather.size,
                lambda k: self.relay(k, gather.at(ahead_on("dp", gather.size - k))).wait(),
            )
            return
        x, y, diagonal = grid_peers()
        self.relay(0, gather.at(x)).wait()
        self.relay(1, gather.at(y)).wait()
        self.relay(2, gather.half(diagonal, 0)).wait()
        self.relay(3, gather.half(diagonal, 1)).wait()


def collect(places_ref, slots_ref, group):
    tok_rows, slot_count = places_ref.shape[1], slots_ref.shape[1]
    tiles = []
    for first in range(0, slot_count, 128):
        wide = min(128, slot_count - first)
        lane = first + lax.broadcasted_iota(jnp.int32, (tok_rows, wide), 1)
        hit = None
        for n in range(first // CAP, (first + wide - 1) // CAP + 1):
            one = places_ref[group, :, n : n + 1] == lane - n * CAP
            hit = one if hit is None else hit | one
        tiles.append(hit.astype(jnp.float32).astype(jnp.bfloat16))
    return jnp.dot(
        jnp.concatenate(tiles, axis=1), slots_ref[group], preferred_element_type=jnp.float32
    )


class GridSum:
    def __init__(self, piece, landed, sems):
        self.piece, self.landed, self.sems = piece, landed, sems
        self.x, self.y, _ = grid_peers()
        self.count = landed.shape[1] // 2

    def half(self, n, which):
        return self.piece(n).at[pl.ds(which * self.count, self.count)]

    def slot(self, j):
        return self.landed.at[j // 2, pl.ds(j % 2 * self.count, self.count)]

    def copy(self, j):
        n, which, peer = (
            (1, 0, self.x),
            (3, 0, self.x),
            (2, 1, self.y),
            (3, 1, self.y),
            (2, 0, self.y),
            (1, 1, self.x),
        )[j]
        return remote(self.half(n, which), self.slot(j), self.sems, j, {"dp": peer})

    def start(self):
        for j in (1, 3, 0, 2):
            self.copy(j).start()

    def forward(self):
        for j, n, which in ((1, 2, 0), (3, 1, 1)):
            self.copy(j).wait_recv()
            half = self.half(n, which)
            half[...] = (
                half[...].astype(jnp.float32) + self.slot(j)[...].astype(jnp.float32)
            ).astype(jnp.bfloat16)
            self.copy(4 + j // 2).start()

    def add_to(self, total):
        for which, slots in ((0, (0, 4)), (1, (2, 5))):
            at = pl.ds(which * self.count, self.count)
            for j in slots:
                self.copy(j).wait_recv()
                total[at, :] += self.slot(j)[...].astype(jnp.float32)

    def finish(self):
        for j in range(6):
            self.copy(j).wait_send()


class RowReturn:
    def __init__(self, part, held, landed, total, sent, came, dp_sems, tp_sems):
        self.part, self.held, self.landed, self.total = part, held, landed, total
        self.sent, self.came, self.dp_sems, self.tp_sems = sent, came, dp_sems, tp_sems
        self.size = lax.axis_size("dp")
        self.mine, self.theirs = halves(part.shape[1])
        self.grid = self.size == 4
        if self.grid:
            self.sum = GridSum(lambda n: held.at[n], landed, dp_sems)

    def group(self, k):
        if not self.grid:
            return ahead_on("dp", k)
        me = lax.axis_index("dp")
        x, y = lax.rem(me, 2), lax.div(me, 2)
        flip_x, flip_y = lax.rem(k, 2), lax.div(k, 2)
        return lax.rem(y + flip_y, 2) * 2 + lax.rem(x + flip_x, 2)

    def swap(self, k):
        return remote(
            self.part.at[self.group(k), self.theirs], self.held.at[k], self.tp_sems, k,
            other_core(),
        )

    def copy(self, k):
        return remote(
            self.held.at[k], self.landed.at[k - 1], self.dp_sems, k, {"dp": ahead_on("dp", k)}
        )

    def last(self):
        return remote(self.sent, self.came, self.tp_sems, self.size, other_core())

    def both(self, k):
        return self.part[self.group(k), self.mine].astype(jnp.float32) + self.held[k].astype(
            jnp.float32
        )

    def start(self, places_ref, slots_ref):
        def one(k):
            k = lax.rem(k, self.size)
            group = self.group(k)
            self.part[group] = collect(places_ref, slots_ref, group).astype(jnp.bfloat16)
            self.swap(k).start()

        each(self.size + 1, one)

    def forward(self):
        def one(k):
            self.swap(k).wait_recv()
            self.held[k] = self.both(k).astype(jnp.bfloat16)
            if not self.grid:
                self.copy(k).start()

        each(self.size, one)
        if self.grid:
            self.sum.start()
        self.swap(0).wait()
        self.total[...] = self.both(0)

    def pass_on(self):
        if self.grid:
            self.sum.forward()

    def gather(self):
        def one(k):
            self.copy(k).wait_recv()
            self.total[...] += self.landed[k - 1].astype(jnp.float32)

        if self.grid:
            self.sum.add_to(self.total)
        else:
            each(self.size, one)
        self.sent[...] = self.total[...].astype(jnp.bfloat16)
        self.last().start()

    def finish(self):
        def one(k):
            self.swap(k).wait_send()
            if not self.grid:
                self.copy(k).wait_send()

        each(self.size, one)
        if self.grid:
            self.sum.finish()
        self.last().wait()


def return_scratch(size, rows, width):
    low = jnp.bfloat16
    return [
        pltpu.VMEM((size, rows, width), low),
        pltpu.VMEM((size, rows // 2, width), low),
        pltpu.VMEM((size - 1, rows // 2, width), low),
        pltpu.VMEM((rows // 2, width), jnp.float32),
        pltpu.VMEM((rows // 2, width), low),
        pltpu.VMEM((rows // 2, width), low),
        *sem_pair(max(size, 6)),
        *sem_pair(size + 1),
    ]


def return_grads_kernel(
    slots_ref, places_ref, hidden_ref, cot_ref, gain_ref, out_w_ref, grad_ref, low_ref, mix_ref,
    gain_grad_ref, part, held, landed, total, sent, came, dp_send, dp_recv, tp_send, tp_recv,
):
    greet(["dp", "tp"])
    rows = RowReturn(
        part, held, landed, total, sent, came, (dp_send, dp_recv), (tp_send, tp_recv)
    )
    rows.start(places_ref, slots_ref)
    rows.forward()
    rows.pass_on()
    rows.gather()

    def turn_back(at, grads):
        x_grad, gain_grad = norm_back(
            hidden_ref[at, :], gain_ref[1:2, :], grads.astype(jnp.float32)
        )
        hidden_grad = cot_ref[at, :].astype(jnp.float32) + x_grad
        grad_ref[at, :] = hidden_grad
        low_ref[at, :] = hidden_grad.astype(jnp.bfloat16)
        piece = out_w_ref.shape[2]
        mix = None
        for i in range(out_w_ref.shape[0]):
            one = lax.dot_general(
                low_ref[at, i * piece : (i + 1) * piece],
                out_w_ref[i],
                NT,
                preferred_element_type=jnp.float32,
            )
            mix = one if mix is None else mix + one
        mix_ref[at, :] = mix.astype(jnp.bfloat16)
        return gain_grad

    gain_mine = turn_back(rows.mine, sent[...])
    rows.finish()
    gain_theirs = turn_back(rows.theirs, came[...])
    gain_grad_ref[...] = gain_mine + gain_theirs


def return_grads(slots, places, hidden, cot, gain, out_w, ident):
    size, (rows, width) = slots.shape[0], hidden.shape
    return pl.pallas_call(
        return_grads_kernel,
        name="return_grads",
        in_specs=whole_vmem(6),
        out_specs=whole_vmem(4),
        out_shape=[
            jax.ShapeDtypeStruct((rows, width), jnp.float32),
            jax.ShapeDtypeStruct((rows, width), jnp.bfloat16),
            jax.ShapeDtypeStruct((rows, out_w.shape[1]), jnp.bfloat16),
            jax.ShapeDtypeStruct((1, width), jnp.float32),
        ],
        scratch_shapes=return_scratch(size, rows, width),
        compiler_params=remote_params(ident),
    )(slots, places, hidden, cot, gain, out_w)


def trade_kernel(
    back, ahead, kv_grad_ref, slots_ref, places_ref, low_ref, mix_ref, kv_ref, out_ref, out_w_ref,
    going, came_kv, line_send, line_recv, part, held, landed, total, sent, came, dp_send, dp_recv,
    tp_send, tp_recv,
):
    me, size = lax.axis_index("ctx"), lax.axis_size("ctx")
    greet(["dp", "tp"], line=True)
    right, left = me + 1, me - 1
    sems = (line_send, line_recv)

    def hop(s, src):
        return remote(src, came_kv.at[s], sems, s, {"ctx": left})

    def forth():
        return remote(
            kv_grad_ref.at[lax.rem(me + 1, size)], came_kv.at[0], sems, 0, {"ctx": right}
        )

    def own_piece(s):
        return kv_grad_ref.at[lax.rem(me + size - s, size)]

    if ahead:

        @pl.when(right < size)
        def _():
            forth().start()

    @pl.when(me - back >= 0)
    def _():
        hop(back, own_piece(back)).start()

    rows = RowReturn(
        part, held, landed, total, sent, came, (dp_send, dp_recv), (tp_send, tp_recv)
    )
    rows.start(places_ref, slots_ref)
    rows.forward()
    turned = jnp.transpose(low_ref[...].astype(jnp.float32)).astype(jnp.bfloat16)
    grad = jnp.dot(turned, mix_ref[...], preferred_element_type=jnp.float32)
    piece = out_w_ref.shape[1]
    for i in range(out_w_ref.shape[0]):
        out_w_ref[i] = grad[i * piece : (i + 1) * piece].astype(jnp.bfloat16)
    rows.pass_on()

    for s in range(back - 1, 0, -1):

        @pl.when((me - s >= 0) & (right < size))
        def _(s=s):
            hop(s + 1, going.at[s]).wait_recv()
            going[s] = (
                own_piece(s)[...].astype(jnp.float32) + came_kv[s + 1].astype(jnp.float32)
            ).astype(going.dtype)
            hop(s, going.at[s]).start()

        @pl.when((me - s >= 0) & (right >= size))
        def _(s=s):
            hop(s, own_piece(s)).start()

    rows.gather()
    kv_ref[...] = kv_grad_ref[me].astype(jnp.float32)

    @pl.when(right < size)
    def _():
        hop(1, going.at[0]).wait_recv()
        kv_ref[...] += came_kv[1].astype(jnp.float32)

    if ahead:

        @pl.when(left >= 0)
        def _():
            forth().wait_recv()
            kv_ref[...] += came_kv[0].astype(jnp.float32)

        @pl.when(right < size)
        def _():
            forth().wait_send()

    for s in range(back, 0, -1):

        @pl.when(me - s >= 0)
        def _(s=s):
            hop(s, going.at[0]).wait_send()

    rows.finish()
    out_ref[rows.mine, :] = sent[...]
    out_ref[rows.theirs, :] = came[...]


def trade(kv_grad, slots, places, low, mix, back, ahead, ident):
    size, (rows, width) = slots.shape[0], low.shape
    kv_shape = kv_grad.shape[1:]
    going = pltpu.VMEM((max(back, 1),) + kv_shape, kv_grad.dtype)
    came = pltpu.VMEM((back + 1,) + kv_shape, kv_grad.dtype)
    return pl.pallas_call(
        functools.partial(trade_kernel, back, ahead),
        name="trade",
        in_specs=whole_vmem(5),
        out_specs=whole_vmem(3),
        out_shape=[
            jax.ShapeDtypeStruct(kv_shape, jnp.float32),
            jax.ShapeDtypeStruct((rows, width), jnp.bfloat16),
            jax.ShapeDtypeStruct((size, width // size, mix.shape[1]), jnp.bfloat16),
        ],
        scratch_shapes=[
            going, came, *sem_pair(back + 1), *return_scratch(size, rows, width)
        ],
        compiler_params=remote_params(ident),
    )(kv_grad, slots, places, low, mix)


class PieceSum:
    def __init__(self, axis, source, landed, sems):
        self.axis, self.source, self.landed, self.sems = axis, source, landed, sems
        self.size = lax.axis_size(axis)

    def copy(self, k):
        peer = ahead_on(self.axis, k)
        return remote(
            self.source.at[peer], self.landed.at[k], self.sems, k, {self.axis: peer}
        )

    def send(self, k):
        self.copy(k).start()

    def start(self):
        each(self.size, self.send)

    def forward(self):
        pass

    def total(self):
        each(self.size, lambda k: self.copy(k).wait_recv())
        whole = self.source[lax.axis_index(self.axis)].astype(jnp.float32)
        for k in range(1, self.size):
            whole += self.landed[k].astype(jnp.float32)
        return whole

    def finish(self):
        each(self.size, lambda k: self.copy(k).wait_send())


class GridPieceSum:
    def __init__(self, source, landed, sems, whole):
        x, y, diagonal = grid_peers()
        places = (lax.axis_index("dp"), x, y, diagonal)
        self.source, self.whole = source, whole
        self.sum = GridSum(lambda n: source.at[places[n]], landed, sems)
        self.start, self.forward, self.finish = self.sum.start, self.sum.forward, self.sum.finish

    def total(self):
        self.whole[...] = self.source[lax.axis_index("dp")].astype(jnp.float32)
        self.sum.add_to(self.whole)
        return self.whole[...]


def dp_sum(source, landed, sems, whole):
    if lax.axis_size("dp") == 4:
        return GridPieceSum(source, landed, sems, whole)
    return PieceSum("dp", source, landed, sems)


class WholeSum:
    def __init__(self, axis, source, landed, sems):
        self.axis, self.source, self.landed, self.sems = axis, source, landed, sems
        self.size = lax.axis_size(axis)

    def copy(self, k):
        return remote(
            self.source, self.landed.at[k], self.sems, k, {self.axis: ahead_on(self.axis, k)}
        )

    def start(self):
        each(self.size, lambda k: self.copy(k).start())

    def total(self):
        each(self.size, lambda k: self.copy(k).wait())
        whole = self.source[...]
        for k in range(1, self.size):
            whole += self.landed[k]
        return whole


def finish_kernel(
    dq_ref, dkv_ref, cos_ref, sin_ref, normed_ref, w_ref, x_ref, gain_ref, out_w_ref, gain_two_ref,
    in_ref, own_ref, gains_ref, joined, turned, part, held, pieces, landed,
    out_pieces, out_landed, whole, out_whole, low, low_landed, gain_rows, gain_landed, gain_more, gain_more_landed, *sems,
):
    greet(["dp", "ctx", "tp"])
    pairs = [sems[2 * i : 2 * i + 2] for i in range(len(sems) // 2)]
    out_pieces[...] = out_w_ref[...]
    out_sum = dp_sum(out_pieces, out_landed, pairs[0], out_whole)
    out_sum.start()
    wide = 2 * HEAD_DIM
    q_width, kv_width = dq_ref.shape[1], dkv_ref.shape[1] // 2
    cosine, sine = block_tables(cos_ref, sin_ref, dq_ref.shape[0], lax.axis_index("ctx"))
    for first in range(0, q_width, wide):
        joined[:, first : first + wide] = turn(
            dq_ref[:, first : first + wide], cosine, sine
        ).astype(jnp.bfloat16)
    for first in range(0, kv_width, wide):
        joined[:, q_width + first : q_width + first + wide] = turn(
            dkv_ref[:, first : first + wide], cosine, sine
        ).astype(jnp.bfloat16)
    joined[:, q_width + kv_width :] = dkv_ref[:, kv_width:].astype(jnp.bfloat16)

    turned[...] = jnp.transpose(normed_ref[...].astype(jnp.float32)).astype(jnp.bfloat16)
    w_sum = dp_sum(pieces, landed, pairs[1], whole)
    rows = pieces.shape[1]

    def piece(k):
        peer = ahead_on("dp", k)
        at = pl.ds(pl.multiple_of(peer * rows, rows), rows)
        pieces[peer] = jnp.dot(
            turned[at, :], joined[...], preferred_element_type=jnp.float32
        ).astype(jnp.bfloat16)

    each(pieces.shape[0], piece)
    w_sum.start()
    out_sum.forward()
    for i in range(w_ref.shape[0]):
        part[:, i * rows : (i + 1) * rows] = lax.dot_general(
            joined[...], w_ref[i], NT, preferred_element_type=jnp.float32
        ).astype(jnp.bfloat16)
    swap = remote(part, held, pairs[2], 0, other_core())
    swap.start()
    me = lax.axis_index("dp")
    own = pl.ds(pl.multiple_of(me * rows, rows), rows)
    pieces[me] = jnp.dot(
        turned[own, :], joined[...], preferred_element_type=jnp.float32
    ).astype(jnp.bfloat16)
    swap.wait()
    x_grad, gain_grad = norm_back(
        x_ref[...].astype(jnp.float32),
        gain_ref[0:1, :],
        part[...].astype(jnp.float32) + held[...].astype(jnp.float32),
    )
    in_ref[...] = x_grad
    gain_rows[...] = jnp.zeros(gain_rows.shape, jnp.float32)
    gain_rows[0:1, :] = gain_grad
    gain_rows[1:2, :] = gain_two_ref[...]
    gain_sum = WholeSum("dp", gain_rows, gain_landed, pairs[3])
    gain_sum.start()
    w_sum.forward()

    out_total = out_sum.total()
    w_total = w_sum.total()
    cols = w_total.shape[1]
    few = low.shape[1]
    for c in range(low.shape[0]):
        low[c, :, :cols] = w_total[c * few : (c + 1) * few].astype(jnp.bfloat16)
        low[c, :, cols:] = out_total[c * few : (c + 1) * few].astype(jnp.bfloat16)
    low_sum = PieceSum("ctx", low, low_landed, pairs[4])
    each(low_sum.size, low_sum.send)
    gain_more[...] = gain_sum.total()
    more_sum = WholeSum("ctx", gain_more, gain_more_landed, pairs[5])
    more_sum.start()
    out_sum.finish()
    w_sum.finish()
    own_ref[...] = low_sum.total()
    low_sum.finish()
    gains_ref[...] = more_sum.total()


def finish(dq, dkv, cosine, sine, normed, w, x, gain, out_w, gain_two, ident):
    rows, width = x.shape
    dp_size, ctx_size = lax.axis_size("dp"), lax.axis_size("ctx")
    cols, out_cols = w.shape[2], out_w.shape[2]
    few = width // dp_size // ctx_size
    low, high = jnp.bfloat16, jnp.float32
    return pl.pallas_call(
        finish_kernel,
        name="finish",
        in_specs=whole_vmem(10),
        out_specs=whole_vmem(3),
        out_shape=[
            jax.ShapeDtypeStruct((rows, width), high),
            jax.ShapeDtypeStruct((few, cols + out_cols), high),
            jax.ShapeDtypeStruct((8, width), high),
        ],
        scratch_shapes=[
            pltpu.VMEM((rows, cols), low),
            pltpu.VMEM((width, rows), low),
            pltpu.VMEM((rows, width), low),
            pltpu.VMEM((rows, width), low),
            pltpu.VMEM((dp_size, width // dp_size, cols), low),
            pltpu.VMEM((dp_size, width // dp_size, cols), low),
            pltpu.VMEM(out_w.shape, low),
            pltpu.VMEM(out_w.shape, low),
            pltpu.VMEM((width // dp_size, cols), high),
            pltpu.VMEM((width // dp_size, out_cols), high),
            pltpu.VMEM((ctx_size, few, cols + out_cols), low),
            pltpu.VMEM((ctx_size, few, cols + out_cols), low),
            pltpu.VMEM((8, width), high),
            pltpu.VMEM((dp_size, 8, width), high),
            pltpu.VMEM((8, width), high),
            pltpu.VMEM((ctx_size, 8, width), high),
            *sem_pair(max(dp_size, 6)),
            *sem_pair(max(dp_size, 6)),
            *sem_pair(1),
            *sem_pair(dp_size),
            *sem_pair(ctx_size),
            *sem_pair(ctx_size),
        ],
        compiler_params=remote_params(ident),
    )(dq, dkv, cosine, sine, normed, w, x, gain, out_w, gain_two)


class Everyone:
    def __init__(self, axis, target, sems):
        self.axis, self.target, self.sems = axis, target, sems
        self.size = lax.axis_size(axis)

    def copy(self, k):
        at = self.target.at[lax.axis_index(self.axis)]
        return remote(at, at, self.sems, k, {self.axis: ahead_on(self.axis, k)})

    def start(self):
        each(self.size, lambda k: self.copy(k).start())

    def arrive(self):
        each(self.size, lambda k: self.copy(k).wait_recv())

    def finish(self):
        each(self.size, lambda k: self.copy(k).wait_send())


def find_places(first, own, routes_ref, gates_ref, earlier, place_ref, gate_ref, column_ref):
    _, tokens = routes_ref.shape[1:]

    def group(g, carry):
        routes, gates = routes_ref[g], gates_ref[g]
        names, values = [], []
        for e in range(own):
            named = routes == first + e
            names.append(jnp.max(named.astype(jnp.float32), axis=0, keepdims=True))
            values.append(jnp.sum(jnp.where(named, gates, 0.0), axis=0, keepdims=True))
        spare = jnp.zeros((8 - own % 8 if own % 8 else 0, tokens), jnp.float32)
        names = jnp.concatenate(names + ([spare] if spare.shape[0] else []), axis=0)
        place = jnp.dot(
            names.astype(jnp.bfloat16), earlier[...], preferred_element_type=jnp.float32
        )
        place = jnp.where((names > 0.0) & (place < CAP), place, -float(CAP * own))
        for e in range(own):
            place_ref[g, e] = place[e : e + 1].astype(jnp.int32)
            gate_ref[g, e] = values[e]
        column_ref[g] = jnp.transpose(place)[:, :own].astype(jnp.int32)
        return carry

    lax.fori_loop(0, routes_ref.shape[0], group, 0)


class LineRows:
    def __init__(self, x_ref, x_all, back, ahead, line_sems, tp_sems):
        self.x_ref, self.x_all, self.back, self.ahead = x_ref, x_all, back, ahead
        self.line_sems, self.tp_sems = line_sems, tp_sems
        self.me, self.size = lax.axis_index("ctx"), lax.axis_size("ctx")
        self.mine, _ = halves(x_ref.shape[0])

    def block(self, s):
        return lax.rem(self.me + self.size - s, self.size)

    def sends(self, s):
        return (self.me + 1 < self.size) & (self.me - s >= 0)

    def hop(self, s):
        at = self.x_all.at[self.block(s), self.mine]
        source = self.x_ref.at[self.mine] if isinstance(s, int) and s == 0 else at
        return remote(source, at, self.line_sems, s, {"ctx": self.me + 1})

    def back_hop(self):
        at = self.x_all.at[self.me, self.mine]
        return remote(
            self.x_ref.at[self.mine], at, self.line_sems, self.back, {"ctx": self.me - 1}
        )

    def relay(self, k, block):
        at = self.x_all.at[block, self.mine]
        return remote(at, at, self.tp_sems, k, other_core())

    def start(self):
        if self.back:
            pl.when(self.sends(0))(lambda: self.hop(0).start())
        if self.ahead:
            pl.when(self.me >= 1)(lambda: self.back_hop().start())

    def step(self, s):
        @pl.when(self.me - s - 1 >= 0)
        def _():
            self.hop(s).wait_recv()
            self.relay(s, self.block(s + 1)).start()

        if s + 1 < self.back:
            pl.when(self.sends(s + 1))(lambda: self.hop(s + 1).start())

    def step_back(self):
        if self.ahead:

            @pl.when(self.me + 1 < self.size)
            def _():
                self.back_hop().wait_recv()
                self.relay(self.back, self.block(self.size - 1)).start()

    def finish(self):
        for s in range(self.back):
            pl.when(self.sends(s))(lambda s=s: self.hop(s).wait_send())
        if self.ahead:
            pl.when(self.me >= 1)(lambda: self.back_hop().wait_send())


def front_kernel(
    back, ahead, own, starts_ref, x_ref, cot_ref, q_w_ref, k_w_ref, v_w_ref, out_w_ref, gains_ref,
    docs_ref, routes_ref, gates_ref, cos_ref, sin_ref, w_out, out_w_out, gain_rows, docs_all,
    normed_out, q_ref, kv_out, mix_ref, full_out, log_ref, hidden_out, rows_out, cot_out,
    place_ref, gate_ref, column_ref, w_all, out_w_all, normed, kv_all, full, hidden, x_all,
    gains_all, routes_all, gates_all, acc, top, total, column, part, held,
    normed_two, *sems,
):
    me, size = lax.axis_index("ctx"), lax.axis_size("ctx")
    dp = lax.axis_index("dp")
    local = sems[-1]
    pairs = [sems[2 * i : 2 * i + 2] for i in range(len(sems) // 2)]
    q_width, kv_width = q_w_ref.shape[1], k_w_ref.shape[1]
    dp_size, piece = w_all.shape[:2]
    block_rows = x_ref.shape[0]

    def flush(i, source, target):
        return pltpu.make_async_copy(source, target, local.at[i])

    w_all[dp, :, :q_width] = q_w_ref[...]
    w_all[dp, :, q_width : q_width + kv_width] = k_w_ref[...]
    w_all[dp, :, q_width + kv_width :] = v_w_ref[...]
    gains_all[dp] = gains_ref[...]
    docs_all[me] = docs_ref[...]
    routes_all[dp] = routes_ref[...]
    gates_all[dp] = gates_ref[...]
    greet(["dp", "ctx", "tp"])
    weights = Gather(w_all, pairs[1])
    gains = Everyone("dp", gains_all, pairs[0])
    docs = Everyone("ctx", docs_all, pairs[2])
    routes = Everyone("dp", routes_all, pairs[3])
    gates = Everyone("dp", gates_all, pairs[4])
    out_w = Gather(out_w_all, pairs[5])
    line = LineRows(x_ref, x_all, back, ahead, pairs[8], pairs[11])
    for one in (gains, weights, line, docs, routes, gates):
        one.start()

    out_w_all[dp] = out_w_ref[...]
    x_all[me] = x_ref[...]
    token = lax.broadcasted_iota(jnp.int32, (block_rows, block_rows), 0)
    later = lax.broadcasted_iota(jnp.int32, (block_rows, block_rows), 1)
    normed_two[:, :block_rows] = (token < later).astype(jnp.float32).astype(jnp.bfloat16)
    top[...] = jnp.full(top.shape, NEG_FILL, jnp.float32)
    total[...] = jnp.zeros(total.shape, jnp.float32)
    acc[...] = jnp.zeros(acc.shape, jnp.float32)
    gains.arrive()
    for i in range(dp_size):
        gain_rows[:, i * piece : (i + 1) * piece] = gains_all[i]

    def norm_rows(source):
        x = source.astype(jnp.float32)
        return (x * row_scale(x) * gain_rows[0:1, :]).astype(jnp.bfloat16)

    normed[...] = norm_rows(x_ref[...])
    flush(0, normed, normed_out).start()
    routes.arrive()
    gates.arrive()
    docs.arrive()
    if back:
        line.step(0)
    weights.forward()
    find_places(
        dp * own, own, routes_all, gates_all, normed_two.at[:, :block_rows], place_ref, gate_ref,
        column_ref,
    )
    weights.arrive()
    flush(1, w_all, w_out).start()
    out_w.start()
    cot_rows = RowGather(cot_ref, cot_out, pairs[6], pairs[7], 0)
    cot_rows.start()
    last = 2 + back + 1 + ahead
    flush(last + 3, cot_ref, cot_out.at[dp]).start()

    wide, tile = 4 * HEAD_DIM, 2 * HEAD_DIM

    def project(source, first):
        whole = jnp.dot(
            source[:, :piece], w_all[0, :, first : first + wide],
            preferred_element_type=jnp.float32,
        )
        for i in range(1, dp_size):
            whole += jnp.dot(
                source[:, i * piece : (i + 1) * piece], w_all[i, :, first : first + wide],
                preferred_element_type=jnp.float32,
            )
        return [whole[:, :tile], whole[:, tile:]]

    def tables(block):
        cosine, sine = block_tables(cos_ref, sin_ref, block_rows, block)
        return cosine, -sine

    here = tables(me)
    for first in range(0, q_width, wide):
        for i, part_of in enumerate(project(normed, first)):
            turned = turn(part_of, *here).astype(jnp.bfloat16)
            at = first + i * tile
            q_ref[:, at : at + tile] = (turned.astype(jnp.float32) * HEAD_DIM**-0.5).astype(
                jnp.bfloat16
            )
    for s in range(1, back):
        line.step(s)
    line.step_back()
    masks = Masks(docs_all, starts_ref, column)

    def visit(s, block):
        @pl.when(s > 0)
        def _():
            line.relay(s - 1, block).wait()

        part[...] = norm_rows(x_all[block])
        there = tables(block)
        for first in range(q_width, q_width + 2 * kv_width, wide):
            for i, part_of in enumerate(project(part, first)):
                if first < q_width + kv_width:
                    part_of = turn(part_of, *there)
                at = first - q_width + i * tile
                kv_all[block, :, at : at + tile] = part_of.astype(jnp.bfloat16)
        flush(2 + s, kv_all.at[block], kv_out.at[block]).start()
        attend_block(masks, block, q_ref, kv_all.at[block], acc, top, total)

    def step(s):
        pl.when(me - s >= 0)(lambda: visit(s, lax.rem(me + size - s, size)))

        @pl.when(s == min(1, back))
        def _():
            out_w.forward()
            cot_rows.forward()

    each(back + 1, step, 0)
    if ahead:

        @pl.when(me + 1 < size)
        def _():
            visit(back + 1, lax.rem(me + 1, size))

    log_ref[...] = top[...] + jnp.log(total[...])
    for h in range(total.shape[0]):
        at = slice(h * HEAD_DIM, (h + 1) * HEAD_DIM)
        acc[at, :] = acc[at, :] / total[h : h + 1, :]
    full[...] = jnp.transpose(acc[...])
    mix_ref[...] = full[...].astype(jnp.bfloat16)
    out_w.arrive()
    cot_rows.arrive()
    for i in range(dp_size):
        part[:, i * piece : (i + 1) * piece] = jnp.dot(
            mix_ref[...], out_w_all[i], preferred_element_type=jnp.float32
        ).astype(jnp.bfloat16)

    mine, theirs = halves(block_rows)
    rows = RowGather(normed_two, rows_out, pairs[9], pairs[10], 2)
    first = remote(part.at[theirs], held.at[theirs], pairs[10], 0, other_core())
    second = remote(part.at[mine], held.at[mine], pairs[10], 1, other_core())
    first.start()
    second.start()
    flush(last, full, full_out).start()
    flush(last + 1, out_w_all, out_w_out).start()

    def norm(at):
        whole = x_ref[at, :].astype(jnp.float32) + (
            part[at, :].astype(jnp.float32) + held[at, :].astype(jnp.float32)
        )
        hidden[at, :] = whole
        normed_two[at, :] = (whole * row_scale(whole) * gain_rows[1:2, :]).astype(jnp.bfloat16)

    first.wait()
    norm(mine)
    rows.start()
    second.wait()
    norm(theirs)
    flush(last + 2, hidden, hidden_out).start()
    flush(last + 4, normed_two, rows_out.at[dp]).start()
    cot_rows.finish()
    for one in (gains, weights, docs, routes, gates, out_w, line):
        one.finish()
    rows.forward()
    rows.arrive()
    rows.finish()
    flush(0, normed, normed_out).wait()
    flush(1, w_all, w_out).wait()

    def kept(s):
        @pl.when(me - s >= 0)
        def _():
            flush(2 + s, kv_all.at[me], kv_out.at[me]).wait()

    each(back + 1, kept, 0)
    if ahead:
        pl.when(me + 1 < size)(lambda: flush(3 + back, kv_all.at[me], kv_out.at[me]).wait())
    flush(last, full, full_out).wait()
    flush(last + 1, out_w_all, out_w_out).wait()
    flush(last + 2, hidden, hidden_out).wait()
    flush(last + 3, cot_ref, cot_out.at[dp]).wait()
    flush(last + 4, normed_two, rows_out.at[dp]).wait()


def front(
    starts, x, cot, q_w, k_w, v_w, out_w, gains, docs, routes, gates, cosine, sine, own, back,
    ahead, ident,
):
    rows, width = x.shape
    dp_size, ctx_size = lax.axis_size("dp"), lax.axis_size("ctx")
    q_width, kv_cols = q_w.shape[1], 2 * k_w.shape[1]
    piece, heads = q_w.shape[0], q_width // HEAD_DIM
    low, high, whole = jnp.bfloat16, jnp.float32, jnp.int32
    far = [
        ((dp_size, piece, q_width + kv_cols), low),
        ((dp_size,) + out_w.shape, low),
        ((rows, width), low),
        ((ctx_size, rows, kv_cols), low),
        ((rows, q_width), high),
        ((rows, width), high),
        ((dp_size, rows, width), low),
        ((dp_size, rows, width), low),
    ]
    shapes = [
        far[0],
        far[1],
        ((2, width), high),
        ((ctx_size, 1, rows), whole),
        far[2],
        ((rows, q_width), low),
        far[3],
        ((rows, q_width), low),
        far[4],
        ((heads, rows), high),
        far[5],
        far[6],
        far[7],
        ((dp_size, own, 1, rows), whole),
        ((dp_size, own, 1, rows), high),
        ((dp_size, rows, own), whole),
    ]
    return pl.pallas_call(
        functools.partial(front_kernel, back, ahead, own),
        name="front",
        in_specs=[pl.BlockSpec(memory_space=pltpu.SMEM)] + whole_vmem(12),
        out_specs=[
            pl.BlockSpec(memory_space=pl.ANY if shape in far else pltpu.VMEM) for shape in shapes
        ],
        out_shape=[jax.ShapeDtypeStruct(*shape) for shape in shapes],
        scratch_shapes=[
            *[pltpu.VMEM(*shape) for shape in far[:6]],
            pltpu.VMEM((ctx_size, rows, width), low),
            pltpu.VMEM((dp_size,) + gains.shape, high),
            pltpu.VMEM((dp_size,) + routes.shape, whole),
            pltpu.VMEM((dp_size,) + gates.shape, high),
            pltpu.VMEM((q_width, rows), high),
            pltpu.VMEM((heads, rows), high),
            pltpu.VMEM((heads, rows), high),
            pltpu.VMEM((rows, 8), whole),
            pltpu.VMEM((rows, width), low),
            pltpu.VMEM((rows, width), low),
            pltpu.VMEM((rows, width), low),
            *sem_pair(dp_size),
            *sem_pair(dp_size),
            *sem_pair(ctx_size),
            *sem_pair(dp_size),
            *sem_pair(dp_size),
            *sem_pair(dp_size),
            *sem_pair(dp_size),
            *sem_pair(dp_size),
            *sem_pair(back + 1),
            *sem_pair(dp_size),
            *sem_pair(dp_size + 2),
            *sem_pair(back + 1),
            pltpu.SemaphoreType.DMA((8 + back + ahead,)),
        ],
        compiler_params=remote_params(ident),
    )(starts, x, cot, q_w, k_w, v_w, out_w, gains, docs, routes, gates, cosine, sine)


GROUPS_AT_ONCE = 4


def experts_kernel(more, rows_ref, grads_ref, weights_ref, place_ref, gate_ref, *refs):
    outs_ref, backs_ref, weight_grad_ref, slots, slot_grads = refs[2 * more :]
    groups, tok_rows, _ = rows_ref.shape
    owners, part = weight_grad_ref.shape[1], weight_grad_ref.shape[5]
    slot_index = lax.broadcasted_iota(jnp.int32, (CAP, tok_rows), 0)
    gates = []
    for g in range(groups):
        picks = slot_index == place_ref[g, 0]
        gates.append(jnp.sum(jnp.where(picks, gate_ref[g, 0], 0.0), axis=1, keepdims=True))
        picks = picks.astype(jnp.float32).astype(jnp.bfloat16)
        at = slice(g * CAP, (g + 1) * CAP)
        slots[at, :] = jnp.dot(
            picks, rows_ref[g], preferred_element_type=jnp.float32
        ).astype(jnp.bfloat16)
        slot_grads[at, :] = (
            jnp.dot(picks, grads_ref[g], preferred_element_type=jnp.float32) * gates[g]
        ).astype(jnp.bfloat16)
    gate_w, up_w, down_w = (weights_ref.at[0, i] for i in range(3))
    gate_pre = jnp.dot(slots[...], gate_w[...], preferred_element_type=jnp.float32)
    up_pre = jnp.dot(slots[...], up_w[...], preferred_element_type=jnp.float32)
    act_grad = jnp.dot(slot_grads[...], down_w[...], preferred_element_type=jnp.float32)
    sig = 1.0 / (1.0 + jnp.exp(-gate_pre))
    silu = gate_pre * sig
    act_low = (silu * up_pre).astype(jnp.bfloat16)
    up_low = (act_grad * silu).astype(jnp.bfloat16)
    gate_low = (act_grad * up_pre * (sig * (1.0 + gate_pre * (1.0 - sig)))).astype(jnp.bfloat16)

    back = lax.dot_general(
        gate_low, gate_w[...], NT, preferred_element_type=jnp.float32
    ) + lax.dot_general(up_low, up_w[...], NT, preferred_element_type=jnp.float32)
    out = lax.dot_general(act_low, down_w[...], NT, preferred_element_type=jnp.float32)
    for g in range(groups):
        at = slice(g * CAP, (g + 1) * CAP)
        backs_ref[g] = back[at].astype(jnp.bfloat16)
        outs_ref[g] = (out[at] * gates[g]).astype(jnp.bfloat16)

    for i, (low, source) in enumerate(
        ((gate_low, slots), (up_low, slots), (act_low, slot_grads))
    ):
        turned = jnp.transpose(low.astype(jnp.float32)).astype(jnp.bfloat16)
        total = jnp.dot(turned, source[...], preferred_element_type=jnp.float32)
        for c in range(owners):
            weight_grad_ref[0, c, 0, i] = total[:, c * part : (c + 1) * part].astype(
                weight_grad_ref.dtype
            )


def experts(weights, place_rows, gate_rows, rows_all, grad_all, first, count, before):
    own, _, model_width, hidden = weights.shape
    groups, tok_rows, _ = rows_all.shape
    owners = lax.axis_size("ctx")
    at_once = min(GROUPS_AT_ONCE, groups)
    chunks = groups // at_once
    part = model_width // owners
    rows_spec = pl.BlockSpec(
        (at_once, tok_rows, model_width), lambda c, e: (c, 0, 0), pipeline_mode=pl.Buffered(1)
    )
    line_spec = pl.BlockSpec((at_once, 1, 1, tok_rows), lambda c, e: (c, e + first, 0, 0))
    slots_spec = pl.BlockSpec((at_once, CAP, model_width), lambda c, e: (c, e + first, 0))
    slots_shape = jax.ShapeDtypeStruct((groups, own * CAP, model_width), jnp.bfloat16)
    flops = count * groups * CAP * model_width * 2 * (9 * hidden + 2 * tok_rows)
    more = before is not None
    outs, backs, weight_part = pl.pallas_call(
        functools.partial(experts_kernel, more),
        name="experts",
        grid=(chunks, count),
        in_specs=[
            rows_spec,
            rows_spec,
            pl.BlockSpec((1, 3, model_width, hidden), lambda c, e: (e + first, 0, 0, 0)),
            line_spec,
            line_spec,
        ]
        + [pl.BlockSpec(memory_space=pl.ANY)] * (2 * more),
        out_specs=[
            slots_spec,
            slots_spec,
            pl.BlockSpec((1, owners, 1, 3, hidden, part), lambda c, e: (c, 0, e, 0, 0, 0)),
        ],
        out_shape=[
            slots_shape,
            slots_shape,
            jax.ShapeDtypeStruct((chunks, owners, count, 3, hidden, part), jnp.bfloat16),
        ],
        scratch_shapes=[
            pltpu.VMEM((at_once * CAP, model_width), jnp.bfloat16),
            pltpu.VMEM((at_once * CAP, model_width), jnp.bfloat16),
        ],
        input_output_aliases={5: 0, 6: 1} if more else {},
        compiler_params=pltpu.CompilerParams(vmem_limit_bytes=LIMIT),
        cost_estimate=pl.CostEstimate(
            flops=flops, bytes_accessed=4 * weights.size, transcendentals=0
        ),
    )(rows_all, grad_all, weights, place_rows, gate_rows, *(before if more else ()))
    if chunks == 1:
        return (outs, backs), weight_part[0]
    return (outs, backs), jnp.sum(weight_part.astype(jnp.float32), axis=0).astype(jnp.bfloat16)


def unfold_kernel(more, sums_ref, *refs):
    out_ref = refs[more]
    for i in range(sums_ref.shape[1]):
        out_ref[0, i] = jnp.transpose(sums_ref[0, i].astype(jnp.float32))


def unfold(sums, own, first, before):
    count, three, hidden, part = sums.shape
    more = before is not None
    return pl.pallas_call(
        functools.partial(unfold_kernel, more),
        name="unfold",
        grid=(count,),
        in_specs=[pl.BlockSpec((1, three, hidden, part), lambda e: (e, 0, 0, 0))]
        + [pl.BlockSpec(memory_space=pl.ANY)] * more,
        out_specs=pl.BlockSpec((1, three, part, hidden), lambda e: (e + first, 0, 0, 0)),
        out_shape=jax.ShapeDtypeStruct((own, three, part, hidden), jnp.float32),
        input_output_aliases={1: 0} if more else {},
        compiler_params=pltpu.CompilerParams(vmem_limit_bytes=LIMIT),
    )(sums, *([before] if more else []))


def rotary_tables(token_positions):
    half_dim = HEAD_DIM // 2
    inverse = THETA ** (-(jnp.arange(half_dim, dtype=jnp.float32) * 2.0 / HEAD_DIM))
    angles = token_positions.astype(jnp.float32)[:, None] * inverse[None, :]
    cosine, sine = jnp.cos(angles), jnp.sin(angles)
    return jnp.concatenate([cosine] * 4, axis=1), jnp.concatenate([sine, -sine] * 2, axis=1)


def expert_counts(own):
    return (1, 6, 1) if own == 8 else (own - own // 2, own // 2)


def scatter(grads):
    return lax.psum_scatter(grads, "ctx", scatter_dimension=0)


def body(
    tokens,
    query_weight,
    key_weight,
    value_weight,
    output_weight,
    gain_attn,
    gain_moe,
    expert_weights,
    routes,
    gate_values,
    documents,
    pic_starts,
    cotangent,
):
    block_len = tokens.shape[1]
    ctx_size = lax.axis_size("ctx")
    length = block_len * ctx_size
    back = back_blocks(ctx_size, block_len, length)
    ahead = ahead_blocks(block_len, length, pic_starts.shape[1])
    q_width, kv_width = query_weight.shape[1], key_weight.shape[1]
    own = expert_weights.shape[0]
    x, cot = tokens[0], cotangent[0]

    inside = jnp.arange(block_len, dtype=jnp.int32)
    starts = jnp.arange(-(-ctx_size // 8) * 8, dtype=jnp.int32) * block_len
    cosine, sine = rotary_tables(jnp.concatenate([inside, starts]))
    (
        w_all,
        out_w_all,
        gain_rows,
        docs_all,
        normed_one,
        query,
        kv_all,
        mixture,
        mix_full,
        log_total,
        hidden,
        rows_all,
        grad_all,
        *places,
    ) = front(
        pic_starts,
        x,
        cot,
        query_weight,
        key_weight,
        value_weight,
        output_weight,
        jnp.stack([gain_attn, gain_moe]).astype(jnp.float32),
        documents,
        routes[0].T,
        gate_values[0].T,
        cosine,
        sine,
        own,
        back,
        ahead,
        1,
    )
    place_rows, gate_rows, places = places
    counts = expert_counts(own)
    slots, sums = None, []
    first = 0
    for n, count in enumerate(counts):
        slots, grads = experts(
            expert_weights, place_rows, gate_rows, rows_all, grad_all, first, count, slots
        )
        if n < len(counts) - 1:
            sums.append((scatter(grads), first))
        first += count
    outs, backs = slots
    hidden_grad, hidden_low, mix_grad, gain_two_grad = return_grads(
        backs, places, hidden, cot, gain_rows, out_w_all, 2
    )
    q_rot_grad, kv_part = attend_back(
        pic_starts, query, kv_all, docs_all, log_total, mix_full, mix_grad, back, ahead
    )
    kv_back, expert_sum, output_grad = trade(
        kv_part,
        outs,
        places,
        hidden_low,
        mixture,
        back,
        ahead,
        3,
    )
    x_grad, owned, gain_sums = finish(
        q_rot_grad,
        kv_back,
        cosine,
        sine,
        normed_one,
        w_all,
        x,
        gain_rows,
        output_grad,
        gain_two_grad,
        4,
    )
    grads, owned = lax.optimization_barrier((grads, owned))
    sums.append((scatter(grads), own - counts[-1]))
    few = owned.shape[0]
    here = (lax.axis_index("dp") * ctx_size + lax.axis_index("ctx")) * few
    gain_sums = lax.dynamic_slice_in_dim(gain_sums, here, few, 1)
    expert_grad = None
    for part, first in sums:
        expert_grad = unfold(part, own, first, expert_grad)
    v_end = q_width + 2 * kv_width
    return (
        (hidden + expert_sum.astype(jnp.float32)).astype(jnp.bfloat16)[None],
        (hidden_grad + x_grad).astype(jnp.bfloat16)[None],
        owned[:, :q_width],
        owned[:, q_width : q_width + kv_width],
        owned[:, q_width + kv_width : v_end],
        owned[:, v_end:].T,
        gain_sums[0],
        gain_sums[1],
        expert_grad,
    )


def solution(mesh):
    return jax.shard_map(
        body,
        mesh=mesh,
        in_specs=(
            P("dp", "ctx", None),
            P("dp", "tp"),
            P("dp", "tp"),
            P("dp", "tp"),
            P("tp", "dp"),
            P("dp"),
            P("dp"),
            P("dp", None, None, "tp"),
            P("dp", "ctx", None),
            P("dp", "ctx", None),
            P("dp", "ctx"),
            P("dp", None),
            P("dp", "ctx", None),
        ),
        out_specs=(
            P("dp", "ctx", None),
            P("dp", "ctx", None),
            P(("dp", "ctx"), "tp"),
            P(("dp", "ctx"), "tp"),
            P(("dp", "ctx"), "tp"),
            P("tp", ("dp", "ctx")),
            P(("dp", "ctx")),
            P(("dp", "ctx")),
            P("dp", None, "ctx", "tp"),
        ),
        check_vma=False,
    )
```

```python
import functools

import jax
import jax.numpy as jnp
from jax import lax
from jax.experimental import pallas as pl
from jax.experimental.pallas import tpu as pltpu
from jax.sharding import PartitionSpec as P

HEAD_DIM = 64
PIC = 256
CAP = 144

EPSILON = 1e-06
THETA = 10000.0
NEG_FILL = -1e30


KEY_ROWS = 256
NT = (((1,), (1,)), ((), ()))
LIMIT = 67043328


def whole_vmem(count):
    return [pl.BlockSpec(memory_space=pltpu.VMEM)] * count


def picture_ids(starts_ref, places):
    ids = jnp.full(places.shape, -1, jnp.int32)
    for j in range(starts_ref.shape[1]):
        start = starts_ref[0, j]
        ids += jnp.where((places >= start) & (places < start + PIC), j + 1, 0)
    return ids


def as_column(row):
    tall = jnp.broadcast_to(row.astype(jnp.float32), (8, row.shape[1]))
    return jnp.transpose(tall)[:, 0:1].astype(jnp.int32)


class Masks:
    def __init__(self, docs_ref, starts_ref, column):
        self.docs_ref, self.starts_ref, self.column = docs_ref, starts_ref, column
        self.rows = docs_ref.shape[2]
        me = lax.axis_index("ctx")
        self.q_doc = docs_ref[me]
        self.q_place = me * self.rows + lax.broadcasted_iota(jnp.int32, (1, self.rows), 1)
        self.q_pic = picture_ids(starts_ref, self.q_place)

    def open(self, block):
        self.column[...] = jnp.broadcast_to(
            as_column(self.docs_ref[block]), self.column.shape
        )

    def bias(self, block, rows, first):
        k_doc = self.column[rows, 0:1]
        k_place = block * self.rows + first + lax.broadcasted_iota(jnp.int32, k_doc.shape, 0)
        k_pic = picture_ids(self.starts_ref, k_place)
        seen = (k_doc == self.q_doc) & (
            (k_place <= self.q_place) | ((k_pic == self.q_pic) & (self.q_pic >= 0))
        )
        return jnp.where(seen, 0.0, NEG_FILL)


def attend_block(masks, block, q_ref, kv_ref, acc, top, total):
    kv_width = kv_ref.shape[1] // 2
    heads, kv_heads = q_ref.shape[1] // HEAD_DIM, kv_width // HEAD_DIM
    masks.open(block)

    def step(j, carry):
        first = pl.multiple_of(j * KEY_ROWS, KEY_ROWS)
        rows = pl.ds(first, KEY_ROWS)
        bias = masks.bias(block, rows, first)
        for g in range(kv_heads):
            key = kv_ref[rows, g * HEAD_DIM : (g + 1) * HEAD_DIM]
            val = kv_ref[rows, kv_width + g * HEAD_DIM : kv_width + (g + 1) * HEAD_DIM]
            val_t = jnp.transpose(val.astype(jnp.float32)).astype(jnp.bfloat16)
            for h in range(g * heads // kv_heads, (g + 1) * heads // kv_heads):
                at = slice(h * HEAD_DIM, (h + 1) * HEAD_DIM)
                scores = bias + lax.dot_general(
                    key, q_ref[:, at], NT, preferred_element_type=jnp.float32
                )
                old = top[h : h + 1, :]
                new = jnp.maximum(old, jnp.max(scores, axis=0, keepdims=True))
                probs = jnp.exp(scores - new)
                fade = jnp.exp(old - new)
                total[h : h + 1, :] = total[h : h + 1, :] * fade + jnp.sum(
                    probs, axis=0, keepdims=True
                )
                acc[at, :] = acc[at, :] * fade + jnp.dot(
                    val_t, probs.astype(jnp.bfloat16), preferred_element_type=jnp.float32
                )
                top[h : h + 1, :] = new
        return carry

    lax.fori_loop(0, kv_ref.shape[0] // KEY_ROWS, step, 0)


def attend_back_block(
    masks, edges, block, q_ref, kv_ref, log_ref, delta, grad_ref, acc, dkv_ref
):
    kv_width = kv_ref.shape[1] // 2
    heads, kv_heads = q_ref.shape[1] // HEAD_DIM, kv_width // HEAD_DIM
    masks.open(block)
    count = kv_ref.shape[0] // KEY_ROWS
    me = lax.axis_index("ctx")
    q_first, q_last = edges[me * count, 0], edges[me * count + count - 1, 1]

    def step(j, carry):
        at = block * count + j
        same = (edges[at, 0] <= q_last) & (edges[at, 1] >= q_first)

        @pl.when(same)
        def _():
            inside(j)

        @pl.when(jnp.logical_not(same))
        def _():
            rows = pl.ds(pl.multiple_of(j * KEY_ROWS, KEY_ROWS), KEY_ROWS)
            dkv_ref[rows, :] = jnp.zeros((KEY_ROWS, dkv_ref.shape[1]), dkv_ref.dtype)

        return carry

    def inside(j):
        first = pl.multiple_of(j * KEY_ROWS, KEY_ROWS)
        rows = pl.ds(first, KEY_ROWS)
        bias = masks.bias(block, rows, first)
        for g in range(kv_heads):
            k_at = slice(g * HEAD_DIM, (g + 1) * HEAD_DIM)
            v_at = slice(kv_width + g * HEAD_DIM, kv_width + (g + 1) * HEAD_DIM)
            key, val = kv_ref[rows, k_at], kv_ref[rows, v_at]
            key_t = jnp.transpose(key.astype(jnp.float32)).astype(jnp.bfloat16)
            dk = jnp.zeros((KEY_ROWS, HEAD_DIM), jnp.float32)
            dv = jnp.zeros((KEY_ROWS, HEAD_DIM), jnp.float32)
            for h in range(g * heads // kv_heads, (g + 1) * heads // kv_heads):
                at = slice(h * HEAD_DIM, (h + 1) * HEAD_DIM)
                q_rows, g_rows = q_ref[:, at], grad_ref[:, at]
                scores = bias + lax.dot_general(
                    key, q_rows, NT, preferred_element_type=jnp.float32
                )
                probs = jnp.exp(scores - log_ref[h : h + 1, :])
                prob_grad = lax.dot_general(val, g_rows, NT, preferred_element_type=jnp.float32)
                slope = (probs * (prob_grad - delta[h : h + 1, :])).astype(jnp.bfloat16)
                dv += jnp.dot(
                    probs.astype(jnp.bfloat16), g_rows, preferred_element_type=jnp.float32
                )
                dk += jnp.dot(slope, q_rows, preferred_element_type=jnp.float32)
                acc[at, :] += jnp.dot(key_t, slope, preferred_element_type=jnp.float32)
            dkv_ref[rows, k_at] = dk.astype(dkv_ref.dtype)
            dkv_ref[rows, v_at] = dv.astype(dkv_ref.dtype)

    lax.fori_loop(0, count, step, 0)


def attend_back_kernel(
    back, ahead, starts_ref, edges, q_ref, kv_ref, docs_ref, log_ref, full_ref, grad_ref, dq_ref,
    dkv_ref, acc, delta, column,
):
    me, size = lax.axis_index("ctx"), lax.axis_size("ctx")
    acc[...] = jnp.transpose(full_ref[...] * grad_ref[...].astype(jnp.float32))
    for h in range(delta.shape[0]):
        delta[h : h + 1, :] = jnp.sum(
            acc[h * HEAD_DIM : (h + 1) * HEAD_DIM, :], axis=0, keepdims=True
        )
    acc[...] = jnp.zeros(acc.shape, jnp.float32)
    masks = Masks(docs_ref, starts_ref, column)

    def step(s, carry):
        block = me + ahead - s

        @pl.when((block >= 0) & (block < size))
        def _():
            attend_back_block(
                masks, edges, block, q_ref, kv_ref.at[block], log_ref, delta, grad_ref, acc,
                dkv_ref.at[block],
            )

        return carry

    lax.fori_loop(0, back + ahead + 1, step, 0)
    dq_ref[...] = jnp.transpose(acc[...]) * (HEAD_DIM**-0.5)


def attend_back(starts, q, kv, docs, log_total, full, grad, back, ahead):
    rows, width = q.shape
    by_block = docs.reshape(-1, KEY_ROWS)
    edges = jnp.concatenate([by_block[:, :1], by_block[:, -1:]], axis=1)
    return pl.pallas_call(
        functools.partial(attend_back_kernel, back, ahead),
        name="attend_back",
        in_specs=[pl.BlockSpec(memory_space=pltpu.SMEM)] * 2 + whole_vmem(6),
        out_specs=whole_vmem(2),
        out_shape=[
            jax.ShapeDtypeStruct((rows, width), jnp.float32),
            jax.ShapeDtypeStruct(kv.shape, jnp.bfloat16),
        ],
        scratch_shapes=[
            pltpu.VMEM((width, rows), jnp.float32),
            pltpu.VMEM((width // HEAD_DIM, rows), jnp.float32),
            pltpu.VMEM((rows, 8), jnp.int32),
        ],
        compiler_params=pltpu.CompilerParams(vmem_limit_bytes=LIMIT),
    )(starts, edges, q, kv, docs, log_total, full, grad)


MESH = pl.DeviceIdType.MESH
HOP_PARTS = 8


def greet(axes_list, line=False):
    barrier = pltpu.get_barrier_semaphore()
    count = 0
    for axis in axes_list:
        me, size = lax.axis_index(axis), lax.axis_size(axis)

        def signal(k, carry, axis=axis, me=me, size=size):
            pl.semaphore_signal(
                barrier, inc=1, device_id={axis: lax.rem(me + k, size)}, device_id_type=MESH
            )
            return carry

        lax.fori_loop(1, size, signal, 0)
        count += size - 1
    if not line:
        pl.semaphore_wait(barrier, count)
        return
    me, size = lax.axis_index("ctx"), lax.axis_size("ctx")
    for step in (1, -1):
        other = me + step

        @pl.when((other >= 0) & (other < size))
        def _(other=other):
            pl.semaphore_signal(barrier, inc=1, device_id={"ctx": other}, device_id_type=MESH)

    inner = (me > 0) & (me < size - 1)

    @pl.when(inner)
    def _():
        pl.semaphore_wait(barrier, count + 2)

    @pl.when(jnp.logical_not(inner))
    def _():
        pl.semaphore_wait(barrier, count + 1)


def remote(src, dst, sems, k, device_id):
    return pltpu.make_async_remote_copy(
        src_ref=src,
        dst_ref=dst,
        send_sem=sems[0].at[k],
        recv_sem=sems[1].at[k],
        device_id=device_id,
        device_id_type=MESH,
    )


def other_core():
    return {"tp": 1 - lax.axis_index("tp")}


def ahead_on(axis, k):
    return lax.rem(lax.axis_index(axis) + k, lax.axis_size(axis))


def each(count, do, first=1):
    def step(k, carry):
        do(k)
        return carry

    lax.fori_loop(first, count, step, 0)


def sem_pair(count):
    return [pltpu.SemaphoreType.DMA((count,)), pltpu.SemaphoreType.DMA((count,))]


def remote_params(ident):
    return pltpu.CompilerParams(
        collective_id=ident, has_side_effects=True, vmem_limit_bytes=LIMIT
    )


def halves(rows):
    half = rows // 2
    core = lax.axis_index("tp")
    return (
        pl.ds(pl.multiple_of(core * half, half), half),
        pl.ds(pl.multiple_of((1 - core) * half, half), half),
    )


def turn(tile, cosine, sine):
    lane = lax.broadcasted_iota(jnp.int32, tile.shape, 1)
    half = HEAD_DIM // 2
    swapped = jnp.where(
        lax.rem(lane, HEAD_DIM) < half,
        pltpu.roll(tile, 2 * HEAD_DIM - half, 1),
        pltpu.roll(tile, half, 1),
    )
    return tile * cosine + swapped * sine


def block_tables(cos_ref, sin_ref, rows, block):
    start = pl.ds(rows + block, 1)
    in_cos, in_sin = cos_ref[:rows, :], sin_ref[:rows, :]
    at_cos, at_sin = cos_ref[start, :], sin_ref[start, :]
    return in_cos * at_cos - in_sin * at_sin, in_sin * at_cos + in_cos * at_sin


def row_scale(x):
    return lax.rsqrt(jnp.mean(x * x, axis=-1, keepdims=True) + EPSILON)


def norm_back(x, gain, grad):
    scale = row_scale(x)
    unit = x * scale
    pull = grad * gain
    return (
        scale * (pull - unit * jnp.mean(pull * unit, axis=-1, keepdims=True)),
        jnp.sum(grad * unit, axis=0, keepdims=True),
    )


def back_blocks(ctx_size, block_len, length):
    return min(ctx_size - 1, -(-(length // 2 - 1) // block_len))


def ahead_blocks(block_len, length, spans):
    return 0 if block_len % (length // spans) == 0 else 1


def grid_peers():
    me = lax.axis_index("dp")
    x, y = lax.rem(me, 2), lax.div(me, 2)
    return y * 2 + 1 - x, (1 - y) * 2 + x, 3 - me


class Gather:
    def __init__(self, target, sems, rows=None, source=None):
        self.target, self.sems, self.rows, self.source = target, sems, rows, source
        self.size = lax.axis_size("dp")
        self.grid = self.size == 4

    def at(self, place):
        return self.target.at[place] if self.rows is None else self.target.at[place, self.rows]

    def half(self, place, n):
        if self.rows is None:
            count = self.target.shape[1] // 2
            return self.target.at[place, pl.ds(n * count, count)]
        count = self.rows.size // 2
        first = pl.multiple_of(self.rows.start + n * count, count)
        return self.target.at[place, pl.ds(first, count)]

    def first(self, k, peer):
        place = self.at(lax.axis_index("dp"))
        source = place if self.source is None else self.source.at[self.rows]
        return remote(source, place, self.sems, k, {"dp": peer})

    def passed(self, k, place, n, peer):
        at = self.half(place, n)
        return remote(at, at, self.sems, k, {"dp": peer})

    def direct(self, k):
        return self.first(k, ahead_on("dp", k))

    def start(self):
        if not self.grid:
            each(self.size, lambda k: self.direct(k).start())
            return
        x, y, _ = grid_peers()
        self.first(0, x).start()
        self.first(1, y).start()

    def forward(self, came=None):
        if not self.grid:
            return
        x, y, _ = grid_peers()
        self.first(0, x).wait_recv()
        self.passed(2, x, 0, y).start()
        if came:
            came(0, self.at(x))
        self.first(1, y).wait_recv()
        self.passed(3, y, 1, x).start()
        if came:
            came(1, self.at(y))

    def arrive(self, came=None):
        if not self.grid:

            def one(k):
                self.direct(k).wait_recv()
                if came:
                    came(k, self.at(ahead_on("dp", self.size - k)))

            each(self.size, one)
            return
        x, _, diagonal = grid_peers()
        for n in range(2):
            self.passed(2 + n, diagonal, n, x).wait_recv()
            if came:
                came(2 + n, self.half(diagonal, n))

    def finish(self):
        if not self.grid:
            each(self.size, lambda k: self.direct(k).wait_send())
            return
        x, y, _ = grid_peers()
        self.first(0, x).wait_send()
        self.first(1, y).wait_send()
        self.passed(2, x, 0, y).wait_send()
        self.passed(3, y, 1, x).wait_send()


class RowGather:
    def __init__(self, source, target, dp_sems, tp_sems, first):
        mine, _ = halves(source.shape[0])
        self.gather = Gather(target, dp_sems, mine, source)
        self.tp_sems, self.after = tp_sems, first

    def relay(self, k, at):
        return remote(at, at, self.tp_sems, self.after + k, other_core())

    def came(self, k, at):
        self.relay(k, at).start()

    def start(self):
        self.gather.start()

    def forward(self):
        self.gather.forward(self.came)

    def arrive(self):
        self.gather.arrive(self.came)

    def finish(self):
        self.gather.finish()
        gather = self.gather
        if not gather.grid:
            each(
                gather.size,
                lambda k: self.relay(k, gather.at(ahead_on("dp", gather.size - k))).wait(),
            )
            return
        x, y, diagonal = grid_peers()
        self.relay(0, gather.at(x)).wait()
        self.relay(1, gather.at(y)).wait()
        self.relay(2, gather.half(diagonal, 0)).wait()
        self.relay(3, gather.half(diagonal, 1)).wait()


def collect(places_ref, slots_ref, group):
    tok_rows, slot_count = places_ref.shape[1], slots_ref.shape[1]
    tiles = []
    for first in range(0, slot_count, 128):
        wide = min(128, slot_count - first)
        lane = first + lax.broadcasted_iota(jnp.int32, (tok_rows, wide), 1)
        hit = None
        for n in range(first // CAP, (first + wide - 1) // CAP + 1):
            one = places_ref[group, :, n : n + 1] == lane - n * CAP
            hit = one if hit is None else hit | one
        tiles.append(hit.astype(jnp.float32).astype(jnp.bfloat16))
    return jnp.dot(
        jnp.concatenate(tiles, axis=1), slots_ref[group], preferred_element_type=jnp.float32
    )


class GridSum:
    def __init__(self, piece, landed, sems):
        self.piece, self.landed, self.sems = piece, landed, sems
        self.x, self.y, _ = grid_peers()
        self.count = landed.shape[1] // 2

    def half(self, n, which):
        return self.piece(n).at[pl.ds(which * self.count, self.count)]

    def slot(self, j):
        return self.landed.at[j // 2, pl.ds(j % 2 * self.count, self.count)]

    def copy(self, j):
        n, which, peer = (
            (1, 0, self.x),
            (3, 0, self.x),
            (2, 1, self.y),
            (3, 1, self.y),
            (2, 0, self.y),
            (1, 1, self.x),
        )[j]
        return remote(self.half(n, which), self.slot(j), self.sems, j, {"dp": peer})

    def start(self):
        for j in (1, 3, 0, 2):
            self.copy(j).start()

    def forward(self):
        for j, n, which in ((1, 2, 0), (3, 1, 1)):
            self.copy(j).wait_recv()
            half = self.half(n, which)
            half[...] = (
                half[...].astype(jnp.float32) + self.slot(j)[...].astype(jnp.float32)
            ).astype(jnp.bfloat16)
            self.copy(4 + j // 2).start()

    def add_to(self, total):
        for which, slots in ((0, (0, 4)), (1, (2, 5))):
            at = pl.ds(which * self.count, self.count)
            for j in slots:
                self.copy(j).wait_recv()
                total[at, :] += self.slot(j)[...].astype(jnp.float32)

    def finish(self):
        for j in range(6):
            self.copy(j).wait_send()


class RowReturn:
    def __init__(self, part, held, landed, total, sent, came, dp_sems, tp_sems):
        self.part, self.held, self.landed, self.total = part, held, landed, total
        self.sent, self.came, self.dp_sems, self.tp_sems = sent, came, dp_sems, tp_sems
        self.size = lax.axis_size("dp")
        self.mine, self.theirs = halves(part.shape[1])
        self.grid = self.size == 4
        if self.grid:
            self.sum = GridSum(lambda n: held.at[n], landed, dp_sems)

    def group(self, k):
        if not self.grid:
            return ahead_on("dp", k)
        me = lax.axis_index("dp")
        x, y = lax.rem(me, 2), lax.div(me, 2)
        flip_x, flip_y = lax.rem(k, 2), lax.div(k, 2)
        return lax.rem(y + flip_y, 2) * 2 + lax.rem(x + flip_x, 2)

    def swap(self, k):
        return remote(
            self.part.at[self.group(k), self.theirs], self.held.at[k], self.tp_sems, k,
            other_core(),
        )

    def copy(self, k):
        return remote(
            self.held.at[k], self.landed.at[k - 1], self.dp_sems, k, {"dp": ahead_on("dp", k)}
        )

    def last(self):
        return remote(self.sent, self.came, self.tp_sems, self.size, other_core())

    def both(self, k):
        return self.part[self.group(k), self.mine].astype(jnp.float32) + self.held[k].astype(
            jnp.float32
        )

    def start(self, places_ref, slots_ref):
        def one(k):
            k = lax.rem(k, self.size)
            group = self.group(k)
            self.part[group] = collect(places_ref, slots_ref, group).astype(jnp.bfloat16)
            self.swap(k).start()

        each(self.size + 1, one)

    def forward(self):
        def one(k):
            self.swap(k).wait_recv()
            self.held[k] = self.both(k).astype(jnp.bfloat16)
            if not self.grid:
                self.copy(k).start()

        each(self.size, one)
        if self.grid:
            self.sum.start()
        self.swap(0).wait()
        self.total[...] = self.both(0)

    def pass_on(self):
        if self.grid:
            self.sum.forward()

    def gather(self):
        def one(k):
            self.copy(k).wait_recv()
            self.total[...] += self.landed[k - 1].astype(jnp.float32)

        if self.grid:
            self.sum.add_to(self.total)
        else:
            each(self.size, one)
        self.sent[...] = self.total[...].astype(jnp.bfloat16)
        self.last().start()

    def finish(self):
        def one(k):
            self.swap(k).wait_send()
            if not self.grid:
                self.copy(k).wait_send()

        each(self.size, one)
        if self.grid:
            self.sum.finish()
        self.last().wait()


def return_scratch(size, rows, width):
    low = jnp.bfloat16
    return [
        pltpu.VMEM((size, rows, width), low),
        pltpu.VMEM((size, rows // 2, width), low),
        pltpu.VMEM((size - 1, rows // 2, width), low),
        pltpu.VMEM((rows // 2, width), jnp.float32),
        pltpu.VMEM((rows // 2, width), low),
        pltpu.VMEM((rows // 2, width), low),
        *sem_pair(max(size, 6)),
        *sem_pair(size + 1),
    ]


def return_grads_kernel(
    slots_ref, places_ref, hidden_ref, cot_ref, gain_ref, out_w_ref, grad_ref, low_ref, mix_ref,
    gain_grad_ref, part, held, landed, total, sent, came, dp_send, dp_recv, tp_send, tp_recv,
):
    greet(["dp", "tp"])
    rows = RowReturn(
        part, held, landed, total, sent, came, (dp_send, dp_recv), (tp_send, tp_recv)
    )
    rows.start(places_ref, slots_ref)
    rows.forward()
    rows.pass_on()
    rows.gather()

    def turn_back(at, grads):
        x_grad, gain_grad = norm_back(
            hidden_ref[at, :], gain_ref[1:2, :], grads.astype(jnp.float32)
        )
        hidden_grad = cot_ref[at, :].astype(jnp.float32) + x_grad
        grad_ref[at, :] = hidden_grad
        low_ref[at, :] = hidden_grad.astype(jnp.bfloat16)
        piece = out_w_ref.shape[2]
        mix = None
        for i in range(out_w_ref.shape[0]):
            one = lax.dot_general(
                low_ref[at, i * piece : (i + 1) * piece],
                out_w_ref[i],
                NT,
                preferred_element_type=jnp.float32,
            )
            mix = one if mix is None else mix + one
        mix_ref[at, :] = mix.astype(jnp.bfloat16)
        return gain_grad

    gain_mine = turn_back(rows.mine, sent[...])
    rows.finish()
    gain_theirs = turn_back(rows.theirs, came[...])
    gain_grad_ref[...] = gain_mine + gain_theirs


def return_grads(slots, places, hidden, cot, gain, out_w, ident):
    size, (rows, width) = slots.shape[0], hidden.shape
    return pl.pallas_call(
        return_grads_kernel,
        name="return_grads",
        in_specs=whole_vmem(6),
        out_specs=whole_vmem(4),
        out_shape=[
            jax.ShapeDtypeStruct((rows, width), jnp.float32),
            jax.ShapeDtypeStruct((rows, width), jnp.bfloat16),
            jax.ShapeDtypeStruct((rows, out_w.shape[1]), jnp.bfloat16),
            jax.ShapeDtypeStruct((1, width), jnp.float32),
        ],
        scratch_shapes=return_scratch(size, rows, width),
        compiler_params=remote_params(ident),
    )(slots, places, hidden, cot, gain, out_w)


def trade_kernel(
    back, ahead, kv_grad_ref, slots_ref, places_ref, low_ref, mix_ref, kv_ref, out_ref, out_w_ref,
    going, came_kv, line_send, line_recv, part, held, landed, total, sent, came, dp_send, dp_recv,
    tp_send, tp_recv,
):
    me, size = lax.axis_index("ctx"), lax.axis_size("ctx")
    greet(["dp", "tp"], line=True)
    right, left = me + 1, me - 1
    sems = (line_send, line_recv)

    step = kv_ref.shape[0] // HOP_PARTS

    def rows_at(j):
        return pl.ds(pl.multiple_of(j * step, step), step)

    def hop(s, src, j):
        at = rows_at(j)
        return remote(
            src.at[at], came_kv.at[s, at], sems, s * HOP_PARTS + j, {"ctx": left}
        )

    def hop_all(s, src):
        each(HOP_PARTS, lambda j: hop(s, src, j).start(), 0)

    def forth():
        return remote(
            kv_grad_ref.at[lax.rem(me + 1, size)], came_kv.at[0], sems, 0, {"ctx": right}
        )

    def own_piece(s):
        return kv_grad_ref.at[lax.rem(me + size - s, size)]

    if ahead:

        @pl.when(right < size)
        def _():
            forth().start()

    @pl.when(me - back >= 0)
    def _():
        hop_all(back, own_piece(back))

    rows = RowReturn(
        part, held, landed, total, sent, came, (dp_send, dp_recv), (tp_send, tp_recv)
    )
    rows.start(places_ref, slots_ref)
    rows.forward()
    turned = jnp.transpose(low_ref[...].astype(jnp.float32)).astype(jnp.bfloat16)
    grad = jnp.dot(turned, mix_ref[...], preferred_element_type=jnp.float32)
    piece = out_w_ref.shape[1]
    for i in range(out_w_ref.shape[0]):
        out_w_ref[i] = grad[i * piece : (i + 1) * piece].astype(jnp.bfloat16)
    rows.pass_on()

    for s in range(back - 1, 0, -1):

        @pl.when((me - s >= 0) & (right < size))
        def _(s=s):
            def one(j):
                at = rows_at(j)
                hop(s + 1, going.at[s], j).wait_recv()
                going[s, at, :] = (
                    own_piece(s)[at, :].astype(jnp.float32)
                    + came_kv[s + 1, at, :].astype(jnp.float32)
                ).astype(going.dtype)
                hop(s, going.at[s], j).start()

            each(HOP_PARTS, one, 0)

        @pl.when((me - s >= 0) & (right >= size))
        def _(s=s):
            hop_all(s, own_piece(s))

    rows.gather()
    kv_ref[...] = kv_grad_ref[me].astype(jnp.float32)

    @pl.when(right < size)
    def _():
        each(HOP_PARTS, lambda j: hop(1, going.at[0], j).wait_recv(), 0)
        kv_ref[...] += came_kv[1].astype(jnp.float32)

    if ahead:

        @pl.when(left >= 0)
        def _():
            forth().wait_recv()
            kv_ref[...] += came_kv[0].astype(jnp.float32)

        @pl.when(right < size)
        def _():
            forth().wait_send()

    for s in range(back, 0, -1):

        @pl.when(me - s >= 0)
        def _(s=s):
            each(HOP_PARTS, lambda j: hop(s, going.at[0], j).wait_send(), 0)

    rows.finish()
    out_ref[rows.mine, :] = sent[...]
    out_ref[rows.theirs, :] = came[...]


def trade(kv_grad, slots, places, low, mix, back, ahead, ident):
    size, (rows, width) = slots.shape[0], low.shape
    kv_shape = kv_grad.shape[1:]
    going = pltpu.VMEM((max(back, 1),) + kv_shape, kv_grad.dtype)
    came = pltpu.VMEM((back + 1,) + kv_shape, kv_grad.dtype)
    return pl.pallas_call(
        functools.partial(trade_kernel, back, ahead),
        name="trade",
        in_specs=whole_vmem(5),
        out_specs=whole_vmem(3),
        out_shape=[
            jax.ShapeDtypeStruct(kv_shape, jnp.float32),
            jax.ShapeDtypeStruct((rows, width), jnp.bfloat16),
            jax.ShapeDtypeStruct((size, width // size, mix.shape[1]), jnp.bfloat16),
        ],
        scratch_shapes=[
            going,
            came,
            *sem_pair((back + 1) * HOP_PARTS),
            *return_scratch(size, rows, width),
        ],
        compiler_params=remote_params(ident),
    )(kv_grad, slots, places, low, mix)


class PieceSum:
    def __init__(self, axis, source, landed, sems, rows):
        self.axis, self.source, self.landed, self.sems = axis, source, landed, sems
        self.size, self.rows = lax.axis_size(axis), rows
        self.parts = source.shape[1] // rows

    def copy(self, k, j):
        peer = ahead_on(self.axis, k)
        at = pl.ds(j * self.rows, self.rows)
        return remote(
            self.source.at[peer, at],
            self.landed.at[k, at],
            self.sems,
            k * self.parts + j,
            {self.axis: peer},
        )

    def every(self, do):
        for j in range(self.parts):
            each(self.size, lambda k, j=j: do(self.copy(k, j)))

    def start(self):
        self.every(lambda copy: copy.start())

    def forward(self):
        pass

    def total(self):
        self.every(lambda copy: copy.wait_recv())
        whole = self.source[lax.axis_index(self.axis)].astype(jnp.float32)
        for k in range(1, self.size):
            whole += self.landed[k].astype(jnp.float32)
        return whole

    def finish(self):
        self.every(lambda copy: copy.wait_send())


class GridPieceSum:
    def __init__(self, source, landed, sems, whole):
        x, y, diagonal = grid_peers()
        places = (lax.axis_index("dp"), x, y, diagonal)
        self.source, self.whole = source, whole
        self.sum = GridSum(lambda n: source.at[places[n]], landed, sems)
        self.start, self.forward, self.finish = self.sum.start, self.sum.forward, self.sum.finish

    def total(self):
        self.whole[...] = self.source[lax.axis_index("dp")].astype(jnp.float32)
        self.sum.add_to(self.whole)
        return self.whole[...]


def dp_sum(source, landed, sems, whole):
    if lax.axis_size("dp") == 4:
        return GridPieceSum(source, landed, sems, whole)
    return PieceSum("dp", source, landed, sems, source.shape[1])


class WholeSum:
    def __init__(self, axis, source, landed, sems):
        self.axis, self.source, self.landed, self.sems = axis, source, landed, sems
        self.size = lax.axis_size(axis)

    def copy(self, k):
        return remote(
            self.source, self.landed.at[k], self.sems, k, {self.axis: ahead_on(self.axis, k)}
        )

    def start(self):
        each(self.size, lambda k: self.copy(k).start())

    def total(self):
        each(self.size, lambda k: self.copy(k).wait())
        whole = self.source[...]
        for k in range(1, self.size):
            whole += self.landed[k]
        return whole


def finish_kernel(
    dq_ref, dkv_ref, cos_ref, sin_ref, normed_ref, w_ref, x_ref, gain_ref, out_w_ref, gain_two_ref,
    in_ref, own_ref, gains_ref, joined, turned, part, held, pieces, landed,
    out_pieces, out_landed, whole, out_whole, low, low_landed, gain_rows, gain_landed, gain_more, gain_more_landed, *sems,
):
    greet(["dp", "ctx", "tp"])
    pairs = [sems[2 * i : 2 * i + 2] for i in range(len(sems) // 2)]
    out_pieces[...] = out_w_ref[...]
    out_sum = dp_sum(out_pieces, out_landed, pairs[0], out_whole)
    out_sum.start()
    wide = 2 * HEAD_DIM
    q_width, kv_width = dq_ref.shape[1], dkv_ref.shape[1] // 2
    cosine, sine = block_tables(cos_ref, sin_ref, dq_ref.shape[0], lax.axis_index("ctx"))
    for first in range(0, q_width, wide):
        joined[:, first : first + wide] = turn(
            dq_ref[:, first : first + wide], cosine, sine
        ).astype(jnp.bfloat16)
    for first in range(0, kv_width, wide):
        joined[:, q_width + first : q_width + first + wide] = turn(
            dkv_ref[:, first : first + wide], cosine, sine
        ).astype(jnp.bfloat16)
    joined[:, q_width + kv_width :] = dkv_ref[:, kv_width:].astype(jnp.bfloat16)

    turned[...] = jnp.transpose(normed_ref[...].astype(jnp.float32)).astype(jnp.bfloat16)
    w_sum = dp_sum(pieces, landed, pairs[1], whole)
    rows = pieces.shape[1]

    def piece(k):
        peer = ahead_on("dp", k)
        at = pl.ds(pl.multiple_of(peer * rows, rows), rows)
        pieces[peer] = jnp.dot(
            turned[at, :], joined[...], preferred_element_type=jnp.float32
        ).astype(jnp.bfloat16)

    each(pieces.shape[0], piece)
    w_sum.start()
    out_sum.forward()
    for i in range(w_ref.shape[0]):
        part[:, i * rows : (i + 1) * rows] = lax.dot_general(
            joined[...], w_ref[i], NT, preferred_element_type=jnp.float32
        ).astype(jnp.bfloat16)
    swap = remote(part, held, pairs[2], 0, other_core())
    swap.start()
    me = lax.axis_index("dp")
    own = pl.ds(pl.multiple_of(me * rows, rows), rows)
    pieces[me] = jnp.dot(
        turned[own, :], joined[...], preferred_element_type=jnp.float32
    ).astype(jnp.bfloat16)
    swap.wait()
    x_grad, gain_grad = norm_back(
        x_ref[...].astype(jnp.float32),
        gain_ref[0:1, :],
        part[...].astype(jnp.float32) + held[...].astype(jnp.float32),
    )
    in_ref[...] = x_grad
    gain_rows[...] = jnp.zeros(gain_rows.shape, jnp.float32)
    gain_rows[0:1, :] = gain_grad
    gain_rows[1:2, :] = gain_two_ref[...]
    gain_sum = WholeSum("dp", gain_rows, gain_landed, pairs[3])
    gain_sum.start()
    w_sum.forward()

    out_total = out_sum.total()
    w_total = w_sum.total()
    cols = w_total.shape[1]
    few = low.shape[1]
    for c in range(low.shape[0]):
        low[c, :, :cols] = w_total[c * few : (c + 1) * few].astype(jnp.bfloat16)
        low[c, :, cols:] = out_total[c * few : (c + 1) * few].astype(jnp.bfloat16)
    low_sum = PieceSum("ctx", low, low_landed, pairs[4], min(few, 16))
    low_sum.start()
    gain_more[...] = gain_sum.total()
    more_sum = WholeSum("ctx", gain_more, gain_more_landed, pairs[5])
    more_sum.start()
    out_sum.finish()
    w_sum.finish()
    own_ref[...] = low_sum.total()
    low_sum.finish()
    gains_ref[...] = more_sum.total()


def finish(dq, dkv, cosine, sine, normed, w, x, gain, out_w, gain_two, ident):
    rows, width = x.shape
    dp_size, ctx_size = lax.axis_size("dp"), lax.axis_size("ctx")
    cols, out_cols = w.shape[2], out_w.shape[2]
    few = width // dp_size // ctx_size
    low, high = jnp.bfloat16, jnp.float32
    return pl.pallas_call(
        finish_kernel,
        name="finish",
        in_specs=whole_vmem(10),
        out_specs=whole_vmem(3),
        out_shape=[
            jax.ShapeDtypeStruct((rows, width), high),
            jax.ShapeDtypeStruct((few, cols + out_cols), high),
            jax.ShapeDtypeStruct((8, width), high),
        ],
        scratch_shapes=[
            pltpu.VMEM((rows, cols), low),
            pltpu.VMEM((width, rows), low),
            pltpu.VMEM((rows, width), low),
            pltpu.VMEM((rows, width), low),
            pltpu.VMEM((dp_size, width // dp_size, cols), low),
            pltpu.VMEM((dp_size, width // dp_size, cols), low),
            pltpu.VMEM(out_w.shape, low),
            pltpu.VMEM(out_w.shape, low),
            pltpu.VMEM((width // dp_size, cols), high),
            pltpu.VMEM((width // dp_size, out_cols), high),
            pltpu.VMEM((ctx_size, few, cols + out_cols), low),
            pltpu.VMEM((ctx_size, few, cols + out_cols), low),
            pltpu.VMEM((8, width), high),
            pltpu.VMEM((dp_size, 8, width), high),
            pltpu.VMEM((8, width), high),
            pltpu.VMEM((ctx_size, 8, width), high),
            *sem_pair(max(dp_size, 6)),
            *sem_pair(max(dp_size, 6)),
            *sem_pair(1),
            *sem_pair(dp_size),
            *sem_pair(ctx_size * (few // min(few, 16))),
            *sem_pair(ctx_size),
        ],
        compiler_params=remote_params(ident),
    )(dq, dkv, cosine, sine, normed, w, x, gain, out_w, gain_two)


class Everyone:
    def __init__(self, axis, target, sems):
        self.axis, self.target, self.sems = axis, target, sems
        self.size = lax.axis_size(axis)

    def copy(self, k):
        at = self.target.at[lax.axis_index(self.axis)]
        return remote(at, at, self.sems, k, {self.axis: ahead_on(self.axis, k)})

    def start(self):
        each(self.size, lambda k: self.copy(k).start())

    def arrive(self):
        each(self.size, lambda k: self.copy(k).wait_recv())

    def finish(self):
        each(self.size, lambda k: self.copy(k).wait_send())


def find_places(first, own, routes_ref, gates_ref, earlier, place_ref, gate_ref, column_ref):
    _, tokens = routes_ref.shape[1:]

    def group(g, carry):
        routes, gates = routes_ref[g], gates_ref[g]
        names, values = [], []
        for e in range(own):
            named = routes == first + e
            names.append(jnp.max(named.astype(jnp.float32), axis=0, keepdims=True))
            values.append(jnp.sum(jnp.where(named, gates, 0.0), axis=0, keepdims=True))
        spare = jnp.zeros((8 - own % 8 if own % 8 else 0, tokens), jnp.float32)
        names = jnp.concatenate(names + ([spare] if spare.shape[0] else []), axis=0)
        place = jnp.dot(
            names.astype(jnp.bfloat16), earlier[...], preferred_element_type=jnp.float32
        )
        place = jnp.where((names > 0.0) & (place < CAP), place, -float(CAP * own))
        for e in range(own):
            place_ref[g, e] = place[e : e + 1].astype(jnp.int32)
            gate_ref[g, e] = values[e]
        column_ref[g] = jnp.transpose(place)[:, :own].astype(jnp.int32)
        return carry

    lax.fori_loop(0, routes_ref.shape[0], group, 0)


class LineRows:
    def __init__(self, x_ref, x_all, back, ahead, line_sems, tp_sems):
        self.x_ref, self.x_all, self.back, self.ahead = x_ref, x_all, back, ahead
        self.line_sems, self.tp_sems = line_sems, tp_sems
        self.me, self.size = lax.axis_index("ctx"), lax.axis_size("ctx")
        self.mine, _ = halves(x_ref.shape[0])

    def block(self, s):
        return lax.rem(self.me + self.size - s, self.size)

    def sends(self, s):
        return (self.me + 1 < self.size) & (self.me - s >= 0)

    def hop(self, s):
        at = self.x_all.at[self.block(s), self.mine]
        source = self.x_ref.at[self.mine] if isinstance(s, int) and s == 0 else at
        return remote(source, at, self.line_sems, s, {"ctx": self.me + 1})

    def back_hop(self):
        at = self.x_all.at[self.me, self.mine]
        return remote(
            self.x_ref.at[self.mine], at, self.line_sems, self.back, {"ctx": self.me - 1}
        )

    def relay(self, k, block):
        at = self.x_all.at[block, self.mine]
        return remote(at, at, self.tp_sems, k, other_core())

    def start(self):
        if self.back:
            pl.when(self.sends(0))(lambda: self.hop(0).start())
        if self.ahead:
            pl.when(self.me >= 1)(lambda: self.back_hop().start())

    def step(self, s):
        @pl.when(self.me - s - 1 >= 0)
        def _():
            self.hop(s).wait_recv()
            self.relay(s, self.block(s + 1)).start()

        if s + 1 < self.back:
            pl.when(self.sends(s + 1))(lambda: self.hop(s + 1).start())

    def step_back(self):
        if self.ahead:

            @pl.when(self.me + 1 < self.size)
            def _():
                self.back_hop().wait_recv()
                self.relay(self.back, self.block(self.size - 1)).start()

    def finish(self):
        for s in range(self.back):
            pl.when(self.sends(s))(lambda s=s: self.hop(s).wait_send())
        if self.ahead:
            pl.when(self.me >= 1)(lambda: self.back_hop().wait_send())


def front_kernel(
    back, ahead, own, starts_ref, x_ref, cot_ref, q_w_ref, k_w_ref, v_w_ref, out_w_ref, gains_ref,
    docs_ref, routes_ref, gates_ref, cos_ref, sin_ref, w_out, out_w_out, gain_rows, docs_all,
    normed_out, q_ref, kv_out, mix_ref, full_out, log_ref, hidden_out, rows_out, cot_out,
    place_ref, gate_ref, column_ref, w_all, out_w_all, normed, kv_all, full, hidden, x_all,
    gains_all, routes_all, gates_all, acc, top, total, column, part, held,
    normed_two, *sems,
):
    me, size = lax.axis_index("ctx"), lax.axis_size("ctx")
    dp = lax.axis_index("dp")
    local = sems[-1]
    pairs = [sems[2 * i : 2 * i + 2] for i in range(len(sems) // 2)]
    q_width, kv_width = q_w_ref.shape[1], k_w_ref.shape[1]
    dp_size, piece = w_all.shape[:2]
    block_rows = x_ref.shape[0]

    def flush(i, source, target):
        return pltpu.make_async_copy(source, target, local.at[i])

    w_all[dp, :, :q_width] = q_w_ref[...]
    w_all[dp, :, q_width : q_width + kv_width] = k_w_ref[...]
    w_all[dp, :, q_width + kv_width :] = v_w_ref[...]
    gains_all[dp] = gains_ref[...]
    docs_all[me] = docs_ref[...]
    routes_all[dp] = routes_ref[...]
    gates_all[dp] = gates_ref[...]
    greet(["dp", "ctx", "tp"])
    weights = Gather(w_all, pairs[1])
    gains = Everyone("dp", gains_all, pairs[0])
    docs = Everyone("ctx", docs_all, pairs[2])
    routes = Everyone("dp", routes_all, pairs[3])
    gates = Everyone("dp", gates_all, pairs[4])
    out_w = Gather(out_w_all, pairs[5])
    line = LineRows(x_ref, x_all, back, ahead, pairs[8], pairs[11])
    for one in (gains, weights, line, docs, routes, gates):
        one.start()

    out_w_all[dp] = out_w_ref[...]
    x_all[me] = x_ref[...]
    token = lax.broadcasted_iota(jnp.int32, (block_rows, block_rows), 0)
    later = lax.broadcasted_iota(jnp.int32, (block_rows, block_rows), 1)
    normed_two[:, :block_rows] = (token < later).astype(jnp.float32).astype(jnp.bfloat16)
    top[...] = jnp.full(top.shape, NEG_FILL, jnp.float32)
    total[...] = jnp.zeros(total.shape, jnp.float32)
    acc[...] = jnp.zeros(acc.shape, jnp.float32)
    gains.arrive()
    for i in range(dp_size):
        gain_rows[:, i * piece : (i + 1) * piece] = gains_all[i]

    def norm_rows(source):
        x = source.astype(jnp.float32)
        return (x * row_scale(x) * gain_rows[0:1, :]).astype(jnp.bfloat16)

    normed[...] = norm_rows(x_ref[...])
    flush(0, normed, normed_out).start()
    routes.arrive()
    gates.arrive()
    docs.arrive()
    if back:
        line.step(0)
    weights.forward()
    find_places(
        dp * own, own, routes_all, gates_all, normed_two.at[:, :block_rows], place_ref, gate_ref,
        column_ref,
    )
    weights.arrive()
    flush(1, w_all, w_out).start()
    out_w.start()
    cot_rows = RowGather(cot_ref, cot_out, pairs[6], pairs[7], 0)
    cot_rows.start()
    last = 2 + back + 1 + ahead
    flush(last + 3, cot_ref, cot_out.at[dp]).start()

    wide, tile = 4 * HEAD_DIM, 2 * HEAD_DIM

    def project(source, first):
        whole = jnp.dot(
            source[:, :piece], w_all[0, :, first : first + wide],
            preferred_element_type=jnp.float32,
        )
        for i in range(1, dp_size):
            whole += jnp.dot(
                source[:, i * piece : (i + 1) * piece], w_all[i, :, first : first + wide],
                preferred_element_type=jnp.float32,
            )
        return [whole[:, :tile], whole[:, tile:]]

    def tables(block):
        cosine, sine = block_tables(cos_ref, sin_ref, block_rows, block)
        return cosine, -sine

    here = tables(me)
    for first in range(0, q_width, wide):
        for i, part_of in enumerate(project(normed, first)):
            turned = turn(part_of, *here).astype(jnp.bfloat16)
            at = first + i * tile
            q_ref[:, at : at + tile] = (turned.astype(jnp.float32) * HEAD_DIM**-0.5).astype(
                jnp.bfloat16
            )
    for s in range(1, back):
        line.step(s)
    line.step_back()
    masks = Masks(docs_all, starts_ref, column)

    def visit(s, block):
        @pl.when(s > 0)
        def _():
            line.relay(s - 1, block).wait()

        part[...] = norm_rows(x_all[block])
        there = tables(block)
        for first in range(q_width, q_width + 2 * kv_width, wide):
            for i, part_of in enumerate(project(part, first)):
                if first < q_width + kv_width:
                    part_of = turn(part_of, *there)
                at = first - q_width + i * tile
                kv_all[block, :, at : at + tile] = part_of.astype(jnp.bfloat16)
        flush(2 + s, kv_all.at[block], kv_out.at[block]).start()
        attend_block(masks, block, q_ref, kv_all.at[block], acc, top, total)

    def step(s):
        pl.when(me - s >= 0)(lambda: visit(s, lax.rem(me + size - s, size)))

        @pl.when(s == min(1, back))
        def _():
            out_w.forward()
            cot_rows.forward()

    each(back + 1, step, 0)
    if ahead:

        @pl.when(me + 1 < size)
        def _():
            visit(back + 1, lax.rem(me + 1, size))

    log_ref[...] = top[...] + jnp.log(total[...])
    for h in range(total.shape[0]):
        at = slice(h * HEAD_DIM, (h + 1) * HEAD_DIM)
        acc[at, :] = acc[at, :] / total[h : h + 1, :]
    full[...] = jnp.transpose(acc[...])
    mix_ref[...] = full[...].astype(jnp.bfloat16)
    out_w.arrive()
    cot_rows.arrive()
    for i in range(dp_size):
        part[:, i * piece : (i + 1) * piece] = jnp.dot(
            mix_ref[...], out_w_all[i], preferred_element_type=jnp.float32
        ).astype(jnp.bfloat16)

    mine, theirs = halves(block_rows)
    rows = RowGather(normed_two, rows_out, pairs[9], pairs[10], 2)
    first = remote(part.at[theirs], held.at[theirs], pairs[10], 0, other_core())
    second = remote(part.at[mine], held.at[mine], pairs[10], 1, other_core())
    first.start()
    second.start()
    flush(last, full, full_out).start()
    flush(last + 1, out_w_all, out_w_out).start()

    def norm(at):
        whole = x_ref[at, :].astype(jnp.float32) + (
            part[at, :].astype(jnp.float32) + held[at, :].astype(jnp.float32)
        )
        hidden[at, :] = whole
        normed_two[at, :] = (whole * row_scale(whole) * gain_rows[1:2, :]).astype(jnp.bfloat16)

    first.wait()
    norm(mine)
    rows.start()
    second.wait()
    norm(theirs)
    flush(last + 2, hidden, hidden_out).start()
    flush(last + 4, normed_two, rows_out.at[dp]).start()
    cot_rows.finish()
    for one in (gains, weights, docs, routes, gates, out_w, line):
        one.finish()
    rows.forward()
    rows.arrive()
    rows.finish()
    flush(0, normed, normed_out).wait()
    flush(1, w_all, w_out).wait()

    def kept(s):
        @pl.when(me - s >= 0)
        def _():
            flush(2 + s, kv_all.at[me], kv_out.at[me]).wait()

    each(back + 1, kept, 0)
    if ahead:
        pl.when(me + 1 < size)(lambda: flush(3 + back, kv_all.at[me], kv_out.at[me]).wait())
    flush(last, full, full_out).wait()
    flush(last + 1, out_w_all, out_w_out).wait()
    flush(last + 2, hidden, hidden_out).wait()
    flush(last + 3, cot_ref, cot_out.at[dp]).wait()
    flush(last + 4, normed_two, rows_out.at[dp]).wait()


def front(
    starts, x, cot, q_w, k_w, v_w, out_w, gains, docs, routes, gates, cosine, sine, own, back,
    ahead, ident,
):
    rows, width = x.shape
    dp_size, ctx_size = lax.axis_size("dp"), lax.axis_size("ctx")
    q_width, kv_cols = q_w.shape[1], 2 * k_w.shape[1]
    piece, heads = q_w.shape[0], q_width // HEAD_DIM
    low, high, whole = jnp.bfloat16, jnp.float32, jnp.int32
    far = [
        ((dp_size, piece, q_width + kv_cols), low),
        ((dp_size,) + out_w.shape, low),
        ((rows, width), low),
        ((ctx_size, rows, kv_cols), low),
        ((rows, q_width), high),
        ((rows, width), high),
        ((dp_size, rows, width), low),
        ((dp_size, rows, width), low),
    ]
    shapes = [
        far[0],
        far[1],
        ((2, width), high),
        ((ctx_size, 1, rows), whole),
        far[2],
        ((rows, q_width), low),
        far[3],
        ((rows, q_width), low),
        far[4],
        ((heads, rows), high),
        far[5],
        far[6],
        far[7],
        ((dp_size, own, 1, rows), whole),
        ((dp_size, own, 1, rows), high),
        ((dp_size, rows, own), whole),
    ]
    return pl.pallas_call(
        functools.partial(front_kernel, back, ahead, own),
        name="front",
        in_specs=[pl.BlockSpec(memory_space=pltpu.SMEM)] + whole_vmem(12),
        out_specs=[
            pl.BlockSpec(memory_space=pl.ANY if shape in far else pltpu.VMEM) for shape in shapes
        ],
        out_shape=[jax.ShapeDtypeStruct(*shape) for shape in shapes],
        scratch_shapes=[
            *[pltpu.VMEM(*shape) for shape in far[:6]],
            pltpu.VMEM((ctx_size, rows, width), low),
            pltpu.VMEM((dp_size,) + gains.shape, high),
            pltpu.VMEM((dp_size,) + routes.shape, whole),
            pltpu.VMEM((dp_size,) + gates.shape, high),
            pltpu.VMEM((q_width, rows), high),
            pltpu.VMEM((heads, rows), high),
            pltpu.VMEM((heads, rows), high),
            pltpu.VMEM((rows, 8), whole),
            pltpu.VMEM((rows, width), low),
            pltpu.VMEM((rows, width), low),
            pltpu.VMEM((rows, width), low),
            *sem_pair(dp_size),
            *sem_pair(dp_size),
            *sem_pair(ctx_size),
            *sem_pair(dp_size),
            *sem_pair(dp_size),
            *sem_pair(dp_size),
            *sem_pair(dp_size),
            *sem_pair(dp_size),
            *sem_pair(back + 1),
            *sem_pair(dp_size),
            *sem_pair(dp_size + 2),
            *sem_pair(back + 1),
            pltpu.SemaphoreType.DMA((8 + back + ahead,)),
        ],
        compiler_params=remote_params(ident),
    )(starts, x, cot, q_w, k_w, v_w, out_w, gains, docs, routes, gates, cosine, sine)


GROUPS_AT_ONCE = 4


def experts_kernel(more, rows_ref, grads_ref, weights_ref, place_ref, gate_ref, *refs):
    outs_ref, backs_ref, weight_grad_ref, slots, slot_grads = refs[2 * more :]
    groups, tok_rows, _ = rows_ref.shape
    owners, part = weight_grad_ref.shape[1], weight_grad_ref.shape[5]
    slot_index = lax.broadcasted_iota(jnp.int32, (CAP, tok_rows), 0)
    gates = []
    for g in range(groups):
        picks = slot_index == place_ref[g, 0]
        gates.append(jnp.sum(jnp.where(picks, gate_ref[g, 0], 0.0), axis=1, keepdims=True))
        picks = picks.astype(jnp.float32).astype(jnp.bfloat16)
        at = slice(g * CAP, (g + 1) * CAP)
        slots[at, :] = jnp.dot(
            picks, rows_ref[g], preferred_element_type=jnp.float32
        ).astype(jnp.bfloat16)
        slot_grads[at, :] = (
            jnp.dot(picks, grads_ref[g], preferred_element_type=jnp.float32) * gates[g]
        ).astype(jnp.bfloat16)
    gate_w, up_w, down_w = (weights_ref.at[0, i] for i in range(3))
    gate_pre = jnp.dot(slots[...], gate_w[...], preferred_element_type=jnp.float32)
    up_pre = jnp.dot(slots[...], up_w[...], preferred_element_type=jnp.float32)
    act_grad = jnp.dot(slot_grads[...], down_w[...], preferred_element_type=jnp.float32)
    sig = 1.0 / (1.0 + jnp.exp(-gate_pre))
    silu = gate_pre * sig
    act_low = (silu * up_pre).astype(jnp.bfloat16)
    up_low = (act_grad * silu).astype(jnp.bfloat16)
    gate_low = (act_grad * up_pre * (sig * (1.0 + gate_pre * (1.0 - sig)))).astype(jnp.bfloat16)

    back = lax.dot_general(
        gate_low, gate_w[...], NT, preferred_element_type=jnp.float32
    ) + lax.dot_general(up_low, up_w[...], NT, preferred_element_type=jnp.float32)
    out = lax.dot_general(act_low, down_w[...], NT, preferred_element_type=jnp.float32)
    for g in range(groups):
        at = slice(g * CAP, (g + 1) * CAP)
        backs_ref[g] = back[at].astype(jnp.bfloat16)
        outs_ref[g] = (out[at] * gates[g]).astype(jnp.bfloat16)

    for i, (low, source) in enumerate(
        ((gate_low, slots), (up_low, slots), (act_low, slot_grads))
    ):
        turned = jnp.transpose(low.astype(jnp.float32)).astype(jnp.bfloat16)
        total = jnp.dot(turned, source[...], preferred_element_type=jnp.float32)
        for c in range(owners):
            weight_grad_ref[0, c, 0, i] = total[:, c * part : (c + 1) * part].astype(
                weight_grad_ref.dtype
            )


def experts(weights, place_rows, gate_rows, rows_all, grad_all, first, count, before):
    own, _, model_width, hidden = weights.shape
    groups, tok_rows, _ = rows_all.shape
    owners = lax.axis_size("ctx")
    at_once = min(GROUPS_AT_ONCE, groups)
    chunks = groups // at_once
    part = model_width // owners
    rows_spec = pl.BlockSpec(
        (at_once, tok_rows, model_width), lambda c, e: (c, 0, 0), pipeline_mode=pl.Buffered(1)
    )
    line_spec = pl.BlockSpec((at_once, 1, 1, tok_rows), lambda c, e: (c, e + first, 0, 0))
    slots_spec = pl.BlockSpec((at_once, CAP, model_width), lambda c, e: (c, e + first, 0))
    slots_shape = jax.ShapeDtypeStruct((groups, own * CAP, model_width), jnp.bfloat16)
    flops = count * groups * CAP * model_width * 2 * (9 * hidden + 2 * tok_rows)
    more = before is not None
    outs, backs, weight_part = pl.pallas_call(
        functools.partial(experts_kernel, more),
        name="experts",
        grid=(chunks, count),
        in_specs=[
            rows_spec,
            rows_spec,
            pl.BlockSpec((1, 3, model_width, hidden), lambda c, e: (e + first, 0, 0, 0)),
            line_spec,
            line_spec,
        ]
        + [pl.BlockSpec(memory_space=pl.ANY)] * (2 * more),
        out_specs=[
            slots_spec,
            slots_spec,
            pl.BlockSpec((1, owners, 1, 3, hidden, part), lambda c, e: (c, 0, e, 0, 0, 0)),
        ],
        out_shape=[
            slots_shape,
            slots_shape,
            jax.ShapeDtypeStruct((chunks, owners, count, 3, hidden, part), jnp.bfloat16),
        ],
        scratch_shapes=[
            pltpu.VMEM((at_once * CAP, model_width), jnp.bfloat16),
            pltpu.VMEM((at_once * CAP, model_width), jnp.bfloat16),
        ],
        input_output_aliases={5: 0, 6: 1} if more else {},
        compiler_params=pltpu.CompilerParams(vmem_limit_bytes=LIMIT),
        cost_estimate=pl.CostEstimate(
            flops=flops, bytes_accessed=4 * weights.size, transcendentals=0
        ),
    )(rows_all, grad_all, weights, place_rows, gate_rows, *(before if more else ()))
    if chunks == 1:
        return (outs, backs), weight_part[0]
    return (outs, backs), jnp.sum(weight_part.astype(jnp.float32), axis=0).astype(jnp.bfloat16)


def unfold_kernel(more, sums_ref, *refs):
    out_ref = refs[more]
    for i in range(sums_ref.shape[1]):
        out_ref[0, i] = jnp.transpose(sums_ref[0, i].astype(jnp.float32))


def unfold(sums, own, first, before):
    count, three, hidden, part = sums.shape
    more = before is not None
    return pl.pallas_call(
        functools.partial(unfold_kernel, more),
        name="unfold",
        grid=(count,),
        in_specs=[pl.BlockSpec((1, three, hidden, part), lambda e: (e, 0, 0, 0))]
        + [pl.BlockSpec(memory_space=pl.ANY)] * more,
        out_specs=pl.BlockSpec((1, three, part, hidden), lambda e: (e + first, 0, 0, 0)),
        out_shape=jax.ShapeDtypeStruct((own, three, part, hidden), jnp.float32),
        input_output_aliases={1: 0} if more else {},
        compiler_params=pltpu.CompilerParams(vmem_limit_bytes=LIMIT),
    )(sums, *([before] if more else []))


def rotary_tables(token_positions):
    half_dim = HEAD_DIM // 2
    inverse = THETA ** (-(jnp.arange(half_dim, dtype=jnp.float32) * 2.0 / HEAD_DIM))
    angles = token_positions.astype(jnp.float32)[:, None] * inverse[None, :]
    cosine, sine = jnp.cos(angles), jnp.sin(angles)
    return jnp.concatenate([cosine] * 4, axis=1), jnp.concatenate([sine, -sine] * 2, axis=1)


def expert_counts(own):
    return (1, 6, 1) if own == 8 else (own - own // 2, own // 2)


def scatter(grads):
    return lax.psum_scatter(grads, "ctx", scatter_dimension=0)


def body(
    tokens,
    query_weight,
    key_weight,
    value_weight,
    output_weight,
    gain_attn,
    gain_moe,
    expert_weights,
    routes,
    gate_values,
    documents,
    pic_starts,
    cotangent,
):
    block_len = tokens.shape[1]
    ctx_size = lax.axis_size("ctx")
    length = block_len * ctx_size
    back = back_blocks(ctx_size, block_len, length)
    ahead = ahead_blocks(block_len, length, pic_starts.shape[1])
    q_width, kv_width = query_weight.shape[1], key_weight.shape[1]
    own = expert_weights.shape[0]
    x, cot = tokens[0], cotangent[0]

    inside = jnp.arange(block_len, dtype=jnp.int32)
    starts = jnp.arange(-(-ctx_size // 8) * 8, dtype=jnp.int32) * block_len
    cosine, sine = rotary_tables(jnp.concatenate([inside, starts]))
    (
        w_all,
        out_w_all,
        gain_rows,
        docs_all,
        normed_one,
        query,
        kv_all,
        mixture,
        mix_full,
        log_total,
        hidden,
        rows_all,
        grad_all,
        *places,
    ) = front(
        pic_starts,
        x,
        cot,
        query_weight,
        key_weight,
        value_weight,
        output_weight,
        jnp.stack([gain_attn, gain_moe]).astype(jnp.float32),
        documents,
        routes[0].T,
        gate_values[0].T,
        cosine,
        sine,
        own,
        back,
        ahead,
        1,
    )
    place_rows, gate_rows, places = places
    counts = expert_counts(own)
    slots, sums = None, []
    first = 0
    for n, count in enumerate(counts):
        slots, grads = experts(
            expert_weights, place_rows, gate_rows, rows_all, grad_all, first, count, slots
        )
        if n < len(counts) - 1:
            sums.append((scatter(grads), first))
        first += count
    outs, backs = slots
    hidden_grad, hidden_low, mix_grad, gain_two_grad = return_grads(
        backs, places, hidden, cot, gain_rows, out_w_all, 2
    )
    q_rot_grad, kv_part = attend_back(
        pic_starts, query, kv_all, docs_all, log_total, mix_full, mix_grad, back, ahead
    )
    kv_back, expert_sum, output_grad = trade(
        kv_part,
        outs,
        places,
        hidden_low,
        mixture,
        back,
        ahead,
        3,
    )
    x_grad, owned, gain_sums = finish(
        q_rot_grad,
        kv_back,
        cosine,
        sine,
        normed_one,
        w_all,
        x,
        gain_rows,
        output_grad,
        gain_two_grad,
        4,
    )
    grads, owned = lax.optimization_barrier((grads, owned))
    sums.append((scatter(grads), own - counts[-1]))
    few = owned.shape[0]
    here = (lax.axis_index("dp") * ctx_size + lax.axis_index("ctx")) * few
    gain_sums = lax.dynamic_slice_in_dim(gain_sums, here, few, 1)
    expert_grad = None
    for part, first in sums:
        expert_grad = unfold(part, own, first, expert_grad)
    v_end = q_width + 2 * kv_width
    return (
        (hidden + expert_sum.astype(jnp.float32)).astype(jnp.bfloat16)[None],
        (hidden_grad + x_grad).astype(jnp.bfloat16)[None],
        owned[:, :q_width],
        owned[:, q_width : q_width + kv_width],
        owned[:, q_width + kv_width : v_end],
        owned[:, v_end:].T,
        gain_sums[0],
        gain_sums[1],
        expert_grad,
    )


def solution(mesh):
    return jax.shard_map(
        body,
        mesh=mesh,
        in_specs=(
            P("dp", "ctx", None),
            P("dp", "tp"),
            P("dp", "tp"),
            P("dp", "tp"),
            P("tp", "dp"),
            P("dp"),
            P("dp"),
            P("dp", None, None, "tp"),
            P("dp", "ctx", None),
            P("dp", "ctx", None),
            P("dp", "ctx"),
            P("dp", None),
            P("dp", "ctx", None),
        ),
        out_specs=(
            P("dp", "ctx", None),
            P("dp", "ctx", None),
            P(("dp", "ctx"), "tp"),
            P(("dp", "ctx"), "tp"),
            P(("dp", "ctx"), "tp"),
            P("tp", ("dp", "ctx")),
            P(("dp", "ctx")),
            P(("dp", "ctx")),
            P("dp", None, "ctx", "tp"),
        ),
        check_vma=False,
    )
```

```python
import functools

import jax
import jax.numpy as jnp
from jax import lax
from jax.experimental import pallas as pl
from jax.experimental.pallas import tpu as pltpu
from jax.sharding import PartitionSpec as P

HEAD_DIM = 64
PIC = 256
CAP = 144

EPSILON = 1e-06
THETA = 10000.0
NEG_FILL = -1e30


KEY_ROWS = 256
NT = (((1,), (1,)), ((), ()))
LIMIT = 67043328


def whole_vmem(count):
    return [pl.BlockSpec(memory_space=pltpu.VMEM)] * count


def picture_ids(starts_ref, places):
    ids = jnp.full(places.shape, -1, jnp.int32)
    for j in range(starts_ref.shape[1]):
        start = starts_ref[0, j]
        ids += jnp.where((places >= start) & (places < start + PIC), j + 1, 0)
    return ids


def as_column(row):
    tall = jnp.broadcast_to(row.astype(jnp.float32), (8, row.shape[1]))
    return jnp.transpose(tall)[:, 0:1].astype(jnp.int32)


class Masks:
    def __init__(self, docs_ref, starts_ref, column):
        self.docs_ref, self.starts_ref, self.column = docs_ref, starts_ref, column
        self.rows = docs_ref.shape[2]
        me = lax.axis_index("ctx")
        self.q_doc = docs_ref[me]
        self.q_place = me * self.rows + lax.broadcasted_iota(jnp.int32, (1, self.rows), 1)
        self.q_pic = picture_ids(starts_ref, self.q_place)

    def open(self, block):
        self.column[...] = jnp.broadcast_to(
            as_column(self.docs_ref[block]), self.column.shape
        )

    def bias(self, block, rows, first):
        k_doc = self.column[rows, 0:1]
        k_place = block * self.rows + first + lax.broadcasted_iota(jnp.int32, k_doc.shape, 0)
        k_pic = picture_ids(self.starts_ref, k_place)
        seen = (k_doc == self.q_doc) & (
            (k_place <= self.q_place) | ((k_pic == self.q_pic) & (self.q_pic >= 0))
        )
        return jnp.where(seen, 0.0, NEG_FILL)


def attend_block(masks, block, q_ref, kv_ref, acc, top, total):
    kv_width = kv_ref.shape[1] // 2
    heads, kv_heads = q_ref.shape[1] // HEAD_DIM, kv_width // HEAD_DIM
    masks.open(block)

    def step(j, carry):
        first = pl.multiple_of(j * KEY_ROWS, KEY_ROWS)
        rows = pl.ds(first, KEY_ROWS)
        bias = masks.bias(block, rows, first)
        for g in range(kv_heads):
            key = kv_ref[rows, g * HEAD_DIM : (g + 1) * HEAD_DIM]
            val = kv_ref[rows, kv_width + g * HEAD_DIM : kv_width + (g + 1) * HEAD_DIM]
            val_t = jnp.transpose(val.astype(jnp.float32)).astype(jnp.bfloat16)
            for h in range(g * heads // kv_heads, (g + 1) * heads // kv_heads):
                at = slice(h * HEAD_DIM, (h + 1) * HEAD_DIM)
                scores = bias + lax.dot_general(
                    key, q_ref[:, at], NT, preferred_element_type=jnp.float32
                )
                old = top[h : h + 1, :]
                new = jnp.maximum(old, jnp.max(scores, axis=0, keepdims=True))
                probs = jnp.exp(scores - new)
                fade = jnp.exp(old - new)
                total[h : h + 1, :] = total[h : h + 1, :] * fade + jnp.sum(
                    probs, axis=0, keepdims=True
                )
                acc[at, :] = acc[at, :] * fade + jnp.dot(
                    val_t, probs.astype(jnp.bfloat16), preferred_element_type=jnp.float32
                )
                top[h : h + 1, :] = new
        return carry

    lax.fori_loop(0, kv_ref.shape[0] // KEY_ROWS, step, 0)


def attend_back_block(
    masks, edges, block, q_ref, kv_ref, log_ref, delta, grad_ref, acc, dkv_ref
):
    kv_width = kv_ref.shape[1] // 2
    heads, kv_heads = q_ref.shape[1] // HEAD_DIM, kv_width // HEAD_DIM
    masks.open(block)
    count = kv_ref.shape[0] // KEY_ROWS
    me = lax.axis_index("ctx")
    q_first, q_last = edges[me * count, 0], edges[me * count + count - 1, 1]

    def step(j, carry):
        at = block * count + j
        same = (edges[at, 0] <= q_last) & (edges[at, 1] >= q_first)

        @pl.when(same)
        def _():
            inside(j)

        @pl.when(jnp.logical_not(same))
        def _():
            rows = pl.ds(pl.multiple_of(j * KEY_ROWS, KEY_ROWS), KEY_ROWS)
            dkv_ref[rows, :] = jnp.zeros((KEY_ROWS, dkv_ref.shape[1]), dkv_ref.dtype)

        return carry

    def inside(j):
        first = pl.multiple_of(j * KEY_ROWS, KEY_ROWS)
        rows = pl.ds(first, KEY_ROWS)
        bias = masks.bias(block, rows, first)
        for g in range(kv_heads):
            k_at = slice(g * HEAD_DIM, (g + 1) * HEAD_DIM)
            v_at = slice(kv_width + g * HEAD_DIM, kv_width + (g + 1) * HEAD_DIM)
            key, val = kv_ref[rows, k_at], kv_ref[rows, v_at]
            key_t = jnp.transpose(key.astype(jnp.float32)).astype(jnp.bfloat16)
            dk = jnp.zeros((KEY_ROWS, HEAD_DIM), jnp.float32)
            dv = jnp.zeros((KEY_ROWS, HEAD_DIM), jnp.float32)
            for h in range(g * heads // kv_heads, (g + 1) * heads // kv_heads):
                at = slice(h * HEAD_DIM, (h + 1) * HEAD_DIM)
                q_rows, g_rows = q_ref[:, at], grad_ref[:, at]
                scores = bias + lax.dot_general(
                    key, q_rows, NT, preferred_element_type=jnp.float32
                )
                probs = jnp.exp(scores - log_ref[h : h + 1, :])
                prob_grad = lax.dot_general(val, g_rows, NT, preferred_element_type=jnp.float32)
                slope = (probs * (prob_grad - delta[h : h + 1, :])).astype(jnp.bfloat16)
                dv += jnp.dot(
                    probs.astype(jnp.bfloat16), g_rows, preferred_element_type=jnp.float32
                )
                dk += jnp.dot(slope, q_rows, preferred_element_type=jnp.float32)
                acc[at, :] += jnp.dot(key_t, slope, preferred_element_type=jnp.float32)
            dkv_ref[rows, k_at] = dk.astype(dkv_ref.dtype)
            dkv_ref[rows, v_at] = dv.astype(dkv_ref.dtype)

    lax.fori_loop(0, count, step, 0)


def attend_back_kernel(
    back, ahead, starts_ref, edges, q_ref, kv_ref, docs_ref, log_ref, full_ref, grad_ref, dq_ref,
    dkv_ref, acc, delta, column,
):
    me, size = lax.axis_index("ctx"), lax.axis_size("ctx")
    acc[...] = jnp.transpose(full_ref[...] * grad_ref[...].astype(jnp.float32))
    for h in range(delta.shape[0]):
        delta[h : h + 1, :] = jnp.sum(
            acc[h * HEAD_DIM : (h + 1) * HEAD_DIM, :], axis=0, keepdims=True
        )
    acc[...] = jnp.zeros(acc.shape, jnp.float32)
    masks = Masks(docs_ref, starts_ref, column)

    def step(s, carry):
        block = me + ahead - s

        @pl.when((block >= 0) & (block < size))
        def _():
            attend_back_block(
                masks, edges, block, q_ref, kv_ref.at[block], log_ref, delta, grad_ref, acc,
                dkv_ref.at[block],
            )

        return carry

    lax.fori_loop(0, back + ahead + 1, step, 0)
    dq_ref[...] = jnp.transpose(acc[...]) * (HEAD_DIM**-0.5)


def attend_back(starts, q, kv, docs, log_total, full, grad, back, ahead):
    rows, width = q.shape
    by_block = docs.reshape(-1, KEY_ROWS)
    edges = jnp.concatenate([by_block[:, :1], by_block[:, -1:]], axis=1)
    return pl.pallas_call(
        functools.partial(attend_back_kernel, back, ahead),
        name="attend_back",
        in_specs=[pl.BlockSpec(memory_space=pltpu.SMEM)] * 2 + whole_vmem(6),
        out_specs=whole_vmem(2),
        out_shape=[
            jax.ShapeDtypeStruct((rows, width), jnp.float32),
            jax.ShapeDtypeStruct(kv.shape, jnp.bfloat16),
        ],
        scratch_shapes=[
            pltpu.VMEM((width, rows), jnp.float32),
            pltpu.VMEM((width // HEAD_DIM, rows), jnp.float32),
            pltpu.VMEM((rows, 8), jnp.int32),
        ],
        compiler_params=pltpu.CompilerParams(vmem_limit_bytes=LIMIT),
    )(starts, edges, q, kv, docs, log_total, full, grad)


MESH = pl.DeviceIdType.MESH


def greet(axes_list, line=False):
    barrier = pltpu.get_barrier_semaphore()
    count = 0
    for axis in axes_list:
        me, size = lax.axis_index(axis), lax.axis_size(axis)

        def signal(k, carry, axis=axis, me=me, size=size):
            pl.semaphore_signal(
                barrier, inc=1, device_id={axis: lax.rem(me + k, size)}, device_id_type=MESH
            )
            return carry

        lax.fori_loop(1, size, signal, 0)
        count += size - 1
    if not line:
        pl.semaphore_wait(barrier, count)
        return
    me, size = lax.axis_index("ctx"), lax.axis_size("ctx")
    for step in (1, -1):
        other = me + step

        @pl.when((other >= 0) & (other < size))
        def _(other=other):
            pl.semaphore_signal(barrier, inc=1, device_id={"ctx": other}, device_id_type=MESH)

    inner = (me > 0) & (me < size - 1)

    @pl.when(inner)
    def _():
        pl.semaphore_wait(barrier, count + 2)

    @pl.when(jnp.logical_not(inner))
    def _():
        pl.semaphore_wait(barrier, count + 1)


def remote(src, dst, sems, k, device_id):
    return pltpu.make_async_remote_copy(
        src_ref=src,
        dst_ref=dst,
        send_sem=sems[0].at[k],
        recv_sem=sems[1].at[k],
        device_id=device_id,
        device_id_type=MESH,
    )


def other_core():
    return {"tp": 1 - lax.axis_index("tp")}


def ahead_on(axis, k):
    return lax.rem(lax.axis_index(axis) + k, lax.axis_size(axis))


def each(count, do, first=1):
    def step(k, carry):
        do(k)
        return carry

    lax.fori_loop(first, count, step, 0)


def sem_pair(count):
    return [pltpu.SemaphoreType.DMA((count,)), pltpu.SemaphoreType.DMA((count,))]


def remote_params(ident):
    return pltpu.CompilerParams(
        collective_id=ident, has_side_effects=True, vmem_limit_bytes=LIMIT
    )


def halves(rows):
    half = rows // 2
    core = lax.axis_index("tp")
    return (
        pl.ds(pl.multiple_of(core * half, half), half),
        pl.ds(pl.multiple_of((1 - core) * half, half), half),
    )


def turn(tile, cosine, sine):
    lane = lax.broadcasted_iota(jnp.int32, tile.shape, 1)
    half = HEAD_DIM // 2
    swapped = jnp.where(
        lax.rem(lane, HEAD_DIM) < half,
        pltpu.roll(tile, 2 * HEAD_DIM - half, 1),
        pltpu.roll(tile, half, 1),
    )
    return tile * cosine + swapped * sine


def block_tables(cos_ref, sin_ref, rows, block):
    start = pl.ds(rows + block, 1)
    in_cos, in_sin = cos_ref[:rows, :], sin_ref[:rows, :]
    at_cos, at_sin = cos_ref[start, :], sin_ref[start, :]
    return in_cos * at_cos - in_sin * at_sin, in_sin * at_cos + in_cos * at_sin


def row_scale(x):
    return lax.rsqrt(jnp.mean(x * x, axis=-1, keepdims=True) + EPSILON)


def norm_back(x, gain, grad):
    scale = row_scale(x)
    unit = x * scale
    pull = grad * gain
    return (
        scale * (pull - unit * jnp.mean(pull * unit, axis=-1, keepdims=True)),
        jnp.sum(grad * unit, axis=0, keepdims=True),
    )


def back_blocks(ctx_size, block_len, length):
    return min(ctx_size - 1, -(-(length // 2 - 1) // block_len))


def ahead_blocks(block_len, length, spans):
    return 0 if block_len % (length // spans) == 0 else 1


def grid_peers():
    me = lax.axis_index("dp")
    x, y = lax.rem(me, 2), lax.div(me, 2)
    return y * 2 + 1 - x, (1 - y) * 2 + x, 3 - me


class Gather:
    def __init__(self, target, sems, rows=None, source=None):
        self.target, self.sems, self.rows, self.source = target, sems, rows, source
        self.size = lax.axis_size("dp")
        self.grid = self.size == 4

    def at(self, place):
        return self.target.at[place] if self.rows is None else self.target.at[place, self.rows]

    def half(self, place, n):
        if self.rows is None:
            count = self.target.shape[1] // 2
            return self.target.at[place, pl.ds(n * count, count)]
        count = self.rows.size // 2
        first = pl.multiple_of(self.rows.start + n * count, count)
        return self.target.at[place, pl.ds(first, count)]

    def first(self, k, peer):
        place = self.at(lax.axis_index("dp"))
        source = place if self.source is None else self.source.at[self.rows]
        return remote(source, place, self.sems, k, {"dp": peer})

    def passed(self, k, place, n, peer):
        at = self.half(place, n)
        return remote(at, at, self.sems, k, {"dp": peer})

    def direct(self, k):
        return self.first(k, ahead_on("dp", k))

    def start(self):
        if not self.grid:
            each(self.size, lambda k: self.direct(k).start())
            return
        x, y, _ = grid_peers()
        self.first(0, x).start()
        self.first(1, y).start()

    def forward(self, came=None):
        if not self.grid:
            return
        x, y, _ = grid_peers()
        self.first(0, x).wait_recv()
        self.passed(2, x, 0, y).start()
        if came:
            came(0, self.at(x))
        self.first(1, y).wait_recv()
        self.passed(3, y, 1, x).start()
        if came:
            came(1, self.at(y))

    def arrive(self, came=None):
        if not self.grid:

            def one(k):
                self.direct(k).wait_recv()
                if came:
                    came(k, self.at(ahead_on("dp", self.size - k)))

            each(self.size, one)
            return
        x, _, diagonal = grid_peers()
        for n in range(2):
            self.passed(2 + n, diagonal, n, x).wait_recv()
            if came:
                came(2 + n, self.half(diagonal, n))

    def finish(self):
        if not self.grid:
            each(self.size, lambda k: self.direct(k).wait_send())
            return
        x, y, _ = grid_peers()
        self.first(0, x).wait_send()
        self.first(1, y).wait_send()
        self.passed(2, x, 0, y).wait_send()
        self.passed(3, y, 1, x).wait_send()


class RowGather:
    def __init__(self, source, target, dp_sems, tp_sems, first):
        mine, _ = halves(source.shape[0])
        self.gather = Gather(target, dp_sems, mine, source)
        self.tp_sems, self.after = tp_sems, first

    def relay(self, k, at):
        return remote(at, at, self.tp_sems, self.after + k, other_core())

    def came(self, k, at):
        self.relay(k, at).start()

    def start(self):
        self.gather.start()

    def forward(self):
        self.gather.forward(self.came)

    def arrive(self):
        self.gather.arrive(self.came)

    def finish(self):
        self.gather.finish()
        gather = self.gather
        if not gather.grid:
            each(
                gather.size,
                lambda k: self.relay(k, gather.at(ahead_on("dp", gather.size - k))).wait(),
            )
            return
        x, y, diagonal = grid_peers()
        self.relay(0, gather.at(x)).wait()
        self.relay(1, gather.at(y)).wait()
        self.relay(2, gather.half(diagonal, 0)).wait()
        self.relay(3, gather.half(diagonal, 1)).wait()


def collect(places_ref, slots_ref, group):
    tok_rows, slot_count = places_ref.shape[1], slots_ref.shape[1]
    tiles = []
    for first in range(0, slot_count, 128):
        wide = min(128, slot_count - first)
        lane = first + lax.broadcasted_iota(jnp.int32, (tok_rows, wide), 1)
        hit = None
        for n in range(first // CAP, (first + wide - 1) // CAP + 1):
            one = places_ref[group, :, n : n + 1] == lane - n * CAP
            hit = one if hit is None else hit | one
        tiles.append(hit.astype(jnp.float32).astype(jnp.bfloat16))
    return jnp.dot(
        jnp.concatenate(tiles, axis=1), slots_ref[group], preferred_element_type=jnp.float32
    )


class GridSum:
    def __init__(self, piece, landed, sems):
        self.piece, self.landed, self.sems = piece, landed, sems
        self.x, self.y, _ = grid_peers()
        self.count = landed.shape[1] // 2

    def half(self, n, which):
        return self.piece(n).at[pl.ds(which * self.count, self.count)]

    def slot(self, j):
        return self.landed.at[j // 2, pl.ds(j % 2 * self.count, self.count)]

    def copy(self, j):
        n, which, peer = (
            (1, 0, self.x),
            (3, 0, self.x),
            (2, 1, self.y),
            (3, 1, self.y),
            (2, 0, self.y),
            (1, 1, self.x),
        )[j]
        return remote(self.half(n, which), self.slot(j), self.sems, j, {"dp": peer})

    def start(self):
        for j in (1, 3, 0, 2):
            self.copy(j).start()

    def forward(self):
        for j, n, which in ((1, 2, 0), (3, 1, 1)):
            self.copy(j).wait_recv()
            half = self.half(n, which)
            half[...] = (
                half[...].astype(jnp.float32) + self.slot(j)[...].astype(jnp.float32)
            ).astype(jnp.bfloat16)
            self.copy(4 + j // 2).start()

    def add_to(self, total):
        for which, slots in ((0, (0, 4)), (1, (2, 5))):
            at = pl.ds(which * self.count, self.count)
            for j in slots:
                self.copy(j).wait_recv()
                total[at, :] += self.slot(j)[...].astype(jnp.float32)

    def finish(self):
        for j in range(6):
            self.copy(j).wait_send()


class RowReturn:
    def __init__(self, part, held, landed, total, sent, came, dp_sems, tp_sems):
        self.part, self.held, self.landed, self.total = part, held, landed, total
        self.sent, self.came, self.dp_sems, self.tp_sems = sent, came, dp_sems, tp_sems
        self.size = lax.axis_size("dp")
        self.mine, self.theirs = halves(part.shape[1])
        self.grid = self.size == 4
        if self.grid:
            self.sum = GridSum(lambda n: held.at[n], landed, dp_sems)

    def group(self, k):
        if not self.grid:
            return ahead_on("dp", k)
        me = lax.axis_index("dp")
        x, y = lax.rem(me, 2), lax.div(me, 2)
        flip_x, flip_y = lax.rem(k, 2), lax.div(k, 2)
        return lax.rem(y + flip_y, 2) * 2 + lax.rem(x + flip_x, 2)

    def swap(self, k):
        return remote(
            self.part.at[self.group(k), self.theirs], self.held.at[k], self.tp_sems, k,
            other_core(),
        )

    def copy(self, k):
        return remote(
            self.held.at[k], self.landed.at[k - 1], self.dp_sems, k, {"dp": ahead_on("dp", k)}
        )

    def last(self):
        return remote(self.sent, self.came, self.tp_sems, self.size, other_core())

    def both(self, k):
        return self.part[self.group(k), self.mine].astype(jnp.float32) + self.held[k].astype(
            jnp.float32
        )

    def start(self, places_ref, slots_ref):
        def one(k):
            k = lax.rem(k, self.size)
            group = self.group(k)
            self.part[group] = collect(places_ref, slots_ref, group).astype(jnp.bfloat16)
            self.swap(k).start()

        each(self.size + 1, one)

    def forward(self):
        def one(k):
            self.swap(k).wait_recv()
            self.held[k] = self.both(k).astype(jnp.bfloat16)
            if not self.grid:
                self.copy(k).start()

        each(self.size, one)
        if self.grid:
            self.sum.start()
        self.swap(0).wait()
        self.total[...] = self.both(0)

    def pass_on(self):
        if self.grid:
            self.sum.forward()

    def gather(self):
        def one(k):
            self.copy(k).wait_recv()
            self.total[...] += self.landed[k - 1].astype(jnp.float32)

        if self.grid:
            self.sum.add_to(self.total)
        else:
            each(self.size, one)
        self.sent[...] = self.total[...].astype(jnp.bfloat16)
        self.last().start()

    def finish(self):
        def one(k):
            self.swap(k).wait_send()
            if not self.grid:
                self.copy(k).wait_send()

        each(self.size, one)
        if self.grid:
            self.sum.finish()
        self.last().wait()


def return_scratch(size, rows, width):
    low = jnp.bfloat16
    return [
        pltpu.VMEM((size, rows, width), low),
        pltpu.VMEM((size, rows // 2, width), low),
        pltpu.VMEM((size - 1, rows // 2, width), low),
        pltpu.VMEM((rows // 2, width), jnp.float32),
        pltpu.VMEM((rows // 2, width), low),
        pltpu.VMEM((rows // 2, width), low),
        *sem_pair(max(size, 6)),
        *sem_pair(size + 1),
    ]


def return_grads_kernel(
    slots_ref, places_ref, hidden_ref, cot_ref, gain_ref, out_w_ref, grad_ref, low_ref, mix_ref,
    gain_grad_ref, part, held, landed, total, sent, came, dp_send, dp_recv, tp_send, tp_recv,
):
    greet(["dp", "tp"])
    rows = RowReturn(
        part, held, landed, total, sent, came, (dp_send, dp_recv), (tp_send, tp_recv)
    )
    rows.start(places_ref, slots_ref)
    rows.forward()
    rows.pass_on()
    rows.gather()

    def turn_back(at, grads):
        x_grad, gain_grad = norm_back(
            hidden_ref[at, :], gain_ref[1:2, :], grads.astype(jnp.float32)
        )
        hidden_grad = cot_ref[at, :].astype(jnp.float32) + x_grad
        grad_ref[at, :] = hidden_grad
        low_ref[at, :] = hidden_grad.astype(jnp.bfloat16)
        piece = out_w_ref.shape[2]
        mix = None
        for i in range(out_w_ref.shape[0]):
            one = lax.dot_general(
                low_ref[at, i * piece : (i + 1) * piece],
                out_w_ref[i],
                NT,
                preferred_element_type=jnp.float32,
            )
            mix = one if mix is None else mix + one
        mix_ref[at, :] = mix.astype(jnp.bfloat16)
        return gain_grad

    gain_mine = turn_back(rows.mine, sent[...])
    rows.finish()
    gain_theirs = turn_back(rows.theirs, came[...])
    gain_grad_ref[...] = gain_mine + gain_theirs


def return_grads(slots, places, hidden, cot, gain, out_w, ident):
    size, (rows, width) = slots.shape[0], hidden.shape
    return pl.pallas_call(
        return_grads_kernel,
        name="return_grads",
        in_specs=whole_vmem(6),
        out_specs=whole_vmem(4),
        out_shape=[
            jax.ShapeDtypeStruct((rows, width), jnp.float32),
            jax.ShapeDtypeStruct((rows, width), jnp.bfloat16),
            jax.ShapeDtypeStruct((rows, out_w.shape[1]), jnp.bfloat16),
            jax.ShapeDtypeStruct((1, width), jnp.float32),
        ],
        scratch_shapes=return_scratch(size, rows, width),
        compiler_params=remote_params(ident),
    )(slots, places, hidden, cot, gain, out_w)


def trade_kernel(
    back, ahead, kv_grad_ref, slots_ref, places_ref, low_ref, mix_ref, kv_ref, out_ref, out_w_ref,
    going, came_kv, line_send, line_recv, part, held, landed, total, sent, came, dp_send, dp_recv,
    tp_send, tp_recv,
):
    me, size = lax.axis_index("ctx"), lax.axis_size("ctx")
    greet(["dp", "tp"], line=True)
    right, left = me + 1, me - 1
    sems = (line_send, line_recv)

    def hop(s, src):
        return remote(src, came_kv.at[s], sems, s, {"ctx": left})

    def forth():
        return remote(
            kv_grad_ref.at[lax.rem(me + 1, size)], came_kv.at[0], sems, 0, {"ctx": right}
        )

    def own_piece(s):
        return kv_grad_ref.at[lax.rem(me + size - s, size)]

    if ahead:

        @pl.when(right < size)
        def _():
            forth().start()

    @pl.when(me - back >= 0)
    def _():
        hop(back, own_piece(back)).start()

    rows = RowReturn(
        part, held, landed, total, sent, came, (dp_send, dp_recv), (tp_send, tp_recv)
    )
    rows.start(places_ref, slots_ref)
    rows.forward()
    turned = jnp.transpose(low_ref[...].astype(jnp.float32)).astype(jnp.bfloat16)
    grad = jnp.dot(turned, mix_ref[...], preferred_element_type=jnp.float32)
    piece = out_w_ref.shape[1]
    for i in range(out_w_ref.shape[0]):
        out_w_ref[i] = grad[i * piece : (i + 1) * piece].astype(jnp.bfloat16)
    rows.pass_on()

    for s in range(back - 1, 0, -1):

        @pl.when((me - s >= 0) & (right < size))
        def _(s=s):
            hop(s + 1, going.at[s]).wait_recv()
            going[s] = (
                own_piece(s)[...].astype(jnp.float32) + came_kv[s + 1].astype(jnp.float32)
            ).astype(going.dtype)
            hop(s, going.at[s]).start()

        @pl.when((me - s >= 0) & (right >= size))
        def _(s=s):
            hop(s, own_piece(s)).start()

    rows.gather()
    kv_ref[...] = kv_grad_ref[me].astype(jnp.float32)

    @pl.when(right < size)
    def _():
        hop(1, going.at[0]).wait_recv()
        kv_ref[...] += came_kv[1].astype(jnp.float32)

    if ahead:

        @pl.when(left >= 0)
        def _():
            forth().wait_recv()
            kv_ref[...] += came_kv[0].astype(jnp.float32)

        @pl.when(right < size)
        def _():
            forth().wait_send()

    for s in range(back, 0, -1):

        @pl.when(me - s >= 0)
        def _(s=s):
            hop(s, going.at[0]).wait_send()

    rows.finish()
    out_ref[rows.mine, :] = sent[...]
    out_ref[rows.theirs, :] = came[...]


def trade(kv_grad, slots, places, low, mix, back, ahead, ident):
    size, (rows, width) = slots.shape[0], low.shape
    kv_shape = kv_grad.shape[1:]
    going = pltpu.VMEM((max(back, 1),) + kv_shape, kv_grad.dtype)
    came = pltpu.VMEM((back + 1,) + kv_shape, kv_grad.dtype)
    return pl.pallas_call(
        functools.partial(trade_kernel, back, ahead),
        name="trade",
        in_specs=whole_vmem(5),
        out_specs=whole_vmem(3),
        out_shape=[
            jax.ShapeDtypeStruct(kv_shape, jnp.float32),
            jax.ShapeDtypeStruct((rows, width), jnp.bfloat16),
            jax.ShapeDtypeStruct((size, width // size, mix.shape[1]), jnp.bfloat16),
        ],
        scratch_shapes=[
            going, came, *sem_pair(back + 1), *return_scratch(size, rows, width)
        ],
        compiler_params=remote_params(ident),
    )(kv_grad, slots, places, low, mix)


class PieceSum:
    def __init__(self, axis, source, landed, sems):
        self.axis, self.source, self.landed, self.sems = axis, source, landed, sems
        self.size = lax.axis_size(axis)

    def copy(self, k):
        peer = ahead_on(self.axis, k)
        return remote(
            self.source.at[peer], self.landed.at[k], self.sems, k, {self.axis: peer}
        )

    def send(self, k):
        self.copy(k).start()

    def start(self):
        each(self.size, self.send)

    def forward(self):
        pass

    def total(self):
        each(self.size, lambda k: self.copy(k).wait_recv())
        whole = self.source[lax.axis_index(self.axis)].astype(jnp.float32)
        for k in range(1, self.size):
            whole += self.landed[k].astype(jnp.float32)
        return whole

    def finish(self):
        each(self.size, lambda k: self.copy(k).wait_send())


class GridPieceSum:
    def __init__(self, source, landed, sems, whole):
        x, y, diagonal = grid_peers()
        places = (lax.axis_index("dp"), x, y, diagonal)
        self.source, self.whole = source, whole
        self.sum = GridSum(lambda n: source.at[places[n]], landed, sems)
        self.start, self.forward, self.finish = self.sum.start, self.sum.forward, self.sum.finish

    def total(self):
        self.whole[...] = self.source[lax.axis_index("dp")].astype(jnp.float32)
        self.sum.add_to(self.whole)
        return self.whole[...]


def dp_sum(source, landed, sems, whole):
    if lax.axis_size("dp") == 4:
        return GridPieceSum(source, landed, sems, whole)
    return PieceSum("dp", source, landed, sems)


class WholeSum:
    def __init__(self, axis, source, landed, sems):
        self.axis, self.source, self.landed, self.sems = axis, source, landed, sems
        self.size = lax.axis_size(axis)

    def copy(self, k):
        return remote(
            self.source, self.landed.at[k], self.sems, k, {self.axis: ahead_on(self.axis, k)}
        )

    def start(self):
        each(self.size, lambda k: self.copy(k).start())

    def total(self):
        each(self.size, lambda k: self.copy(k).wait())
        whole = self.source[...]
        for k in range(1, self.size):
            whole += self.landed[k]
        return whole


def finish_kernel(
    dq_ref, dkv_ref, cos_ref, sin_ref, normed_ref, w_ref, x_ref, gain_ref, out_w_ref, gain_two_ref,
    in_ref, own_ref, gains_ref, joined, turned, part, held, pieces, landed,
    out_pieces, out_landed, whole, out_whole, low, low_landed, gain_rows, gain_landed, gain_more, gain_more_landed, *sems,
):
    greet(["dp", "ctx", "tp"])
    pairs = [sems[2 * i : 2 * i + 2] for i in range(len(sems) // 2)]
    out_pieces[...] = out_w_ref[...]
    out_sum = dp_sum(out_pieces, out_landed, pairs[0], out_whole)
    out_sum.start()
    wide = 2 * HEAD_DIM
    q_width, kv_width = dq_ref.shape[1], dkv_ref.shape[1] // 2
    cosine, sine = block_tables(cos_ref, sin_ref, dq_ref.shape[0], lax.axis_index("ctx"))
    for first in range(0, q_width, wide):
        joined[:, first : first + wide] = turn(
            dq_ref[:, first : first + wide], cosine, sine
        ).astype(jnp.bfloat16)
    for first in range(0, kv_width, wide):
        joined[:, q_width + first : q_width + first + wide] = turn(
            dkv_ref[:, first : first + wide], cosine, sine
        ).astype(jnp.bfloat16)
    joined[:, q_width + kv_width :] = dkv_ref[:, kv_width:].astype(jnp.bfloat16)

    turned[...] = jnp.transpose(normed_ref[...].astype(jnp.float32)).astype(jnp.bfloat16)
    w_sum = dp_sum(pieces, landed, pairs[1], whole)
    rows = pieces.shape[1]

    def piece(k):
        peer = ahead_on("dp", k)
        at = pl.ds(pl.multiple_of(peer * rows, rows), rows)
        pieces[peer] = jnp.dot(
            turned[at, :], joined[...], preferred_element_type=jnp.float32
        ).astype(jnp.bfloat16)

    each(pieces.shape[0], piece)
    w_sum.start()
    out_sum.forward()
    for i in range(w_ref.shape[0]):
        part[:, i * rows : (i + 1) * rows] = lax.dot_general(
            joined[...], w_ref[i], NT, preferred_element_type=jnp.float32
        ).astype(jnp.bfloat16)
    swap = remote(part, held, pairs[2], 0, other_core())
    swap.start()
    me = lax.axis_index("dp")
    own = pl.ds(pl.multiple_of(me * rows, rows), rows)
    pieces[me] = jnp.dot(
        turned[own, :], joined[...], preferred_element_type=jnp.float32
    ).astype(jnp.bfloat16)
    swap.wait()
    x_grad, gain_grad = norm_back(
        x_ref[...].astype(jnp.float32),
        gain_ref[0:1, :],
        part[...].astype(jnp.float32) + held[...].astype(jnp.float32),
    )
    in_ref[...] = x_grad
    gain_rows[...] = jnp.zeros(gain_rows.shape, jnp.float32)
    gain_rows[0:1, :] = gain_grad
    gain_rows[1:2, :] = gain_two_ref[...]
    gain_sum = WholeSum("dp", gain_rows, gain_landed, pairs[3])
    gain_sum.start()
    w_sum.forward()

    out_total = out_sum.total()
    w_total = w_sum.total()
    cols = w_total.shape[1]
    few = low.shape[1]
    for c in range(low.shape[0]):
        low[c, :, :cols] = w_total[c * few : (c + 1) * few].astype(jnp.bfloat16)
        low[c, :, cols:] = out_total[c * few : (c + 1) * few].astype(jnp.bfloat16)
    low_sum = PieceSum("ctx", low, low_landed, pairs[4])
    each(low_sum.size, low_sum.send)
    gain_more[...] = gain_sum.total()
    more_sum = WholeSum("ctx", gain_more, gain_more_landed, pairs[5])
    more_sum.start()
    out_sum.finish()
    w_sum.finish()
    own_ref[...] = low_sum.total()
    low_sum.finish()
    gains_ref[...] = more_sum.total()


def finish(dq, dkv, cosine, sine, normed, w, x, gain, out_w, gain_two, ident):
    rows, width = x.shape
    dp_size, ctx_size = lax.axis_size("dp"), lax.axis_size("ctx")
    cols, out_cols = w.shape[2], out_w.shape[2]
    few = width // dp_size // ctx_size
    low, high = jnp.bfloat16, jnp.float32
    return pl.pallas_call(
        finish_kernel,
        name="finish",
        in_specs=whole_vmem(10),
        out_specs=whole_vmem(3),
        out_shape=[
            jax.ShapeDtypeStruct((rows, width), high),
            jax.ShapeDtypeStruct((few, cols + out_cols), high),
            jax.ShapeDtypeStruct((8, width), high),
        ],
        scratch_shapes=[
            pltpu.VMEM((rows, cols), low),
            pltpu.VMEM((width, rows), low),
            pltpu.VMEM((rows, width), low),
            pltpu.VMEM((rows, width), low),
            pltpu.VMEM((dp_size, width // dp_size, cols), low),
            pltpu.VMEM((dp_size, width // dp_size, cols), low),
            pltpu.VMEM(out_w.shape, low),
            pltpu.VMEM(out_w.shape, low),
            pltpu.VMEM((width // dp_size, cols), high),
            pltpu.VMEM((width // dp_size, out_cols), high),
            pltpu.VMEM((ctx_size, few, cols + out_cols), low),
            pltpu.VMEM((ctx_size, few, cols + out_cols), low),
            pltpu.VMEM((8, width), high),
            pltpu.VMEM((dp_size, 8, width), high),
            pltpu.VMEM((8, width), high),
            pltpu.VMEM((ctx_size, 8, width), high),
            *sem_pair(max(dp_size, 6)),
            *sem_pair(max(dp_size, 6)),
            *sem_pair(1),
            *sem_pair(dp_size),
            *sem_pair(ctx_size),
            *sem_pair(ctx_size),
        ],
        compiler_params=remote_params(ident),
    )(dq, dkv, cosine, sine, normed, w, x, gain, out_w, gain_two)


class Everyone:
    def __init__(self, axis, target, sems):
        self.axis, self.target, self.sems = axis, target, sems
        self.size = lax.axis_size(axis)

    def copy(self, k):
        at = self.target.at[lax.axis_index(self.axis)]
        return remote(at, at, self.sems, k, {self.axis: ahead_on(self.axis, k)})

    def start(self):
        each(self.size, lambda k: self.copy(k).start())

    def arrive(self):
        each(self.size, lambda k: self.copy(k).wait_recv())

    def finish(self):
        each(self.size, lambda k: self.copy(k).wait_send())


def find_places(first, own, routes_ref, gates_ref, earlier, place_ref, gate_ref, column_ref):
    _, tokens = routes_ref.shape[1:]

    def group(g, carry):
        routes, gates = routes_ref[g], gates_ref[g]
        names, values = [], []
        for e in range(own):
            named = routes == first + e
            names.append(jnp.max(named.astype(jnp.float32), axis=0, keepdims=True))
            values.append(jnp.sum(jnp.where(named, gates, 0.0), axis=0, keepdims=True))
        spare = jnp.zeros((8 - own % 8 if own % 8 else 0, tokens), jnp.float32)
        names = jnp.concatenate(names + ([spare] if spare.shape[0] else []), axis=0)
        place = jnp.dot(
            names.astype(jnp.bfloat16), earlier[...], preferred_element_type=jnp.float32
        )
        place = jnp.where((names > 0.0) & (place < CAP), place, -float(CAP * own))
        for e in range(own):
            place_ref[g, e] = place[e : e + 1].astype(jnp.int32)
            gate_ref[g, e] = values[e]
        column_ref[g] = jnp.transpose(place)[:, :own].astype(jnp.int32)
        return carry

    lax.fori_loop(0, routes_ref.shape[0], group, 0)


class LineRows:
    def __init__(self, x_ref, x_all, back, ahead, line_sems, tp_sems):
        self.x_ref, self.x_all, self.back, self.ahead = x_ref, x_all, back, ahead
        self.line_sems, self.tp_sems = line_sems, tp_sems
        self.me, self.size = lax.axis_index("ctx"), lax.axis_size("ctx")
        self.mine, _ = halves(x_ref.shape[0])

    def block(self, s):
        return lax.rem(self.me + self.size - s, self.size)

    def sends(self, s):
        return (self.me + 1 < self.size) & (self.me - s >= 0)

    def hop(self, s):
        at = self.x_all.at[self.block(s), self.mine]
        source = self.x_ref.at[self.mine] if isinstance(s, int) and s == 0 else at
        return remote(source, at, self.line_sems, s, {"ctx": self.me + 1})

    def back_hop(self):
        at = self.x_all.at[self.me, self.mine]
        return remote(
            self.x_ref.at[self.mine], at, self.line_sems, self.back, {"ctx": self.me - 1}
        )

    def relay(self, k, block):
        at = self.x_all.at[block, self.mine]
        return remote(at, at, self.tp_sems, k, other_core())

    def start(self):
        if self.back:
            pl.when(self.sends(0))(lambda: self.hop(0).start())
        if self.ahead:
            pl.when(self.me >= 1)(lambda: self.back_hop().start())

    def step(self, s):
        @pl.when(self.me - s - 1 >= 0)
        def _():
            self.hop(s).wait_recv()
            self.relay(s, self.block(s + 1)).start()

        if s + 1 < self.back:
            pl.when(self.sends(s + 1))(lambda: self.hop(s + 1).start())

    def step_back(self):
        if self.ahead:

            @pl.when(self.me + 1 < self.size)
            def _():
                self.back_hop().wait_recv()
                self.relay(self.back, self.block(self.size - 1)).start()

    def finish(self):
        for s in range(self.back):
            pl.when(self.sends(s))(lambda s=s: self.hop(s).wait_send())
        if self.ahead:
            pl.when(self.me >= 1)(lambda: self.back_hop().wait_send())


def front_kernel(
    back, ahead, own, starts_ref, x_ref, cot_ref, q_w_ref, k_w_ref, v_w_ref, out_w_ref, gains_ref,
    docs_ref, routes_ref, gates_ref, cos_ref, sin_ref, w_out, out_w_out, gain_rows, docs_all,
    normed_out, q_ref, kv_out, mix_ref, full_out, log_ref, hidden_out, rows_out, cot_out,
    place_ref, gate_ref, column_ref, w_all, out_w_all, normed, kv_all, full, hidden, x_all,
    gains_all, routes_all, gates_all, acc, top, total, column, part, held,
    normed_two, *sems,
):
    me, size = lax.axis_index("ctx"), lax.axis_size("ctx")
    dp = lax.axis_index("dp")
    local = sems[-1]
    pairs = [sems[2 * i : 2 * i + 2] for i in range(len(sems) // 2)]
    q_width, kv_width = q_w_ref.shape[1], k_w_ref.shape[1]
    dp_size, piece = w_all.shape[:2]
    block_rows = x_ref.shape[0]

    def flush(i, source, target):
        return pltpu.make_async_copy(source, target, local.at[i])

    w_all[dp, :, :q_width] = q_w_ref[...]
    w_all[dp, :, q_width : q_width + kv_width] = k_w_ref[...]
    w_all[dp, :, q_width + kv_width :] = v_w_ref[...]
    gains_all[dp] = gains_ref[...]
    docs_all[me] = docs_ref[...]
    routes_all[dp] = routes_ref[...]
    gates_all[dp] = gates_ref[...]
    greet(["dp", "ctx", "tp"])
    weights = Gather(w_all, pairs[1])
    gains = Everyone("dp", gains_all, pairs[0])
    docs = Everyone("ctx", docs_all, pairs[2])
    routes = Everyone("dp", routes_all, pairs[3])
    gates = Everyone("dp", gates_all, pairs[4])
    out_w = Gather(out_w_all, pairs[5])
    line = LineRows(x_ref, x_all, back, ahead, pairs[8], pairs[11])
    for one in (gains, weights, line, docs, routes, gates):
        one.start()

    out_w_all[dp] = out_w_ref[...]
    x_all[me] = x_ref[...]
    token = lax.broadcasted_iota(jnp.int32, (block_rows, block_rows), 0)
    later = lax.broadcasted_iota(jnp.int32, (block_rows, block_rows), 1)
    normed_two[:, :block_rows] = (token < later).astype(jnp.float32).astype(jnp.bfloat16)
    top[...] = jnp.full(top.shape, NEG_FILL, jnp.float32)
    total[...] = jnp.zeros(total.shape, jnp.float32)
    acc[...] = jnp.zeros(acc.shape, jnp.float32)
    gains.arrive()
    for i in range(dp_size):
        gain_rows[:, i * piece : (i + 1) * piece] = gains_all[i]

    def norm_rows(source):
        x = source.astype(jnp.float32)
        return (x * row_scale(x) * gain_rows[0:1, :]).astype(jnp.bfloat16)

    normed[...] = norm_rows(x_ref[...])
    flush(0, normed, normed_out).start()
    routes.arrive()
    gates.arrive()
    docs.arrive()
    if back:
        line.step(0)
    weights.forward()
    find_places(
        dp * own, own, routes_all, gates_all, normed_two.at[:, :block_rows], place_ref, gate_ref,
        column_ref,
    )
    weights.arrive()
    flush(1, w_all, w_out).start()
    out_w.start()
    cot_rows = RowGather(cot_ref, cot_out, pairs[6], pairs[7], 0)
    cot_rows.start()
    last = 2 + back + 1 + ahead
    flush(last + 3, cot_ref, cot_out.at[dp]).start()

    wide, tile = 4 * HEAD_DIM, 2 * HEAD_DIM

    def project(source, first):
        whole = jnp.dot(
            source[:, :piece], w_all[0, :, first : first + wide],
            preferred_element_type=jnp.float32,
        )
        for i in range(1, dp_size):
            whole += jnp.dot(
                source[:, i * piece : (i + 1) * piece], w_all[i, :, first : first + wide],
                preferred_element_type=jnp.float32,
            )
        return [whole[:, :tile], whole[:, tile:]]

    def tables(block):
        cosine, sine = block_tables(cos_ref, sin_ref, block_rows, block)
        return cosine, -sine

    here = tables(me)
    for first in range(0, q_width, wide):
        for i, part_of in enumerate(project(normed, first)):
            turned = turn(part_of, *here).astype(jnp.bfloat16)
            at = first + i * tile
            q_ref[:, at : at + tile] = (turned.astype(jnp.float32) * HEAD_DIM**-0.5).astype(
                jnp.bfloat16
            )
    for s in range(1, back):
        line.step(s)
    line.step_back()
    masks = Masks(docs_all, starts_ref, column)

    def visit(s, block):
        @pl.when(s > 0)
        def _():
            line.relay(s - 1, block).wait()

        part[...] = norm_rows(x_all[block])
        there = tables(block)
        for first in range(q_width, q_width + 2 * kv_width, wide):
            for i, part_of in enumerate(project(part, first)):
                if first < q_width + kv_width:
                    part_of = turn(part_of, *there)
                at = first - q_width + i * tile
                kv_all[block, :, at : at + tile] = part_of.astype(jnp.bfloat16)
        flush(2 + s, kv_all.at[block], kv_out.at[block]).start()
        attend_block(masks, block, q_ref, kv_all.at[block], acc, top, total)

    def step(s):
        pl.when(me - s >= 0)(lambda: visit(s, lax.rem(me + size - s, size)))

        @pl.when(s == min(1, back))
        def _():
            out_w.forward()
            cot_rows.forward()

    each(back + 1, step, 0)
    if ahead:

        @pl.when(me + 1 < size)
        def _():
            visit(back + 1, lax.rem(me + 1, size))

    log_ref[...] = top[...] + jnp.log(total[...])
    for h in range(total.shape[0]):
        at = slice(h * HEAD_DIM, (h + 1) * HEAD_DIM)
        acc[at, :] = acc[at, :] / total[h : h + 1, :]
    full[...] = jnp.transpose(acc[...])
    mix_ref[...] = full[...].astype(jnp.bfloat16)
    out_w.arrive()
    cot_rows.arrive()
    for i in range(dp_size):
        part[:, i * piece : (i + 1) * piece] = jnp.dot(
            mix_ref[...], out_w_all[i], preferred_element_type=jnp.float32
        ).astype(jnp.bfloat16)

    mine, theirs = halves(block_rows)
    rows = RowGather(normed_two, rows_out, pairs[9], pairs[10], 2)
    first = remote(part.at[theirs], held.at[theirs], pairs[10], 0, other_core())
    second = remote(part.at[mine], held.at[mine], pairs[10], 1, other_core())
    first.start()
    second.start()
    flush(last, full, full_out).start()
    flush(last + 1, out_w_all, out_w_out).start()

    def norm(at):
        whole = x_ref[at, :].astype(jnp.float32) + (
            part[at, :].astype(jnp.float32) + held[at, :].astype(jnp.float32)
        )
        hidden[at, :] = whole
        normed_two[at, :] = (whole * row_scale(whole) * gain_rows[1:2, :]).astype(jnp.bfloat16)

    first.wait()
    norm(mine)
    rows.start()
    second.wait()
    norm(theirs)
    flush(last + 2, hidden, hidden_out).start()
    flush(last + 4, normed_two, rows_out.at[dp]).start()
    cot_rows.finish()
    for one in (gains, weights, docs, routes, gates, out_w, line):
        one.finish()
    rows.forward()
    rows.arrive()
    rows.finish()
    flush(0, normed, normed_out).wait()
    flush(1, w_all, w_out).wait()

    def kept(s):
        @pl.when(me - s >= 0)
        def _():
            flush(2 + s, kv_all.at[me], kv_out.at[me]).wait()

    each(back + 1, kept, 0)
    if ahead:
        pl.when(me + 1 < size)(lambda: flush(3 + back, kv_all.at[me], kv_out.at[me]).wait())
    flush(last, full, full_out).wait()
    flush(last + 1, out_w_all, out_w_out).wait()
    flush(last + 2, hidden, hidden_out).wait()
    flush(last + 3, cot_ref, cot_out.at[dp]).wait()
    flush(last + 4, normed_two, rows_out.at[dp]).wait()


def front(
    starts, x, cot, q_w, k_w, v_w, out_w, gains, docs, routes, gates, cosine, sine, own, back,
    ahead, ident,
):
    rows, width = x.shape
    dp_size, ctx_size = lax.axis_size("dp"), lax.axis_size("ctx")
    q_width, kv_cols = q_w.shape[1], 2 * k_w.shape[1]
    piece, heads = q_w.shape[0], q_width // HEAD_DIM
    low, high, whole = jnp.bfloat16, jnp.float32, jnp.int32
    far = [
        ((dp_size, piece, q_width + kv_cols), low),
        ((dp_size,) + out_w.shape, low),
        ((rows, width), low),
        ((ctx_size, rows, kv_cols), low),
        ((rows, q_width), high),
        ((rows, width), high),
        ((dp_size, rows, width), low),
        ((dp_size, rows, width), low),
    ]
    shapes = [
        far[0],
        far[1],
        ((2, width), high),
        ((ctx_size, 1, rows), whole),
        far[2],
        ((rows, q_width), low),
        far[3],
        ((rows, q_width), low),
        far[4],
        ((heads, rows), high),
        far[5],
        far[6],
        far[7],
        ((dp_size, own, 1, rows), whole),
        ((dp_size, own, 1, rows), high),
        ((dp_size, rows, own), whole),
    ]
    return pl.pallas_call(
        functools.partial(front_kernel, back, ahead, own),
        name="front",
        in_specs=[pl.BlockSpec(memory_space=pltpu.SMEM)] + whole_vmem(12),
        out_specs=[
            pl.BlockSpec(memory_space=pl.ANY if shape in far else pltpu.VMEM) for shape in shapes
        ],
        out_shape=[jax.ShapeDtypeStruct(*shape) for shape in shapes],
        scratch_shapes=[
            *[pltpu.VMEM(*shape) for shape in far[:6]],
            pltpu.VMEM((ctx_size, rows, width), low),
            pltpu.VMEM((dp_size,) + gains.shape, high),
            pltpu.VMEM((dp_size,) + routes.shape, whole),
            pltpu.VMEM((dp_size,) + gates.shape, high),
            pltpu.VMEM((q_width, rows), high),
            pltpu.VMEM((heads, rows), high),
            pltpu.VMEM((heads, rows), high),
            pltpu.VMEM((rows, 8), whole),
            pltpu.VMEM((rows, width), low),
            pltpu.VMEM((rows, width), low),
            pltpu.VMEM((rows, width), low),
            *sem_pair(dp_size),
            *sem_pair(dp_size),
            *sem_pair(ctx_size),
            *sem_pair(dp_size),
            *sem_pair(dp_size),
            *sem_pair(dp_size),
            *sem_pair(dp_size),
            *sem_pair(dp_size),
            *sem_pair(back + 1),
            *sem_pair(dp_size),
            *sem_pair(dp_size + 2),
            *sem_pair(back + 1),
            pltpu.SemaphoreType.DMA((8 + back + ahead,)),
        ],
        compiler_params=remote_params(ident),
    )(starts, x, cot, q_w, k_w, v_w, out_w, gains, docs, routes, gates, cosine, sine)


GROUPS_AT_ONCE = 4


def experts_kernel(more, rows_in, grads_in, weights_ref, place_ref, gate_ref, *refs):
    refs = refs[2 * more :]
    outs_ref, backs_ref, weight_grad_ref, slots, slot_grads, rows_ref, grads_ref, sems = refs
    groups, tok_rows, _ = rows_ref.shape
    start = pl.program_id(0) * groups
    fresh = pl.program_id(1) == 0

    def load(g):
        return (
            pltpu.make_async_copy(rows_in.at[start + g], rows_ref.at[g], sems.at[0, g]),
            pltpu.make_async_copy(grads_in.at[start + g], grads_ref.at[g], sems.at[1, g]),
        )

    @pl.when(fresh)
    def _():
        for g in range(groups):
            for copy in load(g):
                copy.start()

    owners, part = weight_grad_ref.shape[1], weight_grad_ref.shape[5]
    slot_index = lax.broadcasted_iota(jnp.int32, (CAP, tok_rows), 0)
    gates = []
    for g in range(groups):

        @pl.when(fresh)
        def _(g=g):
            for copy in load(g):
                copy.wait()

        picks = slot_index == place_ref[g, 0]
        gates.append(jnp.sum(jnp.where(picks, gate_ref[g, 0], 0.0), axis=1, keepdims=True))
        picks = picks.astype(jnp.float32).astype(jnp.bfloat16)
        at = slice(g * CAP, (g + 1) * CAP)
        slots[at, :] = jnp.dot(
            picks, rows_ref[g], preferred_element_type=jnp.float32
        ).astype(jnp.bfloat16)
        slot_grads[at, :] = (
            jnp.dot(picks, grads_ref[g], preferred_element_type=jnp.float32) * gates[g]
        ).astype(jnp.bfloat16)
    gate_w, up_w, down_w = (weights_ref.at[0, i] for i in range(3))
    gate_pre = jnp.dot(slots[...], gate_w[...], preferred_element_type=jnp.float32)
    up_pre = jnp.dot(slots[...], up_w[...], preferred_element_type=jnp.float32)
    act_grad = jnp.dot(slot_grads[...], down_w[...], preferred_element_type=jnp.float32)
    sig = 1.0 / (1.0 + jnp.exp(-gate_pre))
    silu = gate_pre * sig
    act_low = (silu * up_pre).astype(jnp.bfloat16)
    up_low = (act_grad * silu).astype(jnp.bfloat16)
    gate_low = (act_grad * up_pre * (sig * (1.0 + gate_pre * (1.0 - sig)))).astype(jnp.bfloat16)

    back = lax.dot_general(
        gate_low, gate_w[...], NT, preferred_element_type=jnp.float32
    ) + lax.dot_general(up_low, up_w[...], NT, preferred_element_type=jnp.float32)
    out = lax.dot_general(act_low, down_w[...], NT, preferred_element_type=jnp.float32)
    for g in range(groups):
        at = slice(g * CAP, (g + 1) * CAP)
        backs_ref[g] = back[at].astype(jnp.bfloat16)
        outs_ref[g] = (out[at] * gates[g]).astype(jnp.bfloat16)

    for i, (low, source) in enumerate(
        ((gate_low, slots), (up_low, slots), (act_low, slot_grads))
    ):
        turned = jnp.transpose(low.astype(jnp.float32)).astype(jnp.bfloat16)
        total = jnp.dot(turned, source[...], preferred_element_type=jnp.float32)
        for c in range(owners):
            weight_grad_ref[0, c, 0, i] = total[:, c * part : (c + 1) * part].astype(
                weight_grad_ref.dtype
            )


def experts(weights, place_rows, gate_rows, rows_all, grad_all, first, count, before):
    own, _, model_width, hidden = weights.shape
    groups, tok_rows, _ = rows_all.shape
    owners = lax.axis_size("ctx")
    at_once = min(GROUPS_AT_ONCE, groups)
    chunks = groups // at_once
    part = model_width // owners
    held = pltpu.VMEM((at_once, tok_rows, model_width), jnp.bfloat16)
    line_spec = pl.BlockSpec((at_once, 1, 1, tok_rows), lambda c, e: (c, e + first, 0, 0))
    slots_spec = pl.BlockSpec((at_once, CAP, model_width), lambda c, e: (c, e + first, 0))
    slots_shape = jax.ShapeDtypeStruct((groups, own * CAP, model_width), jnp.bfloat16)
    flops = count * groups * CAP * model_width * 2 * (9 * hidden + 2 * tok_rows)
    more = before is not None
    outs, backs, weight_part = pl.pallas_call(
        functools.partial(experts_kernel, more),
        name="experts",
        grid=(chunks, count),
        in_specs=[
            pl.BlockSpec(memory_space=pl.ANY),
            pl.BlockSpec(memory_space=pl.ANY),
            pl.BlockSpec((1, 3, model_width, hidden), lambda c, e: (e + first, 0, 0, 0)),
            line_spec,
            line_spec,
        ]
        + [pl.BlockSpec(memory_space=pl.ANY)] * (2 * more),
        out_specs=[
            slots_spec,
            slots_spec,
            pl.BlockSpec((1, owners, 1, 3, hidden, part), lambda c, e: (c, 0, e, 0, 0, 0)),
        ],
        out_shape=[
            slots_shape,
            slots_shape,
            jax.ShapeDtypeStruct((chunks, owners, count, 3, hidden, part), jnp.bfloat16),
        ],
        scratch_shapes=[
            pltpu.VMEM((at_once * CAP, model_width), jnp.bfloat16),
            pltpu.VMEM((at_once * CAP, model_width), jnp.bfloat16),
            held,
            held,
            pltpu.SemaphoreType.DMA((2, at_once)),
        ],
        input_output_aliases={5: 0, 6: 1} if more else {},
        compiler_params=pltpu.CompilerParams(vmem_limit_bytes=LIMIT),
        cost_estimate=pl.CostEstimate(
            flops=flops, bytes_accessed=4 * weights.size, transcendentals=0
        ),
    )(rows_all, grad_all, weights, place_rows, gate_rows, *(before if more else ()))
    if chunks == 1:
        return (outs, backs), weight_part[0]
    return (outs, backs), jnp.sum(weight_part.astype(jnp.float32), axis=0).astype(jnp.bfloat16)


def unfold_kernel(more, sums_ref, *refs):
    out_ref = refs[more]
    for i in range(sums_ref.shape[1]):
        out_ref[0, i] = jnp.transpose(sums_ref[0, i].astype(jnp.float32))


def unfold(sums, own, first, matrix, before):
    count, some, hidden, part = sums.shape
    more = before is not None
    return pl.pallas_call(
        functools.partial(unfold_kernel, more),
        name="unfold",
        grid=(count,),
        in_specs=[pl.BlockSpec((1, some, hidden, part), lambda e: (e, 0, 0, 0))]
        + [pl.BlockSpec(memory_space=pl.ANY)] * more,
        out_specs=pl.BlockSpec((1, some, part, hidden), lambda e: (e + first, matrix // some, 0, 0)),
        out_shape=jax.ShapeDtypeStruct((own, 3, part, hidden), jnp.float32),
        input_output_aliases={1: 0} if more else {},
        compiler_params=pltpu.CompilerParams(vmem_limit_bytes=LIMIT),
    )(sums, *([before] if more else []))


def rotary_tables(token_positions):
    half_dim = HEAD_DIM // 2
    inverse = THETA ** (-(jnp.arange(half_dim, dtype=jnp.float32) * 2.0 / HEAD_DIM))
    angles = token_positions.astype(jnp.float32)[:, None] * inverse[None, :]
    cosine, sine = jnp.cos(angles), jnp.sin(angles)
    return jnp.concatenate([cosine] * 4, axis=1), jnp.concatenate([sine, -sine] * 2, axis=1)


def expert_counts(own):
    return (1, 6, 1) if own == 8 else (own - own // 2, own // 2)


def scatter(grads):
    return lax.psum_scatter(grads, "ctx", scatter_dimension=0)


def body(
    tokens,
    query_weight,
    key_weight,
    value_weight,
    output_weight,
    gain_attn,
    gain_moe,
    expert_weights,
    routes,
    gate_values,
    documents,
    pic_starts,
    cotangent,
):
    block_len = tokens.shape[1]
    ctx_size = lax.axis_size("ctx")
    length = block_len * ctx_size
    back = back_blocks(ctx_size, block_len, length)
    ahead = ahead_blocks(block_len, length, pic_starts.shape[1])
    q_width, kv_width = query_weight.shape[1], key_weight.shape[1]
    own = expert_weights.shape[0]
    x, cot = tokens[0], cotangent[0]

    inside = jnp.arange(block_len, dtype=jnp.int32)
    starts = jnp.arange(-(-ctx_size // 8) * 8, dtype=jnp.int32) * block_len
    cosine, sine = rotary_tables(jnp.concatenate([inside, starts]))
    (
        w_all,
        out_w_all,
        gain_rows,
        docs_all,
        normed_one,
        query,
        kv_all,
        mixture,
        mix_full,
        log_total,
        hidden,
        rows_all,
        grad_all,
        *places,
    ) = front(
        pic_starts,
        x,
        cot,
        query_weight,
        key_weight,
        value_weight,
        output_weight,
        jnp.stack([gain_attn, gain_moe]).astype(jnp.float32),
        documents,
        routes[0].T,
        gate_values[0].T,
        cosine,
        sine,
        own,
        back,
        ahead,
        1,
    )
    place_rows, gate_rows, places = places
    counts = expert_counts(own)
    slots, sums = None, []
    first = 0
    for n, count in enumerate(counts):
        slots, grads = experts(
            expert_weights, place_rows, gate_rows, rows_all, grad_all, first, count, slots
        )
        if n < len(counts) - 1:
            sums.append((scatter(grads), first, 0))
        first += count
    outs, backs = slots
    last = own - counts[-1]
    sums.append((scatter(grads[:, :, 2:]), last, 2))
    hidden_grad, hidden_low, mix_grad, gain_two_grad = return_grads(
        backs, places, hidden, cot, gain_rows, out_w_all, 2
    )
    q_rot_grad, kv_part = attend_back(
        pic_starts, query, kv_all, docs_all, log_total, mix_full, mix_grad, back, ahead
    )
    kv_back, expert_sum, output_grad = trade(
        kv_part,
        outs,
        places,
        hidden_low,
        mixture,
        back,
        ahead,
        3,
    )
    x_grad, owned, gain_sums = finish(
        q_rot_grad,
        kv_back,
        cosine,
        sine,
        normed_one,
        w_all,
        x,
        gain_rows,
        output_grad,
        gain_two_grad,
        4,
    )
    grads, owned = lax.optimization_barrier((grads, owned))
    sums.append((scatter(grads[:, :, :2]), last, 0))
    few = owned.shape[0]
    here = (lax.axis_index("dp") * ctx_size + lax.axis_index("ctx")) * few
    gain_sums = lax.dynamic_slice_in_dim(gain_sums, here, few, 1)
    expert_grad = None
    for part, first, matrix in sums:
        expert_grad = unfold(part, own, first, matrix, expert_grad)
    v_end = q_width + 2 * kv_width
    return (
        (hidden + expert_sum.astype(jnp.float32)).astype(jnp.bfloat16)[None],
        (hidden_grad + x_grad).astype(jnp.bfloat16)[None],
        owned[:, :q_width],
        owned[:, q_width : q_width + kv_width],
        owned[:, q_width + kv_width : v_end],
        owned[:, v_end:].T,
        gain_sums[0],
        gain_sums[1],
        expert_grad,
    )


def solution(mesh):
    return jax.shard_map(
        body,
        mesh=mesh,
        in_specs=(
            P("dp", "ctx", None),
            P("dp", "tp"),
            P("dp", "tp"),
            P("dp", "tp"),
            P("tp", "dp"),
            P("dp"),
            P("dp"),
            P("dp", None, None, "tp"),
            P("dp", "ctx", None),
            P("dp", "ctx", None),
            P("dp", "ctx"),
            P("dp", None),
            P("dp", "ctx", None),
        ),
        out_specs=(
            P("dp", "ctx", None),
            P("dp", "ctx", None),
            P(("dp", "ctx"), "tp"),
            P(("dp", "ctx"), "tp"),
            P(("dp", "ctx"), "tp"),
            P("tp", ("dp", "ctx")),
            P(("dp", "ctx")),
            P(("dp", "ctx")),
            P("dp", None, "ctx", "tp"),
        ),
        check_vma=False,
    )
```

```python
import functools

import jax
import jax.numpy as jnp
from jax import lax
from jax.experimental import pallas as pl
from jax.experimental.pallas import tpu as pltpu
from jax.sharding import PartitionSpec as P

HEAD_DIM = 64
PIC = 256
CAP = 144

EPSILON = 1e-06
THETA = 10000.0
NEG_FILL = -1e30


KEY_ROWS = 256
NT = (((1,), (1,)), ((), ()))
LIMIT = 67043328


def whole_vmem(count):
    return [pl.BlockSpec(memory_space=pltpu.VMEM)] * count


def picture_ids(starts_ref, places):
    ids = jnp.full(places.shape, -1, jnp.int32)
    for j in range(starts_ref.shape[1]):
        start = starts_ref[0, j]
        ids += jnp.where((places >= start) & (places < start + PIC), j + 1, 0)
    return ids


def as_column(row):
    tall = jnp.broadcast_to(row.astype(jnp.float32), (8, row.shape[1]))
    return jnp.transpose(tall)[:, 0:1].astype(jnp.int32)


class Masks:
    def __init__(self, docs_ref, starts_ref, column):
        self.docs_ref, self.starts_ref, self.column = docs_ref, starts_ref, column
        self.rows = docs_ref.shape[2]
        me = lax.axis_index("ctx")
        self.q_doc = docs_ref[me]
        self.q_place = me * self.rows + lax.broadcasted_iota(jnp.int32, (1, self.rows), 1)
        self.q_pic = picture_ids(starts_ref, self.q_place)

    def open(self, block):
        self.column[...] = jnp.broadcast_to(
            as_column(self.docs_ref[block]), self.column.shape
        )

    def bias(self, block, rows, first):
        k_doc = self.column[rows, 0:1]
        k_place = block * self.rows + first + lax.broadcasted_iota(jnp.int32, k_doc.shape, 0)
        k_pic = picture_ids(self.starts_ref, k_place)
        seen = (k_doc == self.q_doc) & (
            (k_place <= self.q_place) | ((k_pic == self.q_pic) & (self.q_pic >= 0))
        )
        return jnp.where(seen, 0.0, NEG_FILL)


def attend_block(masks, block, q_ref, kv_ref, acc, top, total):
    kv_width = kv_ref.shape[1] // 2
    heads, kv_heads = q_ref.shape[1] // HEAD_DIM, kv_width // HEAD_DIM
    masks.open(block)

    def step(j, carry):
        first = pl.multiple_of(j * KEY_ROWS, KEY_ROWS)
        rows = pl.ds(first, KEY_ROWS)
        bias = masks.bias(block, rows, first)
        for g in range(kv_heads):
            key = kv_ref[rows, g * HEAD_DIM : (g + 1) * HEAD_DIM]
            val = kv_ref[rows, kv_width + g * HEAD_DIM : kv_width + (g + 1) * HEAD_DIM]
            val_t = jnp.transpose(val.astype(jnp.float32)).astype(jnp.bfloat16)
            for h in range(g * heads // kv_heads, (g + 1) * heads // kv_heads):
                at = slice(h * HEAD_DIM, (h + 1) * HEAD_DIM)
                scores = bias + lax.dot_general(
                    key, q_ref[:, at], NT, preferred_element_type=jnp.float32
                )
                old = top[h : h + 1, :]
                new = jnp.maximum(old, jnp.max(scores, axis=0, keepdims=True))
                probs = jnp.exp(scores - new)
                fade = jnp.exp(old - new)
                total[h : h + 1, :] = total[h : h + 1, :] * fade + jnp.sum(
                    probs, axis=0, keepdims=True
                )
                acc[at, :] = acc[at, :] * fade + jnp.dot(
                    val_t, probs.astype(jnp.bfloat16), preferred_element_type=jnp.float32
                )
                top[h : h + 1, :] = new
        return carry

    lax.fori_loop(0, kv_ref.shape[0] // KEY_ROWS, step, 0)


def attend_back_block(
    masks, edges, block, q_ref, kv_ref, log_ref, delta, grad_ref, acc, dkv_ref
):
    kv_width = kv_ref.shape[1] // 2
    heads, kv_heads = q_ref.shape[1] // HEAD_DIM, kv_width // HEAD_DIM
    masks.open(block)
    count = kv_ref.shape[0] // KEY_ROWS
    me = lax.axis_index("ctx")
    q_first, q_last = edges[me * count, 0], edges[me * count + count - 1, 1]

    def step(j, carry):
        at = block * count + j
        same = (edges[at, 0] <= q_last) & (edges[at, 1] >= q_first)

        @pl.when(same)
        def _():
            inside(j)

        @pl.when(jnp.logical_not(same))
        def _():
            rows = pl.ds(pl.multiple_of(j * KEY_ROWS, KEY_ROWS), KEY_ROWS)
            dkv_ref[rows, :] = jnp.zeros((KEY_ROWS, dkv_ref.shape[1]), dkv_ref.dtype)

        return carry

    def inside(j):
        first = pl.multiple_of(j * KEY_ROWS, KEY_ROWS)
        rows = pl.ds(first, KEY_ROWS)
        bias = masks.bias(block, rows, first)
        for g in range(kv_heads):
            k_at = slice(g * HEAD_DIM, (g + 1) * HEAD_DIM)
            v_at = slice(kv_width + g * HEAD_DIM, kv_width + (g + 1) * HEAD_DIM)
            key, val = kv_ref[rows, k_at], kv_ref[rows, v_at]
            key_t = jnp.transpose(key.astype(jnp.float32)).astype(jnp.bfloat16)
            dk = jnp.zeros((KEY_ROWS, HEAD_DIM), jnp.float32)
            dv = jnp.zeros((KEY_ROWS, HEAD_DIM), jnp.float32)
            for h in range(g * heads // kv_heads, (g + 1) * heads // kv_heads):
                at = slice(h * HEAD_DIM, (h + 1) * HEAD_DIM)
                q_rows, g_rows = q_ref[:, at], grad_ref[:, at]
                scores = bias + lax.dot_general(
                    key, q_rows, NT, preferred_element_type=jnp.float32
                )
                probs = jnp.exp(scores - log_ref[h : h + 1, :])
                prob_grad = lax.dot_general(val, g_rows, NT, preferred_element_type=jnp.float32)
                slope = (probs * (prob_grad - delta[h : h + 1, :])).astype(jnp.bfloat16)
                dv += jnp.dot(
                    probs.astype(jnp.bfloat16), g_rows, preferred_element_type=jnp.float32
                )
                dk += jnp.dot(slope, q_rows, preferred_element_type=jnp.float32)
                acc[at, :] += jnp.dot(key_t, slope, preferred_element_type=jnp.float32)
            dkv_ref[rows, k_at] = dk.astype(dkv_ref.dtype)
            dkv_ref[rows, v_at] = dv.astype(dkv_ref.dtype)

    lax.fori_loop(0, count, step, 0)


def attend_back_kernel(
    back, ahead, starts_ref, edges, q_ref, kv_ref, docs_ref, log_ref, full_ref, grad_ref, dq_ref,
    dkv_ref, acc, delta, column,
):
    me, size = lax.axis_index("ctx"), lax.axis_size("ctx")
    acc[...] = jnp.transpose(full_ref[...] * grad_ref[...].astype(jnp.float32))
    for h in range(delta.shape[0]):
        delta[h : h + 1, :] = jnp.sum(
            acc[h * HEAD_DIM : (h + 1) * HEAD_DIM, :], axis=0, keepdims=True
        )
    acc[...] = jnp.zeros(acc.shape, jnp.float32)
    masks = Masks(docs_ref, starts_ref, column)

    def step(s, carry):
        block = me + ahead - s

        @pl.when((block >= 0) & (block < size))
        def _():
            attend_back_block(
                masks, edges, block, q_ref, kv_ref.at[block], log_ref, delta, grad_ref, acc,
                dkv_ref.at[block],
            )

        return carry

    lax.fori_loop(0, back + ahead + 1, step, 0)
    dq_ref[...] = jnp.transpose(acc[...]) * (HEAD_DIM**-0.5)


def attend_back(starts, q, kv, docs, log_total, full, grad, back, ahead):
    rows, width = q.shape
    by_block = docs.reshape(-1, KEY_ROWS)
    edges = jnp.concatenate([by_block[:, :1], by_block[:, -1:]], axis=1)
    return pl.pallas_call(
        functools.partial(attend_back_kernel, back, ahead),
        name="attend_back",
        in_specs=[pl.BlockSpec(memory_space=pltpu.SMEM)] * 2 + whole_vmem(6),
        out_specs=whole_vmem(2),
        out_shape=[
            jax.ShapeDtypeStruct((rows, width), jnp.float32),
            jax.ShapeDtypeStruct(kv.shape, jnp.bfloat16),
        ],
        scratch_shapes=[
            pltpu.VMEM((width, rows), jnp.float32),
            pltpu.VMEM((width // HEAD_DIM, rows), jnp.float32),
            pltpu.VMEM((rows, 8), jnp.int32),
        ],
        compiler_params=pltpu.CompilerParams(vmem_limit_bytes=LIMIT),
    )(starts, edges, q, kv, docs, log_total, full, grad)


MESH = pl.DeviceIdType.MESH


def greet(axes_list, line=False):
    barrier = pltpu.get_barrier_semaphore()
    count = 0
    for axis in axes_list:
        me, size = lax.axis_index(axis), lax.axis_size(axis)

        def signal(k, carry, axis=axis, me=me, size=size):
            pl.semaphore_signal(
                barrier, inc=1, device_id={axis: lax.rem(me + k, size)}, device_id_type=MESH
            )
            return carry

        lax.fori_loop(1, size, signal, 0)
        count += size - 1
    if not line:
        pl.semaphore_wait(barrier, count)
        return
    me, size = lax.axis_index("ctx"), lax.axis_size("ctx")
    for step in (1, -1):
        other = me + step

        @pl.when((other >= 0) & (other < size))
        def _(other=other):
            pl.semaphore_signal(barrier, inc=1, device_id={"ctx": other}, device_id_type=MESH)

    inner = (me > 0) & (me < size - 1)

    @pl.when(inner)
    def _():
        pl.semaphore_wait(barrier, count + 2)

    @pl.when(jnp.logical_not(inner))
    def _():
        pl.semaphore_wait(barrier, count + 1)


def remote(src, dst, sems, k, device_id):
    return pltpu.make_async_remote_copy(
        src_ref=src,
        dst_ref=dst,
        send_sem=sems[0].at[k],
        recv_sem=sems[1].at[k],
        device_id=device_id,
        device_id_type=MESH,
    )


def other_core():
    return {"tp": 1 - lax.axis_index("tp")}


def ahead_on(axis, k):
    return lax.rem(lax.axis_index(axis) + k, lax.axis_size(axis))


def each(count, do, first=1):
    def step(k, carry):
        do(k)
        return carry

    lax.fori_loop(first, count, step, 0)


def sem_pair(count):
    return [pltpu.SemaphoreType.DMA((count,)), pltpu.SemaphoreType.DMA((count,))]


def remote_params(ident):
    return pltpu.CompilerParams(
        collective_id=ident, has_side_effects=True, vmem_limit_bytes=LIMIT
    )


def halves(rows):
    half = rows // 2
    core = lax.axis_index("tp")
    return (
        pl.ds(pl.multiple_of(core * half, half), half),
        pl.ds(pl.multiple_of((1 - core) * half, half), half),
    )


def turn(tile, cosine, sine):
    lane = lax.broadcasted_iota(jnp.int32, tile.shape, 1)
    half = HEAD_DIM // 2
    swapped = jnp.where(
        lax.rem(lane, HEAD_DIM) < half,
        pltpu.roll(tile, 2 * HEAD_DIM - half, 1),
        pltpu.roll(tile, half, 1),
    )
    return tile * cosine + swapped * sine


def block_tables(cos_ref, sin_ref, rows, block):
    start = pl.ds(rows + block, 1)
    in_cos, in_sin = cos_ref[:rows, :], sin_ref[:rows, :]
    at_cos, at_sin = cos_ref[start, :], sin_ref[start, :]
    return in_cos * at_cos - in_sin * at_sin, in_sin * at_cos + in_cos * at_sin


def row_scale(x):
    return lax.rsqrt(jnp.mean(x * x, axis=-1, keepdims=True) + EPSILON)


def norm_back(x, gain, grad):
    scale = row_scale(x)
    unit = x * scale
    pull = grad * gain
    return (
        scale * (pull - unit * jnp.mean(pull * unit, axis=-1, keepdims=True)),
        jnp.sum(grad * unit, axis=0, keepdims=True),
    )


def back_blocks(ctx_size, block_len, length):
    return min(ctx_size - 1, -(-(length // 2 - 1) // block_len))


def ahead_blocks(block_len, length, spans):
    return 0 if block_len % (length // spans) == 0 else 1


def grid_peers():
    me = lax.axis_index("dp")
    x, y = lax.rem(me, 2), lax.div(me, 2)
    return y * 2 + 1 - x, (1 - y) * 2 + x, 3 - me


class Gather:
    def __init__(self, target, sems, rows=None, source=None):
        self.target, self.sems, self.rows, self.source = target, sems, rows, source
        self.size = lax.axis_size("dp")
        self.grid = self.size == 4

    def at(self, place):
        return self.target.at[place] if self.rows is None else self.target.at[place, self.rows]

    def half(self, place, n):
        if self.rows is None:
            count = self.target.shape[1] // 2
            return self.target.at[place, pl.ds(n * count, count)]
        count = self.rows.size // 2
        first = pl.multiple_of(self.rows.start + n * count, count)
        return self.target.at[place, pl.ds(first, count)]

    def first(self, k, peer):
        place = self.at(lax.axis_index("dp"))
        source = place if self.source is None else self.source.at[self.rows]
        return remote(source, place, self.sems, k, {"dp": peer})

    def passed(self, k, place, n, peer):
        at = self.half(place, n)
        return remote(at, at, self.sems, k, {"dp": peer})

    def direct(self, k):
        return self.first(k, ahead_on("dp", k))

    def start(self):
        if not self.grid:
            each(self.size, lambda k: self.direct(k).start())
            return
        x, y, _ = grid_peers()
        self.first(0, x).start()
        self.first(1, y).start()

    def forward(self, came=None):
        if not self.grid:
            return
        x, y, _ = grid_peers()
        self.first(0, x).wait_recv()
        self.passed(2, x, 0, y).start()
        if came:
            came(0, self.at(x))
        self.first(1, y).wait_recv()
        self.passed(3, y, 1, x).start()
        if came:
            came(1, self.at(y))

    def arrive(self, came=None):
        if not self.grid:

            def one(k):
                self.direct(k).wait_recv()
                if came:
                    came(k, self.at(ahead_on("dp", self.size - k)))

            each(self.size, one)
            return
        x, _, diagonal = grid_peers()
        for n in range(2):
            self.passed(2 + n, diagonal, n, x).wait_recv()
            if came:
                came(2 + n, self.half(diagonal, n))

    def finish(self):
        if not self.grid:
            each(self.size, lambda k: self.direct(k).wait_send())
            return
        x, y, _ = grid_peers()
        self.first(0, x).wait_send()
        self.first(1, y).wait_send()
        self.passed(2, x, 0, y).wait_send()
        self.passed(3, y, 1, x).wait_send()


class RowGather:
    def __init__(self, source, target, dp_sems, tp_sems, first):
        mine, _ = halves(source.shape[0])
        self.gather = Gather(target, dp_sems, mine, source)
        self.tp_sems, self.after = tp_sems, first

    def relay(self, k, at):
        return remote(at, at, self.tp_sems, self.after + k, other_core())

    def came(self, k, at):
        self.relay(k, at).start()

    def start(self):
        self.gather.start()

    def forward(self):
        self.gather.forward(self.came)

    def arrive(self):
        self.gather.arrive(self.came)

    def finish(self):
        self.gather.finish()
        gather = self.gather
        if not gather.grid:
            each(
                gather.size,
                lambda k: self.relay(k, gather.at(ahead_on("dp", gather.size - k))).wait(),
            )
            return
        x, y, diagonal = grid_peers()
        self.relay(0, gather.at(x)).wait()
        self.relay(1, gather.at(y)).wait()
        self.relay(2, gather.half(diagonal, 0)).wait()
        self.relay(3, gather.half(diagonal, 1)).wait()


def collect(places_ref, slots_ref, group):
    tok_rows, slot_count = places_ref.shape[1], slots_ref.shape[1]
    tiles = []
    for first in range(0, slot_count, 128):
        wide = min(128, slot_count - first)
        lane = first + lax.broadcasted_iota(jnp.int32, (tok_rows, wide), 1)
        hit = None
        for n in range(first // CAP, (first + wide - 1) // CAP + 1):
            one = places_ref[group, :, n : n + 1] == lane - n * CAP
            hit = one if hit is None else hit | one
        tiles.append(hit.astype(jnp.float32).astype(jnp.bfloat16))
    return jnp.dot(
        jnp.concatenate(tiles, axis=1), slots_ref[group], preferred_element_type=jnp.float32
    )


class GridSum:
    def __init__(self, piece, landed, sems):
        self.piece, self.landed, self.sems = piece, landed, sems
        self.x, self.y, _ = grid_peers()
        self.count = landed.shape[1] // 2

    def half(self, n, which):
        return self.piece(n).at[pl.ds(which * self.count, self.count)]

    def slot(self, j):
        return self.landed.at[j // 2, pl.ds(j % 2 * self.count, self.count)]

    def copy(self, j):
        n, which, peer = (
            (1, 0, self.x),
            (3, 0, self.x),
            (2, 1, self.y),
            (3, 1, self.y),
            (2, 0, self.y),
            (1, 1, self.x),
        )[j]
        return remote(self.half(n, which), self.slot(j), self.sems, j, {"dp": peer})

    def start(self):
        for j in (1, 3, 0, 2):
            self.copy(j).start()

    def forward(self):
        for j, n, which in ((1, 2, 0), (3, 1, 1)):
            self.copy(j).wait_recv()
            half = self.half(n, which)
            half[...] = (
                half[...].astype(jnp.float32) + self.slot(j)[...].astype(jnp.float32)
            ).astype(jnp.bfloat16)
            self.copy(4 + j // 2).start()

    def add_to(self, total):
        for which, slots in ((0, (0, 4)), (1, (2, 5))):
            at = pl.ds(which * self.count, self.count)
            for j in slots:
                self.copy(j).wait_recv()
                total[at, :] += self.slot(j)[...].astype(jnp.float32)

    def finish(self):
        for j in range(6):
            self.copy(j).wait_send()


class RowReturn:
    def __init__(self, part, held, landed, total, sent, came, dp_sems, tp_sems):
        self.part, self.held, self.landed, self.total = part, held, landed, total
        self.sent, self.came, self.dp_sems, self.tp_sems = sent, came, dp_sems, tp_sems
        self.size = lax.axis_size("dp")
        self.mine, self.theirs = halves(part.shape[1])
        self.grid = self.size == 4
        if self.grid:
            self.sum = GridSum(lambda n: held.at[n], landed, dp_sems)

    def group(self, k):
        if not self.grid:
            return ahead_on("dp", k)
        me = lax.axis_index("dp")
        x, y = lax.rem(me, 2), lax.div(me, 2)
        flip_x, flip_y = lax.rem(k, 2), lax.div(k, 2)
        return lax.rem(y + flip_y, 2) * 2 + lax.rem(x + flip_x, 2)

    def swap(self, k):
        return remote(
            self.part.at[self.group(k), self.theirs], self.held.at[k], self.tp_sems, k,
            other_core(),
        )

    def copy(self, k):
        return remote(
            self.held.at[k], self.landed.at[k - 1], self.dp_sems, k, {"dp": ahead_on("dp", k)}
        )

    def last(self):
        return remote(self.sent, self.came, self.tp_sems, self.size, other_core())

    def both(self, k):
        return self.part[self.group(k), self.mine].astype(jnp.float32) + self.held[k].astype(
            jnp.float32
        )

    def start(self, places_ref, slots_ref):
        def one(k):
            k = lax.rem(k, self.size)
            group = self.group(k)
            self.part[group] = collect(places_ref, slots_ref, group).astype(jnp.bfloat16)
            self.swap(k).start()

        each(self.size + 1, one)

    def forward(self):
        def one(k):
            self.swap(k).wait_recv()
            self.held[k] = self.both(k).astype(jnp.bfloat16)
            if not self.grid:
                self.copy(k).start()

        each(self.size, one)
        if self.grid:
            self.sum.start()
        self.swap(0).wait()
        self.total[...] = self.both(0)

    def pass_on(self):
        if self.grid:
            self.sum.forward()

    def gather(self):
        def one(k):
            self.copy(k).wait_recv()
            self.total[...] += self.landed[k - 1].astype(jnp.float32)

        if self.grid:
            self.sum.add_to(self.total)
        else:
            each(self.size, one)
        self.sent[...] = self.total[...].astype(jnp.bfloat16)
        self.last().start()

    def finish(self):
        def one(k):
            self.swap(k).wait_send()
            if not self.grid:
                self.copy(k).wait_send()

        each(self.size, one)
        if self.grid:
            self.sum.finish()
        self.last().wait()


def return_scratch(size, rows, width):
    low = jnp.bfloat16
    return [
        pltpu.VMEM((size, rows, width), low),
        pltpu.VMEM((size, rows // 2, width), low),
        pltpu.VMEM((size - 1, rows // 2, width), low),
        pltpu.VMEM((rows // 2, width), jnp.float32),
        pltpu.VMEM((rows // 2, width), low),
        pltpu.VMEM((rows // 2, width), low),
        *sem_pair(max(size, 6)),
        *sem_pair(size + 1),
    ]


def return_grads_kernel(
    slots_ref, places_ref, hidden_ref, cot_ref, gain_ref, out_w_ref, grad_ref, low_ref, mix_ref,
    gain_grad_ref, part, held, landed, total, sent, came, dp_send, dp_recv, tp_send, tp_recv,
):
    greet(["dp", "tp"])
    rows = RowReturn(
        part, held, landed, total, sent, came, (dp_send, dp_recv), (tp_send, tp_recv)
    )
    rows.start(places_ref, slots_ref)
    rows.forward()
    rows.pass_on()
    rows.gather()

    def turn_back(at, grads):
        x_grad, gain_grad = norm_back(
            hidden_ref[at, :], gain_ref[1:2, :], grads.astype(jnp.float32)
        )
        hidden_grad = cot_ref[at, :].astype(jnp.float32) + x_grad
        grad_ref[at, :] = hidden_grad
        low_ref[at, :] = hidden_grad.astype(jnp.bfloat16)
        piece = out_w_ref.shape[2]
        mix = None
        for i in range(out_w_ref.shape[0]):
            one = lax.dot_general(
                low_ref[at, i * piece : (i + 1) * piece],
                out_w_ref[i],
                NT,
                preferred_element_type=jnp.float32,
            )
            mix = one if mix is None else mix + one
        mix_ref[at, :] = mix.astype(jnp.bfloat16)
        return gain_grad

    gain_mine = turn_back(rows.mine, sent[...])
    rows.finish()
    gain_theirs = turn_back(rows.theirs, came[...])
    gain_grad_ref[...] = gain_mine + gain_theirs


def return_grads(slots, places, hidden, cot, gain, out_w, ident):
    size, (rows, width) = slots.shape[0], hidden.shape
    return pl.pallas_call(
        return_grads_kernel,
        name="return_grads",
        in_specs=whole_vmem(6),
        out_specs=whole_vmem(4),
        out_shape=[
            jax.ShapeDtypeStruct((rows, width), jnp.float32),
            jax.ShapeDtypeStruct((rows, width), jnp.bfloat16),
            jax.ShapeDtypeStruct((rows, out_w.shape[1]), jnp.bfloat16),
            jax.ShapeDtypeStruct((1, width), jnp.float32),
        ],
        scratch_shapes=return_scratch(size, rows, width),
        compiler_params=remote_params(ident),
    )(slots, places, hidden, cot, gain, out_w)


def trade_kernel(
    back, ahead, early, kv_grad_ref, slots_ref, places_ref, low_ref, mix_ref, *refs
):
    if early:
        dq_ref, cos_ref, sin_ref, normed_ref, *refs = refs
        kv_ref, out_ref, sums_ref, joined_ref, turned_ref, *refs = refs
        pieces, pieces_landed, whole, sum_send, sum_recv, *refs = refs
    else:
        kv_ref, out_ref, out_w_ref, *refs = refs
    going, came_kv, line_send, line_recv, part, held, landed, total, *refs = refs
    sent, came, dp_send, dp_recv, tp_send, tp_recv = refs
    me, size = lax.axis_index("ctx"), lax.axis_size("ctx")
    greet(["dp", "tp"], line=True)
    right, left = me + 1, me - 1
    sems = (line_send, line_recv)

    def hop(s, src):
        return remote(src, came_kv.at[s], sems, s, {"ctx": left})

    def forth():
        return remote(
            kv_grad_ref.at[lax.rem(me + 1, size)], came_kv.at[0], sems, 0, {"ctx": right}
        )

    def own_piece(s):
        return kv_grad_ref.at[lax.rem(me + size - s, size)]

    if ahead:

        @pl.when(right < size)
        def _():
            forth().start()

    @pl.when(me - back >= 0)
    def _():
        hop(back, own_piece(back)).start()

    rows = RowReturn(
        part, held, landed, total, sent, came, (dp_send, dp_recv), (tp_send, tp_recv)
    )
    rows.start(places_ref, slots_ref)
    rows.forward()
    turned = jnp.transpose(low_ref[...].astype(jnp.float32)).astype(jnp.bfloat16)
    grad = jnp.dot(turned, mix_ref[...], preferred_element_type=jnp.float32)
    if early:
        piece, q_width = pieces.shape[1], dq_ref.shape[1]
        for i in range(pieces.shape[0]):
            pieces[i, :, q_width:] = grad[i * piece : (i + 1) * piece].astype(jnp.bfloat16)
        wide = 2 * HEAD_DIM
        cosine, sine = block_tables(cos_ref, sin_ref, dq_ref.shape[0], me)
        for first in range(0, q_width, wide):
            joined_ref[:, first : first + wide] = turn(
                dq_ref[:, first : first + wide], cosine, sine
            ).astype(jnp.bfloat16)
        turned_ref[...] = jnp.transpose(normed_ref[...].astype(jnp.float32)).astype(jnp.bfloat16)
        rows.pass_on()
        for i in range(pieces.shape[0]):
            pieces[i, :, :q_width] = jnp.dot(
                turned_ref[i * piece : (i + 1) * piece, :], joined_ref[...],
                preferred_element_type=jnp.float32,
            ).astype(jnp.bfloat16)
        sums = GridPieceSum(pieces, pieces_landed, (sum_send, sum_recv), whole)
        sums.start()
    else:
        piece = out_w_ref.shape[1]
        for i in range(out_w_ref.shape[0]):
            out_w_ref[i] = grad[i * piece : (i + 1) * piece].astype(jnp.bfloat16)
        rows.pass_on()

    for s in range(back - 1, 0, -1):

        @pl.when((me - s >= 0) & (right < size))
        def _(s=s):
            hop(s + 1, going.at[s]).wait_recv()
            going[s] = (
                own_piece(s)[...].astype(jnp.float32) + came_kv[s + 1].astype(jnp.float32)
            ).astype(going.dtype)
            hop(s, going.at[s]).start()

        @pl.when((me - s >= 0) & (right >= size))
        def _(s=s):
            hop(s, own_piece(s)).start()

    rows.gather()
    if early:
        sums.forward()
    kv_ref[...] = kv_grad_ref[me].astype(jnp.float32)

    @pl.when(right < size)
    def _():
        hop(1, going.at[0]).wait_recv()
        kv_ref[...] += came_kv[1].astype(jnp.float32)

    if ahead:

        @pl.when(left >= 0)
        def _():
            forth().wait_recv()
            kv_ref[...] += came_kv[0].astype(jnp.float32)

        @pl.when(right < size)
        def _():
            forth().wait_send()

    for s in range(back, 0, -1):

        @pl.when(me - s >= 0)
        def _(s=s):
            hop(s, going.at[0]).wait_send()

    if early:
        sums_ref[...] = sums.total().astype(jnp.bfloat16)
        sums.finish()
    rows.finish()
    out_ref[rows.mine, :] = sent[...]
    out_ref[rows.theirs, :] = came[...]


def trade(kv_grad, slots, places, low, mix, dq, cosine, sine, normed, back, ahead, ident):
    size, (rows, width) = slots.shape[0], low.shape
    kv_shape, out_cols, q_width = kv_grad.shape[1:], mix.shape[1], dq.shape[1]
    going = pltpu.VMEM((max(back, 1),) + kv_shape, kv_grad.dtype)
    came = pltpu.VMEM((back + 1,) + kv_shape, kv_grad.dtype)
    early, piece = size == 4, width // size
    few = jnp.bfloat16
    more_in, more_out, more_scratch = [], [], []
    if early:
        more_in = [dq, cosine, sine, normed]
        more_out = [
            jax.ShapeDtypeStruct((piece, q_width + out_cols), few),
            jax.ShapeDtypeStruct(dq.shape, few),
            jax.ShapeDtypeStruct((width, rows), few),
        ]
        more_scratch = [
            pltpu.VMEM((size, piece, q_width + out_cols), few),
            pltpu.VMEM((size - 1, piece, q_width + out_cols), few),
            pltpu.VMEM((piece, q_width + out_cols), jnp.float32),
            *sem_pair(6),
        ]
    else:
        more_out = [jax.ShapeDtypeStruct((size, piece, out_cols), few)]
    return pl.pallas_call(
        functools.partial(trade_kernel, back, ahead, early),
        name="trade",
        in_specs=whole_vmem(5 + len(more_in)),
        out_specs=whole_vmem(2 + len(more_out)),
        out_shape=[
            jax.ShapeDtypeStruct(kv_shape, jnp.float32),
            jax.ShapeDtypeStruct((rows, width), few),
        ]
        + more_out,
        scratch_shapes=more_scratch
        + [going, came, *sem_pair(back + 1), *return_scratch(size, rows, width)],
        compiler_params=remote_params(ident),
    )(kv_grad, slots, places, low, mix, *more_in)


class PieceSum:
    def __init__(self, axis, source, landed, sems):
        self.axis, self.source, self.landed, self.sems = axis, source, landed, sems
        self.size = lax.axis_size(axis)

    def copy(self, k):
        peer = ahead_on(self.axis, k)
        return remote(
            self.source.at[peer], self.landed.at[k], self.sems, k, {self.axis: peer}
        )

    def send(self, k):
        self.copy(k).start()

    def start(self):
        each(self.size, self.send)

    def forward(self):
        pass

    def total(self):
        each(self.size, lambda k: self.copy(k).wait_recv())
        whole = self.source[lax.axis_index(self.axis)].astype(jnp.float32)
        for k in range(1, self.size):
            whole += self.landed[k].astype(jnp.float32)
        return whole

    def finish(self):
        each(self.size, lambda k: self.copy(k).wait_send())


class GridPieceSum:
    def __init__(self, source, landed, sems, whole):
        x, y, diagonal = grid_peers()
        places = (lax.axis_index("dp"), x, y, diagonal)
        self.source, self.whole = source, whole
        self.sum = GridSum(lambda n: source.at[places[n]], landed, sems)
        self.start, self.forward, self.finish = self.sum.start, self.sum.forward, self.sum.finish

    def total(self):
        self.whole[...] = self.source[lax.axis_index("dp")].astype(jnp.float32)
        self.sum.add_to(self.whole)
        return self.whole[...]


def dp_sum(source, landed, sems, whole):
    if lax.axis_size("dp") == 4:
        return GridPieceSum(source, landed, sems, whole)
    return PieceSum("dp", source, landed, sems)


class WholeSum:
    def __init__(self, axis, source, landed, sems):
        self.axis, self.source, self.landed, self.sems = axis, source, landed, sems
        self.size = lax.axis_size(axis)

    def copy(self, k):
        return remote(
            self.source, self.landed.at[k], self.sems, k, {self.axis: ahead_on(self.axis, k)}
        )

    def start(self):
        each(self.size, lambda k: self.copy(k).start())

    def total(self):
        each(self.size, lambda k: self.copy(k).wait())
        whole = self.source[...]
        for k in range(1, self.size):
            whole += self.landed[k]
        return whole


def finish_kernel(early, dkv_ref, cos_ref, sin_ref, w_ref, x_ref, gain_ref, gain_two_ref, *refs):
    if early:
        sums_ref, joined_q_ref, turned, *refs = refs
    else:
        dq_ref, normed_ref, out_w_ref, *refs = refs
    in_ref, own_ref, gains_ref, joined, part, held, pieces, landed, whole, *refs = refs
    low, low_landed, gain_rows, gain_landed, gain_more, gain_more_landed, *refs = refs
    if not early:
        turned, out_landed, *refs = refs
    greet(["dp", "ctx", "tp"])
    pairs = [refs[2 * i : 2 * i + 2] for i in range(len(refs) // 2)]
    wide = 2 * HEAD_DIM
    kv_width = dkv_ref.shape[1] // 2
    q_width = joined.shape[1] - 2 * kv_width
    cosine, sine = block_tables(cos_ref, sin_ref, dkv_ref.shape[0], lax.axis_index("ctx"))
    if early:
        joined[:, :q_width] = joined_q_ref[...]
        done = q_width
    else:
        out_sum = PieceSum("dp", out_w_ref, out_landed, pairs[5])
        out_sum.start()
        done = 0
        for first in range(0, q_width, wide):
            joined[:, first : first + wide] = turn(
                dq_ref[:, first : first + wide], cosine, sine
            ).astype(jnp.bfloat16)
        turned[...] = jnp.transpose(normed_ref[...].astype(jnp.float32)).astype(jnp.bfloat16)
    for first in range(0, kv_width, wide):
        joined[:, q_width + first : q_width + first + wide] = turn(
            dkv_ref[:, first : first + wide], cosine, sine
        ).astype(jnp.bfloat16)
    joined[:, q_width + kv_width :] = dkv_ref[:, kv_width:].astype(jnp.bfloat16)

    w_sum = dp_sum(pieces, landed, pairs[0], whole)
    rows = pieces.shape[1]

    def piece(k):
        peer = ahead_on("dp", k)
        at = pl.ds(pl.multiple_of(peer * rows, rows), rows)
        pieces[peer] = jnp.dot(
            turned[at, :], joined[:, done:], preferred_element_type=jnp.float32
        ).astype(jnp.bfloat16)

    each(pieces.shape[0], piece)
    w_sum.start()
    for i in range(w_ref.shape[0]):
        part[:, i * rows : (i + 1) * rows] = lax.dot_general(
            joined[...], w_ref[i], NT, preferred_element_type=jnp.float32
        ).astype(jnp.bfloat16)
    swap = remote(part, held, pairs[1], 0, other_core())
    swap.start()
    piece(0)
    swap.wait()
    x_grad, gain_grad = norm_back(
        x_ref[...].astype(jnp.float32),
        gain_ref[0:1, :],
        part[...].astype(jnp.float32) + held[...].astype(jnp.float32),
    )
    in_ref[...] = x_grad
    gain_rows[...] = jnp.zeros(gain_rows.shape, jnp.float32)
    gain_rows[0:1, :] = gain_grad
    gain_rows[1:2, :] = gain_two_ref[...]
    gain_sum = WholeSum("dp", gain_rows, gain_landed, pairs[2])
    gain_sum.start()
    w_sum.forward()

    cols, few = joined.shape[1], low.shape[1]
    w_total = w_sum.total()
    if not early:
        out_total = out_sum.total()
    for c in range(low.shape[0]):
        at = slice(c * few, (c + 1) * few)
        low[c, :, done:cols] = w_total[at].astype(jnp.bfloat16)
        if early:
            low[c, :, :done] = sums_ref[at, :done]
            low[c, :, cols:] = sums_ref[at, done:]
        else:
            low[c, :, cols:] = out_total[at].astype(jnp.bfloat16)
    low_sum = PieceSum("ctx", low, low_landed, pairs[3])
    low_sum.start()
    gain_more[...] = gain_sum.total()
    more_sum = WholeSum("ctx", gain_more, gain_more_landed, pairs[4])
    more_sum.start()
    w_sum.finish()
    if not early:
        out_sum.finish()
    own_ref[...] = low_sum.total()
    low_sum.finish()
    gains_ref[...] = more_sum.total()


def finish(dkv, cosine, sine, w, x, gain, gain_two, given, out_cols, ident):
    rows, width = x.shape
    dp_size, ctx_size = lax.axis_size("dp"), lax.axis_size("ctx")
    early, cols = dp_size == 4, w.shape[2]
    piece = width // dp_size
    few = piece // ctx_size
    mine = dkv.shape[1] if early else cols
    low, high = jnp.bfloat16, jnp.float32
    more_scratch = [] if early else [
        pltpu.VMEM((width, rows), low),
        pltpu.VMEM((dp_size, piece, out_cols), low),
    ]
    return pl.pallas_call(
        functools.partial(finish_kernel, early),
        name="finish",
        in_specs=whole_vmem(7 + len(given)),
        out_specs=whole_vmem(3),
        out_shape=[
            jax.ShapeDtypeStruct((rows, width), high),
            jax.ShapeDtypeStruct((few, cols + out_cols), high),
            jax.ShapeDtypeStruct((8, width), high),
        ],
        scratch_shapes=[
            pltpu.VMEM((rows, cols), low),
            pltpu.VMEM((rows, width), low),
            pltpu.VMEM((rows, width), low),
            pltpu.VMEM((dp_size, piece, mine), low),
            pltpu.VMEM((dp_size, piece, mine), low),
            pltpu.VMEM((piece, mine), high),
            pltpu.VMEM((ctx_size, few, cols + out_cols), low),
            pltpu.VMEM((ctx_size, few, cols + out_cols), low),
            pltpu.VMEM((8, width), high),
            pltpu.VMEM((dp_size, 8, width), high),
            pltpu.VMEM((8, width), high),
            pltpu.VMEM((ctx_size, 8, width), high),
            *more_scratch,
            *sem_pair(max(dp_size, 6)),
            *sem_pair(1),
            *sem_pair(dp_size),
            *sem_pair(ctx_size),
            *sem_pair(ctx_size),
            *(() if early else sem_pair(dp_size)),
        ],
        compiler_params=remote_params(ident),
    )(dkv, cosine, sine, w, x, gain, gain_two, *given)


class Everyone:
    def __init__(self, axis, target, sems):
        self.axis, self.target, self.sems = axis, target, sems
        self.size = lax.axis_size(axis)

    def copy(self, k):
        at = self.target.at[lax.axis_index(self.axis)]
        return remote(at, at, self.sems, k, {self.axis: ahead_on(self.axis, k)})

    def start(self):
        each(self.size, lambda k: self.copy(k).start())

    def arrive(self):
        each(self.size, lambda k: self.copy(k).wait_recv())

    def finish(self):
        each(self.size, lambda k: self.copy(k).wait_send())


def find_places(first, own, routes_ref, gates_ref, earlier, place_ref, gate_ref, column_ref):
    _, tokens = routes_ref.shape[1:]

    def group(g, carry):
        routes, gates = routes_ref[g], gates_ref[g]
        names, values = [], []
        for e in range(own):
            named = routes == first + e
            names.append(jnp.max(named.astype(jnp.float32), axis=0, keepdims=True))
            values.append(jnp.sum(jnp.where(named, gates, 0.0), axis=0, keepdims=True))
        spare = jnp.zeros((8 - own % 8 if own % 8 else 0, tokens), jnp.float32)
        names = jnp.concatenate(names + ([spare] if spare.shape[0] else []), axis=0)
        place = jnp.dot(
            names.astype(jnp.bfloat16), earlier[...], preferred_element_type=jnp.float32
        )
        place = jnp.where((names > 0.0) & (place < CAP), place, -float(CAP * own))
        for e in range(own):
            place_ref[g, e] = place[e : e + 1].astype(jnp.int32)
            gate_ref[g, e] = values[e]
        column_ref[g] = jnp.transpose(place)[:, :own].astype(jnp.int32)
        return carry

    lax.fori_loop(0, routes_ref.shape[0], group, 0)


class LineRows:
    def __init__(self, x_ref, x_all, back, ahead, line_sems, tp_sems):
        self.x_ref, self.x_all, self.back, self.ahead = x_ref, x_all, back, ahead
        self.line_sems, self.tp_sems = line_sems, tp_sems
        self.me, self.size = lax.axis_index("ctx"), lax.axis_size("ctx")
        self.mine, _ = halves(x_ref.shape[0])

    def block(self, s):
        return lax.rem(self.me + self.size - s, self.size)

    def sends(self, s):
        return (self.me + 1 < self.size) & (self.me - s >= 0)

    def hop(self, s):
        at = self.x_all.at[self.block(s), self.mine]
        source = self.x_ref.at[self.mine] if isinstance(s, int) and s == 0 else at
        return remote(source, at, self.line_sems, s, {"ctx": self.me + 1})

    def back_hop(self):
        at = self.x_all.at[self.me, self.mine]
        return remote(
            self.x_ref.at[self.mine], at, self.line_sems, self.back, {"ctx": self.me - 1}
        )

    def relay(self, k, block):
        at = self.x_all.at[block, self.mine]
        return remote(at, at, self.tp_sems, k, other_core())

    def start(self):
        if self.back:
            pl.when(self.sends(0))(lambda: self.hop(0).start())
        if self.ahead:
            pl.when(self.me >= 1)(lambda: self.back_hop().start())

    def step(self, s):
        @pl.when(self.me - s - 1 >= 0)
        def _():
            self.hop(s).wait_recv()
            self.relay(s, self.block(s + 1)).start()

        if s + 1 < self.back:
            pl.when(self.sends(s + 1))(lambda: self.hop(s + 1).start())

    def step_back(self):
        if self.ahead:

            @pl.when(self.me + 1 < self.size)
            def _():
                self.back_hop().wait_recv()
                self.relay(self.back, self.block(self.size - 1)).start()

    def finish(self):
        for s in range(self.back):
            pl.when(self.sends(s))(lambda s=s: self.hop(s).wait_send())
        if self.ahead:
            pl.when(self.me >= 1)(lambda: self.back_hop().wait_send())


def front_kernel(
    back, ahead, own, starts_ref, x_ref, cot_ref, q_w_ref, k_w_ref, v_w_ref, out_w_ref, gains_ref,
    docs_ref, routes_ref, gates_ref, cos_ref, sin_ref, w_out, out_w_out, gain_rows, docs_all,
    normed_out, q_ref, kv_out, mix_ref, full_out, log_ref, hidden_out, rows_out, cot_out,
    place_ref, gate_ref, column_ref, w_all, out_w_all, normed, kv_all, full, hidden, x_all,
    gains_all, routes_all, gates_all, acc, top, total, column, part, held,
    normed_two, *sems,
):
    me, size = lax.axis_index("ctx"), lax.axis_size("ctx")
    dp = lax.axis_index("dp")
    local = sems[-1]
    pairs = [sems[2 * i : 2 * i + 2] for i in range(len(sems) // 2)]
    q_width, kv_width = q_w_ref.shape[1], k_w_ref.shape[1]
    dp_size, piece = w_all.shape[:2]
    block_rows = x_ref.shape[0]

    def flush(i, source, target):
        return pltpu.make_async_copy(source, target, local.at[i])

    w_all[dp, :, :q_width] = q_w_ref[...]
    w_all[dp, :, q_width : q_width + kv_width] = k_w_ref[...]
    w_all[dp, :, q_width + kv_width :] = v_w_ref[...]
    gains_all[dp] = gains_ref[...]
    docs_all[me] = docs_ref[...]
    routes_all[dp] = routes_ref[...]
    gates_all[dp] = gates_ref[...]
    greet(["dp", "ctx", "tp"])
    weights = Gather(w_all, pairs[1])
    gains = Everyone("dp", gains_all, pairs[0])
    docs = Everyone("ctx", docs_all, pairs[2])
    routes = Everyone("dp", routes_all, pairs[3])
    gates = Everyone("dp", gates_all, pairs[4])
    out_w = Gather(out_w_all, pairs[5])
    line = LineRows(x_ref, x_all, back, ahead, pairs[8], pairs[11])
    for one in (gains, weights, line, docs, routes, gates):
        one.start()

    out_w_all[dp] = out_w_ref[...]
    x_all[me] = x_ref[...]
    token = lax.broadcasted_iota(jnp.int32, (block_rows, block_rows), 0)
    later = lax.broadcasted_iota(jnp.int32, (block_rows, block_rows), 1)
    normed_two[:, :block_rows] = (token < later).astype(jnp.float32).astype(jnp.bfloat16)
    top[...] = jnp.full(top.shape, NEG_FILL, jnp.float32)
    total[...] = jnp.zeros(total.shape, jnp.float32)
    acc[...] = jnp.zeros(acc.shape, jnp.float32)
    gains.arrive()
    for i in range(dp_size):
        gain_rows[:, i * piece : (i + 1) * piece] = gains_all[i]

    def norm_rows(source):
        x = source.astype(jnp.float32)
        return (x * row_scale(x) * gain_rows[0:1, :]).astype(jnp.bfloat16)

    normed[...] = norm_rows(x_ref[...])
    flush(0, normed, normed_out).start()
    routes.arrive()
    gates.arrive()
    docs.arrive()
    if back:
        line.step(0)
    weights.forward()
    find_places(
        dp * own, own, routes_all, gates_all, normed_two.at[:, :block_rows], place_ref, gate_ref,
        column_ref,
    )
    weights.arrive()
    flush(1, w_all, w_out).start()
    out_w.start()
    cot_rows = RowGather(cot_ref, cot_out, pairs[6], pairs[7], 0)
    cot_rows.start()
    last = 2 + back + 1 + ahead
    flush(last + 3, cot_ref, cot_out.at[dp]).start()

    wide, tile = 4 * HEAD_DIM, 2 * HEAD_DIM

    def project(source, first):
        whole = jnp.dot(
            source[:, :piece], w_all[0, :, first : first + wide],
            preferred_element_type=jnp.float32,
        )
        for i in range(1, dp_size):
            whole += jnp.dot(
                source[:, i * piece : (i + 1) * piece], w_all[i, :, first : first + wide],
                preferred_element_type=jnp.float32,
            )
        return [whole[:, :tile], whole[:, tile:]]

    def tables(block):
        cosine, sine = block_tables(cos_ref, sin_ref, block_rows, block)
        return cosine, -sine

    here = tables(me)
    for first in range(0, q_width, wide):
        for i, part_of in enumerate(project(normed, first)):
            turned = turn(part_of, *here).astype(jnp.bfloat16)
            at = first + i * tile
            q_ref[:, at : at + tile] = (turned.astype(jnp.float32) * HEAD_DIM**-0.5).astype(
                jnp.bfloat16
            )
    for s in range(1, back):
        line.step(s)
    line.step_back()
    masks = Masks(docs_all, starts_ref, column)

    def visit(s, block):
        @pl.when(s > 0)
        def _():
            line.relay(s - 1, block).wait()

        part[...] = norm_rows(x_all[block])
        there = tables(block)
        for first in range(q_width, q_width + 2 * kv_width, wide):
            for i, part_of in enumerate(project(part, first)):
                if first < q_width + kv_width:
                    part_of = turn(part_of, *there)
                at = first - q_width + i * tile
                kv_all[block, :, at : at + tile] = part_of.astype(jnp.bfloat16)
        flush(2 + s, kv_all.at[block], kv_out.at[block]).start()
        attend_block(masks, block, q_ref, kv_all.at[block], acc, top, total)

    def step(s):
        pl.when(me - s >= 0)(lambda: visit(s, lax.rem(me + size - s, size)))

        @pl.when(s == min(1, back))
        def _():
            out_w.forward()
            cot_rows.forward()

    each(back + 1, step, 0)
    if ahead:

        @pl.when(me + 1 < size)
        def _():
            visit(back + 1, lax.rem(me + 1, size))

    log_ref[...] = top[...] + jnp.log(total[...])
    for h in range(total.shape[0]):
        at = slice(h * HEAD_DIM, (h + 1) * HEAD_DIM)
        acc[at, :] = acc[at, :] / total[h : h + 1, :]
    full[...] = jnp.transpose(acc[...])
    mix_ref[...] = full[...].astype(jnp.bfloat16)
    out_w.arrive()
    cot_rows.arrive()
    for i in range(dp_size):
        part[:, i * piece : (i + 1) * piece] = jnp.dot(
            mix_ref[...], out_w_all[i], preferred_element_type=jnp.float32
        ).astype(jnp.bfloat16)

    mine, theirs = halves(block_rows)
    rows = RowGather(normed_two, rows_out, pairs[9], pairs[10], 2)
    first = remote(part.at[theirs], held.at[theirs], pairs[10], 0, other_core())
    second = remote(part.at[mine], held.at[mine], pairs[10], 1, other_core())
    first.start()
    second.start()
    flush(last, full, full_out).start()
    flush(last + 1, out_w_all, out_w_out).start()

    def norm(at):
        whole = x_ref[at, :].astype(jnp.float32) + (
            part[at, :].astype(jnp.float32) + held[at, :].astype(jnp.float32)
        )
        hidden[at, :] = whole
        normed_two[at, :] = (whole * row_scale(whole) * gain_rows[1:2, :]).astype(jnp.bfloat16)

    first.wait()
    norm(mine)
    rows.start()
    second.wait()
    norm(theirs)
    flush(last + 2, hidden, hidden_out).start()
    flush(last + 4, normed_two, rows_out.at[dp]).start()
    cot_rows.finish()
    for one in (gains, weights, docs, routes, gates, out_w, line):
        one.finish()
    rows.forward()
    rows.arrive()
    rows.finish()
    flush(0, normed, normed_out).wait()
    flush(1, w_all, w_out).wait()

    def kept(s):
        @pl.when(me - s >= 0)
        def _():
            flush(2 + s, kv_all.at[me], kv_out.at[me]).wait()

    each(back + 1, kept, 0)
    if ahead:
        pl.when(me + 1 < size)(lambda: flush(3 + back, kv_all.at[me], kv_out.at[me]).wait())
    flush(last, full, full_out).wait()
    flush(last + 1, out_w_all, out_w_out).wait()
    flush(last + 2, hidden, hidden_out).wait()
    flush(last + 3, cot_ref, cot_out.at[dp]).wait()
    flush(last + 4, normed_two, rows_out.at[dp]).wait()


def front(
    starts, x, cot, q_w, k_w, v_w, out_w, gains, docs, routes, gates, cosine, sine, own, back,
    ahead, ident,
):
    rows, width = x.shape
    dp_size, ctx_size = lax.axis_size("dp"), lax.axis_size("ctx")
    q_width, kv_cols = q_w.shape[1], 2 * k_w.shape[1]
    piece, heads = q_w.shape[0], q_width // HEAD_DIM
    low, high, whole = jnp.bfloat16, jnp.float32, jnp.int32
    far = [
        ((dp_size, piece, q_width + kv_cols), low),
        ((dp_size,) + out_w.shape, low),
        ((rows, width), low),
        ((ctx_size, rows, kv_cols), low),
        ((rows, q_width), high),
        ((rows, width), high),
        ((dp_size, rows, width), low),
        ((dp_size, rows, width), low),
    ]
    shapes = [
        far[0],
        far[1],
        ((2, width), high),
        ((ctx_size, 1, rows), whole),
        far[2],
        ((rows, q_width), low),
        far[3],
        ((rows, q_width), low),
        far[4],
        ((heads, rows), high),
        far[5],
        far[6],
        far[7],
        ((dp_size, own, 1, rows), whole),
        ((dp_size, own, 1, rows), high),
        ((dp_size, rows, own), whole),
    ]
    return pl.pallas_call(
        functools.partial(front_kernel, back, ahead, own),
        name="front",
        in_specs=[pl.BlockSpec(memory_space=pltpu.SMEM)] + whole_vmem(12),
        out_specs=[
            pl.BlockSpec(memory_space=pl.ANY if shape in far else pltpu.VMEM) for shape in shapes
        ],
        out_shape=[jax.ShapeDtypeStruct(*shape) for shape in shapes],
        scratch_shapes=[
            *[pltpu.VMEM(*shape) for shape in far[:6]],
            pltpu.VMEM((ctx_size, rows, width), low),
            pltpu.VMEM((dp_size,) + gains.shape, high),
            pltpu.VMEM((dp_size,) + routes.shape, whole),
            pltpu.VMEM((dp_size,) + gates.shape, high),
            pltpu.VMEM((q_width, rows), high),
            pltpu.VMEM((heads, rows), high),
            pltpu.VMEM((heads, rows), high),
            pltpu.VMEM((rows, 8), whole),
            pltpu.VMEM((rows, width), low),
            pltpu.VMEM((rows, width), low),
            pltpu.VMEM((rows, width), low),
            *sem_pair(dp_size),
            *sem_pair(dp_size),
            *sem_pair(ctx_size),
            *sem_pair(dp_size),
            *sem_pair(dp_size),
            *sem_pair(dp_size),
            *sem_pair(dp_size),
            *sem_pair(dp_size),
            *sem_pair(back + 1),
            *sem_pair(dp_size),
            *sem_pair(dp_size + 2),
            *sem_pair(back + 1),
            pltpu.SemaphoreType.DMA((8 + back + ahead,)),
        ],
        compiler_params=remote_params(ident),
    )(starts, x, cot, q_w, k_w, v_w, out_w, gains, docs, routes, gates, cosine, sine)


GROUPS_AT_ONCE = 4


def experts_kernel(more, rows_ref, grads_ref, weights_ref, place_ref, gate_ref, *refs):
    outs_ref, backs_ref, weight_grad_ref, slots, slot_grads = refs[2 * more :]
    groups, tok_rows, _ = rows_ref.shape
    owners, part = weight_grad_ref.shape[1], weight_grad_ref.shape[5]
    slot_index = lax.broadcasted_iota(jnp.int32, (CAP, tok_rows), 0)
    gates = []
    for g in range(groups):
        picks = slot_index == place_ref[g, 0]
        gates.append(jnp.sum(jnp.where(picks, gate_ref[g, 0], 0.0), axis=1, keepdims=True))
        picks = picks.astype(jnp.float32).astype(jnp.bfloat16)
        at = slice(g * CAP, (g + 1) * CAP)
        slots[at, :] = jnp.dot(
            picks, rows_ref[g], preferred_element_type=jnp.float32
        ).astype(jnp.bfloat16)
        slot_grads[at, :] = (
            jnp.dot(picks, grads_ref[g], preferred_element_type=jnp.float32) * gates[g]
        ).astype(jnp.bfloat16)
    gate_w, up_w, down_w = (weights_ref.at[0, i] for i in range(3))
    gate_pre = jnp.dot(slots[...], gate_w[...], preferred_element_type=jnp.float32)
    up_pre = jnp.dot(slots[...], up_w[...], preferred_element_type=jnp.float32)
    act_grad = jnp.dot(slot_grads[...], down_w[...], preferred_element_type=jnp.float32)
    sig = 1.0 / (1.0 + jnp.exp(-gate_pre))
    silu = gate_pre * sig
    act_low = (silu * up_pre).astype(jnp.bfloat16)
    up_low = (act_grad * silu).astype(jnp.bfloat16)
    gate_low = (act_grad * up_pre * (sig * (1.0 + gate_pre * (1.0 - sig)))).astype(jnp.bfloat16)

    back = lax.dot_general(
        gate_low, gate_w[...], NT, preferred_element_type=jnp.float32
    ) + lax.dot_general(up_low, up_w[...], NT, preferred_element_type=jnp.float32)
    out = lax.dot_general(act_low, down_w[...], NT, preferred_element_type=jnp.float32)
    for g in range(groups):
        at = slice(g * CAP, (g + 1) * CAP)
        backs_ref[g] = back[at].astype(jnp.bfloat16)
        outs_ref[g] = (out[at] * gates[g]).astype(jnp.bfloat16)

    for i, (low, source) in enumerate(
        ((gate_low, slots), (up_low, slots), (act_low, slot_grads))
    ):
        turned = jnp.transpose(low.astype(jnp.float32)).astype(jnp.bfloat16)
        total = jnp.dot(turned, source[...], preferred_element_type=jnp.float32)
        for c in range(owners):
            weight_grad_ref[0, c, 0, i] = total[:, c * part : (c + 1) * part].astype(
                weight_grad_ref.dtype
            )


def experts(weights, place_rows, gate_rows, rows_all, grad_all, first, count, before):
    own, _, model_width, hidden = weights.shape
    groups, tok_rows, _ = rows_all.shape
    owners = lax.axis_size("ctx")
    at_once = min(GROUPS_AT_ONCE, groups)
    chunks = groups // at_once
    part = model_width // owners
    rows_spec = pl.BlockSpec(
        (at_once, tok_rows, model_width), lambda c, e: (c, 0, 0), pipeline_mode=pl.Buffered(1)
    )
    line_spec = pl.BlockSpec((at_once, 1, 1, tok_rows), lambda c, e: (c, e + first, 0, 0))
    slots_spec = pl.BlockSpec((at_once, CAP, model_width), lambda c, e: (c, e + first, 0))
    slots_shape = jax.ShapeDtypeStruct((groups, own * CAP, model_width), jnp.bfloat16)
    flops = count * groups * CAP * model_width * 2 * (9 * hidden + 2 * tok_rows)
    more = before is not None
    outs, backs, weight_part = pl.pallas_call(
        functools.partial(experts_kernel, more),
        name="experts",
        grid=(chunks, count),
        in_specs=[
            rows_spec,
            rows_spec,
            pl.BlockSpec((1, 3, model_width, hidden), lambda c, e: (e + first, 0, 0, 0)),
            line_spec,
            line_spec,
        ]
        + [pl.BlockSpec(memory_space=pl.ANY)] * (2 * more),
        out_specs=[
            slots_spec,
            slots_spec,
            pl.BlockSpec((1, owners, 1, 3, hidden, part), lambda c, e: (c, 0, e, 0, 0, 0)),
        ],
        out_shape=[
            slots_shape,
            slots_shape,
            jax.ShapeDtypeStruct((chunks, owners, count, 3, hidden, part), jnp.bfloat16),
        ],
        scratch_shapes=[
            pltpu.VMEM((at_once * CAP, model_width), jnp.bfloat16),
            pltpu.VMEM((at_once * CAP, model_width), jnp.bfloat16),
        ],
        input_output_aliases={5: 0, 6: 1} if more else {},
        compiler_params=pltpu.CompilerParams(vmem_limit_bytes=LIMIT),
        cost_estimate=pl.CostEstimate(
            flops=flops, bytes_accessed=4 * weights.size, transcendentals=0
        ),
    )(rows_all, grad_all, weights, place_rows, gate_rows, *(before if more else ()))
    if chunks == 1:
        return (outs, backs), weight_part[0]
    return (outs, backs), jnp.sum(weight_part.astype(jnp.float32), axis=0).astype(jnp.bfloat16)


def unfold_kernel(more, sums_ref, *refs):
    out_ref = refs[more]
    for i in range(sums_ref.shape[1]):
        out_ref[0, i] = jnp.transpose(sums_ref[0, i].astype(jnp.float32))


def unfold(sums, own, first, before):
    count, three, hidden, part = sums.shape
    more = before is not None
    return pl.pallas_call(
        functools.partial(unfold_kernel, more),
        name="unfold",
        grid=(count,),
        in_specs=[pl.BlockSpec((1, three, hidden, part), lambda e: (e, 0, 0, 0))]
        + [pl.BlockSpec(memory_space=pl.ANY)] * more,
        out_specs=pl.BlockSpec((1, three, part, hidden), lambda e: (e + first, 0, 0, 0)),
        out_shape=jax.ShapeDtypeStruct((own, three, part, hidden), jnp.float32),
        input_output_aliases={1: 0} if more else {},
        compiler_params=pltpu.CompilerParams(vmem_limit_bytes=LIMIT),
    )(sums, *([before] if more else []))


def rotary_tables(token_positions):
    half_dim = HEAD_DIM // 2
    inverse = THETA ** (-(jnp.arange(half_dim, dtype=jnp.float32) * 2.0 / HEAD_DIM))
    angles = token_positions.astype(jnp.float32)[:, None] * inverse[None, :]
    cosine, sine = jnp.cos(angles), jnp.sin(angles)
    return jnp.concatenate([cosine] * 4, axis=1), jnp.concatenate([sine, -sine] * 2, axis=1)


def expert_counts(own):
    return (1, 6, 1) if own == 8 else (own - own // 2, own // 2)


def scatter(grads):
    return lax.psum_scatter(grads, "ctx", scatter_dimension=0)


def body(
    tokens,
    query_weight,
    key_weight,
    value_weight,
    output_weight,
    gain_attn,
    gain_moe,
    expert_weights,
    routes,
    gate_values,
    documents,
    pic_starts,
    cotangent,
):
    block_len = tokens.shape[1]
    ctx_size = lax.axis_size("ctx")
    length = block_len * ctx_size
    back = back_blocks(ctx_size, block_len, length)
    ahead = ahead_blocks(block_len, length, pic_starts.shape[1])
    q_width, kv_width = query_weight.shape[1], key_weight.shape[1]
    own = expert_weights.shape[0]
    x, cot = tokens[0], cotangent[0]

    inside = jnp.arange(block_len, dtype=jnp.int32)
    starts = jnp.arange(-(-ctx_size // 8) * 8, dtype=jnp.int32) * block_len
    cosine, sine = rotary_tables(jnp.concatenate([inside, starts]))
    (
        w_all,
        out_w_all,
        gain_rows,
        docs_all,
        normed_one,
        query,
        kv_all,
        mixture,
        mix_full,
        log_total,
        hidden,
        rows_all,
        grad_all,
        *places,
    ) = front(
        pic_starts,
        x,
        cot,
        query_weight,
        key_weight,
        value_weight,
        output_weight,
        jnp.stack([gain_attn, gain_moe]).astype(jnp.float32),
        documents,
        routes[0].T,
        gate_values[0].T,
        cosine,
        sine,
        own,
        back,
        ahead,
        1,
    )
    place_rows, gate_rows, places = places
    counts = expert_counts(own)
    slots, sums = None, []
    first = 0
    for n, count in enumerate(counts):
        slots, grads = experts(
            expert_weights, place_rows, gate_rows, rows_all, grad_all, first, count, slots
        )
        if n < len(counts) - 1:
            sums.append((scatter(grads), first))
        first += count
    outs, backs = slots
    hidden_grad, hidden_low, mix_grad, gain_two_grad = return_grads(
        backs, places, hidden, cot, gain_rows, out_w_all, 2
    )
    q_rot_grad, kv_part = attend_back(
        pic_starts, query, kv_all, docs_all, log_total, mix_full, mix_grad, back, ahead
    )
    kv_back, expert_sum, *given = trade(
        kv_part,
        outs,
        places,
        hidden_low,
        mixture,
        q_rot_grad,
        cosine,
        sine,
        normed_one,
        back,
        ahead,
        3,
    )
    if len(given) == 1:
        given = [q_rot_grad, normed_one, given[0]]
    x_grad, owned, gain_sums = finish(
        kv_back, cosine, sine, w_all, x, gain_rows, gain_two_grad, given, mixture.shape[1], 4
    )
    grads, owned = lax.optimization_barrier((grads, owned))
    sums.append((scatter(grads), own - counts[-1]))
    few = owned.shape[0]
    here = (lax.axis_index("dp") * ctx_size + lax.axis_index("ctx")) * few
    gain_sums = lax.dynamic_slice_in_dim(gain_sums, here, few, 1)
    expert_grad = None
    for part, first in sums:
        expert_grad = unfold(part, own, first, expert_grad)
    v_end = q_width + 2 * kv_width
    return (
        (hidden + expert_sum.astype(jnp.float32)).astype(jnp.bfloat16)[None],
        (hidden_grad + x_grad).astype(jnp.bfloat16)[None],
        owned[:, :q_width],
        owned[:, q_width : q_width + kv_width],
        owned[:, q_width + kv_width : v_end],
        owned[:, v_end:].T,
        gain_sums[0],
        gain_sums[1],
        expert_grad,
    )


def solution(mesh):
    return jax.shard_map(
        body,
        mesh=mesh,
        in_specs=(
            P("dp", "ctx", None),
            P("dp", "tp"),
            P("dp", "tp"),
            P("dp", "tp"),
            P("tp", "dp"),
            P("dp"),
            P("dp"),
            P("dp", None, None, "tp"),
            P("dp", "ctx", None),
            P("dp", "ctx", None),
            P("dp", "ctx"),
            P("dp", None),
            P("dp", "ctx", None),
        ),
        out_specs=(
            P("dp", "ctx", None),
            P("dp", "ctx", None),
            P(("dp", "ctx"), "tp"),
            P(("dp", "ctx"), "tp"),
            P(("dp", "ctx"), "tp"),
            P("tp", ("dp", "ctx")),
            P(("dp", "ctx")),
            P(("dp", "ctx")),
            P("dp", None, "ctx", "tp"),
        ),
        check_vma=False,
    )
```

```python
import functools

import jax
import jax.numpy as jnp
from jax import lax
from jax.experimental import pallas as pl
from jax.experimental.pallas import tpu as pltpu
from jax.sharding import PartitionSpec as P

HEAD_DIM = 64
PIC = 256
CAP = 144

EPSILON = 1e-06
THETA = 10000.0
NEG_FILL = -1e30


KEY_ROWS = 256
NT = (((1,), (1,)), ((), ()))
LIMIT = 67043328


def whole_vmem(count):
    return [pl.BlockSpec(memory_space=pltpu.VMEM)] * count


def picture_ids(starts_ref, places):
    ids = jnp.full(places.shape, -1, jnp.int32)
    for j in range(starts_ref.shape[1]):
        start = starts_ref[0, j]
        ids += jnp.where((places >= start) & (places < start + PIC), j + 1, 0)
    return ids


def as_column(row):
    tall = jnp.broadcast_to(row.astype(jnp.float32), (8, row.shape[1]))
    return jnp.transpose(tall)[:, 0:1].astype(jnp.int32)


class Masks:
    def __init__(self, docs_ref, starts_ref, column):
        self.docs_ref, self.starts_ref, self.column = docs_ref, starts_ref, column
        self.rows = docs_ref.shape[2]
        me = lax.axis_index("ctx")
        self.q_doc = docs_ref[me]
        self.q_place = me * self.rows + lax.broadcasted_iota(jnp.int32, (1, self.rows), 1)
        self.q_pic = picture_ids(starts_ref, self.q_place)

    def open(self, block):
        self.column[...] = jnp.broadcast_to(
            as_column(self.docs_ref[block]), self.column.shape
        )

    def bias(self, block, rows, first):
        k_doc = self.column[rows, 0:1]
        k_place = block * self.rows + first + lax.broadcasted_iota(jnp.int32, k_doc.shape, 0)
        k_pic = picture_ids(self.starts_ref, k_place)
        seen = (k_doc == self.q_doc) & (
            (k_place <= self.q_place) | ((k_pic == self.q_pic) & (self.q_pic >= 0))
        )
        return jnp.where(seen, 0.0, NEG_FILL)


def attend_block(masks, block, q_ref, kv_ref, acc, top, total):
    kv_width = kv_ref.shape[1] // 2
    heads, kv_heads = q_ref.shape[1] // HEAD_DIM, kv_width // HEAD_DIM
    masks.open(block)

    def step(j, carry):
        first = pl.multiple_of(j * KEY_ROWS, KEY_ROWS)
        rows = pl.ds(first, KEY_ROWS)
        bias = masks.bias(block, rows, first)
        for g in range(kv_heads):
            key = kv_ref[rows, g * HEAD_DIM : (g + 1) * HEAD_DIM]
            val = kv_ref[rows, kv_width + g * HEAD_DIM : kv_width + (g + 1) * HEAD_DIM]
            val_t = jnp.transpose(val.astype(jnp.float32)).astype(jnp.bfloat16)
            for h in range(g * heads // kv_heads, (g + 1) * heads // kv_heads):
                at = slice(h * HEAD_DIM, (h + 1) * HEAD_DIM)
                scores = bias + lax.dot_general(
                    key, q_ref[:, at], NT, preferred_element_type=jnp.float32
                )
                old = top[h : h + 1, :]
                new = jnp.maximum(old, jnp.max(scores, axis=0, keepdims=True))
                probs = jnp.exp(scores - new)
                fade = jnp.exp(old - new)
                total[h : h + 1, :] = total[h : h + 1, :] * fade + jnp.sum(
                    probs, axis=0, keepdims=True
                )
                acc[at, :] = acc[at, :] * fade + jnp.dot(
                    val_t, probs.astype(jnp.bfloat16), preferred_element_type=jnp.float32
                )
                top[h : h + 1, :] = new
        return carry

    lax.fori_loop(0, kv_ref.shape[0] // KEY_ROWS, step, 0)


def attend_back_block(
    masks, edges, block, q_ref, kv_ref, log_ref, delta, grad_ref, acc, dkv_ref
):
    kv_width = kv_ref.shape[1] // 2
    heads, kv_heads = q_ref.shape[1] // HEAD_DIM, kv_width // HEAD_DIM
    masks.open(block)
    count = kv_ref.shape[0] // KEY_ROWS
    me = lax.axis_index("ctx")
    q_first, q_last = edges[me * count, 0], edges[me * count + count - 1, 1]

    def step(j, carry):
        at = block * count + j
        same = (edges[at, 0] <= q_last) & (edges[at, 1] >= q_first)

        @pl.when(same)
        def _():
            inside(j)

        @pl.when(jnp.logical_not(same))
        def _():
            rows = pl.ds(pl.multiple_of(j * KEY_ROWS, KEY_ROWS), KEY_ROWS)
            dkv_ref[rows, :] = jnp.zeros((KEY_ROWS, dkv_ref.shape[1]), dkv_ref.dtype)

        return carry

    def inside(j):
        first = pl.multiple_of(j * KEY_ROWS, KEY_ROWS)
        rows = pl.ds(first, KEY_ROWS)
        bias = masks.bias(block, rows, first)
        for g in range(kv_heads):
            k_at = slice(g * HEAD_DIM, (g + 1) * HEAD_DIM)
            v_at = slice(kv_width + g * HEAD_DIM, kv_width + (g + 1) * HEAD_DIM)
            key, val = kv_ref[rows, k_at], kv_ref[rows, v_at]
            key_t = jnp.transpose(key.astype(jnp.float32)).astype(jnp.bfloat16)
            dk = jnp.zeros((KEY_ROWS, HEAD_DIM), jnp.float32)
            dv = jnp.zeros((KEY_ROWS, HEAD_DIM), jnp.float32)
            for h in range(g * heads // kv_heads, (g + 1) * heads // kv_heads):
                at = slice(h * HEAD_DIM, (h + 1) * HEAD_DIM)
                q_rows, g_rows = q_ref[:, at], grad_ref[:, at]
                scores = bias + lax.dot_general(
                    key, q_rows, NT, preferred_element_type=jnp.float32
                )
                probs = jnp.exp(scores - log_ref[h : h + 1, :])
                prob_grad = lax.dot_general(val, g_rows, NT, preferred_element_type=jnp.float32)
                slope = (probs * (prob_grad - delta[h : h + 1, :])).astype(jnp.bfloat16)
                dv += jnp.dot(
                    probs.astype(jnp.bfloat16), g_rows, preferred_element_type=jnp.float32
                )
                dk += jnp.dot(slope, q_rows, preferred_element_type=jnp.float32)
                acc[at, :] += jnp.dot(key_t, slope, preferred_element_type=jnp.float32)
            dkv_ref[rows, k_at] = dk.astype(dkv_ref.dtype)
            dkv_ref[rows, v_at] = dv.astype(dkv_ref.dtype)

    lax.fori_loop(0, count, step, 0)


def attend_back_kernel(
    back, ahead, starts_ref, edges, q_ref, kv_ref, docs_ref, log_ref, full_ref, grad_ref, dq_ref,
    dkv_ref, acc, delta, column,
):
    me, size = lax.axis_index("ctx"), lax.axis_size("ctx")
    acc[...] = jnp.transpose(full_ref[...] * grad_ref[...].astype(jnp.float32))
    for h in range(delta.shape[0]):
        delta[h : h + 1, :] = jnp.sum(
            acc[h * HEAD_DIM : (h + 1) * HEAD_DIM, :], axis=0, keepdims=True
        )
    acc[...] = jnp.zeros(acc.shape, jnp.float32)
    masks = Masks(docs_ref, starts_ref, column)

    def step(s, carry):
        block = me + ahead - s

        @pl.when((block >= 0) & (block < size))
        def _():
            attend_back_block(
                masks, edges, block, q_ref, kv_ref.at[block], log_ref, delta, grad_ref, acc,
                dkv_ref.at[block],
            )

        return carry

    lax.fori_loop(0, back + ahead + 1, step, 0)
    dq_ref[...] = jnp.transpose(acc[...]) * (HEAD_DIM**-0.5)


def attend_back(starts, q, kv, docs, log_total, full, grad, back, ahead):
    rows, width = q.shape
    by_block = docs.reshape(-1, KEY_ROWS)
    edges = jnp.concatenate([by_block[:, :1], by_block[:, -1:]], axis=1)
    return pl.pallas_call(
        functools.partial(attend_back_kernel, back, ahead),
        name="attend_back",
        in_specs=[pl.BlockSpec(memory_space=pltpu.SMEM)] * 2 + whole_vmem(6),
        out_specs=whole_vmem(2),
        out_shape=[
            jax.ShapeDtypeStruct((rows, width), jnp.float32),
            jax.ShapeDtypeStruct(kv.shape, jnp.bfloat16),
        ],
        scratch_shapes=[
            pltpu.VMEM((width, rows), jnp.float32),
            pltpu.VMEM((width // HEAD_DIM, rows), jnp.float32),
            pltpu.VMEM((rows, 8), jnp.int32),
        ],
        compiler_params=pltpu.CompilerParams(vmem_limit_bytes=LIMIT),
    )(starts, edges, q, kv, docs, log_total, full, grad)


MESH = pl.DeviceIdType.MESH


def greet(axes_list, line=False):
    barrier = pltpu.get_barrier_semaphore()
    count = 0
    for axis in axes_list:
        me, size = lax.axis_index(axis), lax.axis_size(axis)

        def signal(k, carry, axis=axis, me=me, size=size):
            pl.semaphore_signal(
                barrier, inc=1, device_id={axis: lax.rem(me + k, size)}, device_id_type=MESH
            )
            return carry

        lax.fori_loop(1, size, signal, 0)
        count += size - 1
    if not line:
        pl.semaphore_wait(barrier, count)
        return
    me, size = lax.axis_index("ctx"), lax.axis_size("ctx")
    for step in (1, -1):
        other = me + step

        @pl.when((other >= 0) & (other < size))
        def _(other=other):
            pl.semaphore_signal(barrier, inc=1, device_id={"ctx": other}, device_id_type=MESH)

    inner = (me > 0) & (me < size - 1)

    @pl.when(inner)
    def _():
        pl.semaphore_wait(barrier, count + 2)

    @pl.when(jnp.logical_not(inner))
    def _():
        pl.semaphore_wait(barrier, count + 1)


def remote(src, dst, sems, k, device_id):
    return pltpu.make_async_remote_copy(
        src_ref=src,
        dst_ref=dst,
        send_sem=sems[0].at[k],
        recv_sem=sems[1].at[k],
        device_id=device_id,
        device_id_type=MESH,
    )


def other_core():
    return {"tp": 1 - lax.axis_index("tp")}


def ahead_on(axis, k):
    return lax.rem(lax.axis_index(axis) + k, lax.axis_size(axis))


def each(count, do, first=1):
    def step(k, carry):
        do(k)
        return carry

    lax.fori_loop(first, count, step, 0)


def sem_pair(count):
    return [pltpu.SemaphoreType.DMA((count,)), pltpu.SemaphoreType.DMA((count,))]


def remote_params(ident):
    return pltpu.CompilerParams(
        collective_id=ident, has_side_effects=True, vmem_limit_bytes=LIMIT
    )


def halves(rows):
    half = rows // 2
    core = lax.axis_index("tp")
    return (
        pl.ds(pl.multiple_of(core * half, half), half),
        pl.ds(pl.multiple_of((1 - core) * half, half), half),
    )


def turn(tile, cosine, sine):
    lane = lax.broadcasted_iota(jnp.int32, tile.shape, 1)
    half = HEAD_DIM // 2
    swapped = jnp.where(
        lax.rem(lane, HEAD_DIM) < half,
        pltpu.roll(tile, 2 * HEAD_DIM - half, 1),
        pltpu.roll(tile, half, 1),
    )
    return tile * cosine + swapped * sine


def block_tables(cos_ref, sin_ref, rows, block):
    start = pl.ds(rows + block, 1)
    in_cos, in_sin = cos_ref[:rows, :], sin_ref[:rows, :]
    at_cos, at_sin = cos_ref[start, :], sin_ref[start, :]
    return in_cos * at_cos - in_sin * at_sin, in_sin * at_cos + in_cos * at_sin


def row_scale(x):
    return lax.rsqrt(jnp.mean(x * x, axis=-1, keepdims=True) + EPSILON)


def norm_back(x, gain, grad):
    scale = row_scale(x)
    unit = x * scale
    pull = grad * gain
    return (
        scale * (pull - unit * jnp.mean(pull * unit, axis=-1, keepdims=True)),
        jnp.sum(grad * unit, axis=0, keepdims=True),
    )


def back_blocks(ctx_size, block_len, length):
    return min(ctx_size - 1, -(-(length // 2 - 1) // block_len))


def ahead_blocks(block_len, length, spans):
    return 0 if block_len % (length // spans) == 0 else 1


def grid_peers():
    me = lax.axis_index("dp")
    x, y = lax.rem(me, 2), lax.div(me, 2)
    return y * 2 + 1 - x, (1 - y) * 2 + x, 3 - me


class Gather:
    def __init__(self, target, sems, rows=None, source=None):
        self.target, self.sems, self.rows, self.source = target, sems, rows, source
        self.size = lax.axis_size("dp")
        self.grid = self.size == 4

    def at(self, place):
        return self.target.at[place] if self.rows is None else self.target.at[place, self.rows]

    def half(self, place, n):
        if self.rows is None:
            count = self.target.shape[1] // 2
            return self.target.at[place, pl.ds(n * count, count)]
        count = self.rows.size // 2
        first = pl.multiple_of(self.rows.start + n * count, count)
        return self.target.at[place, pl.ds(first, count)]

    def first(self, k, peer):
        place = self.at(lax.axis_index("dp"))
        source = place if self.source is None else self.source.at[self.rows]
        return remote(source, place, self.sems, k, {"dp": peer})

    def passed(self, k, place, n, peer):
        at = self.half(place, n)
        return remote(at, at, self.sems, k, {"dp": peer})

    def direct(self, k):
        return self.first(k, ahead_on("dp", k))

    def start(self):
        if not self.grid:
            each(self.size, lambda k: self.direct(k).start())
            return
        x, y, _ = grid_peers()
        self.first(0, x).start()
        self.first(1, y).start()

    def forward(self, came=None):
        if not self.grid:
            return
        x, y, _ = grid_peers()
        self.first(0, x).wait_recv()
        self.passed(2, x, 0, y).start()
        if came:
            came(0, self.at(x))
        self.first(1, y).wait_recv()
        self.passed(3, y, 1, x).start()
        if came:
            came(1, self.at(y))

    def arrive(self, came=None):
        if not self.grid:

            def one(k):
                self.direct(k).wait_recv()
                if came:
                    came(k, self.at(ahead_on("dp", self.size - k)))

            each(self.size, one)
            return
        x, _, diagonal = grid_peers()
        for n in range(2):
            self.passed(2 + n, diagonal, n, x).wait_recv()
            if came:
                came(2 + n, self.half(diagonal, n))

    def finish(self):
        if not self.grid:
            each(self.size, lambda k: self.direct(k).wait_send())
            return
        x, y, _ = grid_peers()
        self.first(0, x).wait_send()
        self.first(1, y).wait_send()
        self.passed(2, x, 0, y).wait_send()
        self.passed(3, y, 1, x).wait_send()


class RowGather:
    def __init__(self, source, target, dp_sems, tp_sems, first):
        mine, _ = halves(source.shape[0])
        self.gather = Gather(target, dp_sems, mine, source)
        self.tp_sems, self.after = tp_sems, first

    def relay(self, k, at):
        return remote(at, at, self.tp_sems, self.after + k, other_core())

    def came(self, k, at):
        self.relay(k, at).start()

    def start(self):
        self.gather.start()

    def forward(self):
        self.gather.forward(self.came)

    def arrive(self):
        self.gather.arrive(self.came)

    def finish(self):
        self.gather.finish()
        gather = self.gather
        if not gather.grid:
            each(
                gather.size,
                lambda k: self.relay(k, gather.at(ahead_on("dp", gather.size - k))).wait(),
            )
            return
        x, y, diagonal = grid_peers()
        self.relay(0, gather.at(x)).wait()
        self.relay(1, gather.at(y)).wait()
        self.relay(2, gather.half(diagonal, 0)).wait()
        self.relay(3, gather.half(diagonal, 1)).wait()


def collect(places_ref, slots_ref, group):
    tok_rows, slot_count = places_ref.shape[1], slots_ref.shape[1]
    tiles = []
    for first in range(0, slot_count, 128):
        wide = min(128, slot_count - first)
        lane = first + lax.broadcasted_iota(jnp.int32, (tok_rows, wide), 1)
        hit = None
        for n in range(first // CAP, (first + wide - 1) // CAP + 1):
            one = places_ref[group, :, n : n + 1] == lane - n * CAP
            hit = one if hit is None else hit | one
        tiles.append(hit.astype(jnp.float32).astype(jnp.bfloat16))
    return jnp.dot(
        jnp.concatenate(tiles, axis=1), slots_ref[group], preferred_element_type=jnp.float32
    )


class GridSum:
    def __init__(self, piece, landed, sems):
        self.piece, self.landed, self.sems = piece, landed, sems
        self.x, self.y, _ = grid_peers()
        self.count = landed.shape[1] // 2

    def half(self, n, which):
        return self.piece(n).at[pl.ds(which * self.count, self.count)]

    def slot(self, j):
        return self.landed.at[j // 2, pl.ds(j % 2 * self.count, self.count)]

    def copy(self, j):
        n, which, peer = (
            (1, 0, self.x),
            (3, 0, self.x),
            (2, 1, self.y),
            (3, 1, self.y),
            (2, 0, self.y),
            (1, 1, self.x),
        )[j]
        return remote(self.half(n, which), self.slot(j), self.sems, j, {"dp": peer})

    def start(self):
        for j in (1, 3, 0, 2):
            self.copy(j).start()

    def forward(self):
        for j, n, which in ((1, 2, 0), (3, 1, 1)):
            self.copy(j).wait_recv()
            half = self.half(n, which)
            half[...] = (
                half[...].astype(jnp.float32) + self.slot(j)[...].astype(jnp.float32)
            ).astype(jnp.bfloat16)
            self.copy(4 + j // 2).start()

    def add_to(self, total):
        for which, slots in ((0, (0, 4)), (1, (2, 5))):
            at = pl.ds(which * self.count, self.count)
            for j in slots:
                self.copy(j).wait_recv()
                total[at, :] += self.slot(j)[...].astype(jnp.float32)

    def finish(self):
        for j in range(6):
            self.copy(j).wait_send()


class RowReturn:
    def __init__(self, part, held, landed, total, sent, came, dp_sems, tp_sems):
        self.part, self.held, self.landed, self.total = part, held, landed, total
        self.sent, self.came, self.dp_sems, self.tp_sems = sent, came, dp_sems, tp_sems
        self.size = lax.axis_size("dp")
        self.mine, self.theirs = halves(part.shape[1])
        self.grid = self.size == 4
        if self.grid:
            self.sum = GridSum(lambda n: held.at[n], landed, dp_sems)

    def group(self, k):
        if not self.grid:
            return ahead_on("dp", k)
        me = lax.axis_index("dp")
        x, y = lax.rem(me, 2), lax.div(me, 2)
        flip_x, flip_y = lax.rem(k, 2), lax.div(k, 2)
        return lax.rem(y + flip_y, 2) * 2 + lax.rem(x + flip_x, 2)

    def swap(self, k):
        return remote(
            self.part.at[self.group(k), self.theirs], self.held.at[k], self.tp_sems, k,
            other_core(),
        )

    def copy(self, k):
        return remote(
            self.held.at[k], self.landed.at[k - 1], self.dp_sems, k, {"dp": ahead_on("dp", k)}
        )

    def last(self):
        return remote(self.sent, self.came, self.tp_sems, self.size, other_core())

    def both(self, k):
        return self.part[self.group(k), self.mine].astype(jnp.float32) + self.held[k].astype(
            jnp.float32
        )

    def load(self, slots_in, slots_ref, sems, k):
        group = self.group(k)
        return pltpu.make_async_copy(slots_in.at[group], slots_ref.at[group], sems.at[k])

    def fetch(self, *slots):
        each(self.size + 1, lambda k: self.load(*slots, lax.rem(k, self.size)).start())

    def start(self, places_ref, *slots):
        slots_ref = slots[1]

        def one(k):
            k = lax.rem(k, self.size)
            group = self.group(k)
            self.load(*slots, k).wait()
            self.part[group] = collect(places_ref, slots_ref, group).astype(jnp.bfloat16)
            self.swap(k).start()

        each(self.size + 1, one)

    def forward(self):
        def one(k):
            self.swap(k).wait_recv()
            self.held[k] = self.both(k).astype(jnp.bfloat16)
            if not self.grid:
                self.copy(k).start()

        each(self.size, one)
        if self.grid:
            self.sum.start()
        self.swap(0).wait()
        self.total[...] = self.both(0)

    def pass_on(self):
        if self.grid:
            self.sum.forward()

    def gather(self):
        def one(k):
            self.copy(k).wait_recv()
            self.total[...] += self.landed[k - 1].astype(jnp.float32)

        if self.grid:
            self.sum.add_to(self.total)
        else:
            each(self.size, one)
        self.sent[...] = self.total[...].astype(jnp.bfloat16)
        self.last().start()

    def finish(self):
        def one(k):
            self.swap(k).wait_send()
            if not self.grid:
                self.copy(k).wait_send()

        each(self.size, one)
        if self.grid:
            self.sum.finish()
        self.last().wait()


def return_scratch(size, rows, width):
    low = jnp.bfloat16
    return [
        pltpu.VMEM((size, rows, width), low),
        pltpu.VMEM((size, rows // 2, width), low),
        pltpu.VMEM((size - 1, rows // 2, width), low),
        pltpu.VMEM((rows // 2, width), jnp.float32),
        pltpu.VMEM((rows // 2, width), low),
        pltpu.VMEM((rows // 2, width), low),
        *sem_pair(max(size, 6)),
        *sem_pair(size + 1),
    ]


def return_grads_kernel(
    slots_in, places_ref, hidden_ref, cot_ref, gain_ref, out_w_ref, grad_ref, low_ref, mix_ref,
    gain_grad_ref, slots_ref, slot_sems, part, held, landed, total, sent, came, dp_send, dp_recv, tp_send, tp_recv,
):
    rows = RowReturn(
        part, held, landed, total, sent, came, (dp_send, dp_recv), (tp_send, tp_recv)
    )
    slots = (slots_in, slots_ref, slot_sems)
    rows.fetch(*slots)
    greet(["dp", "tp"])
    rows.start(places_ref, *slots)
    rows.forward()
    rows.pass_on()
    rows.gather()

    def turn_back(at, grads):
        x_grad, gain_grad = norm_back(
            hidden_ref[at, :], gain_ref[1:2, :], grads.astype(jnp.float32)
        )
        hidden_grad = cot_ref[at, :].astype(jnp.float32) + x_grad
        grad_ref[at, :] = hidden_grad
        low_ref[at, :] = hidden_grad.astype(jnp.bfloat16)
        piece = out_w_ref.shape[2]
        mix = None
        for i in range(out_w_ref.shape[0]):
            one = lax.dot_general(
                low_ref[at, i * piece : (i + 1) * piece],
                out_w_ref[i],
                NT,
                preferred_element_type=jnp.float32,
            )
            mix = one if mix is None else mix + one
        mix_ref[at, :] = mix.astype(jnp.bfloat16)
        return gain_grad

    gain_mine = turn_back(rows.mine, sent[...])
    rows.finish()
    gain_theirs = turn_back(rows.theirs, came[...])
    gain_grad_ref[...] = gain_mine + gain_theirs


def return_grads(slots, places, hidden, cot, gain, out_w, ident):
    size, (rows, width) = slots.shape[0], hidden.shape
    return pl.pallas_call(
        return_grads_kernel,
        name="return_grads",
        in_specs=[pl.BlockSpec(memory_space=pl.ANY)] + whole_vmem(5),
        out_specs=whole_vmem(4),
        out_shape=[
            jax.ShapeDtypeStruct((rows, width), jnp.float32),
            jax.ShapeDtypeStruct((rows, width), jnp.bfloat16),
            jax.ShapeDtypeStruct((rows, out_w.shape[1]), jnp.bfloat16),
            jax.ShapeDtypeStruct((1, width), jnp.float32),
        ],
        scratch_shapes=[
            pltpu.VMEM(slots.shape, slots.dtype),
            pltpu.SemaphoreType.DMA((size,)),
            *return_scratch(size, rows, width),
        ],
        compiler_params=remote_params(ident),
    )(slots, places, hidden, cot, gain, out_w)


def trade_kernel(
    back, ahead, early, kv_grad_ref, slots_in, places_ref, low_ref, mix_ref, *refs
):
    if early:
        dq_ref, cos_ref, sin_ref, normed_ref, *refs = refs
        kv_ref, out_ref, sums_ref, joined_ref, turned_ref, *refs = refs
        pieces, pieces_landed, whole, sum_send, sum_recv, *refs = refs
    else:
        kv_ref, out_ref, out_w_ref, *refs = refs
    slots_ref, slot_sems, going, came_kv, line_send, line_recv, part, held, landed, total, *refs = refs
    sent, came, dp_send, dp_recv, tp_send, tp_recv = refs
    me, size = lax.axis_index("ctx"), lax.axis_size("ctx")
    rows = RowReturn(
        part, held, landed, total, sent, came, (dp_send, dp_recv), (tp_send, tp_recv)
    )
    slots = (slots_in, slots_ref, slot_sems)
    rows.fetch(*slots)
    greet(["dp", "tp"], line=True)
    right, left = me + 1, me - 1
    sems = (line_send, line_recv)

    def hop(s, src):
        return remote(src, came_kv.at[s], sems, s, {"ctx": left})

    def forth():
        return remote(
            kv_grad_ref.at[lax.rem(me + 1, size)], came_kv.at[0], sems, 0, {"ctx": right}
        )

    def own_piece(s):
        return kv_grad_ref.at[lax.rem(me + size - s, size)]

    if ahead:

        @pl.when(right < size)
        def _():
            forth().start()

    @pl.when(me - back >= 0)
    def _():
        hop(back, own_piece(back)).start()

    rows.start(places_ref, *slots)
    rows.forward()
    turned = jnp.transpose(low_ref[...].astype(jnp.float32)).astype(jnp.bfloat16)
    grad = jnp.dot(turned, mix_ref[...], preferred_element_type=jnp.float32)
    if early:
        piece, q_width = pieces.shape[1], dq_ref.shape[1]
        for i in range(pieces.shape[0]):
            pieces[i, :, q_width:] = grad[i * piece : (i + 1) * piece].astype(jnp.bfloat16)
        wide = 2 * HEAD_DIM
        cosine, sine = block_tables(cos_ref, sin_ref, dq_ref.shape[0], me)
        for first in range(0, q_width, wide):
            joined_ref[:, first : first + wide] = turn(
                dq_ref[:, first : first + wide], cosine, sine
            ).astype(jnp.bfloat16)
        turned_ref[...] = jnp.transpose(normed_ref[...].astype(jnp.float32)).astype(jnp.bfloat16)
        rows.pass_on()
        for i in range(pieces.shape[0]):
            pieces[i, :, :q_width] = jnp.dot(
                turned_ref[i * piece : (i + 1) * piece, :], joined_ref[...],
                preferred_element_type=jnp.float32,
            ).astype(jnp.bfloat16)
        sums = GridPieceSum(pieces, pieces_landed, (sum_send, sum_recv), whole)
        sums.start()
    else:
        piece = out_w_ref.shape[1]
        for i in range(out_w_ref.shape[0]):
            out_w_ref[i] = grad[i * piece : (i + 1) * piece].astype(jnp.bfloat16)
        rows.pass_on()

    for s in range(back - 1, 0, -1):

        @pl.when((me - s >= 0) & (right < size))
        def _(s=s):
            hop(s + 1, going.at[s]).wait_recv()
            going[s] = (
                own_piece(s)[...].astype(jnp.float32) + came_kv[s + 1].astype(jnp.float32)
            ).astype(going.dtype)
            hop(s, going.at[s]).start()

        @pl.when((me - s >= 0) & (right >= size))
        def _(s=s):
            hop(s, own_piece(s)).start()

    rows.gather()
    if early:
        sums.forward()
    kv_ref[...] = kv_grad_ref[me].astype(jnp.float32)

    @pl.when(right < size)
    def _():
        hop(1, going.at[0]).wait_recv()
        kv_ref[...] += came_kv[1].astype(jnp.float32)

    if ahead:

        @pl.when(left >= 0)
        def _():
            forth().wait_recv()
            kv_ref[...] += came_kv[0].astype(jnp.float32)

        @pl.when(right < size)
        def _():
            forth().wait_send()

    for s in range(back, 0, -1):

        @pl.when(me - s >= 0)
        def _(s=s):
            hop(s, going.at[0]).wait_send()

    if early:
        sums_ref[...] = sums.total().astype(jnp.bfloat16)
        sums.finish()
    rows.finish()
    out_ref[rows.mine, :] = sent[...]
    out_ref[rows.theirs, :] = came[...]


def trade(kv_grad, slots, places, low, mix, dq, cosine, sine, normed, back, ahead, ident):
    size, (rows, width) = slots.shape[0], low.shape
    kv_shape, out_cols, q_width = kv_grad.shape[1:], mix.shape[1], dq.shape[1]
    going = pltpu.VMEM((max(back, 1),) + kv_shape, kv_grad.dtype)
    came = pltpu.VMEM((back + 1,) + kv_shape, kv_grad.dtype)
    early, piece = size == 4, width // size
    few = jnp.bfloat16
    more_in, more_out, more_scratch = [], [], []
    if early:
        more_in = [dq, cosine, sine, normed]
        more_out = [
            jax.ShapeDtypeStruct((piece, q_width + out_cols), few),
            jax.ShapeDtypeStruct(dq.shape, few),
            jax.ShapeDtypeStruct((width, rows), few),
        ]
        more_scratch = [
            pltpu.VMEM((size, piece, q_width + out_cols), few),
            pltpu.VMEM((size - 1, piece, q_width + out_cols), few),
            pltpu.VMEM((piece, q_width + out_cols), jnp.float32),
            *sem_pair(6),
        ]
    else:
        more_out = [jax.ShapeDtypeStruct((size, piece, out_cols), few)]
    return pl.pallas_call(
        functools.partial(trade_kernel, back, ahead, early),
        name="trade",
        in_specs=whole_vmem(1)
        + [pl.BlockSpec(memory_space=pl.ANY)]
        + whole_vmem(3 + len(more_in)),
        out_specs=whole_vmem(2 + len(more_out)),
        out_shape=[
            jax.ShapeDtypeStruct(kv_shape, jnp.float32),
            jax.ShapeDtypeStruct((rows, width), few),
        ]
        + more_out,
        scratch_shapes=more_scratch
        + [pltpu.VMEM(slots.shape, slots.dtype), pltpu.SemaphoreType.DMA((size,))]
        + [going, came, *sem_pair(back + 1), *return_scratch(size, rows, width)],
        compiler_params=remote_params(ident),
    )(kv_grad, slots, places, low, mix, *more_in)


class PieceSum:
    def __init__(self, axis, source, landed, sems):
        self.axis, self.source, self.landed, self.sems = axis, source, landed, sems
        self.size = lax.axis_size(axis)

    def copy(self, k):
        peer = ahead_on(self.axis, k)
        return remote(
            self.source.at[peer], self.landed.at[k], self.sems, k, {self.axis: peer}
        )

    def send(self, k):
        self.copy(k).start()

    def start(self):
        each(self.size, self.send)

    def forward(self):
        pass

    def total(self):
        each(self.size, lambda k: self.copy(k).wait_recv())
        whole = self.source[lax.axis_index(self.axis)].astype(jnp.float32)
        for k in range(1, self.size):
            whole += self.landed[k].astype(jnp.float32)
        return whole

    def finish(self):
        each(self.size, lambda k: self.copy(k).wait_send())


class GridPieceSum:
    def __init__(self, source, landed, sems, whole):
        x, y, diagonal = grid_peers()
        places = (lax.axis_index("dp"), x, y, diagonal)
        self.source, self.whole = source, whole
        self.sum = GridSum(lambda n: source.at[places[n]], landed, sems)
        self.start, self.forward, self.finish = self.sum.start, self.sum.forward, self.sum.finish

    def total(self):
        self.whole[...] = self.source[lax.axis_index("dp")].astype(jnp.float32)
        self.sum.add_to(self.whole)
        return self.whole[...]


def dp_sum(source, landed, sems, whole):
    if lax.axis_size("dp") == 4:
        return GridPieceSum(source, landed, sems, whole)
    return PieceSum("dp", source, landed, sems)


class WholeSum:
    def __init__(self, axis, source, landed, sems):
        self.axis, self.source, self.landed, self.sems = axis, source, landed, sems
        self.size = lax.axis_size(axis)

    def copy(self, k):
        return remote(
            self.source, self.landed.at[k], self.sems, k, {self.axis: ahead_on(self.axis, k)}
        )

    def start(self):
        each(self.size, lambda k: self.copy(k).start())

    def total(self):
        each(self.size, lambda k: self.copy(k).wait())
        whole = self.source[...]
        for k in range(1, self.size):
            whole += self.landed[k]
        return whole


def finish_kernel(early, dkv_ref, cos_ref, sin_ref, w_ref, x_ref, gain_ref, gain_two_ref, *refs):
    if early:
        sums_ref, joined_q_ref, turned, *refs = refs
    else:
        dq_ref, normed_ref, out_w_ref, *refs = refs
    in_ref, own_ref, gains_ref, joined, part, held, pieces, landed, whole, *refs = refs
    low, low_landed, gain_rows, gain_landed, gain_more, gain_more_landed, *refs = refs
    if not early:
        turned, out_landed, *refs = refs
    greet(["dp", "ctx", "tp"])
    pairs = [refs[2 * i : 2 * i + 2] for i in range(len(refs) // 2)]
    wide = 2 * HEAD_DIM
    kv_width = dkv_ref.shape[1] // 2
    q_width = joined.shape[1] - 2 * kv_width
    cosine, sine = block_tables(cos_ref, sin_ref, dkv_ref.shape[0], lax.axis_index("ctx"))
    if early:
        joined[:, :q_width] = joined_q_ref[...]
        done = q_width
    else:
        out_sum = PieceSum("dp", out_w_ref, out_landed, pairs[5])
        out_sum.start()
        done = 0
        for first in range(0, q_width, wide):
            joined[:, first : first + wide] = turn(
                dq_ref[:, first : first + wide], cosine, sine
            ).astype(jnp.bfloat16)
        turned[...] = jnp.transpose(normed_ref[...].astype(jnp.float32)).astype(jnp.bfloat16)
    for first in range(0, kv_width, wide):
        joined[:, q_width + first : q_width + first + wide] = turn(
            dkv_ref[:, first : first + wide], cosine, sine
        ).astype(jnp.bfloat16)
    joined[:, q_width + kv_width :] = dkv_ref[:, kv_width:].astype(jnp.bfloat16)

    w_sum = dp_sum(pieces, landed, pairs[0], whole)
    rows = pieces.shape[1]

    def piece(k):
        peer = ahead_on("dp", k)
        at = pl.ds(pl.multiple_of(peer * rows, rows), rows)
        pieces[peer] = jnp.dot(
            turned[at, :], joined[:, done:], preferred_element_type=jnp.float32
        ).astype(jnp.bfloat16)

    each(pieces.shape[0], piece)
    w_sum.start()
    for i in range(w_ref.shape[0]):
        part[:, i * rows : (i + 1) * rows] = lax.dot_general(
            joined[...], w_ref[i], NT, preferred_element_type=jnp.float32
        ).astype(jnp.bfloat16)
    swap = remote(part, held, pairs[1], 0, other_core())
    swap.start()
    piece(0)
    swap.wait()
    x_grad, gain_grad = norm_back(
        x_ref[...].astype(jnp.float32),
        gain_ref[0:1, :],
        part[...].astype(jnp.float32) + held[...].astype(jnp.float32),
    )
    in_ref[...] = x_grad
    gain_rows[...] = jnp.zeros(gain_rows.shape, jnp.float32)
    gain_rows[0:1, :] = gain_grad
    gain_rows[1:2, :] = gain_two_ref[...]
    gain_sum = WholeSum("dp", gain_rows, gain_landed, pairs[2])
    gain_sum.start()
    w_sum.forward()

    cols, few = joined.shape[1], low.shape[1]
    w_total = w_sum.total()
    if not early:
        out_total = out_sum.total()
    for c in range(low.shape[0]):
        at = slice(c * few, (c + 1) * few)
        low[c, :, done:cols] = w_total[at].astype(jnp.bfloat16)
        if early:
            low[c, :, :done] = sums_ref[at, :done]
            low[c, :, cols:] = sums_ref[at, done:]
        else:
            low[c, :, cols:] = out_total[at].astype(jnp.bfloat16)
    low_sum = PieceSum("ctx", low, low_landed, pairs[3])
    low_sum.start()
    gain_more[...] = gain_sum.total()
    more_sum = WholeSum("ctx", gain_more, gain_more_landed, pairs[4])
    more_sum.start()
    w_sum.finish()
    if not early:
        out_sum.finish()
    own_ref[...] = low_sum.total()
    low_sum.finish()
    gains_ref[...] = more_sum.total()


def finish(dkv, cosine, sine, w, x, gain, gain_two, given, out_cols, ident):
    rows, width = x.shape
    dp_size, ctx_size = lax.axis_size("dp"), lax.axis_size("ctx")
    early, cols = dp_size == 4, w.shape[2]
    piece = width // dp_size
    few = piece // ctx_size
    mine = dkv.shape[1] if early else cols
    low, high = jnp.bfloat16, jnp.float32
    more_scratch = [] if early else [
        pltpu.VMEM((width, rows), low),
        pltpu.VMEM((dp_size, piece, out_cols), low),
    ]
    return pl.pallas_call(
        functools.partial(finish_kernel, early),
        name="finish",
        in_specs=whole_vmem(7 + len(given)),
        out_specs=whole_vmem(3),
        out_shape=[
            jax.ShapeDtypeStruct((rows, width), high),
            jax.ShapeDtypeStruct((few, cols + out_cols), high),
            jax.ShapeDtypeStruct((8, width), high),
        ],
        scratch_shapes=[
            pltpu.VMEM((rows, cols), low),
            pltpu.VMEM((rows, width), low),
            pltpu.VMEM((rows, width), low),
            pltpu.VMEM((dp_size, piece, mine), low),
            pltpu.VMEM((dp_size, piece, mine), low),
            pltpu.VMEM((piece, mine), high),
            pltpu.VMEM((ctx_size, few, cols + out_cols), low),
            pltpu.VMEM((ctx_size, few, cols + out_cols), low),
            pltpu.VMEM((8, width), high),
            pltpu.VMEM((dp_size, 8, width), high),
            pltpu.VMEM((8, width), high),
            pltpu.VMEM((ctx_size, 8, width), high),
            *more_scratch,
            *sem_pair(max(dp_size, 6)),
            *sem_pair(1),
            *sem_pair(dp_size),
            *sem_pair(ctx_size),
            *sem_pair(ctx_size),
            *(() if early else sem_pair(dp_size)),
        ],
        compiler_params=remote_params(ident),
    )(dkv, cosine, sine, w, x, gain, gain_two, *given)


class Everyone:
    def __init__(self, axis, target, sems):
        self.axis, self.target, self.sems = axis, target, sems
        self.size = lax.axis_size(axis)

    def copy(self, k):
        at = self.target.at[lax.axis_index(self.axis)]
        return remote(at, at, self.sems, k, {self.axis: ahead_on(self.axis, k)})

    def start(self):
        each(self.size, lambda k: self.copy(k).start())

    def arrive(self):
        each(self.size, lambda k: self.copy(k).wait_recv())

    def finish(self):
        each(self.size, lambda k: self.copy(k).wait_send())


def find_places(first, own, routes_ref, gates_ref, earlier, place_ref, gate_ref, column_ref):
    _, tokens = routes_ref.shape[1:]

    def group(g, carry):
        routes, gates = routes_ref[g], gates_ref[g]
        names, values = [], []
        for e in range(own):
            named = routes == first + e
            names.append(jnp.max(named.astype(jnp.float32), axis=0, keepdims=True))
            values.append(jnp.sum(jnp.where(named, gates, 0.0), axis=0, keepdims=True))
        spare = jnp.zeros((8 - own % 8 if own % 8 else 0, tokens), jnp.float32)
        names = jnp.concatenate(names + ([spare] if spare.shape[0] else []), axis=0)
        place = jnp.dot(
            names.astype(jnp.bfloat16), earlier[...], preferred_element_type=jnp.float32
        )
        place = jnp.where((names > 0.0) & (place < CAP), place, -float(CAP * own))
        for e in range(own):
            place_ref[g, e] = place[e : e + 1].astype(jnp.int32)
            gate_ref[g, e] = values[e]
        column_ref[g] = jnp.transpose(place)[:, :own].astype(jnp.int32)
        return carry

    lax.fori_loop(0, routes_ref.shape[0], group, 0)


class LineRows:
    def __init__(self, x_ref, x_all, back, ahead, line_sems, tp_sems):
        self.x_ref, self.x_all, self.back, self.ahead = x_ref, x_all, back, ahead
        self.line_sems, self.tp_sems = line_sems, tp_sems
        self.me, self.size = lax.axis_index("ctx"), lax.axis_size("ctx")
        self.mine, _ = halves(x_ref.shape[0])

    def block(self, s):
        return lax.rem(self.me + self.size - s, self.size)

    def sends(self, s):
        return (self.me + 1 < self.size) & (self.me - s >= 0)

    def hop(self, s):
        at = self.x_all.at[self.block(s), self.mine]
        source = self.x_ref.at[self.mine] if isinstance(s, int) and s == 0 else at
        return remote(source, at, self.line_sems, s, {"ctx": self.me + 1})

    def back_hop(self):
        at = self.x_all.at[self.me, self.mine]
        return remote(
            self.x_ref.at[self.mine], at, self.line_sems, self.back, {"ctx": self.me - 1}
        )

    def relay(self, k, block):
        at = self.x_all.at[block, self.mine]
        return remote(at, at, self.tp_sems, k, other_core())

    def start(self):
        if self.back:
            pl.when(self.sends(0))(lambda: self.hop(0).start())
        if self.ahead:
            pl.when(self.me >= 1)(lambda: self.back_hop().start())

    def step(self, s):
        @pl.when(self.me - s - 1 >= 0)
        def _():
            self.hop(s).wait_recv()
            self.relay(s, self.block(s + 1)).start()

        if s + 1 < self.back:
            pl.when(self.sends(s + 1))(lambda: self.hop(s + 1).start())

    def step_back(self):
        if self.ahead:

            @pl.when(self.me + 1 < self.size)
            def _():
                self.back_hop().wait_recv()
                self.relay(self.back, self.block(self.size - 1)).start()

    def finish(self):
        for s in range(self.back):
            pl.when(self.sends(s))(lambda s=s: self.hop(s).wait_send())
        if self.ahead:
            pl.when(self.me >= 1)(lambda: self.back_hop().wait_send())


def front_kernel(
    back, ahead, own, starts_ref, x_ref, cot_ref, q_w_ref, k_w_ref, v_w_ref, out_w_ref, gains_ref,
    docs_ref, routes_ref, gates_ref, cos_ref, sin_ref, w_out, out_w_out, gain_rows, docs_all,
    normed_out, q_ref, kv_out, mix_ref, full_out, log_ref, hidden_out, rows_out, cot_out,
    place_ref, gate_ref, column_ref, w_all, out_w_all, normed, kv_all, full, hidden, x_all,
    gains_all, routes_all, gates_all, acc, top, total, column, part, held,
    normed_two, *sems,
):
    me, size = lax.axis_index("ctx"), lax.axis_size("ctx")
    dp = lax.axis_index("dp")
    local = sems[-1]
    pairs = [sems[2 * i : 2 * i + 2] for i in range(len(sems) // 2)]
    q_width, kv_width = q_w_ref.shape[1], k_w_ref.shape[1]
    dp_size, piece = w_all.shape[:2]
    block_rows = x_ref.shape[0]

    def flush(i, source, target):
        return pltpu.make_async_copy(source, target, local.at[i])

    w_all[dp, :, :q_width] = q_w_ref[...]
    w_all[dp, :, q_width : q_width + kv_width] = k_w_ref[...]
    w_all[dp, :, q_width + kv_width :] = v_w_ref[...]
    gains_all[dp] = gains_ref[...]
    docs_all[me] = docs_ref[...]
    routes_all[dp] = routes_ref[...]
    gates_all[dp] = gates_ref[...]
    greet(["dp", "ctx", "tp"])
    weights = Gather(w_all, pairs[1])
    gains = Everyone("dp", gains_all, pairs[0])
    docs = Everyone("ctx", docs_all, pairs[2])
    routes = Everyone("dp", routes_all, pairs[3])
    gates = Everyone("dp", gates_all, pairs[4])
    out_w = Gather(out_w_all, pairs[5])
    line = LineRows(x_ref, x_all, back, ahead, pairs[8], pairs[11])
    for one in (gains, weights, line, docs, routes, gates):
        one.start()

    out_w_all[dp] = out_w_ref[...]
    x_all[me] = x_ref[...]
    token = lax.broadcasted_iota(jnp.int32, (block_rows, block_rows), 0)
    later = lax.broadcasted_iota(jnp.int32, (block_rows, block_rows), 1)
    normed_two[:, :block_rows] = (token < later).astype(jnp.float32).astype(jnp.bfloat16)
    top[...] = jnp.full(top.shape, NEG_FILL, jnp.float32)
    total[...] = jnp.zeros(total.shape, jnp.float32)
    acc[...] = jnp.zeros(acc.shape, jnp.float32)
    gains.arrive()
    for i in range(dp_size):
        gain_rows[:, i * piece : (i + 1) * piece] = gains_all[i]

    def norm_rows(source):
        x = source.astype(jnp.float32)
        return (x * row_scale(x) * gain_rows[0:1, :]).astype(jnp.bfloat16)

    normed[...] = norm_rows(x_ref[...])
    flush(0, normed, normed_out).start()
    routes.arrive()
    gates.arrive()
    docs.arrive()
    if back:
        line.step(0)
    weights.forward()
    find_places(
        dp * own, own, routes_all, gates_all, normed_two.at[:, :block_rows], place_ref, gate_ref,
        column_ref,
    )
    weights.arrive()
    flush(1, w_all, w_out).start()
    out_w.start()
    cot_rows = RowGather(cot_ref, cot_out, pairs[6], pairs[7], 0)
    cot_rows.start()
    last = 2 + back + 1 + ahead
    flush(last + 3, cot_ref, cot_out.at[dp]).start()

    wide, tile = 4 * HEAD_DIM, 2 * HEAD_DIM

    def project(source, first):
        whole = jnp.dot(
            source[:, :piece], w_all[0, :, first : first + wide],
            preferred_element_type=jnp.float32,
        )
        for i in range(1, dp_size):
            whole += jnp.dot(
                source[:, i * piece : (i + 1) * piece], w_all[i, :, first : first + wide],
                preferred_element_type=jnp.float32,
            )
        return [whole[:, :tile], whole[:, tile:]]

    def tables(block):
        cosine, sine = block_tables(cos_ref, sin_ref, block_rows, block)
        return cosine, -sine

    here = tables(me)
    for first in range(0, q_width, wide):
        for i, part_of in enumerate(project(normed, first)):
            turned = turn(part_of, *here).astype(jnp.bfloat16)
            at = first + i * tile
            q_ref[:, at : at + tile] = (turned.astype(jnp.float32) * HEAD_DIM**-0.5).astype(
                jnp.bfloat16
            )
    for s in range(1, back):
        line.step(s)
    line.step_back()
    masks = Masks(docs_all, starts_ref, column)

    def visit(s, block):
        @pl.when(s > 0)
        def _():
            line.relay(s - 1, block).wait()

        part[...] = norm_rows(x_all[block])
        there = tables(block)
        for first in range(q_width, q_width + 2 * kv_width, wide):
            for i, part_of in enumerate(project(part, first)):
                if first < q_width + kv_width:
                    part_of = turn(part_of, *there)
                at = first - q_width + i * tile
                kv_all[block, :, at : at + tile] = part_of.astype(jnp.bfloat16)
        flush(2 + s, kv_all.at[block], kv_out.at[block]).start()
        attend_block(masks, block, q_ref, kv_all.at[block], acc, top, total)

    def step(s):
        pl.when(me - s >= 0)(lambda: visit(s, lax.rem(me + size - s, size)))

        @pl.when(s == min(1, back))
        def _():
            out_w.forward()
            cot_rows.forward()

    each(back + 1, step, 0)
    if ahead:

        @pl.when(me + 1 < size)
        def _():
            visit(back + 1, lax.rem(me + 1, size))

    log_ref[...] = top[...] + jnp.log(total[...])
    for h in range(total.shape[0]):
        at = slice(h * HEAD_DIM, (h + 1) * HEAD_DIM)
        acc[at, :] = acc[at, :] / total[h : h + 1, :]
    full[...] = jnp.transpose(acc[...])
    mix_ref[...] = full[...].astype(jnp.bfloat16)
    out_w.arrive()
    cot_rows.arrive()
    for i in range(dp_size):
        part[:, i * piece : (i + 1) * piece] = jnp.dot(
            mix_ref[...], out_w_all[i], preferred_element_type=jnp.float32
        ).astype(jnp.bfloat16)

    mine, theirs = halves(block_rows)
    rows = RowGather(normed_two, rows_out, pairs[9], pairs[10], 2)
    first = remote(part.at[theirs], held.at[theirs], pairs[10], 0, other_core())
    second = remote(part.at[mine], held.at[mine], pairs[10], 1, other_core())
    first.start()
    second.start()
    flush(last, full, full_out).start()
    flush(last + 1, out_w_all, out_w_out).start()

    def norm(at):
        whole = x_ref[at, :].astype(jnp.float32) + (
            part[at, :].astype(jnp.float32) + held[at, :].astype(jnp.float32)
        )
        hidden[at, :] = whole
        normed_two[at, :] = (whole * row_scale(whole) * gain_rows[1:2, :]).astype(jnp.bfloat16)

    first.wait()
    norm(mine)
    rows.start()
    second.wait()
    norm(theirs)
    flush(last + 2, hidden, hidden_out).start()
    flush(last + 4, normed_two, rows_out.at[dp]).start()
    cot_rows.finish()
    for one in (gains, weights, docs, routes, gates, out_w, line):
        one.finish()
    rows.forward()
    rows.arrive()
    rows.finish()
    flush(0, normed, normed_out).wait()
    flush(1, w_all, w_out).wait()

    def kept(s):
        @pl.when(me - s >= 0)
        def _():
            flush(2 + s, kv_all.at[me], kv_out.at[me]).wait()

    each(back + 1, kept, 0)
    if ahead:
        pl.when(me + 1 < size)(lambda: flush(3 + back, kv_all.at[me], kv_out.at[me]).wait())
    flush(last, full, full_out).wait()
    flush(last + 1, out_w_all, out_w_out).wait()
    flush(last + 2, hidden, hidden_out).wait()
    flush(last + 3, cot_ref, cot_out.at[dp]).wait()
    flush(last + 4, normed_two, rows_out.at[dp]).wait()


def front(
    starts, x, cot, q_w, k_w, v_w, out_w, gains, docs, routes, gates, cosine, sine, own, back,
    ahead, ident,
):
    rows, width = x.shape
    dp_size, ctx_size = lax.axis_size("dp"), lax.axis_size("ctx")
    q_width, kv_cols = q_w.shape[1], 2 * k_w.shape[1]
    piece, heads = q_w.shape[0], q_width // HEAD_DIM
    low, high, whole = jnp.bfloat16, jnp.float32, jnp.int32
    far = [
        ((dp_size, piece, q_width + kv_cols), low),
        ((dp_size,) + out_w.shape, low),
        ((rows, width), low),
        ((ctx_size, rows, kv_cols), low),
        ((rows, q_width), high),
        ((rows, width), high),
        ((dp_size, rows, width), low),
        ((dp_size, rows, width), low),
    ]
    shapes = [
        far[0],
        far[1],
        ((2, width), high),
        ((ctx_size, 1, rows), whole),
        far[2],
        ((rows, q_width), low),
        far[3],
        ((rows, q_width), low),
        far[4],
        ((heads, rows), high),
        far[5],
        far[6],
        far[7],
        ((dp_size, own, 1, rows), whole),
        ((dp_size, own, 1, rows), high),
        ((dp_size, rows, own), whole),
    ]
    return pl.pallas_call(
        functools.partial(front_kernel, back, ahead, own),
        name="front",
        in_specs=[pl.BlockSpec(memory_space=pltpu.SMEM)] + whole_vmem(12),
        out_specs=[
            pl.BlockSpec(memory_space=pl.ANY if shape in far else pltpu.VMEM) for shape in shapes
        ],
        out_shape=[jax.ShapeDtypeStruct(*shape) for shape in shapes],
        scratch_shapes=[
            *[pltpu.VMEM(*shape) for shape in far[:6]],
            pltpu.VMEM((ctx_size, rows, width), low),
            pltpu.VMEM((dp_size,) + gains.shape, high),
            pltpu.VMEM((dp_size,) + routes.shape, whole),
            pltpu.VMEM((dp_size,) + gates.shape, high),
            pltpu.VMEM((q_width, rows), high),
            pltpu.VMEM((heads, rows), high),
            pltpu.VMEM((heads, rows), high),
            pltpu.VMEM((rows, 8), whole),
            pltpu.VMEM((rows, width), low),
            pltpu.VMEM((rows, width), low),
            pltpu.VMEM((rows, width), low),
            *sem_pair(dp_size),
            *sem_pair(dp_size),
            *sem_pair(ctx_size),
            *sem_pair(dp_size),
            *sem_pair(dp_size),
            *sem_pair(dp_size),
            *sem_pair(dp_size),
            *sem_pair(dp_size),
            *sem_pair(back + 1),
            *sem_pair(dp_size),
            *sem_pair(dp_size + 2),
            *sem_pair(back + 1),
            pltpu.SemaphoreType.DMA((8 + back + ahead,)),
        ],
        compiler_params=remote_params(ident),
    )(starts, x, cot, q_w, k_w, v_w, out_w, gains, docs, routes, gates, cosine, sine)


GROUPS_AT_ONCE = 4


def experts_kernel(more, rows_ref, grads_ref, weights_ref, place_ref, gate_ref, *refs):
    outs_ref, backs_ref, weight_grad_ref, slots, slot_grads = refs[2 * more :]
    groups, tok_rows, _ = rows_ref.shape
    owners, part = weight_grad_ref.shape[1], weight_grad_ref.shape[5]
    slot_index = lax.broadcasted_iota(jnp.int32, (CAP, tok_rows), 0)
    gates = []
    for g in range(groups):
        picks = slot_index == place_ref[g, 0]
        gates.append(jnp.sum(jnp.where(picks, gate_ref[g, 0], 0.0), axis=1, keepdims=True))
        picks = picks.astype(jnp.float32).astype(jnp.bfloat16)
        at = slice(g * CAP, (g + 1) * CAP)
        slots[at, :] = jnp.dot(
            picks, rows_ref[g], preferred_element_type=jnp.float32
        ).astype(jnp.bfloat16)
        slot_grads[at, :] = (
            jnp.dot(picks, grads_ref[g], preferred_element_type=jnp.float32) * gates[g]
        ).astype(jnp.bfloat16)
    gate_w, up_w, down_w = (weights_ref.at[0, i] for i in range(3))
    gate_pre = jnp.dot(slots[...], gate_w[...], preferred_element_type=jnp.float32)
    up_pre = jnp.dot(slots[...], up_w[...], preferred_element_type=jnp.float32)
    act_grad = jnp.dot(slot_grads[...], down_w[...], preferred_element_type=jnp.float32)
    sig = 1.0 / (1.0 + jnp.exp(-gate_pre))
    silu = gate_pre * sig
    act_low = (silu * up_pre).astype(jnp.bfloat16)
    up_low = (act_grad * silu).astype(jnp.bfloat16)
    gate_low = (act_grad * up_pre * (sig * (1.0 + gate_pre * (1.0 - sig)))).astype(jnp.bfloat16)

    back = lax.dot_general(
        gate_low, gate_w[...], NT, preferred_element_type=jnp.float32
    ) + lax.dot_general(up_low, up_w[...], NT, preferred_element_type=jnp.float32)
    out = lax.dot_general(act_low, down_w[...], NT, preferred_element_type=jnp.float32)
    for g in range(groups):
        at = slice(g * CAP, (g + 1) * CAP)
        backs_ref[g] = back[at].astype(jnp.bfloat16)
        outs_ref[g] = (out[at] * gates[g]).astype(jnp.bfloat16)

    for i, (low, source) in enumerate(
        ((gate_low, slots), (up_low, slots), (act_low, slot_grads))
    ):
        turned = jnp.transpose(low.astype(jnp.float32)).astype(jnp.bfloat16)
        total = jnp.dot(turned, source[...], preferred_element_type=jnp.float32)
        for c in range(owners):
            weight_grad_ref[0, c, 0, i] = total[:, c * part : (c + 1) * part].astype(
                weight_grad_ref.dtype
            )


def experts(weights, place_rows, gate_rows, rows_all, grad_all, first, count, before):
    own, _, model_width, hidden = weights.shape
    groups, tok_rows, _ = rows_all.shape
    owners = lax.axis_size("ctx")
    at_once = min(GROUPS_AT_ONCE, groups)
    chunks = groups // at_once
    part = model_width // owners
    rows_spec = pl.BlockSpec(
        (at_once, tok_rows, model_width), lambda c, e: (c, 0, 0), pipeline_mode=pl.Buffered(1)
    )
    line_spec = pl.BlockSpec((at_once, 1, 1, tok_rows), lambda c, e: (c, e + first, 0, 0))
    slots_spec = pl.BlockSpec((at_once, CAP, model_width), lambda c, e: (c, e + first, 0))
    slots_shape = jax.ShapeDtypeStruct((groups, own * CAP, model_width), jnp.bfloat16)
    flops = count * groups * CAP * model_width * 2 * (9 * hidden + 2 * tok_rows)
    more = before is not None
    outs, backs, weight_part = pl.pallas_call(
        functools.partial(experts_kernel, more),
        name="experts",
        grid=(chunks, count),
        in_specs=[
            rows_spec,
            rows_spec,
            pl.BlockSpec((1, 3, model_width, hidden), lambda c, e: (e + first, 0, 0, 0)),
            line_spec,
            line_spec,
        ]
        + [pl.BlockSpec(memory_space=pl.ANY)] * (2 * more),
        out_specs=[
            slots_spec,
            slots_spec,
            pl.BlockSpec((1, owners, 1, 3, hidden, part), lambda c, e: (c, 0, e, 0, 0, 0)),
        ],
        out_shape=[
            slots_shape,
            slots_shape,
            jax.ShapeDtypeStruct((chunks, owners, count, 3, hidden, part), jnp.bfloat16),
        ],
        scratch_shapes=[
            pltpu.VMEM((at_once * CAP, model_width), jnp.bfloat16),
            pltpu.VMEM((at_once * CAP, model_width), jnp.bfloat16),
        ],
        input_output_aliases={5: 0, 6: 1} if more else {},
        compiler_params=pltpu.CompilerParams(vmem_limit_bytes=LIMIT),
        cost_estimate=pl.CostEstimate(
            flops=flops, bytes_accessed=4 * weights.size, transcendentals=0
        ),
    )(rows_all, grad_all, weights, place_rows, gate_rows, *(before if more else ()))
    if chunks == 1:
        return (outs, backs), weight_part[0]
    return (outs, backs), jnp.sum(weight_part.astype(jnp.float32), axis=0).astype(jnp.bfloat16)


def unfold_kernel(more, sums_ref, *refs):
    out_ref = refs[more]
    for i in range(sums_ref.shape[1]):
        out_ref[0, i] = jnp.transpose(sums_ref[0, i].astype(jnp.float32))


def unfold(sums, own, first, before):
    count, three, hidden, part = sums.shape
    more = before is not None
    return pl.pallas_call(
        functools.partial(unfold_kernel, more),
        name="unfold",
        grid=(count,),
        in_specs=[pl.BlockSpec((1, three, hidden, part), lambda e: (e, 0, 0, 0))]
        + [pl.BlockSpec(memory_space=pl.ANY)] * more,
        out_specs=pl.BlockSpec((1, three, part, hidden), lambda e: (e + first, 0, 0, 0)),
        out_shape=jax.ShapeDtypeStruct((own, three, part, hidden), jnp.float32),
        input_output_aliases={1: 0} if more else {},
        compiler_params=pltpu.CompilerParams(vmem_limit_bytes=LIMIT),
    )(sums, *([before] if more else []))


def rotary_tables(token_positions):
    half_dim = HEAD_DIM // 2
    inverse = THETA ** (-(jnp.arange(half_dim, dtype=jnp.float32) * 2.0 / HEAD_DIM))
    angles = token_positions.astype(jnp.float32)[:, None] * inverse[None, :]
    cosine, sine = jnp.cos(angles), jnp.sin(angles)
    return jnp.concatenate([cosine] * 4, axis=1), jnp.concatenate([sine, -sine] * 2, axis=1)


def expert_counts(own):
    return (1, 6, 1) if own == 8 else (own - own // 2, own // 2)


def scatter(grads):
    return lax.psum_scatter(grads, "ctx", scatter_dimension=0)


def body(
    tokens,
    query_weight,
    key_weight,
    value_weight,
    output_weight,
    gain_attn,
    gain_moe,
    expert_weights,
    routes,
    gate_values,
    documents,
    pic_starts,
    cotangent,
):
    block_len = tokens.shape[1]
    ctx_size = lax.axis_size("ctx")
    length = block_len * ctx_size
    back = back_blocks(ctx_size, block_len, length)
    ahead = ahead_blocks(block_len, length, pic_starts.shape[1])
    q_width, kv_width = query_weight.shape[1], key_weight.shape[1]
    own = expert_weights.shape[0]
    x, cot = tokens[0], cotangent[0]

    inside = jnp.arange(block_len, dtype=jnp.int32)
    starts = jnp.arange(-(-ctx_size // 8) * 8, dtype=jnp.int32) * block_len
    cosine, sine = rotary_tables(jnp.concatenate([inside, starts]))
    (
        w_all,
        out_w_all,
        gain_rows,
        docs_all,
        normed_one,
        query,
        kv_all,
        mixture,
        mix_full,
        log_total,
        hidden,
        rows_all,
        grad_all,
        *places,
    ) = front(
        pic_starts,
        x,
        cot,
        query_weight,
        key_weight,
        value_weight,
        output_weight,
        jnp.stack([gain_attn, gain_moe]).astype(jnp.float32),
        documents,
        routes[0].T,
        gate_values[0].T,
        cosine,
        sine,
        own,
        back,
        ahead,
        1,
    )
    place_rows, gate_rows, places = places
    counts = expert_counts(own)
    slots, sums = None, []
    first = 0
    for n, count in enumerate(counts):
        slots, grads = experts(
            expert_weights, place_rows, gate_rows, rows_all, grad_all, first, count, slots
        )
        if n < len(counts) - 1:
            sums.append((scatter(grads), first))
        first += count
    outs, backs = slots
    hidden_grad, hidden_low, mix_grad, gain_two_grad = return_grads(
        backs, places, hidden, cot, gain_rows, out_w_all, 2
    )
    q_rot_grad, kv_part = attend_back(
        pic_starts, query, kv_all, docs_all, log_total, mix_full, mix_grad, back, ahead
    )
    kv_back, expert_sum, *given = trade(
        kv_part,
        outs,
        places,
        hidden_low,
        mixture,
        q_rot_grad,
        cosine,
        sine,
        normed_one,
        back,
        ahead,
        3,
    )
    if len(given) == 1:
        given = [q_rot_grad, normed_one, given[0]]
    x_grad, owned, gain_sums = finish(
        kv_back, cosine, sine, w_all, x, gain_rows, gain_two_grad, given, mixture.shape[1], 4
    )
    grads, owned = lax.optimization_barrier((grads, owned))
    sums.append((scatter(grads), own - counts[-1]))
    few = owned.shape[0]
    here = (lax.axis_index("dp") * ctx_size + lax.axis_index("ctx")) * few
    gain_sums = lax.dynamic_slice_in_dim(gain_sums, here, few, 1)
    expert_grad = None
    for part, first in sums:
        expert_grad = unfold(part, own, first, expert_grad)
    v_end = q_width + 2 * kv_width
    return (
        (hidden + expert_sum.astype(jnp.float32)).astype(jnp.bfloat16)[None],
        (hidden_grad + x_grad).astype(jnp.bfloat16)[None],
        owned[:, :q_width],
        owned[:, q_width : q_width + kv_width],
        owned[:, q_width + kv_width : v_end],
        owned[:, v_end:].T,
        gain_sums[0],
        gain_sums[1],
        expert_grad,
    )


def solution(mesh):
    return jax.shard_map(
        body,
        mesh=mesh,
        in_specs=(
            P("dp", "ctx", None),
            P("dp", "tp"),
            P("dp", "tp"),
            P("dp", "tp"),
            P("tp", "dp"),
            P("dp"),
            P("dp"),
            P("dp", None, None, "tp"),
            P("dp", "ctx", None),
            P("dp", "ctx", None),
            P("dp", "ctx"),
            P("dp", None),
            P("dp", "ctx", None),
        ),
        out_specs=(
            P("dp", "ctx", None),
            P("dp", "ctx", None),
            P(("dp", "ctx"), "tp"),
            P(("dp", "ctx"), "tp"),
            P(("dp", "ctx"), "tp"),
            P("tp", ("dp", "ctx")),
            P(("dp", "ctx")),
            P(("dp", "ctx")),
            P("dp", None, "ctx", "tp"),
        ),
        check_vma=False,
    )
```
